16 devices in a mesh: dp: 4 (over z, y), seq: 4 (over x, core).
Axes of the slice: x: 2, y: 2, z: 2, core: 2. Of those that a mesh axis runs over, the one named last changes fastest.
Arguments:
- enc_out: bfloat16 [256, 8, 640], P('dp', 'seq'), parts along dimension 0
- pred_out: bfloat16 [256, 32, 640], P('dp'), parts along dimension 0
- w_enc: bfloat16 [640, 640], replicated
- w_pred: bfloat16 [640, 640], replicated
- w_out: bfloat16 [640, 1024], replicated
- labels: int32 [256, 31], P('dp'), parts along dimension 0
- frame_len: int32 [256], P('dp'), parts along dimension 0
- label_len: int32 [256], P('dp'), parts along dimension 0
Outputs:
- output 1: float32 [256], P('dp'), parts along dimension 0
- output 2: bfloat16 [256, 8, 640], P('dp', 'seq'), parts along dimension 0
- output 3: float32 [2560, 640], P('dp'), parts along dimension 0
- output 4: float32 [2560, 640], P('dp'), parts along dimension 0
- output 5: float32 [2560, 1024], P('dp'), parts along dimension 0
There are 4 independent parts. The reference program is written for one: setup_inputs(seed, part) draws one part's arguments, and reference() takes and returns one part's arrays. A program takes and returns all parts, laid end to end along the dimension named above; an argument that names none is the same for every part.
All inputs are finite; a program needn't handle non-finite values.
Results may differ from the reference program's by a relative error of at most 0.0138912.
Values are sent between devices in bfloat16 or wider.
A program may use at most 1 GiB of HBM per device.

```python
import jax
import jax.numpy as jnp
from jax import lax

NUM_UTT = 64
NUM_FRAMES = 8
LABEL_POS = 32
ENC_DIM = 640
PRED_DIM = 640
JOINT_DIM = 640
VOCAB_SIZE = 1024
FRAME_BLOCK = 2
NUM_LABELS = LABEL_POS - 1
NUM_BLOCKS = NUM_FRAMES // FRAME_BLOCK
NEG_FILL = -1.0e30


def setup_inputs(seed: int = 0, part: int = 0) -> dict:
    shared_key, part_base = jax.random.split(jax.random.key(seed))
    part_key = jax.random.fold_in(part_base, part)
    k_enc, k_pred, k_lab, k_frames, k_lens = jax.random.split(part_key, 5)
    k_wenc, k_wpred, k_wout = jax.random.split(shared_key, 3)
    enc_out = jax.random.normal(k_enc, (NUM_UTT, NUM_FRAMES, ENC_DIM), jnp.float32).astype(jnp.bfloat16)
    pred_out = jax.random.normal(k_pred, (NUM_UTT, LABEL_POS, PRED_DIM), jnp.float32).astype(jnp.bfloat16)
    w_enc = (jax.random.normal(k_wenc, (ENC_DIM, JOINT_DIM), jnp.float32) * ENC_DIM ** -0.5).astype(jnp.bfloat16)
    w_pred = (jax.random.normal(k_wpred, (PRED_DIM, JOINT_DIM), jnp.float32) * PRED_DIM ** -0.5).astype(jnp.bfloat16)
    w_out = (jax.random.normal(k_wout, (JOINT_DIM, VOCAB_SIZE), jnp.float32) * (1.5 * JOINT_DIM ** -0.5)).astype(jnp.bfloat16)
    labels = jax.random.randint(k_lab, (NUM_UTT, NUM_LABELS), 1, VOCAB_SIZE, jnp.int32)
    frame_len = jax.random.randint(k_frames, (NUM_UTT,), NUM_FRAMES // 4 + 1, NUM_FRAMES + 1, jnp.int32).at[0].set(NUM_FRAMES)
    label_len = jax.random.randint(k_lens, (NUM_UTT,), 1, NUM_LABELS + 1, jnp.int32).at[NUM_UTT - 1].set(NUM_LABELS)
    return {'enc_out': enc_out, 'pred_out': pred_out, 'w_enc': w_enc, 'w_pred': w_pred, 'w_out': w_out, 'labels': labels, 'frame_len': frame_len, 'label_len': label_len}


def joint_block(enc_blk, act_g, w_enc, w_out):
    n_utt, n_blk, _ = enc_blk.shape
    act_f = jnp.dot(enc_blk.reshape(n_utt * n_blk, ENC_DIM), w_enc, preferred_element_type=jnp.float32).astype(jnp.bfloat16).reshape(n_utt, n_blk, JOINT_DIM)
    hidden = jnp.tanh(act_f[:, :, None, :].astype(jnp.float32) + act_g[:, None, :, :].astype(jnp.float32)).astype(jnp.bfloat16)
    logits = jnp.dot(hidden.reshape(n_utt * n_blk * LABEL_POS, JOINT_DIM), w_out, preferred_element_type=jnp.float32).reshape(n_utt, n_blk, LABEL_POS, VOCAB_SIZE)
    return hidden, jax.nn.log_softmax(logits, axis=-1)


def label_prefix(frame_lab):
    zero_col = jnp.zeros_like(frame_lab[:, :1])
    return jnp.concatenate([zero_col, jnp.cumsum(frame_lab, axis=1)], axis=1)


def reference(enc_out, pred_out, w_enc, w_pred, w_out, labels, frame_len, label_len):
    act_g = jnp.dot(pred_out.reshape(NUM_UTT * LABEL_POS, PRED_DIM), w_pred, preferred_element_type=jnp.float32).astype(jnp.bfloat16).reshape(NUM_UTT, LABEL_POS, JOINT_DIM)
    lab_ids = jnp.concatenate([labels, jnp.full((NUM_UTT, 1), -1, jnp.int32)], axis=1)
    lab_index = jnp.broadcast_to(labels[:, None, :, None], (NUM_UTT, FRAME_BLOCK, NUM_LABELS, 1))
    enc_blocks = enc_out.reshape(NUM_UTT, NUM_BLOCKS, FRAME_BLOCK, ENC_DIM).transpose(1, 0, 2, 3)

    def lattice_scores(enc_blk):
        _, log_probs = joint_block(enc_blk, act_g, w_enc, w_out)
        lab_lp = jnp.take_along_axis(log_probs[:, :, :NUM_LABELS, :], lab_index, axis=3)[..., 0]
        return log_probs[..., 0], lab_lp

    blank_blocks, lab_blocks = lax.map(lattice_scores, enc_blocks)
    blank_lp = blank_blocks.transpose(1, 0, 2, 3).reshape(NUM_UTT, NUM_FRAMES, LABEL_POS)
    lab_lp = lab_blocks.transpose(1, 0, 2, 3).reshape(NUM_UTT, NUM_FRAMES, NUM_LABELS)

    pos_ids = jnp.arange(LABEL_POS)[None, :]
    neg_rows = jnp.full((NUM_UTT, LABEL_POS), NEG_FILL, jnp.float32)
    init_x = jnp.where(pos_ids == 0, 0.0, neg_rows)
    boundary = jnp.where(pos_ids == label_len[:, None], 0.0, neg_rows)

    def alpha_step(x_prev, frame_in):
        frame_blank, frame_lab = frame_in
        lab_sum = label_prefix(frame_lab)
        alpha_t = lab_sum + lax.cumlogsumexp(x_prev - lab_sum, axis=1)
        return alpha_t + frame_blank, alpha_t

    _, alphas = lax.scan(alpha_step, init_x, (blank_lp.transpose(1, 0, 2), lab_lp.transpose(1, 0, 2)))
    alphas = alphas.transpose(1, 0, 2)

    def beta_step(next_row, frame_in):
        frame_blank, frame_lab, frame_id = frame_in
        lab_sum = label_prefix(frame_lab)
        beta_row = lax.cumlogsumexp(next_row + frame_blank + lab_sum, axis=1, reverse=True) - lab_sum
        beta_row = jnp.where((frame_id >= frame_len)[:, None], boundary, beta_row)
        return beta_row, (beta_row, next_row)

    first_row, (betas, beta_next) = lax.scan(beta_step, boundary, (blank_lp.transpose(1, 0, 2), lab_lp.transpose(1, 0, 2), jnp.arange(NUM_FRAMES)), reverse=True)
    betas = betas.transpose(1, 0, 2)
    beta_next = beta_next.transpose(1, 0, 2)
    log_prob = first_row[:, 0]

    beta_up = jnp.concatenate([betas[:, :, 1:], jnp.full((NUM_UTT, NUM_FRAMES, 1), NEG_FILL, jnp.float32)], axis=2)
    lab_full = jnp.concatenate([lab_lp, jnp.zeros((NUM_UTT, NUM_FRAMES, 1), jnp.float32)], axis=2)
    frame_ok = (jnp.arange(NUM_FRAMES)[None, :] < frame_len[:, None])[:, :, None]
    norm_shift = log_prob[:, None, None]
    occ_blank = jnp.where(frame_ok, jnp.exp(jnp.minimum(alphas + blank_lp + beta_next - norm_shift, 0.0)), 0.0)
    occ_lab = jnp.where(frame_ok, jnp.exp(jnp.minimum(alphas + lab_full + beta_up - norm_shift, 0.0)), 0.0)

    def to_blocks(arr):
        return arr.reshape(NUM_UTT, NUM_BLOCKS, FRAME_BLOCK, LABEL_POS).transpose(1, 0, 2, 3)

    vocab_ids = jnp.arange(VOCAB_SIZE)

    def grad_step(acc_carry, blk_in):
        gw_enc, gw_out, d_act_g = acc_carry
        enc_blk, occ_b, occ_l = blk_in
        hidden, log_probs = joint_block(enc_blk, act_g, w_enc, w_out)
        d_logits = (jnp.exp(log_probs) * (occ_b + occ_l)[..., None] - jnp.where(vocab_ids == 0, occ_b[..., None], 0.0) - jnp.where(vocab_ids == lab_ids[:, None, :, None], occ_l[..., None], 0.0)).astype(jnp.bfloat16)
        flat_dz = d_logits.reshape(NUM_UTT * FRAME_BLOCK * LABEL_POS, VOCAB_SIZE)
        flat_h = hidden.reshape(NUM_UTT * FRAME_BLOCK * LABEL_POS, JOINT_DIM)
        d_hidden = jnp.dot(flat_dz, w_out.T, preferred_element_type=jnp.float32)
        d_pre = (d_hidden * (1.0 - jnp.square(flat_h.astype(jnp.float32)))).astype(jnp.bfloat16).reshape(NUM_UTT, FRAME_BLOCK, LABEL_POS, JOINT_DIM)
        d_act_f = jnp.sum(d_pre.astype(jnp.float32), axis=2).astype(jnp.bfloat16).reshape(NUM_UTT * FRAME_BLOCK, JOINT_DIM)
        grad_blk = jnp.dot(d_act_f, w_enc.T, preferred_element_type=jnp.float32).astype(jnp.bfloat16).reshape(NUM_UTT, FRAME_BLOCK, ENC_DIM)
        gw_enc = gw_enc + jnp.dot(enc_blk.reshape(NUM_UTT * FRAME_BLOCK, ENC_DIM).T, d_act_f, preferred_element_type=jnp.float32)
        gw_out = gw_out + jnp.dot(flat_h.T, flat_dz, preferred_element_type=jnp.float32)
        d_act_g = d_act_g + jnp.sum(d_pre.astype(jnp.float32), axis=1)
        return (gw_enc, gw_out, d_act_g), grad_blk

    acc_init = (jnp.zeros((ENC_DIM, JOINT_DIM), jnp.float32), jnp.zeros((JOINT_DIM, VOCAB_SIZE), jnp.float32), jnp.zeros((NUM_UTT, LABEL_POS, JOINT_DIM), jnp.float32))
    (gw_enc, gw_out, d_act_g), grad_blocks = lax.scan(grad_step, acc_init, (enc_blocks, to_blocks(occ_blank), to_blocks(occ_lab)))
    grad_enc = grad_blocks.transpose(1, 0, 2, 3).reshape(NUM_UTT, NUM_FRAMES, ENC_DIM)
    gw_pred = jnp.einsum('buh,buj->hj', pred_out.astype(jnp.float32), d_act_g.astype(jnp.float32))
    return -log_prob, grad_enc, gw_enc, gw_pred, gw_out
```

```python
import functools

import jax
import jax.numpy as jnp
from jax import lax
from jax.experimental import pallas as pl
from jax.experimental.pallas import tpu as pltpu
from jax.sharding import PartitionSpec as P

NEG = -1.0e30
ROWS = 256
GRP = 8
KEEP = 22
F32 = jnp.float32
BF16 = jnp.bfloat16
NT = (((1,), (1,)), ((), ()))
NN = (((1,), (0,)), ((), ()))


def dot(a, b, dims=NN):
    return lax.dot_general(a, b, dims, preferred_element_type=F32)


def split3(x):
    hi = x.astype(BF16).astype(F32)
    r1 = x - hi
    mid = r1.astype(BF16).astype(F32)
    return hi, mid, r1 - mid


def logadd(a, b):
    m = jnp.maximum(a, b)
    return m + jnp.log(1.0 + jnp.exp(jnp.minimum(a, b) - m))


def core_kernel(n_utt, n_t, n_u, flen_s, llen_s, flen_v, llen_v, lab_ref, f_ref, g_ref, we_ref, wp_ref, wo_ref,
                loss_ref, gf_ref, gwe_ref, gwp_ref, gwo_ref,
                wot, cat, ylab, hbuf, ebuf, zbuf, stat, idx, dzb, sk, abuf, t1buf, t2buf, gocc, segu, segt, tbl):
    n_grp = n_utt // GRP
    n_j = we_ref.shape[1]
    n_v = wo_ref.shape[1]
    gu = GRP * n_u
    gt = GRP * n_t
    n_diag = n_t + n_u - 1
    n_kt = (n_diag + 1) * n_t

    def grp_step(g, pos):
        total = jnp.int32(0)
        for j in range(GRP):
            total = total + flen_s[g * GRP + j] * (llen_s[g * GRP + j] + 1)
        n_blk = (total + ROWS - 1) // ROWS

        def blk_step(k, p):
            tbl[0, p] = g
            tbl[1, p] = k
            return p + 1
        return lax.fori_loop(0, n_blk, blk_step, pos)
    n_blocks = lax.fori_loop(0, n_grp, grp_step, jnp.int32(0))

    wot[...] = wo_ref[...].T
    c_t = dot(wp_ref[...].T, g_ref[...], NT).astype(BF16)
    a_t = dot(we_ref[...].T, f_ref[...], NT).astype(BF16)
    lab = lab_ref[...]
    for g in range(n_grp):
        cat[g, :, 0:gu] = c_t[:, g * gu:(g + 1) * gu]
        a_g = a_t[:, g * gt:(g + 1) * gt]
        cat[g, :, gu:gu + 128] = jnp.concatenate([a_g, jnp.zeros((n_j, 128 - gt), BF16)], axis=1)
        lab_g = lab[:, g * gu:(g + 1) * gu]
        row = lax.broadcasted_iota(jnp.int32, (16, gu), 0)
        hi = lax.shift_right_arithmetic(lab_g, 5)
        lo = jnp.bitwise_and(lab_g, 31)
        ylab[g] = jnp.where(row == 0, hi, jnp.where(row == 1, lo, 0)).astype(F32).astype(BF16)
    sk[...] = jnp.zeros_like(sk)
    segu[...] = jnp.zeros_like(segu)
    segt[...] = jnp.zeros_like(segt)
    gwo_ref[...] = jnp.zeros_like(gwo_ref)

    def onehot(n, index_row):
        return (lax.broadcasted_iota(jnp.int32, (n, ROWS), 0) == index_row)

    def as_bf16(mask):
        return jnp.where(mask, 1.0, 0.0).astype(BF16)

    n_ch = n_v // 256
    v_iota = lax.broadcasted_iota(jnp.int32, (256, ROWS), 0)

    def fwd(i, carry):
        g = tbl[0, i]
        k = tbl[1, i]
        r = k * ROWS + lax.broadcasted_iota(jnp.int32, (1, ROWS), 1)
        start = jnp.int32(0)
        bl = jnp.full((1, ROWS), -1, jnp.int32)
        w = jnp.zeros((1, ROWS), jnp.int32)
        u1 = jnp.ones((1, ROWS), jnp.int32)
        for j in range(GRP):
            u1_j = llen_s[g * GRP + j] + 1
            end = start + flen_s[g * GRP + j] * u1_j
            inside = (r >= start) & (r < end)
            bl = jnp.where(inside, j, bl)
            w = jnp.where(inside, r - start, w)
            u1 = jnp.where(inside, u1_j, u1)
            start = end
        valid = bl >= 0
        t = jnp.zeros((1, ROWS), jnp.int32)
        for j in range(1, n_t):
            t = t + jnp.where(w >= j * u1, 1, 0)
        u = w - t * u1
        idx_u = jnp.where(valid, bl * n_u + u, -1)
        idx_t = jnp.where(valid, bl * n_t + t, -1)
        idx_kt = jnp.where(valid, (t + u) * n_t + t, -1)
        idx_b = jnp.where(valid, g * GRP + bl, -1)
        oh = jnp.concatenate([as_bf16(onehot(gu, idx_u)), as_bf16(onehot(128, idx_t))], axis=0)
        pre = dot(cat[g], oh)
        h = jnp.tanh(pre).astype(BF16)
        hbuf[i] = h
        yy = dot(ylab[g], oh[0:gu])
        y = (yy[0:1] * 32.0 + yy[1:2]).astype(jnp.int32)
        mx = None
        lz = None
        for c in range(n_ch):
            z = dot(wot[c * 256:(c + 1) * 256, :], h)
            zbuf[c * 256:(c + 1) * 256, :] = z
            zm = jnp.max(z.reshape(32, 8, ROWS), axis=0)
            zl = jnp.sum(jnp.where(v_iota == y - c * 256, z, 0.0).reshape(32, 8, ROWS), axis=0)
            mx = zm if mx is None else jnp.maximum(mx, zm)
            lz = zl if lz is None else lz + zl
        m = jnp.max(mx, axis=0, keepdims=True)
        lab_z = jnp.sum(lz, axis=0, keepdims=True)
        blank_z = zbuf[0:1, :]
        acc = None
        slot = jnp.minimum(i, KEEP)
        for c in range(n_ch):
            e = jnp.exp(zbuf[c * 256:(c + 1) * 256, :] - m)
            ebuf[slot, c * 256:(c + 1) * 256, :] = e
            es = jnp.sum(e.reshape(32, 8, ROWS), axis=0)
            acc = es if acc is None else acc + es
        s = jnp.sum(acc, axis=0, keepdims=True)
        lse = m + jnp.log(s)
        b_parts = split3(blank_z - lse)
        l_parts = split3(lab_z - lse)
        ohb = onehot(32, idx_b)
        vs = [jnp.where(ohb, part, 0.0).astype(BF16) for pair in zip(b_parts, l_parts) for part in pair]
        vs = jnp.concatenate(vs + [jnp.zeros((64, ROWS), BF16)], axis=0)
        okt = as_bf16(onehot(n_kt, idx_kt))
        sk[...] += dot(okt, vs, NT)
        rows8 = lax.broadcasted_iota(jnp.int32, (8, ROWS), 0)
        stat[i] = jnp.where(rows8 == 0, 1.0 / s, m)
        packed = jnp.where(rows8 == 0, idx_u, jnp.where(rows8 == 1, idx_t, jnp.where(rows8 == 2, idx_kt, jnp.where(rows8 == 3, idx_b, y))))
        idx[i] = packed
        return carry

    lax.fori_loop(0, n_blocks, fwd, 0)

    tt = lax.broadcasted_iota(jnp.int32, (n_t, 128), 0)
    t_len = flen_v[...]
    u_len = llen_v[...]

    def scores(k):
        lo = k * n_t
        v0 = sk[lo:lo + n_t, 0:128]
        v1 = sk[lo:lo + n_t, 128:256]
        x = v0 + pltpu.roll(v0, 64, 1) + v1
        uu = k - tt
        ok = (uu >= 0) & (tt < t_len)
        bl_k = jnp.where(ok & (uu <= u_len), x, NEG)
        lb_k = jnp.where(ok & (uu < u_len), pltpu.roll(x, 96, 1), NEG)
        return bl_k, lb_k

    alpha = jnp.where(tt == 0, 0.0, NEG).astype(F32)
    abuf[0] = alpha
    beta = jnp.full((n_t, 128), NEG, F32)
    sc = [scores(k) for k in range(n_diag)]
    for step in range(n_diag):
        if step > 0:
            bl_k, lb_k = sc[step - 1]
            p1 = jnp.where(tt == 0, NEG, pltpu.roll(alpha + bl_k, 1, 0))
            alpha = logadd(p1, alpha + lb_k)
            abuf[step] = alpha
        k = n_diag - 1 - step
        bl_k, lb_k = sc[k]
        up = jnp.where(tt == n_t - 1, jnp.where(u_len == k + 1 - n_t, 0.0, NEG), pltpu.roll(beta, n_t - 1, 0))
        t1 = up + bl_k
        t2 = beta + lb_k
        t1buf[k] = t1
        t2buf[k] = t2
        beta = jnp.where(tt >= t_len, jnp.where(k - tt == u_len, 0.0, NEG), logadd(t1, t2))
    log_p = beta[0:1, :]
    loss_ref[...] = jnp.broadcast_to(-log_p, (8, 128))
    lane_ok = lax.broadcasted_iota(jnp.int32, (n_t, 128), 1) < 32
    for k in range(n_diag):
        for which, buf in enumerate((t1buf, t2buf)):
            occ = jnp.where(lane_ok, jnp.exp(jnp.minimum(abuf[k] + buf[k] - log_p, 0.0)), 0.0)
            hi, mid, lo = split3(occ)
            lo_row = which * n_kt + k * n_t
            gocc[lo_row:lo_row + n_t, :] = hi + pltpu.roll(mid, 32, 1) + pltpu.roll(lo, 64, 1)
    for which in range(2):
        gocc[which * n_kt + n_diag * n_t:(which + 1) * n_kt, :] = jnp.zeros((n_kt - n_diag * n_t, 128), F32)

    def bwd(i, carry):
        g = tbl[0, i]
        packed = idx[i]
        idx_u, idx_t, idx_kt, idx_b, y = (packed[q:q + 1] for q in range(5))
        oh = jnp.concatenate([as_bf16(onehot(gu, idx_u)), as_bf16(onehot(128, idx_t))], axis=0)
        row = lax.broadcasted_iota(jnp.int32, (128, ROWS), 0)
        orep = as_bf16((jnp.bitwise_and(row, 31) == idx_b) & (row < 96))
        okt = onehot(n_kt, idx_kt)
        gath = dot(gocc[...].astype(BF16), orep)
        gb = jnp.sum(jnp.where(okt, gath[0:n_kt], 0.0), axis=0, keepdims=True)
        gl = jnp.sum(jnp.where(okt, gath[n_kt:2 * n_kt], 0.0), axis=0, keepdims=True)
        scale = (gb + gl) * stat[i, 0:1, :]
        h = hbuf[i]
        slot = jnp.minimum(i, KEEP)

        @pl.when(i >= KEEP)
        def _():
            m = stat[i, 1:2, :]
            for c in range(n_ch):
                ebuf[KEEP, c * 256:(c + 1) * 256, :] = jnp.exp(dot(wot[c * 256:(c + 1) * 256, :], h) - m)

        for c in range(n_ch):
            d = ebuf[slot, c * 256:(c + 1) * 256, :] * scale - jnp.where(v_iota == y - c * 256, gl, 0.0)
            if c == 0:
                d = d - jnp.where(v_iota == 0, gb, 0.0)
            dzb[c * 256:(c + 1) * 256, :] = d.astype(BF16)
        hf = h.astype(F32)
        dh = dot(wo_ref[...], dzb[...])
        dp = (dh * (1.0 - hf * hf)).astype(BF16)
        seg = dot(dp, oh, NT)
        segu[g] += seg[:, 0:gu]
        segt[g] += seg[:, gu:gu + 128]
        for c in range(n_ch):
            gwo_ref[:, c * 256:(c + 1) * 256] += dot(h, dzb[c * 256:(c + 1) * 256, :], NT)
        return carry

    lax.fori_loop(0, n_blocks, bwd, 0)

    dc_t = jnp.concatenate([segu[g].astype(BF16) for g in range(n_grp)], axis=1)
    da_t = jnp.concatenate([segt[g][:, 0:gt].astype(BF16) for g in range(n_grp)], axis=1)
    gwp_ref[...] = dot(g_ref[...].T, dc_t, NT)
    gwe_ref[...] = dot(f_ref[...].T, da_t, NT)
    gf_ref[...] = dot(da_t.T, we_ref[...], NT).astype(BF16)


def core_call(f2, g2, w_enc, w_pred, w_out, lab_row, flen, llen, n_t, n_u):
    n_utt = flen.shape[0]
    n_j = w_enc.shape[1]
    n_v = w_out.shape[1]
    n_grp = n_utt // GRP
    max_blk = n_grp * ((GRP * n_t * n_u + ROWS - 1) // ROWS)
    n_kt = (n_t + n_u) * n_t
    pad = lambda x: jnp.broadcast_to(jnp.pad(x, (0, 128 - n_utt))[None, :], (n_t, 128))
    vm = pl.BlockSpec(memory_space=pltpu.VMEM)
    sm = pl.BlockSpec(memory_space=pltpu.SMEM)
    return pl.pallas_call(
        functools.partial(core_kernel, n_utt, n_t, n_u),
        out_shape=(
            jax.ShapeDtypeStruct((8, 128), F32),
            jax.ShapeDtypeStruct((n_utt * n_t, f2.shape[1]), BF16),
            jax.ShapeDtypeStruct(w_enc.shape, F32),
            jax.ShapeDtypeStruct(w_pred.shape, F32),
            jax.ShapeDtypeStruct(w_out.shape, F32),
        ),
        in_specs=[sm, sm] + [vm] * 8,
        out_specs=(vm,) * 5,
        scratch_shapes=[
            pltpu.VMEM((n_v, n_j), BF16),
            pltpu.VMEM((n_grp, n_j, GRP * n_u + 128), BF16),
            pltpu.VMEM((n_grp, 16, GRP * n_u), BF16),
            pltpu.VMEM((max_blk, n_j, ROWS), BF16),
            pltpu.VMEM((min(max_blk, KEEP + 1), n_v, ROWS), F32),
            pltpu.VMEM((n_v, ROWS), F32),
            pltpu.VMEM((max_blk, 8, ROWS), F32),
            pltpu.VMEM((max_blk, 8, ROWS), jnp.int32),
            pltpu.VMEM((n_v, ROWS), BF16),
            pltpu.VMEM((n_kt, 256), F32),
            pltpu.VMEM((n_t + n_u, n_t, 128), F32),
            pltpu.VMEM((n_t + n_u, n_t, 128), F32),
            pltpu.VMEM((n_t + n_u, n_t, 128), F32),
            pltpu.VMEM((2 * n_kt, 128), F32),
            pltpu.VMEM((n_grp, n_j, GRP * n_u), F32),
            pltpu.VMEM((n_grp, n_j, 128), F32),
            pltpu.SMEM((2, max_blk), jnp.int32),
        ],
        compiler_params=pltpu.CompilerParams(vmem_limit_bytes=67043328),
        name="rnnt_core",
    )(flen, llen, pad(flen), pad(llen), lab_row, f2, g2, w_enc, w_pred, w_out)


def solution(mesh):
    seq_size = mesh.shape['seq']

    def local_fn(enc_out, pred_out, w_enc, w_pred, w_out, labels, frame_len, label_len):
        seq_idx = lax.axis_index('seq')
        core = seq_idx % 2
        n_utt, n_loc, n_h = enc_out.shape
        n_u = pred_out.shape[1]
        n_t = n_loc * seq_size
        half = n_utt // 2
        f_all = jnp.zeros((half, seq_size, n_loc, n_h), enc_out.dtype)
        mine = lax.dynamic_slice_in_dim(enc_out, core * half, half, 0)
        f_all = lax.dynamic_update_slice(f_all, mine[:, None], (0, seq_idx, 0, 0))
        for d in range(1, seq_size):
            dst = (seq_idx + d) % seq_size
            piece = lax.dynamic_slice_in_dim(enc_out, (dst % 2) * half, half, 0)
            got = lax.ppermute(piece, 'seq', [(s, (s + d) % seq_size) for s in range(seq_size)])
            f_all = lax.dynamic_update_slice(f_all, got[:, None], (0, (seq_idx - d) % seq_size, 0, 0))
        f2 = f_all.reshape(half * n_t, n_h)
        g2 = lax.dynamic_slice_in_dim(pred_out, core * half, half, 0).reshape(half * n_u, n_h)
        lab = jnp.pad(lax.dynamic_slice_in_dim(labels, core * half, half, 0), ((0, 0), (0, 1)), constant_values=-1)
        flen = lax.dynamic_slice_in_dim(frame_len, core * half, half, 0)
        llen = lax.dynamic_slice_in_dim(label_len, core * half, half, 0)
        loss, gf, gwe, gwp, gwo = core_call(f2, g2, w_enc, w_pred, w_out, lab.reshape(1, half * n_u), flen, llen, n_t, n_u)
        swap = [(s, s ^ 1) for s in range(seq_size)]
        gf = gf.reshape(half, seq_size, n_loc, n_h)
        keep = lax.dynamic_slice_in_dim(gf, seq_idx, 1, 1)[:, 0]
        give = lax.dynamic_slice_in_dim(gf, seq_idx + 1 - 2 * core, 1, 1)[:, 0]
        got = lax.ppermute(give, 'seq', swap)
        grad_enc = jnp.where(core == 0, jnp.concatenate([keep, got], 0), jnp.concatenate([got, keep], 0))
        loss = loss[0, :half]
        other = lax.ppermute(loss, 'seq', swap)
        utt_loss = jnp.where(core == 0, jnp.concatenate([loss, other]), jnp.concatenate([other, loss]))
        gwe = gwe + lax.ppermute(gwe, 'seq', swap)
        gwp = gwp + lax.ppermute(gwp, 'seq', swap)
        gwo = gwo + lax.ppermute(gwo, 'seq', swap)
        return utt_loss, grad_enc, gwe, gwp, gwo

    in_specs = (P('dp', 'seq', None), P('dp', None, None), P(None, None), P(None, None), P(None, None), P('dp', None), P('dp'), P('dp'))
    out_specs = (P('dp'), P('dp', 'seq', None), P('dp', None), P('dp', None), P('dp', None))
    return jax.shard_map(local_fn, mesh=mesh, in_specs=in_specs, out_specs=out_specs, check_vma=False)
```

```python
import functools

import jax
import jax.numpy as jnp
from jax import lax
from jax.experimental import pallas as pl
from jax.experimental.pallas import tpu as pltpu
from jax.sharding import PartitionSpec as P

NEG = -1.0e30
ROWS = 256
WIN = 8
CHUNK = 128
KEEP = 18
F32 = jnp.float32
BF16 = jnp.bfloat16
NT = (((1,), (1,)), ((), ()))
NN = (((1,), (0,)), ((), ()))


def dot(a, b, dims=NN):
    return lax.dot_general(a, b, dims, preferred_element_type=F32)


def split3(x):
    hi = x.astype(BF16).astype(F32)
    r1 = x - hi
    mid = r1.astype(BF16).astype(F32)
    return hi, mid, r1 - mid


def logadd(a, b):
    m = jnp.maximum(a, b)
    return m + jnp.log(1.0 + jnp.exp(jnp.minimum(a, b) - m))


def core_kernel(n_utt, n_t, n_u, flen_s, llen_s, flen_v, llen_v, lab_ref, f_ref, g_ref, we_ref, wp_ref, wo_ref,
                loss_ref, gf_ref, gwe_ref, gwp_ref, gwo_ref,
                wot, c_buf, a_buf, ylab, hbuf, hnew, hcur, ebuf, fac, mch, sch, vsb, idx, dznew, dzcur, sk, abuf, t1buf, t2buf,
                gocc, gocb, segu, segt, tbl, off):
    n_j = we_ref.shape[1]
    n_v = wo_ref.shape[1]
    step_u = WIN // 2 * n_u
    step_t = WIN // 2 * n_t
    gu = WIN * n_u
    n_win = n_utt * 2 // WIN - 1
    n_diag = n_t + n_u - 1
    n_kt = (n_diag + 1) * n_t
    n_ch = n_v // CHUNK

    def off_step(b, total):
        off[b] = total
        return total + flen_s[b] * (llen_s[b] + 1)
    off[n_utt] = lax.fori_loop(0, n_utt, off_step, jnp.int32(0))

    def utt_step(b, carry):
        win = jnp.minimum(b // (WIN // 2), n_win - 1)
        base = off[win * (WIN // 2)]
        last = off[win * (WIN // 2) + WIN]

        def emit(c):
            n, pos = c
            end = jnp.minimum(pos + ROWS, last)
            tbl[0, n] = win
            tbl[1, n] = pos - base
            tbl[2, n] = end - base
            return n + 1, end
        return lax.while_loop(lambda c: c[1] < off[b + 1], emit, carry)
    n_blocks, _ = lax.fori_loop(0, n_utt, utt_step, (jnp.int32(0), jnp.int32(0)))
    tbl[0, n_blocks] = 0
    tbl[1, n_blocks] = 0
    tbl[2, n_blocks] = 0

    wot[...] = wo_ref[...].T
    c_buf[...] = dot(wp_ref[...].T, g_ref[...], NT).astype(BF16)
    a_t = dot(we_ref[...].T, f_ref[...], NT).astype(BF16)
    lab = lab_ref[...]
    for w in range(n_win):
        a_buf[w] = jnp.concatenate([a_t[:, w * step_t:w * step_t + 2 * step_t], jnp.zeros((n_j, 128 - 2 * step_t), BF16)], axis=1)
        lab_w = lab[:, w * step_u:w * step_u + gu]
        row = lax.broadcasted_iota(jnp.int32, (16, gu), 0)
        hi = lax.shift_right_arithmetic(lab_w, 5)
        lo = jnp.bitwise_and(lab_w, 31)
        ylab[w] = jnp.where(row == 0, hi, jnp.where(row == 1, lo, 0)).astype(F32).astype(BF16)
    sk[...] = jnp.zeros_like(sk)
    vsb[...] = jnp.zeros_like(vsb)
    segu[...] = jnp.zeros_like(segu)
    segt[...] = jnp.zeros_like(segt)
    gwo_ref[...] = jnp.zeros_like(gwo_ref)

    def onehot(n, index_row):
        return (lax.broadcasted_iota(jnp.int32, (n, ROWS), 0) == index_row)

    def as_bf16(mask):
        return jnp.where(mask, 1.0, 0.0).astype(BF16)

    v_iota = lax.broadcasted_iota(jnp.int32, (CHUNK, ROWS), 0)
    n_sub = CHUNK // 8

    def lanes_of(win):
        return pl.ds(pl.multiple_of(win * step_u, 128), gu)

    def prepare(i):
        win = tbl[0, i]
        r = tbl[1, i] + lax.broadcasted_iota(jnp.int32, (1, ROWS), 1)
        end_r = tbl[2, i]
        start = jnp.int32(0)
        bl = jnp.full((1, ROWS), -1, jnp.int32)
        w = jnp.zeros((1, ROWS), jnp.int32)
        u1 = jnp.ones((1, ROWS), jnp.int32)
        for j in range(WIN):
            u1_j = llen_s[win * (WIN // 2) + j] + 1
            end = start + flen_s[win * (WIN // 2) + j] * u1_j
            inside = (r >= start) & (r < jnp.minimum(end, end_r))
            bl = jnp.where(inside, j, bl)
            w = jnp.where(inside, r - start, w)
            u1 = jnp.where(inside, u1_j, u1)
            start = end
        valid = bl >= 0
        t = jnp.zeros((1, ROWS), jnp.int32)
        for j in range(1, n_t):
            t = t + jnp.where(w >= j * u1, 1, 0)
        u = w - t * u1
        idx_u = jnp.where(valid, bl * n_u + u, -1)
        idx_t = jnp.where(valid, bl * n_t + t, -1)
        idx_kt = jnp.where(valid, (t + u) * n_t + t, -1)
        idx_b = jnp.where(valid, win * (WIN // 2) + bl, -1)
        ohu = as_bf16(onehot(gu, idx_u))
        oht = as_bf16(onehot(128, idx_t))
        half = n_j // 2
        for q in range(2):
            rows = slice(q * half, (q + 1) * half)
            pre = dot(c_buf[rows, lanes_of(win)], ohu) + dot(a_buf[win, rows], oht)
            hnew[rows] = jnp.tanh(pre).astype(BF16)
        yy = dot(ylab[win], ohu)
        y = (yy[0:1] * 32.0 + yy[1:2]).astype(jnp.int32)
        rows8 = lax.broadcasted_iota(jnp.int32, (8, ROWS), 0)
        idx[i] = jnp.where(rows8 == 0, idx_u, jnp.where(rows8 == 1, idx_t, jnp.where(rows8 == 2, idx_kt, jnp.where(rows8 == 3, idx_b, y))))

    def scatter(i):
        okt = as_bf16(onehot(n_kt, idx[i, 2:3]))
        sk[...] += dot(okt, vsb[...], NT)

    def fwd(i, carry):
        scatter(jnp.maximum(i - 1, 0))
        hcur[...] = hnew[...]
        hbuf[i] = hnew[...]
        y = idx[i, 4:5]
        idx_b = idx[i, 3:4]
        slot = jnp.minimum(i, KEEP)
        prepare(i + 1)
        lz = None
        blank_z = None
        for c in range(n_ch):
            z = dot(wot[c * CHUNK:(c + 1) * CHUNK, :], hcur[...])
            z3 = z.reshape(n_sub, 8, ROWS)
            zl = jnp.sum(jnp.where(v_iota == y - c * CHUNK, z, 0.0).reshape(n_sub, 8, ROWS), axis=0)
            lz = zl if lz is None else lz + zl
            if c == 0:
                blank_z = z[0:1, :]
            m_c = jnp.max(z3, axis=0)
            e3 = jnp.exp(z3 - m_c[None])
            ebuf[slot, c * CHUNK:(c + 1) * CHUNK, :] = e3.reshape(CHUNK, ROWS)
            mch[c * 8:(c + 1) * 8, :] = m_c
            sch[c * 8:(c + 1) * 8, :] = jnp.sum(e3, axis=0)
        m8 = jnp.max(mch[...].reshape(n_ch, 8, ROWS), axis=0)
        m = jnp.max(m8, axis=0, keepdims=True)
        f_all = jnp.exp(mch[...] - m)
        s = jnp.sum(jnp.sum((sch[...] * f_all).reshape(n_ch, 8, ROWS), axis=0), axis=0, keepdims=True)
        fac[i] = f_all * (1.0 / s)
        lab_z = jnp.sum(lz, axis=0, keepdims=True)
        lse = m + jnp.log(s)
        b_parts = split3(blank_z - lse)
        l_parts = split3(lab_z - lse)
        ohb = onehot(32, idx_b)
        for q, (bp, lp) in enumerate(zip(b_parts, l_parts)):
            vsb[q * 64:q * 64 + 32] = jnp.where(ohb, bp, 0.0).astype(BF16)
            vsb[q * 64 + 32:q * 64 + 64] = jnp.where(ohb, lp, 0.0).astype(BF16)
        return carry

    prepare(jnp.int32(0))
    lax.fori_loop(0, n_blocks, fwd, 0)
    scatter(n_blocks - 1)

    tt = lax.broadcasted_iota(jnp.int32, (n_t, 128), 0)
    t_len = flen_v[...]
    u_len = llen_v[...]

    def scores(k):
        lo = k * n_t
        v0 = sk[lo:lo + n_t, 0:128]
        v1 = sk[lo:lo + n_t, 128:256]
        x = v0 + pltpu.roll(v0, 64, 1) + v1
        uu = k - tt
        ok = (uu >= 0) & (tt < t_len)
        bl_k = jnp.where(ok & (uu <= u_len), x, NEG)
        lb_k = jnp.where(ok & (uu < u_len), pltpu.roll(x, 96, 1), NEG)
        return bl_k, lb_k

    alpha = jnp.where(tt == 0, 0.0, NEG).astype(F32)
    abuf[0] = alpha
    beta = jnp.full((n_t, 128), NEG, F32)
    sc = [scores(k) for k in range(n_diag)]
    for step in range(n_diag):
        if step > 0:
            bl_k, lb_k = sc[step - 1]
            p1 = jnp.where(tt == 0, NEG, pltpu.roll(alpha + bl_k, 1, 0))
            alpha = logadd(p1, alpha + lb_k)
            abuf[step] = alpha
        k = n_diag - 1 - step
        bl_k, lb_k = sc[k]
        up = jnp.where(tt == n_t - 1, jnp.where(u_len == k + 1 - n_t, 0.0, NEG), pltpu.roll(beta, n_t - 1, 0))
        t1 = up + bl_k
        t2 = beta + lb_k
        t1buf[k] = t1
        t2buf[k] = t2
        beta = jnp.where(tt >= t_len, jnp.where(k - tt == u_len, 0.0, NEG), logadd(t1, t2))
    log_p = beta[0:1, :]
    loss_ref[...] = jnp.broadcast_to(-log_p, (8, 128))
    lane_ok = lax.broadcasted_iota(jnp.int32, (n_t, 128), 1) < 32
    for k in range(n_diag):
        for which, buf in enumerate((t1buf, t2buf)):
            occ = jnp.where(lane_ok, jnp.exp(jnp.minimum(abuf[k] + buf[k] - log_p, 0.0)), 0.0)
            hi, mid, lo = split3(occ)
            lo_row = which * n_kt + k * n_t
            gocc[lo_row:lo_row + n_t, :] = hi + pltpu.roll(mid, 32, 1) + pltpu.roll(lo, 64, 1)
    for which in range(2):
        gocc[which * n_kt + n_diag * n_t:(which + 1) * n_kt, :] = jnp.zeros((n_kt - n_diag * n_t, 128), F32)
    gocb[...] = gocc[...].astype(BF16)

    def again(i):
        @pl.when(i >= KEEP)
        def _():
            m = None
            for c in range(n_ch):
                z = dot(wot[c * CHUNK:(c + 1) * CHUNK, :], hbuf[i])
                z3 = z.reshape(n_sub, 8, ROWS)
                ebuf[KEEP, c * CHUNK:(c + 1) * CHUNK, :] = jnp.exp(z3 - jnp.max(z3, axis=0)[None]).reshape(CHUNK, ROWS)

    def d_logits(i):
        idx_kt = idx[i, 2:3]
        idx_b = idx[i, 3:4]
        y = idx[i, 4:5]
        row = lax.broadcasted_iota(jnp.int32, (128, ROWS), 0)
        orep = as_bf16((jnp.bitwise_and(row, 31) == idx_b) & (row < 96))
        okt = onehot(n_kt, idx_kt)
        gb = jnp.sum(jnp.where(okt, dot(gocb[0:n_kt], orep), 0.0), axis=0, keepdims=True)
        gl = jnp.sum(jnp.where(okt, dot(gocb[n_kt:2 * n_kt], orep), 0.0), axis=0, keepdims=True)
        occ = gb + gl
        slot = jnp.minimum(i, KEEP)
        for c in range(n_ch):
            sc_c = fac[i, c * 8:(c + 1) * 8, :] * occ
            e3 = ebuf[slot, c * CHUNK:(c + 1) * CHUNK, :].reshape(n_sub, 8, ROWS)
            d = (e3 * sc_c[None]).reshape(CHUNK, ROWS) - jnp.where(v_iota == y - c * CHUNK, gl, 0.0)
            if c == 0:
                d = d - jnp.where(v_iota == 0, gb, 0.0)
            dznew[c * CHUNK:(c + 1) * CHUNK, :] = d.astype(BF16)

    def bwd(i, carry):
        again(i + 1)
        dzcur[...] = dznew[...]
        win = tbl[0, i]
        ohu = as_bf16(onehot(gu, idx[i, 0:1]))
        oht = as_bf16(onehot(128, idx[i, 1:2]))
        half = n_j // 2
        d_logits(i + 1)
        for q in range(2):
            rows = slice(q * half, (q + 1) * half)
            hf = hbuf[i, rows].astype(F32)
            dh = dot(wo_ref[rows], dzcur[...])
            dp = (dh * (1.0 - hf * hf)).astype(BF16)
            segu[rows, lanes_of(win)] += dot(dp, ohu, NT)
            segt[win, rows] += dot(dp, oht, NT)
        for c in range(n_v // 256):
            gwo_ref[:, c * 256:(c + 1) * 256] += dot(hbuf[i], dzcur[c * 256:(c + 1) * 256, :], NT)
        return carry

    again(jnp.int32(0))
    d_logits(jnp.int32(0))
    lax.fori_loop(0, n_blocks, bwd, 0)

    dc_t = segu[...].astype(BF16)
    for w in range(1, n_win):
        segt[w, :, 0:step_t] += segt[w - 1, :, step_t:2 * step_t]
    parts = [segt[w, :, 0:step_t] for w in range(n_win)] + [segt[n_win - 1, :, step_t:2 * step_t]]
    da_t = jnp.concatenate(parts, axis=1).astype(BF16)
    gwp_ref[...] = dot(g_ref[...].T, dc_t, NT)
    gwe_ref[...] = dot(f_ref[...].T, da_t, NT)
    gf_ref[...] = dot(da_t.T, we_ref[...], NT).astype(BF16)


def core_call(f2, g2, w_enc, w_pred, w_out, lab_row, flen, llen, n_t, n_u):
    n_utt = flen.shape[0]
    n_j = w_enc.shape[1]
    n_v = w_out.shape[1]
    n_win = n_utt * 2 // WIN - 1
    max_blk = n_utt * n_t * n_u // ROWS + 2
    n_kt = (n_t + n_u) * n_t
    n_st = n_v // CHUNK * 8
    pad = lambda x: jnp.broadcast_to(jnp.pad(x, (0, 128 - n_utt))[None, :], (n_t, 128))
    vm = pl.BlockSpec(memory_space=pltpu.VMEM)
    sm = pl.BlockSpec(memory_space=pltpu.SMEM)
    return pl.pallas_call(
        functools.partial(core_kernel, n_utt, n_t, n_u),
        out_shape=(
            jax.ShapeDtypeStruct((8, 128), F32),
            jax.ShapeDtypeStruct((n_utt * n_t, f2.shape[1]), BF16),
            jax.ShapeDtypeStruct(w_enc.shape, F32),
            jax.ShapeDtypeStruct(w_pred.shape, F32),
            jax.ShapeDtypeStruct(w_out.shape, F32),
        ),
        in_specs=[sm, sm] + [vm] * 8,
        out_specs=(vm,) * 5,
        scratch_shapes=[
            pltpu.VMEM((n_v, n_j), BF16),
            pltpu.VMEM((n_j, n_utt * n_u), BF16),
            pltpu.VMEM((n_win, n_j, 128), BF16),
            pltpu.VMEM((n_win, 16, WIN * n_u), BF16),
            pltpu.VMEM((max_blk, n_j, ROWS), BF16),
            pltpu.VMEM((n_j, ROWS), BF16),
            pltpu.VMEM((n_j, ROWS), BF16),
            pltpu.VMEM((min(max_blk, KEEP + 1), n_v, ROWS), F32),
            pltpu.VMEM((max_blk, n_st, ROWS), F32),
            pltpu.VMEM((n_st, ROWS), F32),
            pltpu.VMEM((n_st, ROWS), F32),
            pltpu.VMEM((256, ROWS), BF16),
            pltpu.VMEM((max_blk, 8, ROWS), jnp.int32),
            pltpu.VMEM((n_v, ROWS), BF16),
            pltpu.VMEM((n_v, ROWS), BF16),
            pltpu.VMEM((n_kt, 256), F32),
            pltpu.VMEM((n_t + n_u, n_t, 128), F32),
            pltpu.VMEM((n_t + n_u, n_t, 128), F32),
            pltpu.VMEM((n_t + n_u, n_t, 128), F32),
            pltpu.VMEM((2 * n_kt, 128), F32),
            pltpu.VMEM((2 * n_kt, 128), BF16),
            pltpu.VMEM((n_j, n_utt * n_u), F32),
            pltpu.VMEM((n_win, n_j, 128), F32),
            pltpu.SMEM((3, max_blk), jnp.int32),
            pltpu.SMEM((n_utt + 1,), jnp.int32),
        ],
        compiler_params=pltpu.CompilerParams(vmem_limit_bytes=67043328),
        name="rnnt_core",
    )(flen, llen, pad(flen), pad(llen), lab_row, f2, g2, w_enc, w_pred, w_out)


def solution(mesh):
    seq_size = mesh.shape['seq']

    def local_fn(enc_out, pred_out, w_enc, w_pred, w_out, labels, frame_len, label_len):
        seq_idx = lax.axis_index('seq')
        core = seq_idx % 2
        n_utt, n_loc, n_h = enc_out.shape
        n_u = pred_out.shape[1]
        n_t = n_loc * seq_size
        half = n_utt // 2
        f_all = jnp.zeros((half, seq_size, n_loc, n_h), enc_out.dtype)
        mine = lax.dynamic_slice_in_dim(enc_out, core * half, half, 0)
        f_all = lax.dynamic_update_slice(f_all, mine[:, None], (0, seq_idx, 0, 0))
        for d in range(1, seq_size):
            dst = (seq_idx + d) % seq_size
            piece = lax.dynamic_slice_in_dim(enc_out, (dst % 2) * half, half, 0)
            got = lax.ppermute(piece, 'seq', [(s, (s + d) % seq_size) for s in range(seq_size)])
            f_all = lax.dynamic_update_slice(f_all, got[:, None], (0, (seq_idx - d) % seq_size, 0, 0))
        f2 = f_all.reshape(half * n_t, n_h)
        g2 = lax.dynamic_slice_in_dim(pred_out, core * half, half, 0).reshape(half * n_u, n_h)
        lab = jnp.pad(lax.dynamic_slice_in_dim(labels, core * half, half, 0), ((0, 0), (0, 1)), constant_values=-1)
        flen = lax.dynamic_slice_in_dim(frame_len, core * half, half, 0)
        llen = lax.dynamic_slice_in_dim(label_len, core * half, half, 0)
        loss, gf, gwe, gwp, gwo = core_call(f2, g2, w_enc, w_pred, w_out, lab.reshape(1, half * n_u), flen, llen, n_t, n_u)
        swap = [(s, s ^ 1) for s in range(seq_size)]
        gf = gf.reshape(half, seq_size, n_loc, n_h)
        keep = lax.dynamic_slice_in_dim(gf, seq_idx, 1, 1)[:, 0]
        give = lax.dynamic_slice_in_dim(gf, seq_idx + 1 - 2 * core, 1, 1)[:, 0]
        got = lax.ppermute(give, 'seq', swap)
        grad_enc = jnp.where(core == 0, jnp.concatenate([keep, got], 0), jnp.concatenate([got, keep], 0))
        loss = loss[0, :half]
        other = lax.ppermute(loss, 'seq', swap)
        utt_loss = jnp.where(core == 0, jnp.concatenate([loss, other]), jnp.concatenate([other, loss]))
        gwe = gwe + lax.ppermute(gwe, 'seq', swap)
        gwp = gwp + lax.ppermute(gwp, 'seq', swap)
        gwo = gwo + lax.ppermute(gwo, 'seq', swap)
        return utt_loss, grad_enc, gwe, gwp, gwo

    in_specs = (P('dp', 'seq', None), P('dp', None, None), P(None, None), P(None, None), P(None, None), P('dp', None), P('dp'), P('dp'))
    out_specs = (P('dp'), P('dp', 'seq', None), P('dp', None), P('dp', None), P('dp', None))
    return jax.shard_map(local_fn, mesh=mesh, in_specs=in_specs, out_specs=out_specs, check_vma=False)
```

```python
import functools

import jax
import jax.numpy as jnp
from jax import lax
from jax.experimental import pallas as pl
from jax.experimental.pallas import tpu as pltpu
from jax.sharding import PartitionSpec as P

NEG = -1.0e30
ROWS = 256
WIN = 8
CHUNK = 128
CORE_MIN, CORE_MAX = 24, 40
KEEP = 15
F32 = jnp.float32
BF16 = jnp.bfloat16
MESH = pl.DeviceIdType.MESH
NT = (((1,), (1,)), ((), ()))
NN = (((1,), (0,)), ((), ()))


def dot(a, b, dims=NN):
    return lax.dot_general(a, b, dims, preferred_element_type=F32)


def split3(x):
    hi = x.astype(BF16).astype(F32)
    r1 = x - hi
    mid = r1.astype(BF16).astype(F32)
    return hi, mid, r1 - mid


def logadd(a, b):
    m = jnp.maximum(a, b)
    return m + jnp.log(1.0 + jnp.exp(jnp.minimum(a, b) - m))


def gather_kernel(n_t, enc_ref, g_ref, we_ref, wp_ref, wo_ref, c_ref, a_ref, wot_ref, f_ref, fbuf, send_sem, recv_sem):
    me = lax.axis_index('seq')
    n_seq = fbuf.shape[0]
    partner = me + 1 - 2 * (me % 2)
    peer = (me + 2) % n_seq
    barrier = pltpu.get_barrier_semaphore()
    for other in (partner, peer):
        pl.semaphore_signal(barrier, inc=1, device_id={'seq': other}, device_id_type=MESH)
    pl.semaphore_wait(barrier, 2)

    def send(src, slot, sem, other):
        return pltpu.make_async_remote_copy(src_ref=src, dst_ref=fbuf.at[slot], send_sem=send_sem.at[sem], recv_sem=recv_sem.at[sem],
                                            device_id={'seq': other}, device_id_type=MESH)
    to_peer = send(enc_ref, me, 0, peer)
    to_peer.start()
    to_partner = send(enc_ref, me, 1, partner)
    to_partner.start()
    fbuf[me] = enc_ref[...]
    c_ref[...] = dot(wp_ref[...].T, g_ref[...], NT).astype(BF16)
    wot_ref[...] = wo_ref[...].T
    we_t = we_ref[...].T
    to_peer.wait_recv()
    relay = send(fbuf.at[peer], peer, 2, partner)
    relay.start()
    n_f = f_ref.shape[0]
    n_b = n_f // n_t
    n_loc = n_t // n_seq
    row = lax.broadcasted_iota(jnp.int32, (n_f, n_f), 0)
    col = lax.broadcasted_iota(jnp.int32, (n_f, n_f), 1)
    t = row % n_t
    order = jnp.where(col == (t // n_loc) * (n_b * n_loc) + (row // n_t) * n_loc + t % n_loc, 1.0, 0.0).astype(BF16)
    to_partner.wait_recv()
    relay.wait_recv()
    f_bt = dot(order, fbuf[...].reshape(n_f, f_ref.shape[1])).astype(BF16)
    f_ref[...] = f_bt
    a_ref[:, 0:n_f] = dot(we_t, f_bt, NT).astype(BF16)
    a_ref[:, n_f:] = jnp.zeros((a_ref.shape[0], a_ref.shape[1] - n_f), BF16)
    to_peer.wait_send()
    to_partner.wait_send()
    relay.wait_send()


def gather_call(enc, g2, w_enc, w_pred, w_out, n_seq, n_t):
    n_rows, n_h = enc.shape
    n_j = w_enc.shape[1]
    vm = pl.BlockSpec(memory_space=pltpu.VMEM)
    n_f = n_rows * n_seq
    return pl.pallas_call(
        functools.partial(gather_kernel, n_t),
        out_shape=(
            jax.ShapeDtypeStruct((n_j, g2.shape[0]), BF16),
            jax.ShapeDtypeStruct((n_j, n_f + 128), BF16),
            jax.ShapeDtypeStruct(w_out.shape[::-1], BF16),
            jax.ShapeDtypeStruct((n_f, n_h), BF16),
        ),
        in_specs=[vm] * 5,
        out_specs=(vm,) * 4,
        scratch_shapes=[
            pltpu.VMEM((n_seq, n_rows, n_h), BF16),
            pltpu.SemaphoreType.DMA((3,)),
            pltpu.SemaphoreType.DMA((3,)),
        ],
        compiler_params=pltpu.CompilerParams(collective_id=0, has_side_effects=True, vmem_limit_bytes=40 << 20),
        name="rnnt_gather",
    )(enc, g2, w_enc, w_pred, w_out)


def reduce_kernel(n_t, gwo_p, dc_p, da_p, loss_p, g_p, f_p, we_p, loss_ref, gf_ref, gwe_ref, gwp_ref, gwo_ref,
                  gwo_v, dc_v, da_v, loss_v, g_v, f_v, we_v, gwp_v, rgwo, rgwp, rda, rloss, in_sem, send_sem, recv_sem):
    me = lax.axis_index('seq')
    partner = me + 1 - 2 * (me % 2)
    loads = [pltpu.make_async_copy(src, dst, in_sem.at[q]) for q, (src, dst) in enumerate(
        ((dc_p, dc_v), (g_p, g_v), (da_p, da_v), (loss_p, loss_v), (f_p, f_v), (we_p, we_v), (gwo_p, gwo_v)))]
    for load in loads:
        load.start()
    barrier = pltpu.get_barrier_semaphore()
    pl.semaphore_signal(barrier, inc=1, device_id={'seq': partner}, device_id_type=MESH)
    pl.semaphore_wait(barrier, 1)

    def send(src, dst, sem):
        return pltpu.make_async_remote_copy(src_ref=src, dst_ref=dst, send_sem=send_sem.at[sem], recv_sem=recv_sem.at[sem],
                                            device_id={'seq': partner}, device_id_type=MESH)
    n_part = 4
    rows = gwo_p.shape[0] // n_part
    sends = [send(da_p, rda, 0), send(loss_p, rloss, 1)]
    sends += [send(gwo_p.at[pl.ds(q * rows, rows)], rgwo.at[pl.ds(q * rows, rows)], 2 + q) for q in range(n_part)]
    for s in sends:
        s.start()
    loads[0].wait()
    loads[1].wait()
    gwp_v[...] = dot(g_v[...].T, dc_v[...], NT)
    s_gwp = send(gwp_v, rgwp, 2 + n_part)
    for load in loads[2:]:
        load.wait()
    sends[0].wait_recv()
    sends[1].wait_recv()
    loss_ref[...] = loss_v[...] + rloss[...]
    da = (da_v[...].astype(F32) + rda[...].astype(F32)).astype(BF16)
    s_gwp.start()
    gwe_ref[...] = dot(f_v[...].T, da, NT)
    n_f = da.shape[1]
    n_own = gf_ref.shape[0]
    n_loc = n_own * n_t // n_f
    row = lax.broadcasted_iota(jnp.int32, (n_own, n_f), 0)
    col = lax.broadcasted_iota(jnp.int32, (n_own, n_f), 1)
    own = jnp.where(col == (row // n_loc) * n_t + me * n_loc + row % n_loc, 1.0, 0.0).astype(BF16)
    gf_ref[...] = dot(dot(own, da, NT).astype(BF16), we_v[...], NT).astype(BF16)
    for q in range(n_part):
        sends[2 + q].wait_recv()
        part = slice(q * rows, (q + 1) * rows)
        gwo_ref[part] = gwo_v[part] + rgwo[part]
    s_gwp.wait_recv()
    gwp_ref[...] = gwp_v[...] + rgwp[...]
    for s in sends + [s_gwp]:
        s.wait_send()


def reduce_call(gwo, dc_t, da_t, loss, g2, f2, w_enc, n_own, n_t):
    vm = pl.BlockSpec(memory_space=pltpu.VMEM)
    like = lambda x: pltpu.VMEM(x.shape, x.dtype)
    gwp_shape = (g2.shape[1], dc_t.shape[0])
    return pl.pallas_call(
        functools.partial(reduce_kernel, n_t),
        out_shape=(
            jax.ShapeDtypeStruct(loss.shape, F32),
            jax.ShapeDtypeStruct((n_own, w_enc.shape[0]), BF16),
            jax.ShapeDtypeStruct(w_enc.shape, F32),
            jax.ShapeDtypeStruct(gwp_shape, F32),
            jax.ShapeDtypeStruct(gwo.shape, F32),
        ),
        in_specs=[pl.BlockSpec(memory_space=pl.ANY)] * 7,
        out_specs=(vm,) * 5,
        scratch_shapes=[like(x) for x in (gwo, dc_t, da_t, loss, g2, f2, w_enc)] + [
            pltpu.VMEM(gwp_shape, F32), like(gwo), pltpu.VMEM(gwp_shape, F32), like(da_t), like(loss),
            pltpu.SemaphoreType.DMA((7,)),
            pltpu.SemaphoreType.DMA((7,)),
            pltpu.SemaphoreType.DMA((7,)),
        ],
        compiler_params=pltpu.CompilerParams(collective_id=1, has_side_effects=True, vmem_limit_bytes=40 << 20),
        name="rnnt_reduce",
    )(gwo, dc_t, da_t, loss, g2, f2, w_enc)


def core_kernel(n_t, n_u, flen_s, llen_s, flen_v, llen_v, lab_ref, c_buf, a_buf, wot, wo_ref,
                loss_ref, dc_ref, da_ref, gwo_ref,
                ylab, hbuf, hnew, hcur, ebuf, fac, mch, sch, vsb, idx, dznew, dzcur, sk, abuf, t1buf, t2buf,
                gocc, gocb, segu, segt, tbl, off):
    n_utt = flen_s.shape[0]
    n_j = c_buf.shape[0]
    n_v = wo_ref.shape[1]
    step_u = WIN // 2 * n_u
    step_t = WIN // 2 * n_t
    per_tile = 128 // step_t
    gu = WIN * n_u
    n_win = n_utt * 2 // WIN - 1
    n_diag = n_t + n_u - 1
    n_kt = (n_diag + 1) * n_t
    n_ch = n_v // CHUNK

    def off_step(b, total):
        off[b] = total
        return total + flen_s[b] * (llen_s[b] + 1)
    off[n_utt] = lax.fori_loop(0, n_utt, off_step, jnp.int32(0))

    total = off[n_utt]
    cut = lax.fori_loop(CORE_MIN, CORE_MAX, lambda b, n: n + jnp.where(off[b] + off[b + 1] <= total, 1, 0), jnp.int32(CORE_MIN))
    first_core = lax.axis_index('seq') % 2 == 0
    u_lo = jnp.where(first_core, 0, cut)
    u_hi = jnp.where(first_core, cut, n_utt)
    stop = off[u_hi]

    def utt_step(b, carry):
        win = jnp.minimum(b // (WIN // 2), n_win - 1)
        base = off[win * (WIN // 2)]
        last = jnp.minimum(off[win * (WIN // 2) + WIN], stop)

        def emit(c):
            n, pos = c
            end = jnp.minimum(pos + ROWS, last)
            tbl[0, n] = win
            tbl[1, n] = pos - base
            tbl[2, n] = end - base
            return n + 1, end
        return lax.while_loop(lambda c: c[1] < off[b + 1], emit, carry)
    n_blocks, _ = lax.fori_loop(u_lo, u_hi, utt_step, (jnp.int32(0), off[u_lo]))
    tbl[0, n_blocks] = 0
    tbl[1, n_blocks] = 0
    tbl[2, n_blocks] = 0

    lab = lab_ref[...]
    n_lab = lab.shape[1]
    place = jnp.where(lax.broadcasted_iota(jnp.int32, (n_lab, n_utt * n_u), 1) % n_u
                      == lax.broadcasted_iota(jnp.int32, (n_lab, n_utt * n_u), 0), 1.0, 0.0).astype(BF16)
    mine = (lax.broadcasted_iota(jnp.int32, (n_utt, n_utt * n_u), 1) // n_u
            == lax.broadcasted_iota(jnp.int32, (n_utt, n_utt * n_u), 0))
    flat = []
    for part in (lax.shift_right_arithmetic(lab, 5), jnp.bitwise_and(lab, 31)):
        spread = dot(part.astype(F32).astype(BF16), place)
        flat.append(jnp.sum(jnp.where(mine, spread, 0.0), axis=0, keepdims=True))
    for w in range(n_win):
        row = lax.broadcasted_iota(jnp.int32, (16, gu), 0)
        hi, lo = (x[:, w * step_u:w * step_u + gu] for x in flat)
        ylab[w] = jnp.where(row == 0, hi, jnp.where(row == 1, lo, 0.0)).astype(BF16)
    sk[...] = jnp.zeros_like(sk)
    vsb[...] = jnp.zeros_like(vsb)
    segu[...] = jnp.zeros_like(segu)
    segt[...] = jnp.zeros_like(segt)
    gwo_ref[...] = jnp.zeros_like(gwo_ref)

    def onehot(n, index_row):
        return (lax.broadcasted_iota(jnp.int32, (n, ROWS), 0) == index_row)

    def as_bf16(mask):
        return jnp.where(mask, 1.0, 0.0).astype(BF16)

    v_iota = lax.broadcasted_iota(jnp.int32, (CHUNK, ROWS), 0)
    n_sub = CHUNK // 8

    def lanes_of(win):
        return pl.ds(pl.multiple_of(win * step_u, 128), gu)

    def frame_lanes_of(win):
        return pl.ds(pl.multiple_of(win // per_tile * 128, 128), 256)

    part_row = lax.broadcasted_iota(jnp.int32, (128, ROWS), 0)

    def spread3(idx_b, parts):
        out = jnp.zeros((128, ROWS), F32)
        for q, part in enumerate(parts):
            out = jnp.where(part_row == idx_b + q * CORE_MAX, part, out)
        return out.astype(BF16)

    def prepare(i):
        win = tbl[0, i]
        r = tbl[1, i] + lax.broadcasted_iota(jnp.int32, (1, ROWS), 1)
        end_r = tbl[2, i]
        start = jnp.int32(0)
        bl = jnp.full((1, ROWS), -1, jnp.int32)
        w = jnp.zeros((1, ROWS), jnp.int32)
        u1 = jnp.ones((1, ROWS), jnp.int32)
        for j in range(WIN):
            u1_j = llen_s[win * (WIN // 2) + j] + 1
            end = start + flen_s[win * (WIN // 2) + j] * u1_j
            inside = (r >= start) & (r < jnp.minimum(end, end_r))
            bl = jnp.where(inside, j, bl)
            w = jnp.where(inside, r - start, w)
            u1 = jnp.where(inside, u1_j, u1)
            start = end
        valid = bl >= 0
        t = jnp.zeros((1, ROWS), jnp.int32)
        for j in range(1, n_t):
            t = t + jnp.where(w >= j * u1, 1, 0)
        u = w - t * u1
        idx_u = jnp.where(valid, bl * n_u + u, -1)
        idx_t = jnp.where(valid, bl * n_t + t + win % per_tile * step_t, -1)
        idx_kt = jnp.where(valid, (t + u) * n_t + t, -1)
        idx_b = jnp.where(valid, win * (WIN // 2) + bl - u_lo, -1024)
        ohu = as_bf16(onehot(gu, idx_u))
        oht = as_bf16(onehot(256, idx_t))
        half = n_j // 2
        for q in range(2):
            rows = slice(q * half, (q + 1) * half)
            pre = dot(c_buf[rows, lanes_of(win)], ohu) + dot(a_buf[rows, frame_lanes_of(win)], oht)
            hnew[rows] = jnp.tanh(pre).astype(BF16)
        yy = dot(ylab[win], ohu)
        y = (yy[0:1] * 32.0 + yy[1:2]).astype(jnp.int32)
        rows8 = lax.broadcasted_iota(jnp.int32, (8, ROWS), 0)
        idx[i] = jnp.where(rows8 == 0, idx_u, jnp.where(rows8 == 1, idx_t, jnp.where(rows8 == 2, idx_kt, jnp.where(rows8 == 3, idx_b, y))))

    def scatter(i):
        okt = as_bf16(onehot(n_kt, idx[i, 2:3]))
        sk[...] += dot(okt, vsb[...], NT)

    def fwd(i, carry):
        scatter(jnp.maximum(i - 1, 0))
        hcur[...] = hnew[...]
        hbuf[i] = hnew[...]
        y = idx[i, 4:5]
        idx_b = idx[i, 3:4]
        slot = jnp.minimum(i, KEEP)
        prepare(i + 1)
        lz = None
        blank_z = None
        for c in range(n_ch):
            z = dot(wot[c * CHUNK:(c + 1) * CHUNK, :], hcur[...])
            z3 = z.reshape(n_sub, 8, ROWS)
            zl = jnp.sum(jnp.where(v_iota == y - c * CHUNK, z, 0.0).reshape(n_sub, 8, ROWS), axis=0)
            lz = zl if lz is None else lz + zl
            if c == 0:
                blank_z = z[0:1, :]
            m_c = jnp.max(z3, axis=0)
            e3 = jnp.exp(z3 - m_c[None])
            ebuf[slot, c * CHUNK:(c + 1) * CHUNK, :] = e3.reshape(CHUNK, ROWS)
            mch[c * 8:(c + 1) * 8, :] = m_c
            sch[c * 8:(c + 1) * 8, :] = jnp.sum(e3, axis=0)
        m8 = jnp.max(mch[...].reshape(n_ch, 8, ROWS), axis=0)
        m = jnp.max(m8, axis=0, keepdims=True)
        f_all = jnp.exp(mch[...] - m)
        s = jnp.sum(jnp.sum((sch[...] * f_all).reshape(n_ch, 8, ROWS), axis=0), axis=0, keepdims=True)
        fac[i] = f_all * (1.0 / s)
        lab_z = jnp.sum(lz, axis=0, keepdims=True)
        lse = m + jnp.log(s)
        b_parts = split3(blank_z - lse)
        l_parts = split3(lab_z - lse)
        vsb[0:128] = spread3(idx_b, b_parts)
        vsb[128:256] = spread3(idx_b, l_parts)
        return carry

    prepare(jnp.int32(0))
    lax.fori_loop(0, n_blocks, fwd, 0)
    scatter(n_blocks - 1)

    tt = lax.broadcasted_iota(jnp.int32, (n_t, 128), 0)
    def own_lanes(ref):
        x = jnp.concatenate([ref[...], jnp.zeros((1, 128 - n_utt), jnp.int32)], axis=1).astype(F32)
        return pltpu.roll(jnp.broadcast_to(x, (n_t, 128)), (128 - u_lo) % 128, 1).astype(jnp.int32)
    t_len = own_lanes(flen_v)
    u_len = own_lanes(llen_v)

    def scores(k):
        lo = k * n_t
        x, y = (v + pltpu.roll(v, 128 - CORE_MAX, 1) + pltpu.roll(v, 128 - 2 * CORE_MAX, 1)
                for v in (sk[lo:lo + n_t, 0:128], sk[lo:lo + n_t, 128:256]))
        uu = k - tt
        ok = (uu >= 0) & (tt < t_len)
        bl_k = jnp.where(ok & (uu <= u_len), x, NEG)
        lb_k = jnp.where(ok & (uu < u_len), y, NEG)
        return bl_k, lb_k

    alpha = jnp.where(tt == 0, 0.0, NEG).astype(F32)
    abuf[0] = alpha
    beta = jnp.full((n_t, 128), NEG, F32)
    sc = [scores(k) for k in range(n_diag)]
    for step in range(n_diag):
        if step > 0:
            bl_k, lb_k = sc[step - 1]
            p1 = jnp.where(tt == 0, NEG, pltpu.roll(alpha + bl_k, 1, 0))
            alpha = logadd(p1, alpha + lb_k)
            abuf[step] = alpha
        k = n_diag - 1 - step
        bl_k, lb_k = sc[k]
        up = jnp.where(tt == n_t - 1, jnp.where(u_len == k + 1 - n_t, 0.0, NEG), pltpu.roll(beta, n_t - 1, 0))
        t1 = up + bl_k
        t2 = beta + lb_k
        t1buf[k] = t1
        t2buf[k] = t2
        beta = jnp.where(tt >= t_len, jnp.where(k - tt == u_len, 0.0, NEG), logadd(t1, t2))
    log_p = beta[0:1, :]
    lane = lax.broadcasted_iota(jnp.int32, (n_t, 128), 1)
    loss_ref[...] = pltpu.roll(jnp.where(lane < u_hi - u_lo, -log_p, 0.0), u_lo, 1)
    lane_ok = lane < CORE_MAX
    for k in range(n_diag):
        for which, buf in enumerate((t1buf, t2buf)):
            occ = jnp.where(lane_ok, jnp.exp(jnp.minimum(abuf[k] + buf[k] - log_p, 0.0)), 0.0)
            hi, mid, lo = split3(occ)
            lo_row = which * n_kt + k * n_t
            gocc[lo_row:lo_row + n_t, :] = hi + pltpu.roll(mid, CORE_MAX, 1) + pltpu.roll(lo, 2 * CORE_MAX, 1)
    for which in range(2):
        gocc[which * n_kt + n_diag * n_t:(which + 1) * n_kt, :] = jnp.zeros((n_kt - n_diag * n_t, 128), F32)
    gocb[...] = gocc[...].astype(BF16)

    def again(i):
        @pl.when(i >= KEEP)
        def _():
            m = None
            for c in range(n_ch):
                z = dot(wot[c * CHUNK:(c + 1) * CHUNK, :], hbuf[i])
                z3 = z.reshape(n_sub, 8, ROWS)
                ebuf[KEEP, c * CHUNK:(c + 1) * CHUNK, :] = jnp.exp(z3 - jnp.max(z3, axis=0)[None]).reshape(CHUNK, ROWS)

    def d_logits(i):
        idx_kt = idx[i, 2:3]
        idx_b = idx[i, 3:4]
        y = idx[i, 4:5]
        orep = spread3(idx_b, (1.0, 1.0, 1.0))
        okt = onehot(n_kt, idx_kt)
        gb = jnp.sum(jnp.where(okt, dot(gocb[0:n_kt], orep), 0.0), axis=0, keepdims=True)
        gl = jnp.sum(jnp.where(okt, dot(gocb[n_kt:2 * n_kt], orep), 0.0), axis=0, keepdims=True)
        occ = gb + gl
        slot = jnp.minimum(i, KEEP)
        for c in range(n_ch):
            sc_c = fac[i, c * 8:(c + 1) * 8, :] * occ
            e3 = ebuf[slot, c * CHUNK:(c + 1) * CHUNK, :].reshape(n_sub, 8, ROWS)
            d = (e3 * sc_c[None]).reshape(CHUNK, ROWS) - jnp.where(v_iota == y - c * CHUNK, gl, 0.0)
            if c == 0:
                d = d - jnp.where(v_iota == 0, gb, 0.0)
            dznew[c * CHUNK:(c + 1) * CHUNK, :] = d.astype(BF16)

    def bwd(i, carry):
        again(i + 1)
        dzcur[...] = dznew[...]
        win = tbl[0, i]
        ohu = as_bf16(onehot(gu, idx[i, 0:1]))
        oht = as_bf16(onehot(256, idx[i, 1:2]))
        half = n_j // 2
        d_logits(i + 1)
        for q in range(2):
            rows = slice(q * half, (q + 1) * half)
            hf = hbuf[i, rows].astype(F32)
            dh = dot(wo_ref[rows], dzcur[...])
            dp = (dh * (1.0 - hf * hf)).astype(BF16)
            segu[rows, lanes_of(win)] += dot(dp, ohu, NT)
            segt[rows, frame_lanes_of(win)] += dot(dp, oht, NT)
        for c in range(n_v // 256):
            gwo_ref[:, c * 256:(c + 1) * 256] += dot(hbuf[i], dzcur[c * 256:(c + 1) * 256, :], NT)
        return carry

    again(jnp.int32(0))
    d_logits(jnp.int32(0))
    lax.fori_loop(0, n_blocks, bwd, 0)

    dc_ref[...] = segu[...].astype(BF16)
    da_ref[...] = segt[:, 0:n_utt * n_t].astype(BF16)


def core_call(c_t, a_t, wot, w_out, labels, flen, llen, n_t, n_u):
    n_utt = flen.shape[0]
    n_j = c_t.shape[0]
    n_v = w_out.shape[1]
    n_win = n_utt * 2 // WIN - 1
    max_blk = n_utt // 2 * n_t * n_u // ROWS + 4
    n_kt = (n_t + n_u) * n_t
    n_st = n_v // CHUNK * 8
    vm = pl.BlockSpec(memory_space=pltpu.VMEM)
    sm = pl.BlockSpec(memory_space=pltpu.SMEM)
    return pl.pallas_call(
        functools.partial(core_kernel, n_t, n_u),
        out_shape=(
            jax.ShapeDtypeStruct((8, 128), F32),
            jax.ShapeDtypeStruct((n_j, n_utt * n_u), BF16),
            jax.ShapeDtypeStruct((n_j, n_utt * n_t), BF16),
            jax.ShapeDtypeStruct(w_out.shape, F32),
        ),
        in_specs=[sm, sm] + [vm] * 7,
        out_specs=(vm,) * 4,
        scratch_shapes=[
            pltpu.VMEM((n_win, 16, WIN * n_u), BF16),
            pltpu.VMEM((max_blk, n_j, ROWS), BF16),
            pltpu.VMEM((n_j, ROWS), BF16),
            pltpu.VMEM((n_j, ROWS), BF16),
            pltpu.VMEM((min(max_blk, KEEP + 1), n_v, ROWS), F32),
            pltpu.VMEM((max_blk, n_st, ROWS), F32),
            pltpu.VMEM((n_st, ROWS), F32),
            pltpu.VMEM((n_st, ROWS), F32),
            pltpu.VMEM((256, ROWS), BF16),
            pltpu.VMEM((max_blk, 8, ROWS), jnp.int32),
            pltpu.VMEM((n_v, ROWS), BF16),
            pltpu.VMEM((n_v, ROWS), BF16),
            pltpu.VMEM((n_kt, 256), F32),
            pltpu.VMEM((n_t + n_u, n_t, 128), F32),
            pltpu.VMEM((n_t + n_u, n_t, 128), F32),
            pltpu.VMEM((n_t + n_u, n_t, 128), F32),
            pltpu.VMEM((2 * n_kt, 128), F32),
            pltpu.VMEM((2 * n_kt, 128), BF16),
            pltpu.VMEM((n_j, n_utt * n_u), F32),
            pltpu.VMEM((n_j, n_utt * n_t + 128), F32),
            pltpu.SMEM((3, max_blk), jnp.int32),
            pltpu.SMEM((n_utt + 1,), jnp.int32),
        ],
        compiler_params=pltpu.CompilerParams(vmem_limit_bytes=67043328),
        name="rnnt_core",
    )(flen, llen, flen.reshape(1, n_utt), llen.reshape(1, n_utt), labels, c_t, a_t, wot, w_out)


def solution(mesh):
    seq_size = mesh.shape['seq']

    def local_fn(enc_out, pred_out, w_enc, w_pred, w_out, labels, frame_len, label_len):
        n_utt, n_loc, n_h = enc_out.shape
        n_u = pred_out.shape[1]
        n_t = n_loc * seq_size
        g2 = pred_out.reshape(n_utt * n_u, n_h)
        c_t, a_t, wot, f2 = gather_call(enc_out.reshape(n_utt * n_loc, n_h), g2, w_enc, w_pred, w_out, seq_size, n_t)
        loss, dc_t, da_t, gwo = core_call(c_t, a_t, wot, w_out, labels, frame_len, label_len, n_t, n_u)
        loss, gf, gwe, gwp, gwo = reduce_call(gwo, dc_t, da_t, loss, g2, f2, w_enc, n_utt * n_loc, n_t)
        return loss[0, :n_utt], gf.reshape(n_utt, n_loc, n_h), gwe, gwp, gwo

    in_specs = (P('dp', 'seq', None), P('dp', None, None), P(None, None), P(None, None), P(None, None), P('dp', None), P('dp'), P('dp'))
    out_specs = (P('dp'), P('dp', 'seq', None), P('dp', None), P('dp', None), P('dp', None))
    return jax.shard_map(local_fn, mesh=mesh, in_specs=in_specs, out_specs=out_specs, check_vma=False)
```

```python
import functools

import jax
import jax.numpy as jnp
from jax import lax
from jax.experimental import pallas as pl
from jax.experimental.pallas import tpu as pltpu
from jax.sharding import PartitionSpec as P

NEG = -1.0e30
ROWS = 256
WIN = 8
CHUNK = 128
CORE_MIN, CORE_MAX = 24, 40
GATHER_VMEM = 40 << 20
CORE_VMEM = 51 << 20
REDUCE_VMEM = 36 << 20
STORE_VMEM = 1 << 20
KEEP = 15
F32 = jnp.float32
BF16 = jnp.bfloat16
MESH = pl.DeviceIdType.MESH
NT = (((1,), (1,)), ((), ()))
NN = (((1,), (0,)), ((), ()))


def dot(a, b, dims=NN):
    return lax.dot_general(a, b, dims, preferred_element_type=F32)


def in_hbm(x):
    return pltpu.with_memory_space_constraint(x, pltpu.HBM)


def split3(x):
    hi = x.astype(BF16).astype(F32)
    r1 = x - hi
    mid = r1.astype(BF16).astype(F32)
    return hi, mid, r1 - mid


def logadd(a, b):
    m = jnp.maximum(a, b)
    return m + jnp.log(1.0 + jnp.exp(jnp.minimum(a, b) - m))


def gather_kernel(n_t, enc_h, g_h, we_h, wp_h, wo_h, c_ref, a_ref, wot_ref, f_ref, enc_ref, g_ref, we_ref, wp_ref, wo_ref, fbuf,
                  in_sem, send_sem, recv_sem):
    me = lax.axis_index('seq')
    n_seq = fbuf.shape[0]
    partner = me + 1 - 2 * (me % 2)
    peer = (me + 2) % n_seq
    load_enc, load_wo, load_wp, load_g, load_we = loads = [pltpu.make_async_copy(src, dst, in_sem.at[q]) for q, (src, dst) in enumerate(
        ((enc_h, enc_ref), (wo_h, wo_ref), (wp_h, wp_ref), (g_h, g_ref), (we_h, we_ref)))]
    for load in loads:
        load.start()
    barrier = pltpu.get_barrier_semaphore()
    for other in (partner, peer):
        pl.semaphore_signal(barrier, inc=1, device_id={'seq': other}, device_id_type=MESH)
    pl.semaphore_wait(barrier, 2)

    def send(src, slot, sem, other):
        return pltpu.make_async_remote_copy(src_ref=src, dst_ref=fbuf.at[slot], send_sem=send_sem.at[sem], recv_sem=recv_sem.at[sem],
                                            device_id={'seq': other}, device_id_type=MESH)
    load_enc.wait()
    to_peer = send(enc_ref, me, 0, peer)
    to_peer.start()
    to_partner = send(enc_ref, me, 1, partner)
    to_partner.start()
    fbuf[me] = enc_ref[...]
    load_wo.wait()
    wot_ref[...] = wo_ref[...].T
    load_wp.wait()
    load_g.wait()
    c_ref[...] = dot(wp_ref[...].T, g_ref[...], NT).astype(BF16)
    load_we.wait()
    we_t = we_ref[...].T
    to_peer.wait_recv()
    relay = send(fbuf.at[peer], peer, 2, partner)
    relay.start()
    n_f = f_ref.shape[0]
    n_b = n_f // n_t
    n_loc = n_t // n_seq
    row = lax.broadcasted_iota(jnp.int32, (n_f, n_f), 0)
    col = lax.broadcasted_iota(jnp.int32, (n_f, n_f), 1)
    t = row % n_t
    order = jnp.where(col == (t // n_loc) * (n_b * n_loc) + (row // n_t) * n_loc + t % n_loc, 1.0, 0.0).astype(BF16)
    to_partner.wait_recv()
    relay.wait_recv()
    f_bt = dot(order, fbuf[...].reshape(n_f, f_ref.shape[1])).astype(BF16)
    f_ref[...] = f_bt
    a_ref[:, 0:n_f] = dot(we_t, f_bt, NT).astype(BF16)
    a_ref[:, n_f:] = jnp.zeros((a_ref.shape[0], a_ref.shape[1] - n_f), BF16)
    to_peer.wait_send()
    to_partner.wait_send()
    relay.wait_send()


def gather_call(enc, g2, w_enc, w_pred, w_out, n_seq, n_t):
    n_rows, n_h = enc.shape
    n_j = w_enc.shape[1]
    vm = pl.BlockSpec(memory_space=pltpu.VMEM)
    n_f = n_rows * n_seq
    args = [in_hbm(x) for x in (enc, g2, w_enc, w_pred, w_out)]
    return pl.pallas_call(
        functools.partial(gather_kernel, n_t),
        out_shape=(
            pltpu.VMEM((n_j, g2.shape[0]), BF16),
            pltpu.VMEM((n_j, n_f + 128), BF16),
            pltpu.VMEM(w_out.shape[::-1], BF16),
            pltpu.VMEM((n_f, n_h), BF16),
        ),
        in_specs=[pl.BlockSpec(memory_space=pltpu.HBM)] * 5,
        out_specs=(vm,) * 4,
        scratch_shapes=[pltpu.VMEM(x.shape, x.dtype) for x in (enc, g2, w_enc, w_pred, w_out)] + [
            pltpu.VMEM((n_seq, n_rows, n_h), BF16),
            pltpu.SemaphoreType.DMA((5,)),
            pltpu.SemaphoreType.DMA((3,)),
            pltpu.SemaphoreType.DMA((3,)),
        ],
        compiler_params=pltpu.CompilerParams(collective_id=0, has_side_effects=True, vmem_limit_bytes=GATHER_VMEM),
        name="rnnt_gather",
    )(*args)


def reduce_kernel(n_t, gwo_v, dc_v, da_v, loss_v, f_v, g_p, we_p, loss_ref, gf_ref, gwe_ref, gwp_ref, gwo_ref,
                  g_v, we_v, gwp_v, rgwo, rgwp, rda, rloss, in_sem, send_sem, recv_sem):
    me = lax.axis_index('seq')
    partner = me + 1 - 2 * (me % 2)
    loads = [pltpu.make_async_copy(src, dst, in_sem.at[q]) for q, (src, dst) in enumerate(((g_p, g_v), (we_p, we_v)))]
    for load in loads:
        load.start()
    barrier = pltpu.get_barrier_semaphore()
    pl.semaphore_signal(barrier, inc=1, device_id={'seq': partner}, device_id_type=MESH)
    pl.semaphore_wait(barrier, 1)

    def send(src, dst, sem):
        return pltpu.make_async_remote_copy(src_ref=src, dst_ref=dst, send_sem=send_sem.at[sem], recv_sem=recv_sem.at[sem],
                                            device_id={'seq': partner}, device_id_type=MESH)
    n_part = 4
    rows = gwo_v.shape[0] // n_part
    sends = [send(da_v, rda, 0), send(loss_v, rloss, 1)]
    sends += [send(gwo_v.at[pl.ds(q * rows, rows)], rgwo.at[pl.ds(q * rows, rows)], 2 + q) for q in range(n_part)]
    for s in sends:
        s.start()
    loads[0].wait()
    gwp_v[...] = dot(g_v[...].T, dc_v[...], NT)
    s_gwp = send(gwp_v, rgwp, 2 + n_part)
    loads[1].wait()
    sends[0].wait_recv()
    sends[1].wait_recv()
    loss_ref[...] = loss_v[...] + rloss[...]
    da = (da_v[...].astype(F32) + rda[...].astype(F32)).astype(BF16)
    s_gwp.start()
    gwe_ref[...] = dot(f_v[...].T, da, NT)
    n_f = da.shape[1]
    n_own = gf_ref.shape[0]
    n_loc = n_own * n_t // n_f
    row = lax.broadcasted_iota(jnp.int32, (n_own, n_f), 0)
    col = lax.broadcasted_iota(jnp.int32, (n_own, n_f), 1)
    own = jnp.where(col == (row // n_loc) * n_t + me * n_loc + row % n_loc, 1.0, 0.0).astype(BF16)
    gf_ref[...] = dot(dot(own, da, NT).astype(BF16), we_v[...], NT).astype(BF16)
    for q in range(n_part):
        sends[2 + q].wait_recv()
        part = slice(q * rows, (q + 1) * rows)
        gwo_ref[part] = gwo_v[part] + rgwo[part]
    s_gwp.wait_recv()
    gwp_ref[...] = gwp_v[...] + rgwp[...]
    for s in sends + [s_gwp]:
        s.wait_send()


def reduce_call(gwo, dc_t, da_t, loss, g2, f2, w_enc, n_own, n_t):
    vm = pl.BlockSpec(memory_space=pltpu.VMEM)
    like = lambda x: pltpu.VMEM(x.shape, x.dtype)
    gwp_shape = (g2.shape[1], dc_t.shape[0])
    return pl.pallas_call(
        functools.partial(reduce_kernel, n_t),
        out_shape=(
            pltpu.VMEM(loss.shape, F32),
            pltpu.VMEM((n_own, w_enc.shape[0]), BF16),
            pltpu.VMEM(w_enc.shape, F32),
            pltpu.VMEM(gwp_shape, F32),
            pltpu.VMEM(gwo.shape, F32),
        ),
        in_specs=[vm] * 5 + [pl.BlockSpec(memory_space=pltpu.HBM)] * 2,
        out_specs=(vm,) * 5,
        scratch_shapes=[like(x) for x in (g2, w_enc)] + [
            pltpu.VMEM(gwp_shape, F32), like(gwo), pltpu.VMEM(gwp_shape, F32), like(da_t), like(loss),
            pltpu.SemaphoreType.DMA((2,)),
            pltpu.SemaphoreType.DMA((7,)),
            pltpu.SemaphoreType.DMA((7,)),
        ],
        compiler_params=pltpu.CompilerParams(collective_id=1, has_side_effects=True, vmem_limit_bytes=REDUCE_VMEM),
        name="rnnt_reduce",
    )(gwo, dc_t, da_t, loss, f2, in_hbm(g2), in_hbm(w_enc))


def store_kernel(n, *refs):
    sems = refs[2 * n]
    copies = [pltpu.make_async_copy(refs[q], refs[n + q], sems.at[q]) for q in range(n)]
    for copy in copies:
        copy.start()
    for copy in copies:
        copy.wait()


def store_call(arrays):
    n = len(arrays)
    return pl.pallas_call(
        functools.partial(store_kernel, n),
        out_shape=tuple(pltpu.HBM(x.shape, x.dtype) for x in arrays),
        in_specs=[pl.BlockSpec(memory_space=pltpu.VMEM)] * n,
        out_specs=(pl.BlockSpec(memory_space=pltpu.HBM),) * n,
        scratch_shapes=[pltpu.SemaphoreType.DMA((n,))],
        compiler_params=pltpu.CompilerParams(vmem_limit_bytes=STORE_VMEM),
        name="rnnt_store",
    )(*arrays)


def core_kernel(n_t, n_u, flen_s, llen_s, flen_v, llen_v, lab_ref, c_buf, a_buf, wot, wo_h,
                loss_ref, dc_ref, da_ref, gwo_ref,
                wo_ref, wo_sem, ylab, hbuf, hnew, hcur, ebuf, fac, mch, sch, vsb, idx, dznew, dzcur, sk, abuf, t1buf, t2buf,
                gocc, gocb, segu, segt, tbl, off):
    n_utt = flen_s.shape[0]
    n_j = c_buf.shape[0]
    n_v = wo_ref.shape[1]
    step_u = WIN // 2 * n_u
    step_t = WIN // 2 * n_t
    per_tile = 128 // step_t
    gu = WIN * n_u
    n_win = n_utt * 2 // WIN - 1
    n_diag = n_t + n_u - 1
    n_kt = (n_diag + 1) * n_t
    n_ch = n_v // CHUNK

    load_wo = pltpu.make_async_copy(wo_h, wo_ref, wo_sem)
    load_wo.start()

    def off_step(b, total):
        off[b] = total
        return total + flen_s[b] * (llen_s[b] + 1)
    off[n_utt] = lax.fori_loop(0, n_utt, off_step, jnp.int32(0))

    total = off[n_utt]
    cut = lax.fori_loop(CORE_MIN, CORE_MAX, lambda b, n: n + jnp.where(off[b] + off[b + 1] <= total, 1, 0), jnp.int32(CORE_MIN))
    first_core = lax.axis_index('seq') % 2 == 0
    u_lo = jnp.where(first_core, 0, cut)
    u_hi = jnp.where(first_core, cut, n_utt)
    stop = off[u_hi]

    def utt_step(b, carry):
        win = jnp.minimum(b // (WIN // 2), n_win - 1)
        base = off[win * (WIN // 2)]
        last = jnp.minimum(off[win * (WIN // 2) + WIN], stop)

        def emit(c):
            n, pos = c
            end = jnp.minimum(pos + ROWS, last)
            tbl[0, n] = win
            tbl[1, n] = pos - base
            tbl[2, n] = end - base
            return n + 1, end
        return lax.while_loop(lambda c: c[1] < off[b + 1], emit, carry)
    n_blocks, _ = lax.fori_loop(u_lo, u_hi, utt_step, (jnp.int32(0), off[u_lo]))
    tbl[0, n_blocks] = 0
    tbl[1, n_blocks] = 0
    tbl[2, n_blocks] = 0

    lab = lab_ref[...]
    place = jnp.where(lax.broadcasted_iota(jnp.int32, (n_utt, n_utt * n_u), 1) // n_u
                      == lax.broadcasted_iota(jnp.int32, (n_utt, n_utt * n_u), 0), 1.0, 0.0).astype(BF16)
    mine = (lax.broadcasted_iota(jnp.int32, (lab.shape[0], n_utt * n_u), 1) % n_u
            == lax.broadcasted_iota(jnp.int32, (lab.shape[0], n_utt * n_u), 0))
    flat = []
    for part in (lax.shift_right_arithmetic(lab, 5), jnp.bitwise_and(lab, 31)):
        spread = dot(part.astype(F32).astype(BF16), place)
        flat.append(jnp.sum(jnp.where(mine, spread, 0.0), axis=0, keepdims=True))
    for w in range(n_win):
        row = lax.broadcasted_iota(jnp.int32, (16, gu), 0)
        hi, lo = (x[:, w * step_u:w * step_u + gu] for x in flat)
        ylab[w] = jnp.where(row == 0, hi, jnp.where(row == 1, lo, 0.0)).astype(BF16)
    sk[...] = jnp.zeros_like(sk)
    vsb[...] = jnp.zeros_like(vsb)
    segu[...] = jnp.zeros_like(segu)
    segt[...] = jnp.zeros_like(segt)
    gwo_ref[...] = jnp.zeros_like(gwo_ref)

    def onehot(n, index_row):
        return (lax.broadcasted_iota(jnp.int32, (n, ROWS), 0) == index_row)

    def as_bf16(mask):
        return jnp.where(mask, 1.0, 0.0).astype(BF16)

    v_iota = lax.broadcasted_iota(jnp.int32, (CHUNK, ROWS), 0)
    n_sub = CHUNK // 8

    def lanes_of(win):
        return pl.ds(pl.multiple_of(win * step_u, 128), gu)

    def frame_lanes_of(win):
        return pl.ds(pl.multiple_of(win // per_tile * 128, 128), 256)

    part_row = lax.broadcasted_iota(jnp.int32, (128, ROWS), 0)

    def spread3(idx_b, parts):
        out = jnp.zeros((128, ROWS), F32)
        for q, part in enumerate(parts):
            out = jnp.where(part_row == idx_b + q * CORE_MAX, part, out)
        return out.astype(BF16)

    def prepare(i):
        win = tbl[0, i]
        r = tbl[1, i] + lax.broadcasted_iota(jnp.int32, (1, ROWS), 1)
        end_r = tbl[2, i]
        start = jnp.int32(0)
        bl = jnp.full((1, ROWS), -1, jnp.int32)
        w = jnp.zeros((1, ROWS), jnp.int32)
        u1 = jnp.ones((1, ROWS), jnp.int32)
        for j in range(WIN):
            u1_j = llen_s[win * (WIN // 2) + j] + 1
            end = start + flen_s[win * (WIN // 2) + j] * u1_j
            inside = (r >= start) & (r < jnp.minimum(end, end_r))
            bl = jnp.where(inside, j, bl)
            w = jnp.where(inside, r - start, w)
            u1 = jnp.where(inside, u1_j, u1)
            start = end
        valid = bl >= 0
        t = jnp.zeros((1, ROWS), jnp.int32)
        for j in range(1, n_t):
            t = t + jnp.where(w >= j * u1, 1, 0)
        u = w - t * u1
        idx_u = jnp.where(valid, bl * n_u + u, -1)
        idx_t = jnp.where(valid, bl * n_t + t + win % per_tile * step_t, -1)
        idx_kt = jnp.where(valid, (t + u) * n_t + t, -1)
        idx_b = jnp.where(valid, win * (WIN // 2) + bl - u_lo, -1024)
        ohu = as_bf16(onehot(gu, idx_u))
        oht = as_bf16(onehot(256, idx_t))
        half = n_j // 2
        for q in range(2):
            rows = slice(q * half, (q + 1) * half)
            pre = dot(c_buf[rows, lanes_of(win)], ohu) + dot(a_buf[rows, frame_lanes_of(win)], oht)
            hnew[rows] = jnp.tanh(pre).astype(BF16)
        yy = dot(ylab[win], ohu)
        y = (yy[0:1] * 32.0 + yy[1:2]).astype(jnp.int32)
        rows8 = lax.broadcasted_iota(jnp.int32, (8, ROWS), 0)
        idx[i] = jnp.where(rows8 == 0, idx_u, jnp.where(rows8 == 1, idx_t, jnp.where(rows8 == 2, idx_kt, jnp.where(rows8 == 3, idx_b, y))))

    def scatter(i):
        okt = as_bf16(onehot(n_kt, idx[i, 2:3]))
        sk[...] += dot(okt, vsb[...], NT)

    def fwd(i, carry):
        scatter(jnp.maximum(i - 1, 0))
        hcur[...] = hnew[...]
        hbuf[i] = hnew[...]
        y = idx[i, 4:5]
        idx_b = idx[i, 3:4]
        slot = jnp.minimum(i, KEEP)
        prepare(i + 1)
        lz = None
        blank_z = None
        for c in range(n_ch):
            z = dot(wot[c * CHUNK:(c + 1) * CHUNK, :], hcur[...])
            z3 = z.reshape(n_sub, 8, ROWS)
            zl = jnp.sum(jnp.where(v_iota == y - c * CHUNK, z, 0.0).reshape(n_sub, 8, ROWS), axis=0)
            lz = zl if lz is None else lz + zl
            if c == 0:
                blank_z = z[0:1, :]
            m_c = jnp.max(z3, axis=0)
            e3 = jnp.exp(z3 - m_c[None])
            ebuf[slot, c * CHUNK:(c + 1) * CHUNK, :] = e3.reshape(CHUNK, ROWS)
            mch[c * 8:(c + 1) * 8, :] = m_c
            sch[c * 8:(c + 1) * 8, :] = jnp.sum(e3, axis=0)
        m8 = jnp.max(mch[...].reshape(n_ch, 8, ROWS), axis=0)
        m = jnp.max(m8, axis=0, keepdims=True)
        f_all = jnp.exp(mch[...] - m)
        s = jnp.sum(jnp.sum((sch[...] * f_all).reshape(n_ch, 8, ROWS), axis=0), axis=0, keepdims=True)
        fac[i] = f_all * (1.0 / s)
        lab_z = jnp.sum(lz, axis=0, keepdims=True)
        lse = m + jnp.log(s)
        b_parts = split3(blank_z - lse)
        l_parts = split3(lab_z - lse)
        vsb[0:128] = spread3(idx_b, b_parts)
        vsb[128:256] = spread3(idx_b, l_parts)
        return carry

    prepare(jnp.int32(0))
    lax.fori_loop(0, n_blocks, fwd, 0)
    scatter(n_blocks - 1)

    tt = lax.broadcasted_iota(jnp.int32, (n_t, 128), 0)
    def own_lanes(ref):
        x = jnp.concatenate([ref[...], jnp.zeros((1, 128 - n_utt), jnp.int32)], axis=1).astype(F32)
        return pltpu.roll(jnp.broadcast_to(x, (n_t, 128)), (128 - u_lo) % 128, 1).astype(jnp.int32)
    t_len = own_lanes(flen_v)
    u_len = own_lanes(llen_v)

    def scores(k):
        lo = k * n_t
        x, y = (v + pltpu.roll(v, 128 - CORE_MAX, 1) + pltpu.roll(v, 128 - 2 * CORE_MAX, 1)
                for v in (sk[lo:lo + n_t, 0:128], sk[lo:lo + n_t, 128:256]))
        uu = k - tt
        ok = (uu >= 0) & (tt < t_len)
        bl_k = jnp.where(ok & (uu <= u_len), x, NEG)
        lb_k = jnp.where(ok & (uu < u_len), y, NEG)
        return bl_k, lb_k

    alpha = jnp.where(tt == 0, 0.0, NEG).astype(F32)
    abuf[0] = alpha
    beta = jnp.full((n_t, 128), NEG, F32)
    sc = [scores(k) for k in range(n_diag)]
    for step in range(n_diag):
        if step > 0:
            bl_k, lb_k = sc[step - 1]
            p1 = jnp.where(tt == 0, NEG, pltpu.roll(alpha + bl_k, 1, 0))
            alpha = logadd(p1, alpha + lb_k)
            abuf[step] = alpha
        k = n_diag - 1 - step
        bl_k, lb_k = sc[k]
        up = jnp.where(tt == n_t - 1, jnp.where(u_len == k + 1 - n_t, 0.0, NEG), pltpu.roll(beta, n_t - 1, 0))
        t1 = up + bl_k
        t2 = beta + lb_k
        t1buf[k] = t1
        t2buf[k] = t2
        beta = jnp.where(tt >= t_len, jnp.where(k - tt == u_len, 0.0, NEG), logadd(t1, t2))
    log_p = beta[0:1, :]
    lane = lax.broadcasted_iota(jnp.int32, (n_t, 128), 1)
    loss_ref[...] = pltpu.roll(jnp.where(lane < u_hi - u_lo, -log_p, 0.0), u_lo, 1)
    lane_ok = lane < CORE_MAX
    for k in range(n_diag):
        for which, buf in enumerate((t1buf, t2buf)):
            occ = jnp.where(lane_ok, jnp.exp(jnp.minimum(abuf[k] + buf[k] - log_p, 0.0)), 0.0)
            hi, mid, lo = split3(occ)
            lo_row = which * n_kt + k * n_t
            gocc[lo_row:lo_row + n_t, :] = hi + pltpu.roll(mid, CORE_MAX, 1) + pltpu.roll(lo, 2 * CORE_MAX, 1)
    for which in range(2):
        gocc[which * n_kt + n_diag * n_t:(which + 1) * n_kt, :] = jnp.zeros((n_kt - n_diag * n_t, 128), F32)
    gocb[...] = gocc[...].astype(BF16)

    def again(i):
        @pl.when(i >= KEEP)
        def _():
            m = None
            for c in range(n_ch):
                z = dot(wot[c * CHUNK:(c + 1) * CHUNK, :], hbuf[i])
                z3 = z.reshape(n_sub, 8, ROWS)
                ebuf[KEEP, c * CHUNK:(c + 1) * CHUNK, :] = jnp.exp(z3 - jnp.max(z3, axis=0)[None]).reshape(CHUNK, ROWS)

    def d_logits(i):
        idx_kt = idx[i, 2:3]
        idx_b = idx[i, 3:4]
        y = idx[i, 4:5]
        orep = spread3(idx_b, (1.0, 1.0, 1.0))
        okt = onehot(n_kt, idx_kt)
        gb = jnp.sum(jnp.where(okt, dot(gocb[0:n_kt], orep), 0.0), axis=0, keepdims=True)
        gl = jnp.sum(jnp.where(okt, dot(gocb[n_kt:2 * n_kt], orep), 0.0), axis=0, keepdims=True)
        occ = gb + gl
        slot = jnp.minimum(i, KEEP)
        for c in range(n_ch):
            sc_c = fac[i, c * 8:(c + 1) * 8, :] * occ
            e3 = ebuf[slot, c * CHUNK:(c + 1) * CHUNK, :].reshape(n_sub, 8, ROWS)
            d = (e3 * sc_c[None]).reshape(CHUNK, ROWS) - jnp.where(v_iota == y - c * CHUNK, gl, 0.0)
            if c == 0:
                d = d - jnp.where(v_iota == 0, gb, 0.0)
            dznew[c * CHUNK:(c + 1) * CHUNK, :] = d.astype(BF16)

    def bwd(i, carry):
        again(i + 1)
        dzcur[...] = dznew[...]
        win = tbl[0, i]
        ohu = as_bf16(onehot(gu, idx[i, 0:1]))
        oht = as_bf16(onehot(256, idx[i, 1:2]))
        half = n_j // 2
        d_logits(i + 1)
        for q in range(2):
            rows = slice(q * half, (q + 1) * half)
            hf = hbuf[i, rows].astype(F32)
            dh = dot(wo_ref[rows], dzcur[...])
            dp = (dh * (1.0 - hf * hf)).astype(BF16)
            segu[rows, lanes_of(win)] += dot(dp, ohu, NT)
            segt[rows, frame_lanes_of(win)] += dot(dp, oht, NT)
        for c in range(n_v // 256):
            gwo_ref[:, c * 256:(c + 1) * 256] += dot(hbuf[i], dzcur[c * 256:(c + 1) * 256, :], NT)
        return carry

    load_wo.wait()
    again(jnp.int32(0))
    d_logits(jnp.int32(0))
    lax.fori_loop(0, n_blocks, bwd, 0)

    dc_ref[...] = segu[...].astype(BF16)
    da_ref[...] = segt[:, 0:n_utt * n_t].astype(BF16)


def core_call(c_t, a_t, wot, w_out, labels, flen, llen, n_t, n_u):
    n_utt = flen.shape[0]
    n_j = c_t.shape[0]
    n_v = w_out.shape[1]
    n_win = n_utt * 2 // WIN - 1
    max_blk = n_utt // 2 * n_t * n_u // ROWS + 4
    n_kt = (n_t + n_u) * n_t
    n_st = n_v // CHUNK * 8
    vm = pl.BlockSpec(memory_space=pltpu.VMEM)
    sm = pl.BlockSpec(memory_space=pltpu.SMEM)
    return pl.pallas_call(
        functools.partial(core_kernel, n_t, n_u),
        out_shape=(
            pltpu.VMEM((8, 128), F32),
            pltpu.VMEM((n_j, n_utt * n_u), BF16),
            pltpu.VMEM((n_j, n_utt * n_t), BF16),
            pltpu.VMEM(w_out.shape, F32),
        ),
        in_specs=[sm, sm] + [vm] * 6 + [pl.BlockSpec(memory_space=pltpu.HBM)],
        out_specs=(vm,) * 4,
        scratch_shapes=[
            pltpu.VMEM(w_out.shape, BF16),
            pltpu.SemaphoreType.DMA,
            pltpu.VMEM((n_win, 16, WIN * n_u), BF16),
            pltpu.VMEM((max_blk, n_j, ROWS), BF16),
            pltpu.VMEM((n_j, ROWS), BF16),
            pltpu.VMEM((n_j, ROWS), BF16),
            pltpu.VMEM((min(max_blk, KEEP + 1), n_v, ROWS), F32),
            pltpu.VMEM((max_blk, n_st, ROWS), F32),
            pltpu.VMEM((n_st, ROWS), F32),
            pltpu.VMEM((n_st, ROWS), F32),
            pltpu.VMEM((256, ROWS), BF16),
            pltpu.VMEM((max_blk, 8, ROWS), jnp.int32),
            pltpu.VMEM((n_v, ROWS), BF16),
            pltpu.VMEM((n_v, ROWS), BF16),
            pltpu.VMEM((n_kt, 256), F32),
            pltpu.VMEM((n_t + n_u, n_t, 128), F32),
            pltpu.VMEM((n_t + n_u, n_t, 128), F32),
            pltpu.VMEM((n_t + n_u, n_t, 128), F32),
            pltpu.VMEM((2 * n_kt, 128), F32),
            pltpu.VMEM((2 * n_kt, 128), BF16),
            pltpu.VMEM((n_j, n_utt * n_u), F32),
            pltpu.VMEM((n_j, n_utt * n_t + 128), F32),
            pltpu.SMEM((3, max_blk), jnp.int32),
            pltpu.SMEM((n_utt + 1,), jnp.int32),
        ],
        compiler_params=pltpu.CompilerParams(vmem_limit_bytes=CORE_VMEM),
        name="rnnt_core",
    )(flen, llen, flen.reshape(1, n_utt), llen.reshape(1, n_utt), labels.T, c_t, a_t, wot, in_hbm(w_out))


def solution(mesh):
    seq_size = mesh.shape['seq']

    def local_fn(enc_out, pred_out, w_enc, w_pred, w_out, labels, frame_len, label_len):
        n_utt, n_loc, n_h = enc_out.shape
        n_u = pred_out.shape[1]
        n_t = n_loc * seq_size
        g2 = pred_out.reshape(n_utt * n_u, n_h)
        c_t, a_t, wot, f2 = gather_call(enc_out.reshape(n_utt * n_loc, n_h), g2, w_enc, w_pred, w_out, seq_size, n_t)
        loss, dc_t, da_t, gwo = core_call(c_t, a_t, wot, w_out, labels, frame_len, label_len, n_t, n_u)
        loss, gf, gwe, gwp, gwo = store_call(reduce_call(gwo, dc_t, da_t, loss, g2, f2, w_enc, n_utt * n_loc, n_t))
        return loss[0, :n_utt], gf.reshape(n_utt, n_loc, n_h), gwe, gwp, gwo

    in_specs = (P('dp', 'seq', None), P('dp', None, None), P(None, None), P(None, None), P(None, None), P('dp', None), P('dp'), P('dp'))
    out_specs = (P('dp'), P('dp', 'seq', None), P('dp', None), P('dp', None), P('dp', None))
    return jax.shard_map(local_fn, mesh=mesh, in_specs=in_specs, out_specs=out_specs, check_vma=False)
```

```python
import functools

import jax
import jax.numpy as jnp
from jax import lax
from jax.experimental import pallas as pl
from jax.experimental.pallas import tpu as pltpu
from jax.sharding import PartitionSpec as P

NEG = -1.0e30
ROWS = 256
WIN = 8
CHUNK = 128
CORE_MIN, CORE_MAX = 24, 40
GATHER_VMEM = 40 << 20
CORE_VMEM = 51 << 20
REDUCE_VMEM = 36 << 20
STORE_VMEM = 1 << 20
KEEP = 15
F32 = jnp.float32
BF16 = jnp.bfloat16
MESH = pl.DeviceIdType.MESH
NT = (((1,), (1,)), ((), ()))
NN = (((1,), (0,)), ((), ()))


def dot(a, b, dims=NN):
    return lax.dot_general(a, b, dims, preferred_element_type=F32)


def in_hbm(x):
    return pltpu.with_memory_space_constraint(x, pltpu.HBM)


def in_vmem(x):
    return pltpu.with_memory_space_constraint(x, pltpu.VMEM)


def split3(x):
    hi = x.astype(BF16).astype(F32)
    r1 = x - hi
    mid = r1.astype(BF16).astype(F32)
    return hi, mid, r1 - mid


def logadd(a, b):
    m = jnp.maximum(a, b)
    return m + jnp.log(1.0 + jnp.exp(jnp.minimum(a, b) - m))


def gather_kernel(n_t, enc_h, g_h, we_h, wp_h, wo_h, c_ref, a_ref, wot_ref, f_ref, enc_ref, g_ref, we_ref, wp_ref, wo_ref, fbuf,
                  in_sem, send_sem, recv_sem):
    me = lax.axis_index('seq')
    n_seq = fbuf.shape[0]
    partner = me + 1 - 2 * (me % 2)
    peer = (me + 2) % n_seq
    load_enc, load_wo, load_wp, load_g, load_we = loads = [pltpu.make_async_copy(src, dst, in_sem.at[q]) for q, (src, dst) in enumerate(
        ((enc_h, enc_ref), (wo_h, wo_ref), (wp_h, wp_ref), (g_h, g_ref), (we_h, we_ref)))]
    for load in loads:
        load.start()
    barrier = pltpu.get_barrier_semaphore()
    for other in (partner, peer):
        pl.semaphore_signal(barrier, inc=1, device_id={'seq': other}, device_id_type=MESH)
    pl.semaphore_wait(barrier, 2)

    def send(src, slot, sem, other):
        return pltpu.make_async_remote_copy(src_ref=src, dst_ref=fbuf.at[slot], send_sem=send_sem.at[sem], recv_sem=recv_sem.at[sem],
                                            device_id={'seq': other}, device_id_type=MESH)
    load_enc.wait()
    to_peer = send(enc_ref, me, 0, peer)
    to_peer.start()
    to_partner = send(enc_ref, me, 1, partner)
    to_partner.start()
    fbuf[me] = enc_ref[...]
    load_wo.wait()
    wot_ref[...] = wo_ref[...].T
    load_wp.wait()
    load_g.wait()
    c_ref[...] = dot(wp_ref[...].T, g_ref[...], NT).astype(BF16)
    load_we.wait()
    we_t = we_ref[...].T
    to_peer.wait_recv()
    relay = send(fbuf.at[peer], peer, 2, partner)
    relay.start()
    n_f = f_ref.shape[0]
    n_b = n_f // n_t
    n_loc = n_t // n_seq
    row = lax.broadcasted_iota(jnp.int32, (n_f, n_f), 0)
    col = lax.broadcasted_iota(jnp.int32, (n_f, n_f), 1)
    t = row % n_t
    order = jnp.where(col == (t // n_loc) * (n_b * n_loc) + (row // n_t) * n_loc + t % n_loc, 1.0, 0.0).astype(BF16)
    to_partner.wait_recv()
    relay.wait_recv()
    f_bt = dot(order, fbuf[...].reshape(n_f, f_ref.shape[1])).astype(BF16)
    f_ref[...] = f_bt
    a_ref[:, 0:n_f] = dot(we_t, f_bt, NT).astype(BF16)
    a_ref[:, n_f:] = jnp.zeros((a_ref.shape[0], a_ref.shape[1] - n_f), BF16)
    to_peer.wait_send()
    to_partner.wait_send()
    relay.wait_send()


def gather_call(enc, g2, w_enc, w_pred, w_out, n_seq, n_t):
    n_rows, n_h = enc.shape
    n_j = w_enc.shape[1]
    vm = pl.BlockSpec(memory_space=pltpu.VMEM)
    n_f = n_rows * n_seq
    args = [in_hbm(x) for x in (enc, g2, w_enc, w_pred, w_out)]
    return pl.pallas_call(
        functools.partial(gather_kernel, n_t),
        out_shape=(
            pltpu.VMEM((n_j, g2.shape[0]), BF16),
            pltpu.VMEM((n_j, n_f + 128), BF16),
            pltpu.VMEM(w_out.shape[::-1], BF16),
            pltpu.VMEM((n_f, n_h), BF16),
        ),
        in_specs=[pl.BlockSpec(memory_space=pltpu.HBM)] * 5,
        out_specs=(vm,) * 4,
        scratch_shapes=[pltpu.VMEM(x.shape, x.dtype) for x in (enc, g2, w_enc, w_pred, w_out)] + [
            pltpu.VMEM((n_seq, n_rows, n_h), BF16),
            pltpu.SemaphoreType.DMA((5,)),
            pltpu.SemaphoreType.DMA((3,)),
            pltpu.SemaphoreType.DMA((3,)),
        ],
        compiler_params=pltpu.CompilerParams(collective_id=0, has_side_effects=True, vmem_limit_bytes=GATHER_VMEM),
        name="rnnt_gather",
    )(*args)


def reduce_kernel(n_t, gwo_v, dc_v, da_v, loss_v, f_v, g_p, we_p, loss_ref, gf_ref, gwe_ref, gwp_ref, gwo_ref,
                  g_v, we_v, gwp_v, rgwo, rgwp, rda, rloss, in_sem, send_sem, recv_sem):
    me = lax.axis_index('seq')
    partner = me + 1 - 2 * (me % 2)
    loads = [pltpu.make_async_copy(src, dst, in_sem.at[q]) for q, (src, dst) in enumerate(((g_p, g_v), (we_p, we_v)))]
    for load in loads:
        load.start()
    barrier = pltpu.get_barrier_semaphore()
    pl.semaphore_signal(barrier, inc=1, device_id={'seq': partner}, device_id_type=MESH)
    pl.semaphore_wait(barrier, 1)

    def send(src, dst, sem):
        return pltpu.make_async_remote_copy(src_ref=src, dst_ref=dst, send_sem=send_sem.at[sem], recv_sem=recv_sem.at[sem],
                                            device_id={'seq': partner}, device_id_type=MESH)
    n_part = 4
    rows = gwo_v.shape[0] // n_part
    sends = [send(da_v, rda, 0), send(loss_v, rloss, 1)]
    sends += [send(gwo_v.at[pl.ds(q * rows, rows)], rgwo.at[pl.ds(q * rows, rows)], 2 + q) for q in range(n_part)]
    for s in sends:
        s.start()
    loads[0].wait()
    gwp_v[...] = dot(g_v[...].T, dc_v[...], NT)
    s_gwp = send(gwp_v, rgwp, 2 + n_part)
    loads[1].wait()
    sends[0].wait_recv()
    sends[1].wait_recv()
    loss_ref[...] = (loss_v[0:1, :] + rloss[0:1, :])[:, 0:loss_ref.shape[1]]
    da = (da_v[...].astype(F32) + rda[...].astype(F32)).astype(BF16)
    s_gwp.start()
    gwe_ref[...] = dot(f_v[...].T, da, NT)
    n_f = da.shape[1]
    n_own = gf_ref.shape[0]
    n_loc = n_own * n_t // n_f
    row = lax.broadcasted_iota(jnp.int32, (n_own, n_f), 0)
    col = lax.broadcasted_iota(jnp.int32, (n_own, n_f), 1)
    own = jnp.where(col == (row // n_loc) * n_t + me * n_loc + row % n_loc, 1.0, 0.0).astype(BF16)
    gf_ref[...] = dot(dot(own, da, NT).astype(BF16), we_v[...], NT).astype(BF16)
    for q in range(n_part):
        sends[2 + q].wait_recv()
        part = slice(q * rows, (q + 1) * rows)
        gwo_ref[part] = gwo_v[part] + rgwo[part]
    s_gwp.wait_recv()
    gwp_ref[...] = gwp_v[...] + rgwp[...]
    for s in sends + [s_gwp]:
        s.wait_send()


def reduce_call(gwo, dc_t, da_t, loss, g2, f2, w_enc, n_own, n_t):
    vm = pl.BlockSpec(memory_space=pltpu.VMEM)
    like = lambda x: pltpu.VMEM(x.shape, x.dtype)
    gwp_shape = (g2.shape[1], dc_t.shape[0])
    return pl.pallas_call(
        functools.partial(reduce_kernel, n_t),
        out_shape=(
            pltpu.VMEM((1, f2.shape[0] // n_t), F32),
            pltpu.VMEM((n_own, w_enc.shape[0]), BF16),
            pltpu.VMEM(w_enc.shape, F32),
            pltpu.VMEM(gwp_shape, F32),
            pltpu.VMEM(gwo.shape, F32),
        ),
        in_specs=[vm] * 5 + [pl.BlockSpec(memory_space=pltpu.HBM)] * 2,
        out_specs=(vm,) * 5,
        scratch_shapes=[like(x) for x in (g2, w_enc)] + [
            pltpu.VMEM(gwp_shape, F32), like(gwo), pltpu.VMEM(gwp_shape, F32), like(da_t), like(loss),
            pltpu.SemaphoreType.DMA((2,)),
            pltpu.SemaphoreType.DMA((7,)),
            pltpu.SemaphoreType.DMA((7,)),
        ],
        compiler_params=pltpu.CompilerParams(collective_id=1, has_side_effects=True, vmem_limit_bytes=REDUCE_VMEM),
        name="rnnt_reduce",
    )(in_vmem(gwo), in_vmem(dc_t), in_vmem(da_t), in_vmem(loss), in_vmem(f2), in_hbm(g2), in_hbm(w_enc))


def store_kernel(n, *refs):
    sems = refs[2 * n]
    copies = [pltpu.make_async_copy(refs[q], refs[n + q], sems.at[q]) for q in range(n)]
    for copy in copies:
        copy.start()
    for copy in copies:
        copy.wait()


def store_call(arrays):
    n = len(arrays)
    return pl.pallas_call(
        functools.partial(store_kernel, n),
        out_shape=tuple(pltpu.HBM(x.shape, x.dtype) for x in arrays),
        in_specs=[pl.BlockSpec(memory_space=pltpu.VMEM)] * n,
        out_specs=(pl.BlockSpec(memory_space=pltpu.HBM),) * n,
        scratch_shapes=[pltpu.SemaphoreType.DMA((n,))],
        compiler_params=pltpu.CompilerParams(vmem_limit_bytes=STORE_VMEM),
        name="rnnt_store",
    )(*[in_vmem(x) for x in arrays])


def core_kernel(n_t, n_u, flen_s, llen_s, flen_v, llen_v, lab_ref, c_buf, a_buf, wot, wo_h,
                loss_ref, dc_ref, da_ref, gwo_ref,
                wo_ref, wo_sem, ylab, hbuf, hnew, hcur, ebuf, fac, mch, sch, idx, dznew, dzcur, dpb, zrow, sk, abuf, t1buf, t2buf,
                gocc, gocb, segu, segt, tbl, off):
    n_utt = flen_s.shape[0]
    n_j = c_buf.shape[0]
    n_v = wo_ref.shape[1]
    step_u = WIN // 2 * n_u
    step_t = WIN // 2 * n_t
    per_tile = 128 // step_t
    gu = WIN * n_u
    n_win = n_utt * 2 // WIN - 1
    n_diag = n_t + n_u - 1
    n_kt = (n_diag + 1) * n_t
    n_ch = n_v // CHUNK

    load_wo = pltpu.make_async_copy(wo_h, wo_ref, wo_sem)
    load_wo.start()

    def off_step(b, total):
        off[b] = total
        return total + flen_s[b] * (llen_s[b] + 1)
    off[n_utt] = lax.fori_loop(0, n_utt, off_step, jnp.int32(0))

    total = off[n_utt]
    cut = lax.fori_loop(CORE_MIN, CORE_MAX, lambda b, n: n + jnp.where(off[b] + off[b + 1] <= total, 1, 0), jnp.int32(CORE_MIN))
    first_core = lax.axis_index('seq') % 2 == 0
    u_lo = jnp.where(first_core, 0, cut)
    u_hi = jnp.where(first_core, cut, n_utt)
    stop = off[u_hi]

    def utt_step(b, carry):
        win = jnp.minimum(b // (WIN // 2), n_win - 1)
        base = off[win * (WIN // 2)]
        last = jnp.minimum(off[win * (WIN // 2) + WIN], stop)

        def emit(c):
            n, pos = c
            end = jnp.minimum(pos + ROWS, last)
            tbl[0, n] = win
            tbl[1, n] = pos - base
            tbl[2, n] = end - base
            return n + 1, end
        return lax.while_loop(lambda c: c[1] < off[b + 1], emit, carry)
    n_blocks, _ = lax.fori_loop(u_lo, u_hi, utt_step, (jnp.int32(0), off[u_lo]))
    tbl[0, n_blocks] = 0
    tbl[1, n_blocks] = 0
    tbl[2, n_blocks] = 0

    lab = lab_ref[...]
    place = jnp.where(lax.broadcasted_iota(jnp.int32, (n_utt, n_utt * n_u), 1) // n_u
                      == lax.broadcasted_iota(jnp.int32, (n_utt, n_utt * n_u), 0), 1.0, 0.0).astype(BF16)
    mine = (lax.broadcasted_iota(jnp.int32, (lab.shape[0], n_utt * n_u), 1) % n_u
            == lax.broadcasted_iota(jnp.int32, (lab.shape[0], n_utt * n_u), 0))
    flat = []
    for part in (lax.shift_right_arithmetic(lab, 5), jnp.bitwise_and(lab, 31)):
        spread = dot(part.astype(F32).astype(BF16), place)
        flat.append(jnp.sum(jnp.where(mine, spread, 0.0), axis=0, keepdims=True))
    for w in range(n_win):
        row = lax.broadcasted_iota(jnp.int32, (16, gu), 0)
        hi, lo = (x[:, w * step_u:w * step_u + gu] for x in flat)
        ylab[w] = jnp.where(row == 0, hi, jnp.where(row == 1, lo, 0.0)).astype(BF16)
    sk[...] = jnp.zeros_like(sk)
    mch[...] = jnp.zeros_like(mch)
    sch[...] = jnp.ones_like(sch)
    zrow[...] = jnp.zeros_like(zrow)
    dpb[...] = jnp.zeros_like(dpb)
    segu[...] = jnp.zeros_like(segu)
    segt[...] = jnp.zeros_like(segt)
    gwo_ref[...] = jnp.zeros_like(gwo_ref)

    def onehot(n, index_row):
        return (lax.broadcasted_iota(jnp.int32, (n, ROWS), 0) == index_row)

    def as_bf16(mask):
        return jnp.where(mask, 1.0, 0.0).astype(BF16)

    def frame_onehot(index_row):
        n = WIN * n_t + 128 - step_t
        return jnp.concatenate([as_bf16(onehot(n, index_row)), jnp.zeros((256 - n, ROWS), BF16)], axis=0)

    v_iota = lax.broadcasted_iota(jnp.int32, (CHUNK, ROWS), 0)
    n_sub = CHUNK // 8

    def lanes_of(win):
        return pl.ds(pl.multiple_of(win * step_u, 128), gu)

    def frame_lanes_of(win):
        return pl.ds(pl.multiple_of(win // per_tile * 128, 128), 256)

    part_row = lax.broadcasted_iota(jnp.int32, (128, ROWS), 0)

    def spread3(idx_b, parts):
        out = jnp.zeros((128, ROWS), F32)
        for q, part in enumerate(parts):
            out = jnp.where(part_row == idx_b + q * CORE_MAX, part, out)
        return out.astype(BF16)

    def prepare(i):
        win = tbl[0, i]
        r = tbl[1, i] + lax.broadcasted_iota(jnp.int32, (1, ROWS), 1)
        end_r = tbl[2, i]
        start = jnp.int32(0)
        bl = jnp.full((1, ROWS), -1, jnp.int32)
        w = jnp.zeros((1, ROWS), jnp.int32)
        u1 = jnp.ones((1, ROWS), jnp.int32)
        for j in range(WIN):
            u1_j = llen_s[win * (WIN // 2) + j] + 1
            end = start + flen_s[win * (WIN // 2) + j] * u1_j
            inside = (r >= start) & (r < jnp.minimum(end, end_r))
            bl = jnp.where(inside, j, bl)
            w = jnp.where(inside, r - start, w)
            u1 = jnp.where(inside, u1_j, u1)
            start = end
        valid = bl >= 0
        t = jnp.zeros((1, ROWS), jnp.int32)
        for j in range(1, n_t):
            t = t + jnp.where(w >= j * u1, 1, 0)
        u = w - t * u1
        idx_u = jnp.where(valid, bl * n_u + u, -1)
        idx_t = jnp.where(valid, bl * n_t + t + win % per_tile * step_t, -1)
        idx_kt = jnp.where(valid, (t + u) * n_t + t, -1)
        idx_b = jnp.where(valid, win * (WIN // 2) + bl - u_lo, -1024)
        ohu = as_bf16(onehot(gu, idx_u))
        oht = frame_onehot(idx_t)
        half = n_j // 2
        for q in range(2):
            rows = slice(q * half, (q + 1) * half)
            pre = dot(c_buf[rows, lanes_of(win)], ohu) + dot(a_buf[rows, frame_lanes_of(win)], oht)
            hnew[rows] = jnp.tanh(pre).astype(BF16)
        yy = dot(ylab[win], ohu)
        y = (yy[0:1] * 32.0 + yy[1:2]).astype(jnp.int32)
        rows8 = lax.broadcasted_iota(jnp.int32, (8, ROWS), 0)
        idx[i] = jnp.where(rows8 == 0, idx_u, jnp.where(rows8 == 1, idx_t, jnp.where(rows8 == 2, idx_kt, jnp.where(rows8 == 3, idx_b, y))))

    def finish(i, live):
        idx_b = idx[i, 3:4]
        m_all = mch[...]
        m8 = jnp.max(m_all.reshape(n_ch, 8, ROWS), axis=0)
        m = jnp.max(m8, axis=0, keepdims=True)
        f_all = jnp.exp(m_all - m)
        s = jnp.sum(jnp.sum((sch[...] * f_all).reshape(n_ch, 8, ROWS), axis=0), axis=0, keepdims=True)
        fac[i] = f_all * (1.0 / s)
        lse = m + jnp.log(s)
        b_parts = split3(zrow[8:9] - lse)
        l_parts = split3(jnp.sum(zrow[0:8], axis=0, keepdims=True) - lse)
        vs = jnp.concatenate([spread3(idx_b, b_parts), spread3(idx_b, l_parts)], axis=0)
        okt = as_bf16(onehot(n_kt, jnp.where(live, idx[i, 2:3], -1)))
        half = n_kt // 2
        for q in range(2):
            sk[q * half:(q + 1) * half] += dot(okt[q * half:(q + 1) * half], vs, NT)

    def fwd(i, carry):
        finish(jnp.maximum(i - 1, 0), i > 0)
        hcur[...] = hnew[...]
        hbuf[i] = hnew[...]
        y = idx[i, 4:5]
        slot = jnp.minimum(i, KEEP)
        prepare(i + 1)
        lz = None
        for c in range(n_ch):
            z = dot(wot[c * CHUNK:(c + 1) * CHUNK, :], hcur[...])
            z3 = z.reshape(n_sub, 8, ROWS)
            zl = jnp.sum(jnp.where(v_iota == y - c * CHUNK, z, 0.0).reshape(n_sub, 8, ROWS), axis=0)
            lz = zl if lz is None else lz + zl
            if c == 0:
                zrow[8:16] = z[0:8, :]
            m_c = jnp.max(z3, axis=0)
            e3 = jnp.exp(z3 - m_c[None])
            ebuf[slot, c * CHUNK:(c + 1) * CHUNK, :] = e3.reshape(CHUNK, ROWS)
            mch[c * 8:(c + 1) * 8, :] = m_c
            sch[c * 8:(c + 1) * 8, :] = jnp.sum(e3, axis=0)
        zrow[0:8] = lz
        return carry

    prepare(jnp.int32(0))
    lax.fori_loop(0, n_blocks, fwd, 0)
    finish(n_blocks - 1, True)

    tt = lax.broadcasted_iota(jnp.int32, (n_t, 128), 0)
    def own_lanes(ref):
        x = jnp.concatenate([ref[...], jnp.zeros((1, 128 - n_utt), jnp.int32)], axis=1).astype(F32)
        return pltpu.roll(jnp.broadcast_to(x, (n_t, 128)), (128 - u_lo) % 128, 1).astype(jnp.int32)
    t_len = own_lanes(flen_v)
    u_len = own_lanes(llen_v)

    def scores(k):
        lo = k * n_t
        x, y = (v + pltpu.roll(v, 128 - CORE_MAX, 1) + pltpu.roll(v, 128 - 2 * CORE_MAX, 1)
                for v in (sk[lo:lo + n_t, 0:128], sk[lo:lo + n_t, 128:256]))
        uu = k - tt
        ok = (uu >= 0) & (tt < t_len)
        bl_k = jnp.where(ok & (uu <= u_len), x, NEG)
        lb_k = jnp.where(ok & (uu < u_len), y, NEG)
        return bl_k, lb_k

    alpha = jnp.where(tt == 0, 0.0, NEG).astype(F32)
    abuf[0] = alpha
    beta = jnp.full((n_t, 128), NEG, F32)
    sc = [scores(k) for k in range(n_diag)]
    for step in range(n_diag):
        if step > 0:
            bl_k, lb_k = sc[step - 1]
            p1 = jnp.where(tt == 0, NEG, pltpu.roll(alpha + bl_k, 1, 0))
            alpha = logadd(p1, alpha + lb_k)
            abuf[step] = alpha
        k = n_diag - 1 - step
        bl_k, lb_k = sc[k]
        up = jnp.where(tt == n_t - 1, jnp.where(u_len == k + 1 - n_t, 0.0, NEG), pltpu.roll(beta, n_t - 1, 0))
        t1 = up + bl_k
        t2 = beta + lb_k
        t1buf[k] = t1
        t2buf[k] = t2
        beta = jnp.where(tt >= t_len, jnp.where(k - tt == u_len, 0.0, NEG), logadd(t1, t2))
    log_p = beta[0:1, :]
    lane = lax.broadcasted_iota(jnp.int32, (n_t, 128), 1)
    loss_ref[...] = pltpu.roll(jnp.where(lane < u_hi - u_lo, -log_p, 0.0), u_lo, 1)
    lane_ok = lane < CORE_MAX
    for k in range(n_diag):
        for which, buf in enumerate((t1buf, t2buf)):
            occ = jnp.where(lane_ok, jnp.exp(jnp.minimum(abuf[k] + buf[k] - log_p, 0.0)), 0.0)
            hi, mid, lo = split3(occ)
            lo_row = which * n_kt + k * n_t
            gocc[lo_row:lo_row + n_t, :] = hi + pltpu.roll(mid, CORE_MAX, 1) + pltpu.roll(lo, 2 * CORE_MAX, 1)
    for which in range(2):
        gocc[which * n_kt + n_diag * n_t:(which + 1) * n_kt, :] = jnp.zeros((n_kt - n_diag * n_t, 128), F32)
    gocb[...] = gocc[...].astype(BF16)

    def again(i):
        @pl.when(i >= KEEP)
        def _():
            m = None
            for c in range(n_ch):
                z = dot(wot[c * CHUNK:(c + 1) * CHUNK, :], hbuf[i])
                z3 = z.reshape(n_sub, 8, ROWS)
                ebuf[KEEP, c * CHUNK:(c + 1) * CHUNK, :] = jnp.exp(z3 - jnp.max(z3, axis=0)[None]).reshape(CHUNK, ROWS)

    def d_logits(i):
        idx_kt = idx[i, 2:3]
        idx_b = idx[i, 3:4]
        y = idx[i, 4:5]
        orep = spread3(idx_b, (1.0, 1.0, 1.0))
        okt = onehot(n_kt, idx_kt)
        gb = jnp.sum(jnp.where(okt, dot(gocb[0:n_kt], orep), 0.0), axis=0, keepdims=True)
        gl = jnp.sum(jnp.where(okt, dot(gocb[n_kt:2 * n_kt], orep), 0.0), axis=0, keepdims=True)
        occ = gb + gl
        slot = jnp.minimum(i, KEEP)
        for c in range(n_ch):
            sc_c = fac[i, c * 8:(c + 1) * 8, :] * occ
            e3 = ebuf[slot, c * CHUNK:(c + 1) * CHUNK, :].reshape(n_sub, 8, ROWS)
            d = (e3 * sc_c[None]).reshape(CHUNK, ROWS) - jnp.where(v_iota == y - c * CHUNK, gl, 0.0)
            if c == 0:
                d = d - jnp.where(v_iota == 0, gb, 0.0)
            dznew[c * CHUNK:(c + 1) * CHUNK, :] = d.astype(BF16)

    half = n_j // 2

    def segments(i):
        win = tbl[0, i]
        ohu = as_bf16(onehot(gu, idx[i, 0:1]))
        oht = frame_onehot(idx[i, 1:2])
        for q in range(2):
            rows = slice(q * half, (q + 1) * half)
            segu[rows, lanes_of(win)] += dot(dpb[rows], ohu, NT)
            segt[rows, frame_lanes_of(win)] += dot(dpb[rows], oht, NT)

    def bwd(i, carry):
        again(i + 1)
        segments(jnp.maximum(i - 1, 0))
        dzcur[...] = dznew[...]
        for q in range(2):
            rows = slice(q * half, (q + 1) * half)
            hf = hbuf[i, rows].astype(F32)
            dh = dot(wo_ref[rows], dzcur[...])
            dpb[rows] = (dh * (1.0 - hf * hf)).astype(BF16)
        for c in range(n_v // 256):
            gwo_ref[:, c * 256:(c + 1) * 256] += dot(hbuf[i], dzcur[c * 256:(c + 1) * 256, :], NT)
        d_logits(i + 1)
        return carry

    load_wo.wait()
    again(jnp.int32(0))
    d_logits(jnp.int32(0))
    lax.fori_loop(0, n_blocks, bwd, 0)
    segments(n_blocks - 1)

    dc_ref[...] = segu[...].astype(BF16)
    da_ref[...] = segt[:, 0:n_utt * n_t].astype(BF16)


def core_call(c_t, a_t, wot, w_out, labels, flen, llen, n_t, n_u):
    n_utt = flen.shape[0]
    n_j = c_t.shape[0]
    n_v = w_out.shape[1]
    n_win = n_utt * 2 // WIN - 1
    max_blk = n_utt // 2 * n_t * n_u // ROWS + 4
    n_kt = (n_t + n_u) * n_t
    n_st = n_v // CHUNK * 8
    vm = pl.BlockSpec(memory_space=pltpu.VMEM)
    sm = pl.BlockSpec(memory_space=pltpu.SMEM)
    return pl.pallas_call(
        functools.partial(core_kernel, n_t, n_u),
        out_shape=(
            pltpu.VMEM((8, 128), F32),
            pltpu.VMEM((n_j, n_utt * n_u), BF16),
            pltpu.VMEM((n_j, n_utt * n_t), BF16),
            pltpu.VMEM(w_out.shape, F32),
        ),
        in_specs=[sm, sm] + [vm] * 6 + [pl.BlockSpec(memory_space=pltpu.HBM)],
        out_specs=(vm,) * 4,
        scratch_shapes=[
            pltpu.VMEM(w_out.shape, BF16),
            pltpu.SemaphoreType.DMA,
            pltpu.VMEM((n_win, 16, WIN * n_u), BF16),
            pltpu.VMEM((max_blk, n_j, ROWS), BF16),
            pltpu.VMEM((n_j, ROWS), BF16),
            pltpu.VMEM((n_j, ROWS), BF16),
            pltpu.VMEM((min(max_blk, KEEP + 1), n_v, ROWS), F32),
            pltpu.VMEM((max_blk, n_st, ROWS), F32),
            pltpu.VMEM((n_st, ROWS), F32),
            pltpu.VMEM((n_st, ROWS), F32),
            pltpu.VMEM((max_blk, 8, ROWS), jnp.int32),
            pltpu.VMEM((n_v, ROWS), BF16),
            pltpu.VMEM((n_v, ROWS), BF16),
            pltpu.VMEM((n_j, ROWS), BF16),
            pltpu.VMEM((16, ROWS), F32),
            pltpu.VMEM((n_kt, 256), F32),
            pltpu.VMEM((n_t + n_u, n_t, 128), F32),
            pltpu.VMEM((n_t + n_u, n_t, 128), F32),
            pltpu.VMEM((n_t + n_u, n_t, 128), F32),
            pltpu.VMEM((2 * n_kt, 128), F32),
            pltpu.VMEM((2 * n_kt, 128), BF16),
            pltpu.VMEM((n_j, n_utt * n_u), F32),
            pltpu.VMEM((n_j, n_utt * n_t + 128), F32),
            pltpu.SMEM((3, max_blk), jnp.int32),
            pltpu.SMEM((n_utt + 1,), jnp.int32),
        ],
        compiler_params=pltpu.CompilerParams(vmem_limit_bytes=CORE_VMEM),
        name="rnnt_core",
    )(flen, llen, flen.reshape(1, n_utt), llen.reshape(1, n_utt), labels.T, in_vmem(c_t), in_vmem(a_t), in_vmem(wot), in_hbm(w_out))


def solution(mesh):
    seq_size = mesh.shape['seq']

    def local_fn(enc_out, pred_out, w_enc, w_pred, w_out, labels, frame_len, label_len):
        n_utt, n_loc, n_h = enc_out.shape
        n_u = pred_out.shape[1]
        n_t = n_loc * seq_size
        g2 = pred_out.reshape(n_utt * n_u, n_h)
        c_t, a_t, wot, f2 = gather_call(enc_out.reshape(n_utt * n_loc, n_h), g2, w_enc, w_pred, w_out, seq_size, n_t)
        loss, dc_t, da_t, gwo = core_call(c_t, a_t, wot, w_out, labels, frame_len, label_len, n_t, n_u)
        loss, gf, gwe, gwp, gwo = store_call(reduce_call(gwo, dc_t, da_t, loss, g2, f2, w_enc, n_utt * n_loc, n_t))
        return loss.reshape(n_utt), gf.reshape(n_utt, n_loc, n_h), gwe, gwp, gwo

    in_specs = (P('dp', 'seq', None), P('dp', None, None), P(None, None), P(None, None), P(None, None), P('dp', None), P('dp'), P('dp'))
    out_specs = (P('dp'), P('dp', 'seq', None), P('dp', None), P('dp', None), P('dp', None))
    return jax.shard_map(local_fn, mesh=mesh, in_specs=in_specs, out_specs=out_specs, check_vma=False)
```

```python
import functools

import jax
import jax.numpy as jnp
from jax import lax
from jax.experimental import pallas as pl
from jax.experimental.pallas import tpu as pltpu
from jax.sharding import PartitionSpec as P

NEG = -1.0e30
ROWS = 256
WIN = 8
CHUNK = 128
CORE_MIN, CORE_MAX = 24, 40
GATHER_VMEM = 40 << 20
CORE_VMEM = 51 << 20
REDUCE_VMEM = 36 << 20
STORE_VMEM = 1 << 20
KEEP = 15
F32 = jnp.float32
BF16 = jnp.bfloat16
MESH = pl.DeviceIdType.MESH
NT = (((1,), (1,)), ((), ()))
NN = (((1,), (0,)), ((), ()))


def dot(a, b, dims=NN):
    return lax.dot_general(a, b, dims, preferred_element_type=F32)


def in_hbm(x):
    return pltpu.with_memory_space_constraint(x, pltpu.HBM)


def in_vmem(x):
    return pltpu.with_memory_space_constraint(x, pltpu.VMEM)


def split3(x):
    hi = x.astype(BF16).astype(F32)
    r1 = x - hi
    mid = r1.astype(BF16).astype(F32)
    return hi, mid, r1 - mid


def logadd(a, b):
    m = jnp.maximum(a, b)
    return m + jnp.log(1.0 + jnp.exp(jnp.minimum(a, b) - m))


def gather_kernel(n_t, enc_h, g_h, we_h, wp_h, wo_h, c_ref, a_ref, wot_ref, f_ref, enc_ref, g_ref, we_ref, wp_ref, wo_ref, fbuf,
                  in_sem, send_sem, recv_sem):
    me = lax.axis_index('seq')
    n_seq = fbuf.shape[0]
    partner = me + 1 - 2 * (me % 2)
    peer = (me + 2) % n_seq
    load_enc, load_wo, load_wp, load_g, load_we = loads = [pltpu.make_async_copy(src, dst, in_sem.at[q]) for q, (src, dst) in enumerate(
        ((enc_h, enc_ref), (wo_h, wo_ref), (wp_h, wp_ref), (g_h, g_ref), (we_h, we_ref)))]
    for load in loads:
        load.start()
    barrier = pltpu.get_barrier_semaphore()
    for other in (partner, peer):
        pl.semaphore_signal(barrier, inc=1, device_id={'seq': other}, device_id_type=MESH)
    pl.semaphore_wait(barrier, 2)

    def send(src, slot, sem, other):
        return pltpu.make_async_remote_copy(src_ref=src, dst_ref=fbuf.at[slot], send_sem=send_sem.at[sem], recv_sem=recv_sem.at[sem],
                                            device_id={'seq': other}, device_id_type=MESH)
    load_enc.wait()
    to_peer = send(enc_ref, me, 0, peer)
    to_peer.start()
    to_partner = send(enc_ref, me, 1, partner)
    to_partner.start()
    fbuf[me] = enc_ref[...]
    load_wo.wait()
    wot_ref[...] = wo_ref[...].T
    load_wp.wait()
    load_g.wait()
    c_ref[...] = dot(wp_ref[...].T, g_ref[...], NT).astype(BF16)
    load_we.wait()
    we_t = we_ref[...].T
    to_peer.wait_recv()
    relay = send(fbuf.at[peer], peer, 2, partner)
    relay.start()
    n_f = f_ref.shape[0]
    n_b = n_f // n_t
    n_loc = n_t // n_seq
    row = lax.broadcasted_iota(jnp.int32, (n_f, n_f), 0)
    col = lax.broadcasted_iota(jnp.int32, (n_f, n_f), 1)
    t = row % n_t
    order = jnp.where(col == (t // n_loc) * (n_b * n_loc) + (row // n_t) * n_loc + t % n_loc, 1.0, 0.0).astype(BF16)
    to_partner.wait_recv()
    relay.wait_recv()
    f_bt = dot(order, fbuf[...].reshape(n_f, f_ref.shape[1])).astype(BF16)
    f_ref[...] = f_bt
    a_ref[:, 0:n_f] = dot(we_t, f_bt, NT).astype(BF16)
    a_ref[:, n_f:] = jnp.zeros((a_ref.shape[0], a_ref.shape[1] - n_f), BF16)
    to_peer.wait_send()
    to_partner.wait_send()
    relay.wait_send()


def gather_call(enc, g2, w_enc, w_pred, w_out, n_seq, n_t):
    n_rows, n_h = enc.shape
    n_j = w_enc.shape[1]
    vm = pl.BlockSpec(memory_space=pltpu.VMEM)
    n_f = n_rows * n_seq
    args = [in_hbm(x) for x in (enc, g2, w_enc, w_pred, w_out)]
    return pl.pallas_call(
        functools.partial(gather_kernel, n_t),
        out_shape=(
            pltpu.VMEM((n_j, g2.shape[0]), BF16),
            pltpu.VMEM((n_j, n_f + 128), BF16),
            pltpu.VMEM(w_out.shape[::-1], BF16),
            pltpu.VMEM((n_f, n_h), BF16),
        ),
        in_specs=[pl.BlockSpec(memory_space=pltpu.HBM)] * 5,
        out_specs=(vm,) * 4,
        scratch_shapes=[pltpu.VMEM(x.shape, x.dtype) for x in (enc, g2, w_enc, w_pred, w_out)] + [
            pltpu.VMEM((n_seq, n_rows, n_h), BF16),
            pltpu.SemaphoreType.DMA((5,)),
            pltpu.SemaphoreType.DMA((3,)),
            pltpu.SemaphoreType.DMA((3,)),
        ],
        compiler_params=pltpu.CompilerParams(collective_id=0, has_side_effects=True, vmem_limit_bytes=GATHER_VMEM),
        name="rnnt_gather",
    )(*args)


def reduce_kernel(n_t, gwo_v, dc_v, da_v, loss_v, f_v, g_p, we_p, loss_ref, gf_ref, gwe_ref, gwp_ref, gwo_ref,
                  g_v, we_v, gwp_v, rgwo, rgwp, rda, rloss, in_sem, send_sem, recv_sem):
    me = lax.axis_index('seq')
    partner = me + 1 - 2 * (me % 2)
    loads = [pltpu.make_async_copy(src, dst, in_sem.at[q]) for q, (src, dst) in enumerate(((g_p, g_v), (we_p, we_v)))]
    for load in loads:
        load.start()
    barrier = pltpu.get_barrier_semaphore()
    pl.semaphore_signal(barrier, inc=1, device_id={'seq': partner}, device_id_type=MESH)
    pl.semaphore_wait(barrier, 1)

    def send(src, dst, sem):
        return pltpu.make_async_remote_copy(src_ref=src, dst_ref=dst, send_sem=send_sem.at[sem], recv_sem=recv_sem.at[sem],
                                            device_id={'seq': partner}, device_id_type=MESH)
    n_part = 4
    rows = gwo_v.shape[0] // n_part
    sends = [send(da_v, rda, 0), send(loss_v, rloss, 1)]
    sends += [send(gwo_v.at[pl.ds(q * rows, rows)], rgwo.at[pl.ds(q * rows, rows)], 2 + q) for q in range(n_part)]
    for s in sends:
        s.start()
    loads[0].wait()
    gwp_v[...] = dot(g_v[...].T, dc_v[...], NT)
    s_gwp = send(gwp_v, rgwp, 2 + n_part)
    loads[1].wait()
    sends[0].wait_recv()
    sends[1].wait_recv()
    loss_ref[...] = (loss_v[0:1, :] + rloss[0:1, :])[:, 0:loss_ref.shape[1]]
    da = (da_v[...].astype(F32) + rda[...].astype(F32)).astype(BF16)
    s_gwp.start()
    gwe_ref[...] = dot(f_v[...].T, da, NT)
    n_f = da.shape[1]
    n_own = gf_ref.shape[0]
    n_loc = n_own * n_t // n_f
    row = lax.broadcasted_iota(jnp.int32, (n_own, n_f), 0)
    col = lax.broadcasted_iota(jnp.int32, (n_own, n_f), 1)
    own = jnp.where(col == (row // n_loc) * n_t + me * n_loc + row % n_loc, 1.0, 0.0).astype(BF16)
    gf_ref[...] = dot(dot(own, da, NT).astype(BF16), we_v[...], NT).astype(BF16)
    for q in range(n_part):
        sends[2 + q].wait_recv()
        part = slice(q * rows, (q + 1) * rows)
        gwo_ref[part] = gwo_v[part] + rgwo[part]
    s_gwp.wait_recv()
    gwp_ref[...] = gwp_v[...] + rgwp[...]
    for s in sends + [s_gwp]:
        s.wait_send()


def reduce_call(gwo, dc_t, da_t, loss, g2, f2, w_enc, n_own, n_t):
    vm = pl.BlockSpec(memory_space=pltpu.VMEM)
    like = lambda x: pltpu.VMEM(x.shape, x.dtype)
    gwp_shape = (g2.shape[1], dc_t.shape[0])
    return pl.pallas_call(
        functools.partial(reduce_kernel, n_t),
        out_shape=(
            pltpu.VMEM((1, f2.shape[0] // n_t), F32),
            pltpu.VMEM((n_own, w_enc.shape[0]), BF16),
            pltpu.VMEM(w_enc.shape, F32),
            pltpu.VMEM(gwp_shape, F32),
            pltpu.VMEM(gwo.shape, F32),
        ),
        in_specs=[vm] * 5 + [pl.BlockSpec(memory_space=pltpu.HBM)] * 2,
        out_specs=(vm,) * 5,
        scratch_shapes=[like(x) for x in (g2, w_enc)] + [
            pltpu.VMEM(gwp_shape, F32), like(gwo), pltpu.VMEM(gwp_shape, F32), like(da_t), like(loss),
            pltpu.SemaphoreType.DMA((2,)),
            pltpu.SemaphoreType.DMA((7,)),
            pltpu.SemaphoreType.DMA((7,)),
        ],
        compiler_params=pltpu.CompilerParams(collective_id=1, has_side_effects=True, vmem_limit_bytes=REDUCE_VMEM),
        name="rnnt_reduce",
    )(in_vmem(gwo), in_vmem(dc_t), in_vmem(da_t), in_vmem(loss), in_vmem(f2), in_hbm(g2), in_hbm(w_enc))


def store_kernel(n, *refs):
    sems = refs[2 * n]
    copies = [pltpu.make_async_copy(refs[q], refs[n + q], sems.at[q]) for q in range(n)]
    for copy in copies:
        copy.start()
    for copy in copies:
        copy.wait()


def store_call(arrays):
    n = len(arrays)
    return pl.pallas_call(
        functools.partial(store_kernel, n),
        out_shape=tuple(pltpu.HBM(x.shape, x.dtype) for x in arrays),
        in_specs=[pl.BlockSpec(memory_space=pltpu.VMEM)] * n,
        out_specs=(pl.BlockSpec(memory_space=pltpu.HBM),) * n,
        scratch_shapes=[pltpu.SemaphoreType.DMA((n,))],
        compiler_params=pltpu.CompilerParams(vmem_limit_bytes=STORE_VMEM),
        name="rnnt_store",
    )(*[in_vmem(x) for x in arrays])


def core_kernel(n_t, n_u, flen_s, llen_s, flen_v, llen_v, lab_ref, c_buf, a_buf, wot, wo_h,
                loss_ref, dc_ref, da_ref, gwo_ref,
                wo_ref, wo_sem, ylab, hbuf, hnew, hcur, ebuf, fac, mch, sch, vsb, ynew, ybuf, idx, dznew, dzcur, dpb, zrow, sk, abuf, t1buf, t2buf,
                gocc, gocb, segu, segt, tbl, off):
    n_utt = flen_s.shape[0]
    n_j = c_buf.shape[0]
    n_v = wo_ref.shape[1]
    step_u = WIN // 2 * n_u
    step_t = WIN // 2 * n_t
    per_tile = 128 // step_t
    gu = WIN * n_u
    n_win = n_utt * 2 // WIN - 1
    n_diag = n_t + n_u - 1
    n_kt = (n_diag + 1) * n_t
    n_ch = n_v // CHUNK

    load_wo = pltpu.make_async_copy(wo_h, wo_ref, wo_sem)
    load_wo.start()

    def off_step(b, total):
        off[b] = total
        return total + flen_s[b] * (llen_s[b] + 1)
    off[n_utt] = lax.fori_loop(0, n_utt, off_step, jnp.int32(0))

    total = off[n_utt]
    cut = lax.fori_loop(CORE_MIN, CORE_MAX, lambda b, n: n + jnp.where(off[b] + off[b + 1] <= total, 1, 0), jnp.int32(CORE_MIN))
    first_core = lax.axis_index('seq') % 2 == 0
    u_lo = jnp.where(first_core, 0, cut)
    u_hi = jnp.where(first_core, cut, n_utt)
    stop = off[u_hi]

    def utt_step(b, carry):
        win = jnp.minimum(b // (WIN // 2), n_win - 1)
        base = off[win * (WIN // 2)]
        last = jnp.minimum(off[win * (WIN // 2) + WIN], stop)

        def emit(c):
            n, pos = c
            end = jnp.minimum(pos + ROWS, last)
            tbl[0, n] = win
            tbl[1, n] = pos - base
            tbl[2, n] = end - base
            return n + 1, end
        return lax.while_loop(lambda c: c[1] < off[b + 1], emit, carry)
    n_blocks, _ = lax.fori_loop(u_lo, u_hi, utt_step, (jnp.int32(0), off[u_lo]))
    for past in range(2):
        for q in range(3):
            tbl[q, n_blocks + past] = 0

    lab = lab_ref[...]
    place = jnp.where(lax.broadcasted_iota(jnp.int32, (n_utt, n_utt * n_u), 1) // n_u
                      == lax.broadcasted_iota(jnp.int32, (n_utt, n_utt * n_u), 0), 1.0, 0.0).astype(BF16)
    mine = (lax.broadcasted_iota(jnp.int32, (lab.shape[0], n_utt * n_u), 1) % n_u
            == lax.broadcasted_iota(jnp.int32, (lab.shape[0], n_utt * n_u), 0))
    flat = []
    for part in (lax.shift_right_arithmetic(lab, 5), jnp.bitwise_and(lab, 31)):
        spread = dot(part.astype(F32).astype(BF16), place)
        flat.append(jnp.sum(jnp.where(mine, spread, 0.0), axis=0, keepdims=True))
    for w in range(n_win):
        row = lax.broadcasted_iota(jnp.int32, (16, gu), 0)
        hi, lo = (x[:, w * step_u:w * step_u + gu] for x in flat)
        ylab[w] = jnp.where(row == 0, hi, jnp.where(row == 1, lo, 0.0)).astype(BF16)
    sk[...] = jnp.zeros_like(sk)
    mch[...] = jnp.zeros_like(mch)
    sch[...] = jnp.ones_like(sch)
    zrow[...] = jnp.zeros_like(zrow)
    vsb[...] = jnp.zeros_like(vsb)
    dpb[...] = jnp.zeros_like(dpb)
    segu[...] = jnp.zeros_like(segu)
    segt[...] = jnp.zeros_like(segt)
    gwo_ref[...] = jnp.zeros_like(gwo_ref)

    def onehot(n, index_row):
        return (lax.broadcasted_iota(jnp.int32, (n, ROWS), 0) == index_row)

    def as_bf16(mask):
        return jnp.where(mask, 1.0, 0.0).astype(BF16)

    def frame_onehot(index_row):
        n = WIN * n_t + 128 - step_t
        return jnp.concatenate([as_bf16(onehot(n, index_row)), jnp.zeros((256 - n, ROWS), BF16)], axis=0)

    v_iota = lax.broadcasted_iota(jnp.int32, (CHUNK, ROWS), 0)
    n_sub = CHUNK // 8

    def lanes_of(win):
        return pl.ds(pl.multiple_of(win * step_u, 128), gu)

    def frame_lanes_of(win):
        return pl.ds(pl.multiple_of(win // per_tile * 128, 128), 256)

    part_row = lax.broadcasted_iota(jnp.int32, (128, ROWS), 0)

    def spread3(idx_b, parts):
        out = jnp.zeros((128, ROWS), F32)
        for q, part in enumerate(parts):
            out = jnp.where(part_row == idx_b + q * CORE_MAX, part, out)
        return out.astype(BF16)

    def locate(i):
        win = tbl[0, i]
        r = tbl[1, i] + lax.broadcasted_iota(jnp.int32, (1, ROWS), 1)
        end_r = tbl[2, i]
        start = jnp.int32(0)
        bl = jnp.full((1, ROWS), -1, jnp.int32)
        w = jnp.zeros((1, ROWS), jnp.int32)
        u1 = jnp.ones((1, ROWS), jnp.int32)
        for j in range(WIN):
            u1_j = llen_s[win * (WIN // 2) + j] + 1
            end = start + flen_s[win * (WIN // 2) + j] * u1_j
            inside = (r >= start) & (r < jnp.minimum(end, end_r))
            bl = jnp.where(inside, j, bl)
            w = jnp.where(inside, r - start, w)
            u1 = jnp.where(inside, u1_j, u1)
            start = end
        valid = bl >= 0
        t = jnp.zeros((1, ROWS), jnp.int32)
        for j in range(1, n_t):
            t = t + jnp.where(w >= j * u1, 1, 0)
        u = w - t * u1
        idx_u = jnp.where(valid, bl * n_u + u, -1)
        idx_t = jnp.where(valid, bl * n_t + t + win % per_tile * step_t, -1)
        idx_kt = jnp.where(valid, (t + u) * n_t + t, -1)
        idx_b = jnp.where(valid, win * (WIN // 2) + bl - u_lo, -1024)
        rows8 = lax.broadcasted_iota(jnp.int32, (8, ROWS), 0)
        idx[i] = jnp.where(rows8 == 0, idx_u, jnp.where(rows8 == 1, idx_t, jnp.where(rows8 == 2, idx_kt, idx_b)))

    half = n_j // 2

    def hidden(i):
        win = tbl[0, i]
        ohu = as_bf16(onehot(gu, idx[i, 0:1]))
        oht = frame_onehot(idx[i, 1:2])
        for q in range(2):
            rows = slice(q * half, (q + 1) * half)
            pre = dot(c_buf[rows, lanes_of(win)], ohu) + dot(a_buf[rows, frame_lanes_of(win)], oht)
            hnew[rows] = jnp.tanh(pre).astype(BF16)
        yy = dot(ylab[win], ohu)
        ynew[...] = jnp.broadcast_to((yy[0:1] * 32.0 + yy[1:2]).astype(jnp.int32), (8, ROWS))

    def finish(i):
        idx_b = idx[i, 3:4]
        m_all = mch[...]
        m8 = jnp.max(m_all.reshape(n_ch, 8, ROWS), axis=0)
        m = jnp.max(m8, axis=0, keepdims=True)
        f_all = jnp.exp(m_all - m)
        s = jnp.sum(jnp.sum((sch[...] * f_all).reshape(n_ch, 8, ROWS), axis=0), axis=0, keepdims=True)
        fac[i] = f_all * (1.0 / s)
        lse = m + jnp.log(s)
        b_parts = split3(zrow[8:9] - lse)
        l_parts = split3(jnp.sum(zrow[0:8], axis=0, keepdims=True) - lse)
        vsb[0:128] = spread3(idx_b, b_parts)
        vsb[128:256] = spread3(idx_b, l_parts)

    def scatter(i, live):
        okt = as_bf16(onehot(n_kt, jnp.where(live, idx[i, 2:3], -1)))
        part = n_kt // 2
        for q in range(2):
            sk[q * part:(q + 1) * part] += dot(okt[q * part:(q + 1) * part], vsb[...], NT)

    def fwd(i, carry):
        scatter(jnp.maximum(i - 2, 0), i > 1)
        finish(jnp.maximum(i - 1, 0))
        hcur[...] = hnew[...]
        hbuf[i] = hnew[...]
        y = ynew[0:1]
        ybuf[i] = ynew[...]
        slot = jnp.minimum(i, KEEP)
        lz = None
        for c in range(n_ch):
            z = dot(wot[c * CHUNK:(c + 1) * CHUNK, :], hcur[...])
            z3 = z.reshape(n_sub, 8, ROWS)
            zl = jnp.sum(jnp.where(v_iota == y - c * CHUNK, z, 0.0).reshape(n_sub, 8, ROWS), axis=0)
            lz = zl if lz is None else lz + zl
            if c == 0:
                zrow[8:16] = z[0:8, :]
            m_c = jnp.max(z3, axis=0)
            e3 = jnp.exp(z3 - m_c[None])
            ebuf[slot, c * CHUNK:(c + 1) * CHUNK, :] = e3.reshape(CHUNK, ROWS)
            mch[c * 8:(c + 1) * 8, :] = m_c
            sch[c * 8:(c + 1) * 8, :] = jnp.sum(e3, axis=0)
        zrow[0:8] = lz
        hidden(i + 1)
        locate(i + 2)
        return carry

    locate(jnp.int32(0))
    locate(jnp.int32(1))
    hidden(jnp.int32(0))
    lax.fori_loop(0, n_blocks, fwd, 0)
    scatter(jnp.maximum(n_blocks - 2, 0), n_blocks > 1)
    finish(n_blocks - 1)
    scatter(n_blocks - 1, True)

    tt = lax.broadcasted_iota(jnp.int32, (n_t, 128), 0)
    def own_lanes(ref):
        x = jnp.concatenate([ref[...], jnp.zeros((1, 128 - n_utt), jnp.int32)], axis=1).astype(F32)
        return pltpu.roll(jnp.broadcast_to(x, (n_t, 128)), (128 - u_lo) % 128, 1).astype(jnp.int32)
    t_len = own_lanes(flen_v)
    u_len = own_lanes(llen_v)

    def scores(k):
        lo = k * n_t
        x, y = (v + pltpu.roll(v, 128 - CORE_MAX, 1) + pltpu.roll(v, 128 - 2 * CORE_MAX, 1)
                for v in (sk[lo:lo + n_t, 0:128], sk[lo:lo + n_t, 128:256]))
        uu = k - tt
        ok = (uu >= 0) & (tt < t_len)
        bl_k = jnp.where(ok & (uu <= u_len), x, NEG)
        lb_k = jnp.where(ok & (uu < u_len), y, NEG)
        return bl_k, lb_k

    alpha = jnp.where(tt == 0, 0.0, NEG).astype(F32)
    abuf[0] = alpha
    beta = jnp.full((n_t, 128), NEG, F32)
    sc = [scores(k) for k in range(n_diag)]
    for step in range(n_diag):
        if step > 0:
            bl_k, lb_k = sc[step - 1]
            p1 = jnp.where(tt == 0, NEG, pltpu.roll(alpha + bl_k, 1, 0))
            alpha = logadd(p1, alpha + lb_k)
            abuf[step] = alpha
        k = n_diag - 1 - step
        bl_k, lb_k = sc[k]
        up = jnp.where(tt == n_t - 1, jnp.where(u_len == k + 1 - n_t, 0.0, NEG), pltpu.roll(beta, n_t - 1, 0))
        t1 = up + bl_k
        t2 = beta + lb_k
        t1buf[k] = t1
        t2buf[k] = t2
        beta = jnp.where(tt >= t_len, jnp.where(k - tt == u_len, 0.0, NEG), logadd(t1, t2))
    log_p = beta[0:1, :]
    lane = lax.broadcasted_iota(jnp.int32, (n_t, 128), 1)
    loss_ref[...] = pltpu.roll(jnp.where(lane < u_hi - u_lo, -log_p, 0.0), u_lo, 1)
    lane_ok = lane < CORE_MAX
    for k in range(n_diag):
        for which, buf in enumerate((t1buf, t2buf)):
            occ = jnp.where(lane_ok, jnp.exp(jnp.minimum(abuf[k] + buf[k] - log_p, 0.0)), 0.0)
            hi, mid, lo = split3(occ)
            lo_row = which * n_kt + k * n_t
            gocc[lo_row:lo_row + n_t, :] = hi + pltpu.roll(mid, CORE_MAX, 1) + pltpu.roll(lo, 2 * CORE_MAX, 1)
    for which in range(2):
        gocc[which * n_kt + n_diag * n_t:(which + 1) * n_kt, :] = jnp.zeros((n_kt - n_diag * n_t, 128), F32)
    gocb[...] = gocc[...].astype(BF16)

    def again(i):
        @pl.when(i >= KEEP)
        def _():
            m = None
            for c in range(n_ch):
                z = dot(wot[c * CHUNK:(c + 1) * CHUNK, :], hbuf[i])
                z3 = z.reshape(n_sub, 8, ROWS)
                ebuf[KEEP, c * CHUNK:(c + 1) * CHUNK, :] = jnp.exp(z3 - jnp.max(z3, axis=0)[None]).reshape(CHUNK, ROWS)

    def occupancy(i):
        orep = spread3(idx[i, 3:4], (1.0, 1.0, 1.0))
        okt = onehot(n_kt, idx[i, 2:3])
        for which in range(2):
            gath = dot(gocb[which * n_kt:(which + 1) * n_kt], orep)
            occ = jnp.sum(jnp.where(okt, gath, 0.0), axis=0, keepdims=True)
            zrow[which * 8:which * 8 + 8] = jnp.broadcast_to(occ, (8, ROWS))

    def d_logits(i):
        y = ybuf[i, 0:1]
        gb = zrow[0:1]
        gl = zrow[8:9]
        occ = gb + gl
        slot = jnp.minimum(i, KEEP)
        for c in range(n_ch):
            sc_c = fac[i, c * 8:(c + 1) * 8, :] * occ
            e3 = ebuf[slot, c * CHUNK:(c + 1) * CHUNK, :].reshape(n_sub, 8, ROWS)
            d = (e3 * sc_c[None]).reshape(CHUNK, ROWS) - jnp.where(v_iota == y - c * CHUNK, gl, 0.0)
            if c == 0:
                d = d - jnp.where(v_iota == 0, gb, 0.0)
            dznew[c * CHUNK:(c + 1) * CHUNK, :] = d.astype(BF16)

    def segments(i):
        win = tbl[0, i]
        ohu = as_bf16(onehot(gu, idx[i, 0:1]))
        oht = frame_onehot(idx[i, 1:2])
        for q in range(2):
            rows = slice(q * half, (q + 1) * half)
            segu[rows, lanes_of(win)] += dot(dpb[rows], ohu, NT)
            segt[rows, frame_lanes_of(win)] += dot(dpb[rows], oht, NT)

    def bwd(i, carry):
        again(i + 1)
        segments(jnp.maximum(i - 1, 0))
        dzcur[...] = dznew[...]
        for q in range(2):
            rows = slice(q * half, (q + 1) * half)
            hf = hbuf[i, rows].astype(F32)
            dh = dot(wo_ref[rows], dzcur[...])
            dpb[rows] = (dh * (1.0 - hf * hf)).astype(BF16)
        for c in range(n_v // 256):
            gwo_ref[:, c * 256:(c + 1) * 256] += dot(hbuf[i], dzcur[c * 256:(c + 1) * 256, :], NT)
        d_logits(i + 1)
        occupancy(i + 2)
        return carry

    load_wo.wait()
    again(jnp.int32(0))
    occupancy(jnp.int32(0))
    d_logits(jnp.int32(0))
    occupancy(jnp.int32(1))
    lax.fori_loop(0, n_blocks, bwd, 0)
    segments(n_blocks - 1)

    dc_ref[...] = segu[...].astype(BF16)
    da_ref[...] = segt[:, 0:n_utt * n_t].astype(BF16)


def core_call(c_t, a_t, wot, w_out, labels, flen, llen, n_t, n_u):
    n_utt = flen.shape[0]
    n_j = c_t.shape[0]
    n_v = w_out.shape[1]
    n_win = n_utt * 2 // WIN - 1
    max_blk = n_utt // 2 * n_t * n_u // ROWS + 5
    n_kt = (n_t + n_u) * n_t
    n_st = n_v // CHUNK * 8
    vm = pl.BlockSpec(memory_space=pltpu.VMEM)
    sm = pl.BlockSpec(memory_space=pltpu.SMEM)
    return pl.pallas_call(
        functools.partial(core_kernel, n_t, n_u),
        out_shape=(
            pltpu.VMEM((8, 128), F32),
            pltpu.VMEM((n_j, n_utt * n_u), BF16),
            pltpu.VMEM((n_j, n_utt * n_t), BF16),
            pltpu.VMEM(w_out.shape, F32),
        ),
        in_specs=[sm, sm] + [vm] * 6 + [pl.BlockSpec(memory_space=pltpu.HBM)],
        out_specs=(vm,) * 4,
        scratch_shapes=[
            pltpu.VMEM(w_out.shape, BF16),
            pltpu.SemaphoreType.DMA,
            pltpu.VMEM((n_win, 16, WIN * n_u), BF16),
            pltpu.VMEM((max_blk, n_j, ROWS), BF16),
            pltpu.VMEM((n_j, ROWS), BF16),
            pltpu.VMEM((n_j, ROWS), BF16),
            pltpu.VMEM((min(max_blk, KEEP + 1), n_v, ROWS), F32),
            pltpu.VMEM((max_blk, n_st, ROWS), F32),
            pltpu.VMEM((n_st, ROWS), F32),
            pltpu.VMEM((n_st, ROWS), F32),
            pltpu.VMEM((256, ROWS), BF16),
            pltpu.VMEM((8, ROWS), jnp.int32),
            pltpu.VMEM((max_blk, 8, ROWS), jnp.int32),
            pltpu.VMEM((max_blk, 8, ROWS), jnp.int32),
            pltpu.VMEM((n_v, ROWS), BF16),
            pltpu.VMEM((n_v, ROWS), BF16),
            pltpu.VMEM((n_j, ROWS), BF16),
            pltpu.VMEM((16, ROWS), F32),
            pltpu.VMEM((n_kt, 256), F32),
            pltpu.VMEM((n_t + n_u, n_t, 128), F32),
            pltpu.VMEM((n_t + n_u, n_t, 128), F32),
            pltpu.VMEM((n_t + n_u, n_t, 128), F32),
            pltpu.VMEM((2 * n_kt, 128), F32),
            pltpu.VMEM((2 * n_kt, 128), BF16),
            pltpu.VMEM((n_j, n_utt * n_u), F32),
            pltpu.VMEM((n_j, n_utt * n_t + 128), F32),
            pltpu.SMEM((3, max_blk), jnp.int32),
            pltpu.SMEM((n_utt + 1,), jnp.int32),
        ],
        compiler_params=pltpu.CompilerParams(vmem_limit_bytes=CORE_VMEM),
        name="rnnt_core",
    )(flen, llen, flen.reshape(1, n_utt), llen.reshape(1, n_utt), labels.T, in_vmem(c_t), in_vmem(a_t), in_vmem(wot), in_hbm(w_out))


def solution(mesh):
    seq_size = mesh.shape['seq']

    def local_fn(enc_out, pred_out, w_enc, w_pred, w_out, labels, frame_len, label_len):
        n_utt, n_loc, n_h = enc_out.shape
        n_u = pred_out.shape[1]
        n_t = n_loc * seq_size
        g2 = pred_out.reshape(n_utt * n_u, n_h)
        c_t, a_t, wot, f2 = gather_call(enc_out.reshape(n_utt * n_loc, n_h), g2, w_enc, w_pred, w_out, seq_size, n_t)
        loss, dc_t, da_t, gwo = core_call(c_t, a_t, wot, w_out, labels, frame_len, label_len, n_t, n_u)
        loss, gf, gwe, gwp, gwo = store_call(reduce_call(gwo, dc_t, da_t, loss, g2, f2, w_enc, n_utt * n_loc, n_t))
        return loss.reshape(n_utt), gf.reshape(n_utt, n_loc, n_h), gwe, gwp, gwo

    in_specs = (P('dp', 'seq', None), P('dp', None, None), P(None, None), P(None, None), P(None, None), P('dp', None), P('dp'), P('dp'))
    out_specs = (P('dp'), P('dp', 'seq', None), P('dp', None), P('dp', None), P('dp', None))
    return jax.shard_map(local_fn, mesh=mesh, in_specs=in_specs, out_specs=out_specs, check_vma=False)
```

```python
import functools

import jax
import jax.numpy as jnp
from jax import lax
from jax.experimental import pallas as pl
from jax.experimental.pallas import tpu as pltpu
from jax.sharding import PartitionSpec as P

NEG = -1.0e30
ROWS = 256
WIN = 8
CHUNK = 128
CORE_MIN, CORE_MAX = 24, 40
GATHER_VMEM = 40 << 20
CORE_VMEM = 51 << 20
REDUCE_VMEM = 36 << 20
STORE_VMEM = 1 << 20
KEEP = 15
F32 = jnp.float32
BF16 = jnp.bfloat16
MESH = pl.DeviceIdType.MESH
NT = (((1,), (1,)), ((), ()))
NN = (((1,), (0,)), ((), ()))


def dot(a, b, dims=NN):
    return lax.dot_general(a, b, dims, preferred_element_type=F32)


def in_hbm(x):
    return pltpu.with_memory_space_constraint(x, pltpu.HBM)


def in_vmem(x):
    return pltpu.with_memory_space_constraint(x, pltpu.VMEM)


def split3(x):
    hi = x.astype(BF16).astype(F32)
    r1 = x - hi
    mid = r1.astype(BF16).astype(F32)
    return hi, mid, r1 - mid


def logadd(a, b):
    m = jnp.maximum(a, b)
    return m + jnp.log(1.0 + jnp.exp(jnp.minimum(a, b) - m))


def gather_kernel(n_t, enc_h, g_h, we_h, wp_h, wo_h, c_ref, a_ref, wot_ref, f_ref, enc_ref, g_ref, we_ref, wp_ref, wo_ref, fbuf,
                  in_sem, send_sem, recv_sem):
    me = lax.axis_index('seq')
    n_seq = fbuf.shape[0]
    partner = me + 1 - 2 * (me % 2)
    peer = (me + 2) % n_seq
    load_enc, load_wo, load_wp, load_g, load_we = loads = [pltpu.make_async_copy(src, dst, in_sem.at[q]) for q, (src, dst) in enumerate(
        ((enc_h, enc_ref), (wo_h, wo_ref), (wp_h, wp_ref), (g_h, g_ref), (we_h, we_ref)))]
    for load in loads:
        load.start()
    barrier = pltpu.get_barrier_semaphore()
    for other in (partner, peer):
        pl.semaphore_signal(barrier, inc=1, device_id={'seq': other}, device_id_type=MESH)
    pl.semaphore_wait(barrier, 2)

    def send(src, slot, sem, other):
        return pltpu.make_async_remote_copy(src_ref=src, dst_ref=fbuf.at[slot], send_sem=send_sem.at[sem], recv_sem=recv_sem.at[sem],
                                            device_id={'seq': other}, device_id_type=MESH)
    load_enc.wait()
    to_peer = send(enc_ref, me, 0, peer)
    to_peer.start()
    to_partner = send(enc_ref, me, 1, partner)
    to_partner.start()
    fbuf[me] = enc_ref[...]
    load_wo.wait()
    wot_ref[...] = wo_ref[...].T
    load_wp.wait()
    load_g.wait()
    c_ref[...] = dot(wp_ref[...].T, g_ref[...], NT).astype(BF16)
    load_we.wait()
    we_t = we_ref[...].T
    to_peer.wait_recv()
    relay = send(fbuf.at[peer], peer, 2, partner)
    relay.start()
    n_f = f_ref.shape[0]
    n_b = n_f // n_t
    n_loc = n_t // n_seq
    row = lax.broadcasted_iota(jnp.int32, (n_f, n_f), 0)
    col = lax.broadcasted_iota(jnp.int32, (n_f, n_f), 1)
    t = row % n_t
    order = jnp.where(col == (t // n_loc) * (n_b * n_loc) + (row // n_t) * n_loc + t % n_loc, 1.0, 0.0).astype(BF16)
    to_partner.wait_recv()
    relay.wait_recv()
    f_bt = dot(order, fbuf[...].reshape(n_f, f_ref.shape[1])).astype(BF16)
    f_ref[...] = f_bt
    a_ref[:, 0:n_f] = dot(we_t, f_bt, NT).astype(BF16)
    a_ref[:, n_f:] = jnp.zeros((a_ref.shape[0], a_ref.shape[1] - n_f), BF16)
    to_peer.wait_send()
    to_partner.wait_send()
    relay.wait_send()


def gather_call(enc, g2, w_enc, w_pred, w_out, n_seq, n_t):
    n_rows, n_h = enc.shape
    n_j = w_enc.shape[1]
    vm = pl.BlockSpec(memory_space=pltpu.VMEM)
    n_f = n_rows * n_seq
    args = [in_hbm(x) for x in (enc, g2, w_enc, w_pred, w_out)]
    return pl.pallas_call(
        functools.partial(gather_kernel, n_t),
        out_shape=(
            pltpu.VMEM((n_j, g2.shape[0]), BF16),
            pltpu.VMEM((n_j, n_f + 128), BF16),
            pltpu.VMEM(w_out.shape[::-1], BF16),
            pltpu.VMEM((n_f, n_h), BF16),
        ),
        in_specs=[pl.BlockSpec(memory_space=pltpu.HBM)] * 5,
        out_specs=(vm,) * 4,
        scratch_shapes=[pltpu.VMEM(x.shape, x.dtype) for x in (enc, g2, w_enc, w_pred, w_out)] + [
            pltpu.VMEM((n_seq, n_rows, n_h), BF16),
            pltpu.SemaphoreType.DMA((5,)),
            pltpu.SemaphoreType.DMA((3,)),
            pltpu.SemaphoreType.DMA((3,)),
        ],
        compiler_params=pltpu.CompilerParams(collective_id=0, has_side_effects=True, vmem_limit_bytes=GATHER_VMEM),
        name="rnnt_gather",
    )(*args)


def reduce_kernel(n_t, gwo_v, dc_v, da_v, loss_v, f_v, g_p, we_p, loss_ref, gf_ref, gwe_ref, gwp_ref, gwo_ref,
                  g_v, we_v, gwp_v, rgwo, rgwp, rda, rloss, in_sem, send_sem, recv_sem):
    me = lax.axis_index('seq')
    partner = me + 1 - 2 * (me % 2)
    loads = [pltpu.make_async_copy(src, dst, in_sem.at[q]) for q, (src, dst) in enumerate(((g_p, g_v), (we_p, we_v)))]
    for load in loads:
        load.start()
    barrier = pltpu.get_barrier_semaphore()
    pl.semaphore_signal(barrier, inc=1, device_id={'seq': partner}, device_id_type=MESH)
    pl.semaphore_wait(barrier, 1)

    def send(src, dst, sem):
        return pltpu.make_async_remote_copy(src_ref=src, dst_ref=dst, send_sem=send_sem.at[sem], recv_sem=recv_sem.at[sem],
                                            device_id={'seq': partner}, device_id_type=MESH)
    n_part = 4
    rows = gwo_v.shape[0] // n_part
    sends = [send(da_v, rda, 0), send(loss_v, rloss, 1)]
    sends += [send(gwo_v.at[pl.ds(q * rows, rows)], rgwo.at[pl.ds(q * rows, rows)], 2 + q) for q in range(n_part)]
    for s in sends:
        s.start()
    loads[0].wait()
    gwp_v[...] = dot(g_v[...].T, dc_v[...], NT)
    s_gwp = send(gwp_v, rgwp, 2 + n_part)
    loads[1].wait()
    sends[0].wait_recv()
    sends[1].wait_recv()
    loss_ref[...] = (loss_v[0:1, :] + rloss[0:1, :])[:, 0:loss_ref.shape[1]]
    da = (da_v[...].astype(F32) + rda[...].astype(F32)).astype(BF16)
    s_gwp.start()
    gwe_ref[...] = dot(f_v[...].T, da, NT)
    n_f = da.shape[1]
    n_own = gf_ref.shape[0]
    n_loc = n_own * n_t // n_f
    row = lax.broadcasted_iota(jnp.int32, (n_own, n_f), 0)
    col = lax.broadcasted_iota(jnp.int32, (n_own, n_f), 1)
    own = jnp.where(col == (row // n_loc) * n_t + me * n_loc + row % n_loc, 1.0, 0.0).astype(BF16)
    gf_ref[...] = dot(dot(own, da, NT).astype(BF16), we_v[...], NT).astype(BF16)
    for q in range(n_part):
        sends[2 + q].wait_recv()
        part = slice(q * rows, (q + 1) * rows)
        gwo_ref[part] = gwo_v[part] + rgwo[part]
    s_gwp.wait_recv()
    gwp_ref[...] = gwp_v[...] + rgwp[...]
    for s in sends + [s_gwp]:
        s.wait_send()


def reduce_call(gwo, dc_t, da_t, loss, g2, f2, w_enc, n_own, n_t):
    vm = pl.BlockSpec(memory_space=pltpu.VMEM)
    like = lambda x: pltpu.VMEM(x.shape, x.dtype)
    gwp_shape = (g2.shape[1], dc_t.shape[0])
    return pl.pallas_call(
        functools.partial(reduce_kernel, n_t),
        out_shape=(
            pltpu.VMEM((1, f2.shape[0] // n_t), F32),
            pltpu.VMEM((n_own, w_enc.shape[0]), BF16),
            pltpu.VMEM(w_enc.shape, F32),
            pltpu.VMEM(gwp_shape, F32),
            pltpu.VMEM(gwo.shape, F32),
        ),
        in_specs=[vm] * 5 + [pl.BlockSpec(memory_space=pltpu.HBM)] * 2,
        out_specs=(vm,) * 5,
        scratch_shapes=[like(x) for x in (g2, w_enc)] + [
            pltpu.VMEM(gwp_shape, F32), like(gwo), pltpu.VMEM(gwp_shape, F32), like(da_t), like(loss),
            pltpu.SemaphoreType.DMA((2,)),
            pltpu.SemaphoreType.DMA((7,)),
            pltpu.SemaphoreType.DMA((7,)),
        ],
        compiler_params=pltpu.CompilerParams(collective_id=1, has_side_effects=True, vmem_limit_bytes=REDUCE_VMEM),
        name="rnnt_reduce",
    )(in_vmem(gwo), in_vmem(dc_t), in_vmem(da_t), in_vmem(loss), in_vmem(f2), in_hbm(g2), in_hbm(w_enc))


def store_kernel(n, *refs):
    sems = refs[2 * n]
    copies = [pltpu.make_async_copy(refs[q], refs[n + q], sems.at[q]) for q in range(n)]
    for copy in copies:
        copy.start()
    for copy in copies:
        copy.wait()


def store_call(arrays):
    n = len(arrays)
    return pl.pallas_call(
        functools.partial(store_kernel, n),
        out_shape=tuple(pltpu.HBM(x.shape, x.dtype) for x in arrays),
        in_specs=[pl.BlockSpec(memory_space=pltpu.VMEM)] * n,
        out_specs=(pl.BlockSpec(memory_space=pltpu.HBM),) * n,
        scratch_shapes=[pltpu.SemaphoreType.DMA((n,))],
        compiler_params=pltpu.CompilerParams(vmem_limit_bytes=STORE_VMEM),
        name="rnnt_store",
    )(*[in_vmem(x) for x in arrays])


def core_kernel(n_t, n_u, flen_s, llen_s, flen_v, llen_v, lab_ref, c_buf, a_buf, wot, wo_h,
                loss_ref, dc_ref, da_ref, gwo_ref,
                wo_ref, wo_sem, ylab, hbuf, hpar, ebuf, fac, mch, sch, vsb, ypar, ybuf, idx, dzb, dpb, zrow, sk, abuf, t1buf, t2buf,
                gocc, gocb, segu, segt, tbl, off):
    n_utt = flen_s.shape[0]
    n_j = c_buf.shape[0]
    n_v = wo_ref.shape[1]
    step_u = WIN // 2 * n_u
    step_t = WIN // 2 * n_t
    per_tile = 128 // step_t
    gu = WIN * n_u
    n_win = n_utt * 2 // WIN - 1
    n_diag = n_t + n_u - 1
    n_kt = (n_diag + 1) * n_t
    n_ch = n_v // CHUNK

    load_wo = pltpu.make_async_copy(wo_h, wo_ref, wo_sem)
    load_wo.start()

    def off_step(b, total):
        off[b] = total
        return total + flen_s[b] * (llen_s[b] + 1)
    off[n_utt] = lax.fori_loop(0, n_utt, off_step, jnp.int32(0))

    total = off[n_utt]
    cut = lax.fori_loop(CORE_MIN, CORE_MAX, lambda b, n: n + jnp.where(off[b] + off[b + 1] <= total, 1, 0), jnp.int32(CORE_MIN))
    first_core = lax.axis_index('seq') % 2 == 0
    u_lo = jnp.where(first_core, 0, cut)
    u_hi = jnp.where(first_core, cut, n_utt)
    stop = off[u_hi]

    def utt_step(b, carry):
        win = jnp.minimum(b // (WIN // 2), n_win - 1)
        base = off[win * (WIN // 2)]
        last = jnp.minimum(off[win * (WIN // 2) + WIN], stop)

        def emit(c):
            n, pos = c
            end = jnp.minimum(pos + ROWS, last)
            tbl[0, n] = win
            tbl[1, n] = pos - base
            tbl[2, n] = end - base
            return n + 1, end
        return lax.while_loop(lambda c: c[1] < off[b + 1], emit, carry)
    n_blocks, _ = lax.fori_loop(u_lo, u_hi, utt_step, (jnp.int32(0), off[u_lo]))
    for past in range(3):
        for q in range(3):
            tbl[q, n_blocks + past] = 0

    lab = lab_ref[...]
    place = jnp.where(lax.broadcasted_iota(jnp.int32, (n_utt, n_utt * n_u), 1) // n_u
                      == lax.broadcasted_iota(jnp.int32, (n_utt, n_utt * n_u), 0), 1.0, 0.0).astype(BF16)
    mine = (lax.broadcasted_iota(jnp.int32, (lab.shape[0], n_utt * n_u), 1) % n_u
            == lax.broadcasted_iota(jnp.int32, (lab.shape[0], n_utt * n_u), 0))
    flat = []
    for part in (lax.shift_right_arithmetic(lab, 5), jnp.bitwise_and(lab, 31)):
        spread = dot(part.astype(F32).astype(BF16), place)
        flat.append(jnp.sum(jnp.where(mine, spread, 0.0), axis=0, keepdims=True))
    for w in range(n_win):
        row = lax.broadcasted_iota(jnp.int32, (16, gu), 0)
        hi, lo = (x[:, w * step_u:w * step_u + gu] for x in flat)
        ylab[w] = jnp.where(row == 0, hi, jnp.where(row == 1, lo, 0.0)).astype(BF16)
    sk[...] = jnp.zeros_like(sk)
    mch[...] = jnp.zeros_like(mch)
    sch[...] = jnp.ones_like(sch)
    zrow[...] = jnp.zeros_like(zrow)
    vsb[...] = jnp.zeros_like(vsb)
    dpb[...] = jnp.zeros_like(dpb)
    segu[...] = jnp.zeros_like(segu)
    segt[...] = jnp.zeros_like(segt)
    gwo_ref[...] = jnp.zeros_like(gwo_ref)

    def onehot(n, index_row):
        return (lax.broadcasted_iota(jnp.int32, (n, ROWS), 0) == index_row)

    def as_bf16(mask):
        return jnp.where(mask, 1.0, 0.0).astype(BF16)

    def frame_onehot(index_row):
        n = WIN * n_t + 128 - step_t
        return jnp.concatenate([as_bf16(onehot(n, index_row)), jnp.zeros((256 - n, ROWS), BF16)], axis=0)

    v_iota = lax.broadcasted_iota(jnp.int32, (CHUNK, ROWS), 0)
    n_sub = CHUNK // 8

    def lanes_of(win):
        return pl.ds(pl.multiple_of(win * step_u, 128), gu)

    def frame_lanes_of(win):
        return pl.ds(pl.multiple_of(win // per_tile * 128, 128), 256)

    part_row = lax.broadcasted_iota(jnp.int32, (128, ROWS), 0)

    def spread3(idx_b, parts):
        out = jnp.zeros((128, ROWS), F32)
        for q, part in enumerate(parts):
            out = jnp.where(part_row == idx_b + q * CORE_MAX, part, out)
        return out.astype(BF16)

    def locate(i):
        win = tbl[0, i]
        r = tbl[1, i] + lax.broadcasted_iota(jnp.int32, (1, ROWS), 1)
        end_r = tbl[2, i]
        start = jnp.int32(0)
        bl = jnp.full((1, ROWS), -1, jnp.int32)
        w = jnp.zeros((1, ROWS), jnp.int32)
        u1 = jnp.ones((1, ROWS), jnp.int32)
        for j in range(WIN):
            u1_j = llen_s[win * (WIN // 2) + j] + 1
            end = start + flen_s[win * (WIN // 2) + j] * u1_j
            inside = (r >= start) & (r < jnp.minimum(end, end_r))
            bl = jnp.where(inside, j, bl)
            w = jnp.where(inside, r - start, w)
            u1 = jnp.where(inside, u1_j, u1)
            start = end
        valid = bl >= 0
        t = jnp.zeros((1, ROWS), jnp.int32)
        for j in range(1, n_t):
            t = t + jnp.where(w >= j * u1, 1, 0)
        u = w - t * u1
        idx_u = jnp.where(valid, bl * n_u + u, -1)
        idx_t = jnp.where(valid, bl * n_t + t + win % per_tile * step_t, -1)
        idx_kt = jnp.where(valid, (t + u) * n_t + t, -1)
        idx_b = jnp.where(valid, win * (WIN // 2) + bl - u_lo, -1024)
        rows8 = lax.broadcasted_iota(jnp.int32, (8, ROWS), 0)
        idx[i] = jnp.where(rows8 == 0, idx_u, jnp.where(rows8 == 1, idx_t, jnp.where(rows8 == 2, idx_kt, idx_b)))

    half = n_j // 2

    def hidden(i, par):
        win = tbl[0, i]
        ohu = as_bf16(onehot(gu, idx[i, 0:1]))
        oht = frame_onehot(idx[i, 1:2])
        for q in range(2):
            rows = slice(q * half, (q + 1) * half)
            pre = dot(c_buf[rows, lanes_of(win)], ohu) + dot(a_buf[rows, frame_lanes_of(win)], oht)
            h = jnp.tanh(pre).astype(BF16)
            hpar[par, rows] = h
            hbuf[i, rows] = h
        yy = dot(ylab[win], ohu)
        y8 = jnp.broadcast_to((yy[0:1] * 32.0 + yy[1:2]).astype(jnp.int32), (8, ROWS))
        ypar[par] = y8
        ybuf[i] = y8

    def finish(i, par):
        idx_b = idx[i, 3:4]
        m_all = mch[par]
        m8 = jnp.max(m_all.reshape(n_ch, 8, ROWS), axis=0)
        m = jnp.max(m8, axis=0, keepdims=True)
        f_all = jnp.exp(m_all - m)
        s = jnp.sum(jnp.sum((sch[par] * f_all).reshape(n_ch, 8, ROWS), axis=0), axis=0, keepdims=True)
        fac[i] = f_all * (1.0 / s)
        lse = m + jnp.log(s)
        b_parts = split3(zrow[par, 8:9] - lse)
        l_parts = split3(jnp.sum(zrow[par, 0:8], axis=0, keepdims=True) - lse)
        vsb[par, 0:128] = spread3(idx_b, b_parts)
        vsb[par, 128:256] = spread3(idx_b, l_parts)

    def scatter(i, par, live):
        okt = as_bf16(onehot(n_kt, jnp.where(live, idx[i, 2:3], -1)))
        part = n_kt // 2
        for q in range(2):
            sk[q * part:(q + 1) * part] += dot(okt[q * part:(q + 1) * part], vsb[par], NT)

    def slot_of(i):
        return jnp.where(i < KEEP, i, KEEP + i % 2)

    def scores_of(i, par):
        y = ypar[par, 0:1]
        slot = slot_of(i)
        lz = None
        for c in range(n_ch):
            z = dot(wot[c * CHUNK:(c + 1) * CHUNK, :], hpar[par])
            z3 = z.reshape(n_sub, 8, ROWS)
            zl = jnp.sum(jnp.where(v_iota == y - c * CHUNK, z, 0.0).reshape(n_sub, 8, ROWS), axis=0)
            lz = zl if lz is None else lz + zl
            if c == 0:
                zrow[par, 8:16] = z[0:8, :]
            m_c = jnp.max(z3, axis=0)
            e3 = jnp.exp(z3 - m_c[None])
            ebuf[slot, c * CHUNK:(c + 1) * CHUNK, :] = e3.reshape(CHUNK, ROWS)
            mch[par, c * 8:(c + 1) * 8, :] = m_c
            sch[par, c * 8:(c + 1) * 8, :] = jnp.sum(e3, axis=0)
        zrow[par, 0:8] = lz

    def fwd_pair(p, carry):
        i = 2 * p
        hidden(i + 1, 1)
        finish(jnp.maximum(i - 1, 0), 1)
        scatter(jnp.maximum(i - 2, 0), 0, i > 1)
        scores_of(i, 0)
        scatter(jnp.maximum(i - 1, 0), 1, i > 0)
        hidden(i + 2, 0)
        finish(i, 0)
        scores_of(i + 1, 1)
        locate(i + 3)
        locate(i + 4)
        return carry

    def fwd_odd(p, carry):
        i = n_blocks - 1
        finish(jnp.maximum(i - 1, 0), 1)
        scatter(jnp.maximum(i - 2, 0), 0, i > 1)
        scores_of(i, 0)
        scatter(jnp.maximum(i - 1, 0), 1, i > 0)
        finish(i, 0)
        scatter(i, 0, True)
        return carry

    def fwd_even(p, carry):
        finish(n_blocks - 1, 1)
        scatter(n_blocks - 2, 0, True)
        scatter(n_blocks - 1, 1, True)
        return carry

    for first in range(3):
        locate(jnp.int32(first))
    hidden(jnp.int32(0), 0)
    lax.fori_loop(0, n_blocks // 2, fwd_pair, 0)
    lax.fori_loop(0, n_blocks % 2, fwd_odd, 0)
    lax.fori_loop(0, 1 - n_blocks % 2, fwd_even, 0)

    tt = lax.broadcasted_iota(jnp.int32, (n_t, 128), 0)
    def own_lanes(ref):
        x = jnp.concatenate([ref[...], jnp.zeros((1, 128 - n_utt), jnp.int32)], axis=1).astype(F32)
        return pltpu.roll(jnp.broadcast_to(x, (n_t, 128)), (128 - u_lo) % 128, 1).astype(jnp.int32)
    t_len = own_lanes(flen_v)
    u_len = own_lanes(llen_v)

    def scores(k):
        lo = k * n_t
        x, y = (v + pltpu.roll(v, 128 - CORE_MAX, 1) + pltpu.roll(v, 128 - 2 * CORE_MAX, 1)
                for v in (sk[lo:lo + n_t, 0:128], sk[lo:lo + n_t, 128:256]))
        uu = k - tt
        ok = (uu >= 0) & (tt < t_len)
        bl_k = jnp.where(ok & (uu <= u_len), x, NEG)
        lb_k = jnp.where(ok & (uu < u_len), y, NEG)
        return bl_k, lb_k

    alpha = jnp.where(tt == 0, 0.0, NEG).astype(F32)
    abuf[0] = alpha
    beta = jnp.full((n_t, 128), NEG, F32)
    sc = [scores(k) for k in range(n_diag)]
    for step in range(n_diag):
        if step > 0:
            bl_k, lb_k = sc[step - 1]
            p1 = jnp.where(tt == 0, NEG, pltpu.roll(alpha + bl_k, 1, 0))
            alpha = logadd(p1, alpha + lb_k)
            abuf[step] = alpha
        k = n_diag - 1 - step
        bl_k, lb_k = sc[k]
        up = jnp.where(tt == n_t - 1, jnp.where(u_len == k + 1 - n_t, 0.0, NEG), pltpu.roll(beta, n_t - 1, 0))
        t1 = up + bl_k
        t2 = beta + lb_k
        t1buf[k] = t1
        t2buf[k] = t2
        beta = jnp.where(tt >= t_len, jnp.where(k - tt == u_len, 0.0, NEG), logadd(t1, t2))
    log_p = beta[0:1, :]
    lane = lax.broadcasted_iota(jnp.int32, (n_t, 128), 1)
    loss_ref[...] = pltpu.roll(jnp.where(lane < u_hi - u_lo, -log_p, 0.0), u_lo, 1)
    lane_ok = lane < CORE_MAX
    for k in range(n_diag):
        for which, buf in enumerate((t1buf, t2buf)):
            occ = jnp.where(lane_ok, jnp.exp(jnp.minimum(abuf[k] + buf[k] - log_p, 0.0)), 0.0)
            hi, mid, lo = split3(occ)
            lo_row = which * n_kt + k * n_t
            gocc[lo_row:lo_row + n_t, :] = hi + pltpu.roll(mid, CORE_MAX, 1) + pltpu.roll(lo, 2 * CORE_MAX, 1)
    for which in range(2):
        gocc[which * n_kt + n_diag * n_t:(which + 1) * n_kt, :] = jnp.zeros((n_kt - n_diag * n_t, 128), F32)
    gocb[...] = gocc[...].astype(BF16)

    def again(first, count):
        def one(q, carry):
            i = first + q

            @pl.when(i >= KEEP)
            def _():
                def chunk(c, carry):
                    rows = pl.ds(pl.multiple_of(c * CHUNK, CHUNK), CHUNK)
                    z3 = dot(wot[rows, :], hbuf[i]).reshape(n_sub, 8, ROWS)
                    ebuf[KEEP + i % 2, rows, :] = jnp.exp(z3 - jnp.max(z3, axis=0)[None]).reshape(CHUNK, ROWS)
                    return carry
                lax.fori_loop(0, n_ch, chunk, 0)
            return carry
        lax.fori_loop(0, count, one, 0)

    def occupancy(i, par):
        orep = spread3(idx[i, 3:4], (1.0, 1.0, 1.0))
        okt = onehot(n_kt, idx[i, 2:3])
        for which in range(2):
            gath = dot(gocb[which * n_kt:(which + 1) * n_kt], orep)
            occ = jnp.sum(jnp.where(okt, gath, 0.0), axis=0, keepdims=True)
            zrow[par, which * 8:which * 8 + 8] = jnp.broadcast_to(occ, (8, ROWS))

    def d_logits(i, par):
        y = ybuf[i, 0:1]
        gb = zrow[par, 0:1]
        gl = zrow[par, 8:9]
        occ = gb + gl
        slot = slot_of(i)
        for c in range(n_ch):
            sc_c = fac[i, c * 8:(c + 1) * 8, :] * occ
            e3 = ebuf[slot, c * CHUNK:(c + 1) * CHUNK, :].reshape(n_sub, 8, ROWS)
            d = (e3 * sc_c[None]).reshape(CHUNK, ROWS) - jnp.where(v_iota == y - c * CHUNK, gl, 0.0)
            if c == 0:
                d = d - jnp.where(v_iota == 0, gb, 0.0)
            dzb[par, c * CHUNK:(c + 1) * CHUNK, :] = d.astype(BF16)

    def segments(i, par):
        win = tbl[0, i]
        ohu = as_bf16(onehot(gu, idx[i, 0:1]))
        oht = frame_onehot(idx[i, 1:2])
        for q in range(2):
            rows = slice(q * half, (q + 1) * half)
            segu[rows, lanes_of(win)] += dot(dpb[par, rows], ohu, NT)
            segt[rows, frame_lanes_of(win)] += dot(dpb[par, rows], oht, NT)

    def d_hidden(i, par):
        for q in range(2):
            rows = slice(q * half, (q + 1) * half)
            hf = hbuf[i, rows].astype(F32)
            dh = dot(wo_ref[rows], dzb[par])
            dpb[par, rows] = (dh * (1.0 - hf * hf)).astype(BF16)

    def out_grad(blocks):
        for c in range(n_v // 256):
            cols = slice(c * 256, (c + 1) * 256)
            new = None
            for i, par in blocks:
                term = dot(hbuf[i], dzb[par, cols, :], NT)
                new = term if new is None else new + term
            gwo_ref[:, cols] += new

    def bwd_pair(p, carry):
        i = 2 * p
        again(i + 2, 2)
        d_hidden(i, 0)
        d_hidden(i + 1, 1)
        out_grad(((i, 0), (i + 1, 1)))
        d_logits(i + 2, 0)
        segments(i, 0)
        d_logits(i + 3, 1)
        segments(i + 1, 1)
        occupancy(i + 4, 0)
        occupancy(i + 5, 1)
        return carry

    def bwd_odd(p, carry):
        d_hidden(n_blocks - 1, 0)
        out_grad(((n_blocks - 1, 0),))
        segments(n_blocks - 1, 0)
        return carry

    load_wo.wait()
    again(0, 2)
    for first in range(2):
        occupancy(jnp.int32(first), first)
        d_logits(jnp.int32(first), first)
        occupancy(jnp.int32(first + 2), first)
    lax.fori_loop(0, n_blocks // 2, bwd_pair, 0)
    lax.fori_loop(0, n_blocks % 2, bwd_odd, 0)

    dc_ref[...] = segu[...].astype(BF16)
    da_ref[...] = segt[:, 0:n_utt * n_t].astype(BF16)


def core_call(c_t, a_t, wot, w_out, labels, flen, llen, n_t, n_u):
    n_utt = flen.shape[0]
    n_j = c_t.shape[0]
    n_v = w_out.shape[1]
    n_win = n_utt * 2 // WIN - 1
    max_blk = n_utt // 2 * n_t * n_u // ROWS + 6
    n_kt = (n_t + n_u) * n_t
    n_st = n_v // CHUNK * 8
    vm = pl.BlockSpec(memory_space=pltpu.VMEM)
    sm = pl.BlockSpec(memory_space=pltpu.SMEM)
    return pl.pallas_call(
        functools.partial(core_kernel, n_t, n_u),
        out_shape=(
            pltpu.VMEM((8, 128), F32),
            pltpu.VMEM((n_j, n_utt * n_u), BF16),
            pltpu.VMEM((n_j, n_utt * n_t), BF16),
            pltpu.VMEM(w_out.shape, F32),
        ),
        in_specs=[sm, sm] + [vm] * 6 + [pl.BlockSpec(memory_space=pltpu.HBM)],
        out_specs=(vm,) * 4,
        scratch_shapes=[
            pltpu.VMEM(w_out.shape, BF16),
            pltpu.SemaphoreType.DMA,
            pltpu.VMEM((n_win, 16, WIN * n_u), BF16),
            pltpu.VMEM((max_blk, n_j, ROWS), BF16),
            pltpu.VMEM((2, n_j, ROWS), BF16),
            pltpu.VMEM((min(max_blk, KEEP + 2), n_v, ROWS), F32),
            pltpu.VMEM((max_blk, n_st, ROWS), F32),
            pltpu.VMEM((2, n_st, ROWS), F32),
            pltpu.VMEM((2, n_st, ROWS), F32),
            pltpu.VMEM((2, 256, ROWS), BF16),
            pltpu.VMEM((2, 8, ROWS), jnp.int32),
            pltpu.VMEM((max_blk, 8, ROWS), jnp.int32),
            pltpu.VMEM((max_blk, 8, ROWS), jnp.int32),
            pltpu.VMEM((2, n_v, ROWS), BF16),
            pltpu.VMEM((2, n_j, ROWS), BF16),
            pltpu.VMEM((2, 16, ROWS), F32),
            pltpu.VMEM((n_kt, 256), F32),
            pltpu.VMEM((n_t + n_u, n_t, 128), F32),
            pltpu.VMEM((n_t + n_u, n_t, 128), F32),
            pltpu.VMEM((n_t + n_u, n_t, 128), F32),
            pltpu.VMEM((2 * n_kt, 128), F32),
            pltpu.VMEM((2 * n_kt, 128), BF16),
            pltpu.VMEM((n_j, n_utt * n_u), F32),
            pltpu.VMEM((n_j, n_utt * n_t + 128), F32),
            pltpu.SMEM((3, max_blk), jnp.int32),
            pltpu.SMEM((n_utt + 1,), jnp.int32),
        ],
        compiler_params=pltpu.CompilerParams(vmem_limit_bytes=CORE_VMEM),
        name="rnnt_core",
    )(flen, llen, flen.reshape(1, n_utt), llen.reshape(1, n_utt), labels.T, in_vmem(c_t), in_vmem(a_t), in_vmem(wot), in_hbm(w_out))


def solution(mesh):
    seq_size = mesh.shape['seq']

    def local_fn(enc_out, pred_out, w_enc, w_pred, w_out, labels, frame_len, label_len):
        n_utt, n_loc, n_h = enc_out.shape
        n_u = pred_out.shape[1]
        n_t = n_loc * seq_size
        g2 = pred_out.reshape(n_utt * n_u, n_h)
        c_t, a_t, wot, f2 = gather_call(enc_out.reshape(n_utt * n_loc, n_h), g2, w_enc, w_pred, w_out, seq_size, n_t)
        loss, dc_t, da_t, gwo = core_call(c_t, a_t, wot, w_out, labels, frame_len, label_len, n_t, n_u)
        loss, gf, gwe, gwp, gwo = store_call(reduce_call(gwo, dc_t, da_t, loss, g2, f2, w_enc, n_utt * n_loc, n_t))
        return loss.reshape(n_utt), gf.reshape(n_utt, n_loc, n_h), gwe, gwp, gwo

    in_specs = (P('dp', 'seq', None), P('dp', None, None), P(None, None), P(None, None), P(None, None), P('dp', None), P('dp'), P('dp'))
    out_specs = (P('dp'), P('dp', 'seq', None), P('dp', None), P('dp', None), P('dp', None))
    return jax.shard_map(local_fn, mesh=mesh, in_specs=in_specs, out_specs=out_specs, check_vma=False)
```

```python
import functools

import jax
import jax.numpy as jnp
from jax import lax
from jax.experimental import pallas as pl
from jax.experimental.pallas import tpu as pltpu
from jax.sharding import PartitionSpec as P

NEG = -1.0e30
ROWS = 256
WIN = 8
CHUNK = 128
CORE_MIN, CORE_MAX = 24, 40
GATHER_VMEM = 40 << 20
CORE_VMEM = 51 << 20
REDUCE_VMEM = 36 << 20
STORE_VMEM = 1 << 20
KEEP = 15
F32 = jnp.float32
BF16 = jnp.bfloat16
MESH = pl.DeviceIdType.MESH
NT = (((1,), (1,)), ((), ()))
NN = (((1,), (0,)), ((), ()))


def dot(a, b, dims=NN):
    return lax.dot_general(a, b, dims, preferred_element_type=F32)


def in_hbm(x):
    return pltpu.with_memory_space_constraint(x, pltpu.HBM)


def in_vmem(x):
    return pltpu.with_memory_space_constraint(x, pltpu.VMEM)


def split3(x):
    hi = x.astype(BF16).astype(F32)
    r1 = x - hi
    mid = r1.astype(BF16).astype(F32)
    return hi, mid, r1 - mid


def logadd(a, b):
    m = jnp.maximum(a, b)
    return m + jnp.log(1.0 + jnp.exp(jnp.minimum(a, b) - m))


def gather_kernel(n_t, enc_h, g_h, we_h, wp_h, wo_h, c_ref, a_ref, wot_ref, f_ref, enc_ref, g_ref, we_ref, wp_ref, wo_ref, fbuf,
                  in_sem, send_sem, recv_sem):
    me = lax.axis_index('seq')
    n_seq = fbuf.shape[0]
    partner = me + 1 - 2 * (me % 2)
    peer = (me + 2) % n_seq
    load_enc, load_wo, load_wp, load_g, load_we = loads = [pltpu.make_async_copy(src, dst, in_sem.at[q]) for q, (src, dst) in enumerate(
        ((enc_h, enc_ref), (wo_h, wo_ref), (wp_h, wp_ref), (g_h, g_ref), (we_h, we_ref)))]
    for load in loads:
        load.start()
    barrier = pltpu.get_barrier_semaphore()
    for other in (partner, peer):
        pl.semaphore_signal(barrier, inc=1, device_id={'seq': other}, device_id_type=MESH)
    pl.semaphore_wait(barrier, 2)

    def send(src, slot, sem, other):
        return pltpu.make_async_remote_copy(src_ref=src, dst_ref=fbuf.at[slot], send_sem=send_sem.at[sem], recv_sem=recv_sem.at[sem],
                                            device_id={'seq': other}, device_id_type=MESH)
    load_enc.wait()
    to_peer = send(enc_ref, me, 0, peer)
    to_peer.start()
    to_partner = send(enc_ref, me, 1, partner)
    to_partner.start()
    fbuf[me] = enc_ref[...]
    load_wo.wait()
    wot_ref[...] = wo_ref[...].T
    load_wp.wait()
    load_g.wait()
    c_ref[...] = dot(wp_ref[...].T, g_ref[...], NT).astype(BF16)
    load_we.wait()
    we_t = we_ref[...].T
    to_peer.wait_recv()
    relay = send(fbuf.at[peer], peer, 2, partner)
    relay.start()
    n_f, n_h = f_ref.shape
    n_b = n_f // n_t
    n_loc = n_t // n_seq
    row = lax.broadcasted_iota(jnp.int32, (n_f, n_f), 0)
    col = lax.broadcasted_iota(jnp.int32, (n_f, n_f), 1)
    t = row % n_t
    order = jnp.where(col == (t // n_loc) * (n_b * n_loc) + (row // n_t) * n_loc + t % n_loc, 1.0, 0.0).astype(BF16)
    to_partner.wait_recv()
    relay.wait_recv()
    f_bt = dot(order, fbuf[...].reshape(n_f, n_h)).astype(BF16)
    f_ref[...] = f_bt
    a_ref[:, 0:n_f] = dot(we_t, f_bt, NT).astype(BF16)
    a_ref[:, n_f:] = jnp.zeros((a_ref.shape[0], a_ref.shape[1] - n_f), BF16)
    to_peer.wait_send()
    to_partner.wait_send()
    relay.wait_send()


def gather_call(enc, g2, w_enc, w_pred, w_out, n_seq, n_t):
    n_utt, n_loc, n_h = enc.shape
    n_j = w_enc.shape[1]
    vm = pl.BlockSpec(memory_space=pltpu.VMEM)
    n_f = n_utt * n_loc * n_seq
    args = [in_hbm(x) for x in (enc, g2, w_enc, w_pred, w_out)]
    return pl.pallas_call(
        functools.partial(gather_kernel, n_t),
        out_shape=(
            pltpu.VMEM((n_j, g2.shape[0]), BF16),
            pltpu.VMEM((n_j, n_f + 128), BF16),
            pltpu.VMEM(w_out.shape[::-1], BF16),
            pltpu.VMEM((n_f, n_h), BF16),
        ),
        in_specs=[pl.BlockSpec(memory_space=pltpu.HBM)] * 5,
        out_specs=(vm,) * 4,
        scratch_shapes=[pltpu.VMEM(x.shape, x.dtype) for x in (enc, g2, w_enc, w_pred, w_out)] + [
            pltpu.VMEM((n_seq, n_utt, n_loc, n_h), BF16),
            pltpu.SemaphoreType.DMA((5,)),
            pltpu.SemaphoreType.DMA((3,)),
            pltpu.SemaphoreType.DMA((3,)),
        ],
        compiler_params=pltpu.CompilerParams(collective_id=0, has_side_effects=True, vmem_limit_bytes=GATHER_VMEM),
        name="rnnt_gather",
    )(*args)


def reduce_kernel(n_t, gwo_v, dc_v, da_v, loss_v, f_v, g_p, we_p, loss_ref, gf_ref, gwe_ref, gwp_ref, gwo_ref,
                  g_v, we_v, gwp_v, rgwo, rgwp, rda, rloss, in_sem, send_sem, recv_sem):
    me = lax.axis_index('seq')
    partner = me + 1 - 2 * (me % 2)
    loads = [pltpu.make_async_copy(src, dst, in_sem.at[q]) for q, (src, dst) in enumerate(((g_p, g_v), (we_p, we_v)))]
    for load in loads:
        load.start()
    barrier = pltpu.get_barrier_semaphore()
    pl.semaphore_signal(barrier, inc=1, device_id={'seq': partner}, device_id_type=MESH)
    pl.semaphore_wait(barrier, 1)

    def send(src, dst, sem):
        return pltpu.make_async_remote_copy(src_ref=src, dst_ref=dst, send_sem=send_sem.at[sem], recv_sem=recv_sem.at[sem],
                                            device_id={'seq': partner}, device_id_type=MESH)
    n_part = 4
    rows = gwo_v.shape[0] // n_part
    sends = [send(da_v, rda, 0), send(loss_v, rloss, 1)]
    sends += [send(gwo_v.at[pl.ds(q * rows, rows)], rgwo.at[pl.ds(q * rows, rows)], 2 + q) for q in range(n_part)]
    for s in sends:
        s.start()
    loads[0].wait()
    gwp_v[...] = dot(g_v[...].T, dc_v[...], NT)
    s_gwp = send(gwp_v, rgwp, 2 + n_part)
    loads[1].wait()
    sends[0].wait_recv()
    sends[1].wait_recv()
    loss_ref[...] = (loss_v[0:1, :] + rloss[0:1, :])[:, 0:loss_ref.shape[1]]
    da = (da_v[...].astype(F32) + rda[...].astype(F32)).astype(BF16)
    s_gwp.start()
    gwe_ref[...] = dot(f_v[...].T, da, NT)
    n_f = da.shape[1]
    n_own = gf_ref.shape[0] * gf_ref.shape[1]
    n_loc = gf_ref.shape[1]
    row = lax.broadcasted_iota(jnp.int32, (n_own, n_f), 0)
    col = lax.broadcasted_iota(jnp.int32, (n_own, n_f), 1)
    own = jnp.where(col == (row // n_loc) * n_t + me * n_loc + row % n_loc, 1.0, 0.0).astype(BF16)
    gf_ref[...] = dot(dot(own, da, NT).astype(BF16), we_v[...], NT).astype(BF16).reshape(gf_ref.shape)
    for q in range(n_part):
        sends[2 + q].wait_recv()
        part = slice(q * rows, (q + 1) * rows)
        gwo_ref[part] = gwo_v[part] + rgwo[part]
    s_gwp.wait_recv()
    gwp_ref[...] = gwp_v[...] + rgwp[...]
    for s in sends + [s_gwp]:
        s.wait_send()


def reduce_call(gwo, dc_t, da_t, loss, g2, f2, w_enc, gf_shape, n_t):
    vm = pl.BlockSpec(memory_space=pltpu.VMEM)
    like = lambda x: pltpu.VMEM(x.shape, x.dtype)
    gwp_shape = (g2.shape[1], dc_t.shape[0])
    return pl.pallas_call(
        functools.partial(reduce_kernel, n_t),
        out_shape=(
            pltpu.VMEM((1, f2.shape[0] // n_t), F32),
            pltpu.VMEM(gf_shape, BF16),
            pltpu.VMEM(w_enc.shape, F32),
            pltpu.VMEM(gwp_shape, F32),
            pltpu.VMEM(gwo.shape, F32),
        ),
        in_specs=[vm] * 5 + [pl.BlockSpec(memory_space=pltpu.HBM)] * 2,
        out_specs=(vm,) * 5,
        scratch_shapes=[like(x) for x in (g2, w_enc)] + [
            pltpu.VMEM(gwp_shape, F32), like(gwo), pltpu.VMEM(gwp_shape, F32), like(da_t), like(loss),
            pltpu.SemaphoreType.DMA((2,)),
            pltpu.SemaphoreType.DMA((7,)),
            pltpu.SemaphoreType.DMA((7,)),
        ],
        compiler_params=pltpu.CompilerParams(collective_id=1, has_side_effects=True, vmem_limit_bytes=REDUCE_VMEM),
        name="rnnt_reduce",
    )(in_vmem(gwo), in_vmem(dc_t), in_vmem(da_t), in_vmem(loss), in_vmem(f2), in_hbm(g2), in_hbm(w_enc))


def store_kernel(n, *refs):
    sems = refs[2 * n]
    copies = [pltpu.make_async_copy(refs[q], refs[n + q], sems.at[q]) for q in range(n)]
    for copy in copies:
        copy.start()
    for copy in copies:
        copy.wait()


def store_call(arrays):
    n = len(arrays)
    return pl.pallas_call(
        functools.partial(store_kernel, n),
        out_shape=tuple(pltpu.HBM(x.shape, x.dtype) for x in arrays),
        in_specs=[pl.BlockSpec(memory_space=pltpu.VMEM)] * n,
        out_specs=(pl.BlockSpec(memory_space=pltpu.HBM),) * n,
        scratch_shapes=[pltpu.SemaphoreType.DMA((n,))],
        compiler_params=pltpu.CompilerParams(vmem_limit_bytes=STORE_VMEM),
        name="rnnt_store",
    )(*[in_vmem(x) for x in arrays])


def core_kernel(n_t, n_u, flen_s, llen_s, flen_v, llen_v, lab_ref, c_buf, a_buf, wot, wo_h,
                loss_ref, dc_ref, da_ref, gwo_ref,
                wo_ref, wo_sem, ylab, hbuf, hpar, ebuf, fac, mch, sch, vsb, ypar, ybuf, idx, dzb, dpb, zrow, sk, abuf, t1buf, t2buf,
                gocc, gocb, segu, segt, tbl, off):
    n_utt = flen_s.shape[0]
    n_j = c_buf.shape[0]
    n_v = wo_ref.shape[1]
    step_u = WIN // 2 * n_u
    step_t = WIN // 2 * n_t
    per_tile = 128 // step_t
    gu = WIN * n_u
    n_win = n_utt * 2 // WIN - 1
    n_diag = n_t + n_u - 1
    n_kt = (n_diag + 1) * n_t
    n_ch = n_v // CHUNK

    load_wo = pltpu.make_async_copy(wo_h, wo_ref, wo_sem)
    load_wo.start()

    def off_step(b, total):
        off[b] = total
        return total + flen_s[b] * (llen_s[b] + 1)
    off[n_utt] = lax.fori_loop(0, n_utt, off_step, jnp.int32(0))

    total = off[n_utt]
    cut = lax.fori_loop(CORE_MIN, CORE_MAX, lambda b, n: n + jnp.where(off[b] + off[b + 1] <= total, 1, 0), jnp.int32(CORE_MIN))
    first_core = lax.axis_index('seq') % 2 == 0
    u_lo = jnp.where(first_core, 0, cut)
    u_hi = jnp.where(first_core, cut, n_utt)
    stop = off[u_hi]

    def utt_step(b, carry):
        win = jnp.minimum(b // (WIN // 2), n_win - 1)
        base = off[win * (WIN // 2)]
        last = jnp.minimum(off[win * (WIN // 2) + WIN], stop)

        def emit(c):
            n, pos = c
            end = jnp.minimum(pos + ROWS, last)
            tbl[0, n] = win
            tbl[1, n] = pos - base
            tbl[2, n] = end - base
            return n + 1, end
        return lax.while_loop(lambda c: c[1] < off[b + 1], emit, carry)
    n_blocks, _ = lax.fori_loop(u_lo, u_hi, utt_step, (jnp.int32(0), off[u_lo]))
    for past in range(3):
        for q in range(3):
            tbl[q, n_blocks + past] = 0

    lab = lab_ref[...]
    place = jnp.where(lax.broadcasted_iota(jnp.int32, (n_utt, n_utt * n_u), 1) // n_u
                      == lax.broadcasted_iota(jnp.int32, (n_utt, n_utt * n_u), 0), 1.0, 0.0).astype(BF16)
    mine = (lax.broadcasted_iota(jnp.int32, (lab.shape[0], n_utt * n_u), 1) % n_u
            == lax.broadcasted_iota(jnp.int32, (lab.shape[0], n_utt * n_u), 0))
    flat = []
    for part in (lax.shift_right_arithmetic(lab, 5), jnp.bitwise_and(lab, 31)):
        spread = dot(part.astype(F32).astype(BF16), place)
        flat.append(jnp.sum(jnp.where(mine, spread, 0.0), axis=0, keepdims=True))
    for w in range(n_win):
        row = lax.broadcasted_iota(jnp.int32, (16, gu), 0)
        hi, lo = (x[:, w * step_u:w * step_u + gu] for x in flat)
        ylab[w] = jnp.where(row == 0, hi, jnp.where(row == 1, lo, 0.0)).astype(BF16)
    sk[...] = jnp.zeros_like(sk)
    mch[...] = jnp.zeros_like(mch)
    sch[...] = jnp.ones_like(sch)
    zrow[...] = jnp.zeros_like(zrow)
    vsb[...] = jnp.zeros_like(vsb)
    dpb[...] = jnp.zeros_like(dpb)

    def onehot(n, index_row):
        return (lax.broadcasted_iota(jnp.int32, (n, ROWS), 0) == index_row)

    def as_bf16(mask):
        return jnp.where(mask, 1.0, 0.0).astype(BF16)

    def frame_onehot(index_row):
        n = WIN * n_t + 128 - step_t
        return jnp.concatenate([as_bf16(onehot(n, index_row)), jnp.zeros((256 - n, ROWS), BF16)], axis=0)

    sub8 = lax.broadcasted_iota(jnp.int32, (8, ROWS), 0)
    n_sub = CHUNK // 8

    def lanes_of(win):
        return pl.ds(pl.multiple_of(win * step_u, 128), gu)

    def frame_lanes_of(win):
        return pl.ds(pl.multiple_of(win // per_tile * 128, 128), 256)

    def spread3(idx_b, parts):
        mask = lax.broadcasted_iota(jnp.int32, (CORE_MAX, ROWS), 0) == idx_b
        return jnp.concatenate([jnp.where(mask, part, 0.0) for part in parts]
                               + [jnp.zeros((128 - 3 * CORE_MAX, ROWS), F32)], axis=0).astype(BF16)

    def locate(i):
        win = tbl[0, i]
        r = tbl[1, i] + lax.broadcasted_iota(jnp.int32, (1, ROWS), 1)
        end_r = tbl[2, i]
        start = jnp.int32(0)
        bl = jnp.full((1, ROWS), -1, jnp.int32)
        w = jnp.zeros((1, ROWS), jnp.int32)
        u1 = jnp.ones((1, ROWS), jnp.int32)
        for j in range(WIN):
            u1_j = llen_s[win * (WIN // 2) + j] + 1
            end = start + flen_s[win * (WIN // 2) + j] * u1_j
            inside = (r >= start) & (r < jnp.minimum(end, end_r))
            bl = jnp.where(inside, j, bl)
            w = jnp.where(inside, r - start, w)
            u1 = jnp.where(inside, u1_j, u1)
            start = end
        valid = bl >= 0
        t = jnp.zeros((1, ROWS), jnp.int32)
        for j in range(1, n_t):
            t = t + jnp.where(w >= j * u1, 1, 0)
        u = w - t * u1
        idx_u = jnp.where(valid, bl * n_u + u, -1)
        idx_t = jnp.where(valid, bl * n_t + t + win % per_tile * step_t, -1)
        idx_kt = jnp.where(valid, (t + u) * n_t + t, -1)
        idx_b = jnp.where(valid, win * (WIN // 2) + bl - u_lo, -1024)
        rows8 = lax.broadcasted_iota(jnp.int32, (8, ROWS), 0)
        idx[i] = jnp.where(rows8 == 0, idx_u, jnp.where(rows8 == 1, idx_t, jnp.where(rows8 == 2, idx_kt, idx_b)))

    half = n_j // 2

    def hidden(i, par):
        win = tbl[0, i]
        ohu = as_bf16(onehot(gu, idx[i, 0:1]))
        oht = frame_onehot(idx[i, 1:2])
        for q in range(2):
            rows = slice(q * half, (q + 1) * half)
            pre = dot(c_buf[rows, lanes_of(win)], ohu) + dot(a_buf[rows, frame_lanes_of(win)], oht)
            h = jnp.tanh(pre).astype(BF16)
            hpar[par, rows] = h
            hbuf[i, rows] = h
        yy = dot(ylab[win], ohu)
        y8 = jnp.broadcast_to((yy[0:1] * 32.0 + yy[1:2]).astype(jnp.int32), (8, ROWS))
        ypar[par] = y8
        ybuf[i] = y8

    def finish(i, par):
        idx_b = idx[i, 3:4]
        m_all = mch[par]
        m8 = jnp.max(m_all.reshape(n_ch, 8, ROWS), axis=0)
        m = jnp.max(m8, axis=0, keepdims=True)
        f_all = jnp.exp(m_all - m)
        s = jnp.sum(jnp.sum((sch[par] * f_all).reshape(n_ch, 8, ROWS), axis=0), axis=0, keepdims=True)
        fac[i] = f_all * (1.0 / s)
        lse = m + jnp.log(s)
        b_parts = split3(zrow[par, 8:9] - lse)
        l_parts = split3(jnp.sum(zrow[par, 0:8], axis=0, keepdims=True) - lse)
        vsb[par, 0:128] = spread3(idx_b, b_parts)
        vsb[par, 128:256] = spread3(idx_b, l_parts)

    def scatter(i, par, live):
        okt = as_bf16(onehot(n_kt, jnp.where(live, idx[i, 2:3], -1)))
        part = n_kt // 2
        for q in range(2):
            sk[q * part:(q + 1) * part] += dot(okt[q * part:(q + 1) * part], vsb[par], NT)

    def slot_of(i):
        return jnp.where(i < KEEP, i, KEEP + i % 2)

    def scores_of(i, par):
        y8 = ypar[par]
        y_tile = lax.shift_right_logical(y8, 3)
        slot = slot_of(i)
        lz = jnp.zeros((8, ROWS), F32)
        for c in range(n_ch):
            z = dot(wot[c * CHUNK:(c + 1) * CHUNK, :], hpar[par])
            z3 = z.reshape(n_sub, 8, ROWS)
            for k in range(n_sub):
                lz = jnp.where(y_tile == c * n_sub + k, z3[k], lz)
            if c == 0:
                zrow[par, 8:16] = z[0:8, :]
            m_c = jnp.max(z3, axis=0)
            e3 = jnp.exp(z3 - m_c[None])
            ebuf[slot, c * CHUNK:(c + 1) * CHUNK, :] = e3.reshape(CHUNK, ROWS)
            mch[par, c * 8:(c + 1) * 8, :] = m_c
            sch[par, c * 8:(c + 1) * 8, :] = jnp.sum(e3, axis=0)
        zrow[par, 0:8] = jnp.where(sub8 == jnp.bitwise_and(y8, 7), lz, 0.0)

    def fwd_pair(p, carry):
        i = 2 * p
        hidden(i + 1, 1)
        finish(jnp.maximum(i - 1, 0), 1)
        scatter(jnp.maximum(i - 2, 0), 0, i > 1)
        scores_of(i, 0)
        scatter(jnp.maximum(i - 1, 0), 1, i > 0)
        hidden(i + 2, 0)
        finish(i, 0)
        scores_of(i + 1, 1)
        locate(i + 3)
        locate(i + 4)
        return carry

    def fwd_odd(p, carry):
        i = n_blocks - 1
        finish(jnp.maximum(i - 1, 0), 1)
        scatter(jnp.maximum(i - 2, 0), 0, i > 1)
        scores_of(i, 0)
        scatter(jnp.maximum(i - 1, 0), 1, i > 0)
        finish(i, 0)
        scatter(i, 0, True)
        return carry

    def fwd_even(p, carry):
        finish(n_blocks - 1, 1)
        scatter(n_blocks - 2, 0, True)
        scatter(n_blocks - 1, 1, True)
        return carry

    for first in range(3):
        locate(jnp.int32(first))
    hidden(jnp.int32(0), 0)
    lax.fori_loop(0, n_blocks // 2, fwd_pair, 0)
    lax.fori_loop(0, n_blocks % 2, fwd_odd, 0)
    lax.fori_loop(0, 1 - n_blocks % 2, fwd_even, 0)

    tt = lax.broadcasted_iota(jnp.int32, (n_t, 128), 0)
    def own_lanes(ref):
        x = jnp.concatenate([ref[...], jnp.zeros((1, 128 - n_utt), jnp.int32)], axis=1).astype(F32)
        return pltpu.roll(jnp.broadcast_to(x, (n_t, 128)), (128 - u_lo) % 128, 1).astype(jnp.int32)
    t_len = own_lanes(flen_v)
    u_len = own_lanes(llen_v)

    def scores(k):
        lo = k * n_t
        x, y = (v + pltpu.roll(v, 128 - CORE_MAX, 1) + pltpu.roll(v, 128 - 2 * CORE_MAX, 1)
                for v in (sk[lo:lo + n_t, 0:128], sk[lo:lo + n_t, 128:256]))
        uu = k - tt
        ok = (uu >= 0) & (tt < t_len)
        bl_k = jnp.where(ok & (uu <= u_len), x, NEG)
        lb_k = jnp.where(ok & (uu < u_len), y, NEG)
        return bl_k, lb_k

    segu[...] = jnp.zeros_like(segu)
    segt[...] = jnp.zeros_like(segt)
    gwo_ref[...] = jnp.zeros_like(gwo_ref)
    alpha = jnp.where(tt == 0, 0.0, NEG).astype(F32)
    abuf[0] = alpha
    beta = jnp.full((n_t, 128), NEG, F32)
    sc = [scores(k) for k in range(n_diag)]
    for step in range(n_diag):
        if step > 0:
            bl_k, lb_k = sc[step - 1]
            p1 = jnp.where(tt == 0, NEG, pltpu.roll(alpha + bl_k, 1, 0))
            alpha = logadd(p1, alpha + lb_k)
            abuf[step] = alpha
        k = n_diag - 1 - step
        bl_k, lb_k = sc[k]
        up = jnp.where(tt == n_t - 1, jnp.where(u_len == k + 1 - n_t, 0.0, NEG), pltpu.roll(beta, n_t - 1, 0))
        t1 = up + bl_k
        t2 = beta + lb_k
        t1buf[k] = t1
        t2buf[k] = t2
        beta = jnp.where(tt >= t_len, jnp.where(k - tt == u_len, 0.0, NEG), logadd(t1, t2))
    log_p = beta[0:1, :]
    lane = lax.broadcasted_iota(jnp.int32, (n_t, 128), 1)
    loss_ref[...] = pltpu.roll(jnp.where(lane < u_hi - u_lo, -log_p, 0.0), u_lo, 1)
    lane_ok = lane < CORE_MAX
    for k in range(n_diag):
        for which, buf in enumerate((t1buf, t2buf)):
            occ = jnp.where(lane_ok, jnp.exp(jnp.minimum(abuf[k] + buf[k] - log_p, 0.0)), 0.0)
            hi, mid, lo = split3(occ)
            lo_row = which * n_kt + k * n_t
            gocc[lo_row:lo_row + n_t, :] = hi + pltpu.roll(mid, CORE_MAX, 1) + pltpu.roll(lo, 2 * CORE_MAX, 1)
    for which in range(2):
        gocc[which * n_kt + n_diag * n_t:(which + 1) * n_kt, :] = jnp.zeros((n_kt - n_diag * n_t, 128), F32)
    gocb[...] = gocc[...].astype(BF16)

    def again(first, count):
        def one(q, carry):
            i = first + q

            @pl.when(i >= KEEP)
            def _():
                def chunk(c, carry):
                    rows = pl.ds(pl.multiple_of(c * CHUNK, CHUNK), CHUNK)
                    z3 = dot(wot[rows, :], hbuf[i]).reshape(n_sub, 8, ROWS)
                    ebuf[KEEP + i % 2, rows, :] = jnp.exp(z3 - jnp.max(z3, axis=0)[None]).reshape(CHUNK, ROWS)
                    return carry
                lax.fori_loop(0, n_ch, chunk, 0)
            return carry
        lax.fori_loop(0, count, one, 0)

    def occupancy(i, par):
        orep = spread3(idx[i, 3:4], (1.0, 1.0, 1.0))
        kt8 = jnp.broadcast_to(idx[i, 2:3], (8, ROWS))
        kt_tile = lax.shift_right_arithmetic(kt8, 3)
        kt_sub = sub8 == jnp.bitwise_and(kt8, 7)
        for which in range(2):
            gath = dot(gocb[which * n_kt:(which + 1) * n_kt], orep).reshape(n_kt // 8, 8, ROWS)
            occ = jnp.zeros((8, ROWS), F32)
            for k in range(n_diag):
                occ = jnp.where(kt_tile == k, gath[k], occ)
            occ = jnp.sum(jnp.where(kt_sub, occ, 0.0), axis=0, keepdims=True)
            zrow[par, which * 8:which * 8 + 8] = jnp.broadcast_to(occ, (8, ROWS))

    def d_logits(i, par):
        y8 = ybuf[i]
        y_tile = lax.shift_right_logical(y8, 3)
        gb = zrow[par, 0:8]
        gl = zrow[par, 8:16]
        occ = gb + gl
        gl_y = jnp.where(sub8 == jnp.bitwise_and(y8, 7), gl, 0.0)
        gb_0 = jnp.where(sub8 == 0, gb, 0.0)
        slot = slot_of(i)
        for c in range(n_ch):
            sc_c = fac[i, c * 8:(c + 1) * 8, :] * occ
            e3 = ebuf[slot, c * CHUNK:(c + 1) * CHUNK, :].reshape(n_sub, 8, ROWS)
            tiles = []
            for k in range(n_sub):
                d = e3[k] * sc_c
                if c == 0 and k == 0:
                    d = d - gb_0
                tiles.append(d - jnp.where(y_tile == c * n_sub + k, gl_y, 0.0))
            d = jnp.concatenate(tiles, axis=0)
            dzb[par, c * CHUNK:(c + 1) * CHUNK, :] = d.astype(BF16)

    def segments(i, par):
        win = tbl[0, i]
        ohu = as_bf16(onehot(gu, idx[i, 0:1]))
        oht = frame_onehot(idx[i, 1:2])
        for q in range(2):
            rows = slice(q * half, (q + 1) * half)
            segu[rows, lanes_of(win)] += dot(dpb[par, rows], ohu, NT)
            segt[rows, frame_lanes_of(win)] += dot(dpb[par, rows], oht, NT)

    def d_hidden(i, par):
        for q in range(2):
            rows = slice(q * half, (q + 1) * half)
            hf = hbuf[i, rows].astype(F32)
            dh = dot(wo_ref[rows], dzb[par])
            dpb[par, rows] = (dh * (1.0 - hf * hf)).astype(BF16)

    def out_grad(blocks):
        for c in range(n_v // 256):
            cols = slice(c * 256, (c + 1) * 256)
            new = None
            for i, par in blocks:
                term = dot(hbuf[i], dzb[par, cols, :], NT)
                new = term if new is None else new + term
            gwo_ref[:, cols] += new

    def bwd_pair(p, carry):
        i = 2 * p
        again(i + 2, 2)
        d_hidden(i, 0)
        d_hidden(i + 1, 1)
        out_grad(((i, 0), (i + 1, 1)))
        d_logits(i + 2, 0)
        segments(i, 0)
        d_logits(i + 3, 1)
        segments(i + 1, 1)
        occupancy(i + 4, 0)
        occupancy(i + 5, 1)
        return carry

    def bwd_odd(p, carry):
        d_hidden(n_blocks - 1, 0)
        out_grad(((n_blocks - 1, 0),))
        segments(n_blocks - 1, 0)
        return carry

    load_wo.wait()
    again(0, 2)
    for first in range(2):
        occupancy(jnp.int32(first), first)
        d_logits(jnp.int32(first), first)
        occupancy(jnp.int32(first + 2), first)
    lax.fori_loop(0, n_blocks // 2, bwd_pair, 0)
    lax.fori_loop(0, n_blocks % 2, bwd_odd, 0)

    dc_ref[...] = segu[...].astype(BF16)
    da_ref[...] = segt[:, 0:n_utt * n_t].astype(BF16)


def core_call(c_t, a_t, wot, w_out, labels, flen, llen, n_t, n_u):
    n_utt = flen.shape[0]
    n_j = c_t.shape[0]
    n_v = w_out.shape[1]
    n_win = n_utt * 2 // WIN - 1
    max_blk = n_utt // 2 * n_t * n_u // ROWS + 6
    n_kt = (n_t + n_u) * n_t
    n_st = n_v // CHUNK * 8
    vm = pl.BlockSpec(memory_space=pltpu.VMEM)
    sm = pl.BlockSpec(memory_space=pltpu.SMEM)
    return pl.pallas_call(
        functools.partial(core_kernel, n_t, n_u),
        out_shape=(
            pltpu.VMEM((8, 128), F32),
            pltpu.VMEM((n_j, n_utt * n_u), BF16),
            pltpu.VMEM((n_j, n_utt * n_t), BF16),
            pltpu.VMEM(w_out.shape, F32),
        ),
        in_specs=[sm, sm] + [vm] * 6 + [pl.BlockSpec(memory_space=pltpu.HBM)],
        out_specs=(vm,) * 4,
        scratch_shapes=[
            pltpu.VMEM(w_out.shape, BF16),
            pltpu.SemaphoreType.DMA,
            pltpu.VMEM((n_win, 16, WIN * n_u), BF16),
            pltpu.VMEM((max_blk, n_j, ROWS), BF16),
            pltpu.VMEM((2, n_j, ROWS), BF16),
            pltpu.VMEM((min(max_blk, KEEP + 2), n_v, ROWS), F32),
            pltpu.VMEM((max_blk, n_st, ROWS), F32),
            pltpu.VMEM((2, n_st, ROWS), F32),
            pltpu.VMEM((2, n_st, ROWS), F32),
            pltpu.VMEM((2, 256, ROWS), BF16),
            pltpu.VMEM((2, 8, ROWS), jnp.int32),
            pltpu.VMEM((max_blk, 8, ROWS), jnp.int32),
            pltpu.VMEM((max_blk, 8, ROWS), jnp.int32),
            pltpu.VMEM((2, n_v, ROWS), BF16),
            pltpu.VMEM((2, n_j, ROWS), BF16),
            pltpu.VMEM((2, 16, ROWS), F32),
            pltpu.VMEM((n_kt, 256), F32),
            pltpu.VMEM((n_t + n_u, n_t, 128), F32),
            pltpu.VMEM((n_t + n_u, n_t, 128), F32),
            pltpu.VMEM((n_t + n_u, n_t, 128), F32),
            pltpu.VMEM((2 * n_kt, 128), F32),
            pltpu.VMEM((2 * n_kt, 128), BF16),
            pltpu.VMEM((n_j, n_utt * n_u), F32),
            pltpu.VMEM((n_j, n_utt * n_t + 128), F32),
            pltpu.SMEM((3, max_blk), jnp.int32),
            pltpu.SMEM((n_utt + 1,), jnp.int32),
        ],
        compiler_params=pltpu.CompilerParams(vmem_limit_bytes=CORE_VMEM),
        name="rnnt_core",
    )(flen, llen, flen.reshape(1, n_utt), llen.reshape(1, n_utt), labels.T, in_vmem(c_t), in_vmem(a_t), in_vmem(wot), in_hbm(w_out))


def solution(mesh):
    seq_size = mesh.shape['seq']

    def local_fn(enc_out, pred_out, w_enc, w_pred, w_out, labels, frame_len, label_len):
        n_utt, n_loc, n_h = enc_out.shape
        n_u = pred_out.shape[1]
        n_t = n_loc * seq_size
        g2 = pred_out.reshape(n_utt * n_u, n_h)
        c_t, a_t, wot, f2 = gather_call(enc_out, g2, w_enc, w_pred, w_out, seq_size, n_t)
        loss, dc_t, da_t, gwo = core_call(c_t, a_t, wot, w_out, labels, frame_len, label_len, n_t, n_u)
        loss, gf, gwe, gwp, gwo = store_call(reduce_call(gwo, dc_t, da_t, loss, g2, f2, w_enc, enc_out.shape, n_t))
        return loss.reshape(n_utt), gf, gwe, gwp, gwo

    in_specs = (P('dp', 'seq', None), P('dp', None, None), P(None, None), P(None, None), P(None, None), P('dp', None), P('dp'), P('dp'))
    out_specs = (P('dp'), P('dp', 'seq', None), P('dp', None), P('dp', None), P('dp', None))
    return jax.shard_map(local_fn, mesh=mesh, in_specs=in_specs, out_specs=out_specs, check_vma=False)
```

```python
import functools

import jax
import jax.numpy as jnp
from jax import lax
from jax.experimental import pallas as pl
from jax.experimental.pallas import tpu as pltpu
from jax.sharding import PartitionSpec as P

NEG = -1.0e30
ROWS = 256
WIN = 8
CHUNK = 128
CORE_MIN, CORE_MAX = 24, 40
GATHER_VMEM = 40 << 20
CORE_VMEM = 44 << 20
REDUCE_VMEM = 36 << 20
STORE_VMEM = 1 << 20
KEEP = 15
F32 = jnp.float32
BF16 = jnp.bfloat16
MESH = pl.DeviceIdType.MESH
NT = (((1,), (1,)), ((), ()))
NN = (((1,), (0,)), ((), ()))


def dot(a, b, dims=NN):
    return lax.dot_general(a, b, dims, preferred_element_type=F32)


def in_hbm(x):
    return pltpu.with_memory_space_constraint(x, pltpu.HBM)


def in_vmem(x):
    return pltpu.with_memory_space_constraint(x, pltpu.VMEM)


def split3(x):
    hi = x.astype(BF16).astype(F32)
    r1 = x - hi
    mid = r1.astype(BF16).astype(F32)
    return hi, mid, r1 - mid


def logadd(a, b):
    m = jnp.maximum(a, b)
    return m + jnp.log(1.0 + jnp.exp(jnp.minimum(a, b) - m))


def label_rows(n_u, lab_ref, ylab):
    n_utt = lab_ref.shape[1]
    step_u = WIN // 2 * n_u
    gu = WIN * n_u
    n_win = ylab.shape[0]
    lab = lab_ref[...]
    place = jnp.where(lax.broadcasted_iota(jnp.int32, (n_utt, n_utt * n_u), 1) // n_u
                      == lax.broadcasted_iota(jnp.int32, (n_utt, n_utt * n_u), 0), 1.0, 0.0).astype(BF16)
    mine = (lax.broadcasted_iota(jnp.int32, (lab.shape[0], n_utt * n_u), 1) % n_u
            == lax.broadcasted_iota(jnp.int32, (lab.shape[0], n_utt * n_u), 0))
    flat = []
    for part in (lax.shift_right_arithmetic(lab, 5), jnp.bitwise_and(lab, 31)):
        spread = dot(part.astype(F32).astype(BF16), place)
        flat.append(jnp.sum(jnp.where(mine, spread, 0.0), axis=0, keepdims=True))
    for w in range(n_win):
        row = lax.broadcasted_iota(jnp.int32, (16, gu), 0)
        hi, lo = (x[:, w * step_u:w * step_u + gu] for x in flat)
        ylab[w] = jnp.where(row == 0, hi, jnp.where(row == 1, lo, 0.0)).astype(BF16)


def gather_kernel(n_t, n_u, enc_h, g_h, we_h, wp_h, wo_h, lab_ref, c_ref, a_ref, wot_ref, f_ref, ylab, gwo_ref, segu, segt,
                  enc_ref, g_ref, we_ref, wp_ref, wo_ref, fbuf, in_sem, send_sem, recv_sem):
    me = lax.axis_index('seq')
    n_seq = fbuf.shape[0]
    partner = me + 1 - 2 * (me % 2)
    peer = (me + 2) % n_seq
    load_enc, load_wo, load_wp, load_g, load_we = loads = [pltpu.make_async_copy(src, dst, in_sem.at[q]) for q, (src, dst) in enumerate(
        ((enc_h, enc_ref), (wo_h, wo_ref), (wp_h, wp_ref), (g_h, g_ref), (we_h, we_ref)))]
    for load in loads:
        load.start()
    barrier = pltpu.get_barrier_semaphore()
    for other in (partner, peer):
        pl.semaphore_signal(barrier, inc=1, device_id={'seq': other}, device_id_type=MESH)
    pl.semaphore_wait(barrier, 2)

    def send(src, slot, sem, other):
        return pltpu.make_async_remote_copy(src_ref=src, dst_ref=fbuf.at[slot], send_sem=send_sem.at[sem], recv_sem=recv_sem.at[sem],
                                            device_id={'seq': other}, device_id_type=MESH)
    load_enc.wait()
    to_peer = send(enc_ref, me, 0, peer)
    to_peer.start()
    to_partner = send(enc_ref, me, 1, partner)
    to_partner.start()
    fbuf[me] = enc_ref[...]
    load_wo.wait()
    wot_ref[...] = wo_ref[...].T
    load_wp.wait()
    load_g.wait()
    c_ref[...] = dot(wp_ref[...].T, g_ref[...], NT).astype(BF16)
    load_we.wait()
    we_t = we_ref[...].T
    gwo_ref[...] = jnp.zeros_like(gwo_ref)
    segu[...] = jnp.zeros_like(segu)
    segt[...] = jnp.zeros_like(segt)
    label_rows(n_u, lab_ref, ylab)
    n_f, n_h = f_ref.shape
    n_own = n_f // n_seq
    n_loc = n_t // n_seq
    row = lax.broadcasted_iota(jnp.int32, (n_own, n_f), 0)
    col = lax.broadcasted_iota(jnp.int32, (n_own, n_f), 1)

    def piece(p):
        rows = fbuf[p].reshape(n_own, n_h)
        f_ref[pl.ds(pl.multiple_of(p * n_own, n_own), n_own), :] = rows
        order = jnp.where(col == row // n_loc * n_t + p * n_loc + row % n_loc, 1.0, 0.0).astype(BF16)
        return dot(dot(we_t, rows, NT).astype(BF16), order)
    a_t = piece(me)
    to_partner.wait_recv()
    a_t = a_t + piece(partner)
    to_peer.wait_recv()
    relay = send(fbuf.at[peer], peer, 2, partner)
    relay.start()
    a_t = a_t + piece(peer)
    relay.wait_recv()
    a_ref[:, 0:n_f] = (a_t + piece((partner + 2) % n_seq)).astype(BF16)
    a_ref[:, n_f:] = jnp.zeros((a_ref.shape[0], a_ref.shape[1] - n_f), BF16)
    to_peer.wait_send()
    to_partner.wait_send()
    relay.wait_send()


def gather_call(enc, g2, w_enc, w_pred, w_out, labels_t, n_seq, n_t, n_u):
    n_utt, n_loc, n_h = enc.shape
    n_j = w_enc.shape[1]
    vm = pl.BlockSpec(memory_space=pltpu.VMEM)
    n_f = n_utt * n_loc * n_seq
    args = [in_hbm(x) for x in (enc, g2, w_enc, w_pred, w_out)]
    return pl.pallas_call(
        functools.partial(gather_kernel, n_t, n_u),
        out_shape=(
            pltpu.VMEM((n_j, g2.shape[0]), BF16),
            pltpu.VMEM((n_j, n_f + 128), BF16),
            pltpu.VMEM(w_out.shape[::-1], BF16),
            pltpu.VMEM((n_f, n_h), BF16),
            pltpu.VMEM((n_utt * 2 // WIN - 1, 16, WIN * n_u), BF16),
            pltpu.VMEM(w_out.shape, F32),
            pltpu.VMEM((n_j, g2.shape[0]), F32),
            pltpu.VMEM((n_j, n_f + 128), F32),
        ),
        in_specs=[pl.BlockSpec(memory_space=pltpu.HBM)] * 5 + [vm],
        out_specs=(vm,) * 8,
        scratch_shapes=[pltpu.VMEM(x.shape, x.dtype) for x in (enc, g2, w_enc, w_pred, w_out)] + [
            pltpu.VMEM((n_seq, n_utt, n_loc, n_h), BF16),
            pltpu.SemaphoreType.DMA((5,)),
            pltpu.SemaphoreType.DMA((3,)),
            pltpu.SemaphoreType.DMA((3,)),
        ],
        compiler_params=pltpu.CompilerParams(collective_id=0, has_side_effects=True, vmem_limit_bytes=GATHER_VMEM),
        name="rnnt_gather",
    )(*args, labels_t)


def reduce_kernel(n_t, gwo_v, dc_v, da_v, loss_v, f_v, g_p, we_p, loss_ref, gf_ref, gwe_ref, gwp_ref, gwo_ref,
                  g_v, we_v, gwp_v, rgwo, rgwp, rda, rloss, da_rows, in_sem, send_sem, recv_sem):
    me = lax.axis_index('seq')
    partner = me + 1 - 2 * (me % 2)
    loads = [pltpu.make_async_copy(src, dst, in_sem.at[q]) for q, (src, dst) in enumerate(((g_p, g_v), (we_p, we_v)))]
    for load in loads:
        load.start()
    barrier = pltpu.get_barrier_semaphore()
    pl.semaphore_signal(barrier, inc=1, device_id={'seq': partner}, device_id_type=MESH)
    pl.semaphore_wait(barrier, 1)

    def send(src, dst, sem):
        return pltpu.make_async_remote_copy(src_ref=src, dst_ref=dst, send_sem=send_sem.at[sem], recv_sem=recv_sem.at[sem],
                                            device_id={'seq': partner}, device_id_type=MESH)
    n_part = 4
    rows = gwo_v.shape[0] // n_part
    sends = [send(da_v, rda, 0), send(loss_v, rloss, 1)]
    sends += [send(gwo_v.at[pl.ds(q * rows, rows)], rgwo.at[pl.ds(q * rows, rows)], 2 + q) for q in range(n_part)]
    for s in sends:
        s.start()
    loads[0].wait()
    gwp_v[...] = dot(g_v[...].T, dc_v[...], NT)
    s_gwp = send(gwp_v, rgwp, 2 + n_part)
    loads[1].wait()
    sends[0].wait_recv()
    sends[1].wait_recv()
    loss_ref[...] = (loss_v[0:1, :] + rloss[0:1, :])[:, 0:loss_ref.shape[1]]
    da = (da_v[...].astype(F32) + rda[...].astype(F32)).astype(BF16)
    s_gwp.start()
    n_f = da.shape[1]
    n_loc = gf_ref.shape[1]
    n_own = gf_ref.shape[0] * n_loc
    row = lax.broadcasted_iota(jnp.int32, (n_f, n_f), 0)
    col = lax.broadcasted_iota(jnp.int32, (n_f, n_f), 1)
    order = jnp.where(col == row % n_own // n_loc * n_t + row // n_own * n_loc + row % n_loc, 1.0, 0.0).astype(BF16)
    da_f = dot(order, da, NT).astype(BF16)
    da_rows[...] = da_f
    gwe_ref[...] = dot(f_v[...].T, da_f)
    own = da_rows[pl.ds(pl.multiple_of(me * n_own, n_own), n_own), :]
    gf_ref[...] = dot(own, we_v[...], NT).astype(BF16).reshape(gf_ref.shape)
    for q in range(n_part):
        sends[2 + q].wait_recv()
        part = slice(q * rows, (q + 1) * rows)
        gwo_ref[part] = gwo_v[part] + rgwo[part]
    s_gwp.wait_recv()
    gwp_ref[...] = gwp_v[...] + rgwp[...]
    for s in sends + [s_gwp]:
        s.wait_send()


def reduce_call(gwo, dc_t, da_t, loss, g2, f2, w_enc, gf_shape, n_t):
    vm = pl.BlockSpec(memory_space=pltpu.VMEM)
    like = lambda x: pltpu.VMEM(x.shape, x.dtype)
    gwp_shape = (g2.shape[1], dc_t.shape[0])
    return pl.pallas_call(
        functools.partial(reduce_kernel, n_t),
        out_shape=(
            pltpu.VMEM((1, f2.shape[0] // n_t), F32),
            pltpu.VMEM(gf_shape, BF16),
            pltpu.VMEM(w_enc.shape, F32),
            pltpu.VMEM(gwp_shape, F32),
            pltpu.VMEM(gwo.shape, F32),
        ),
        in_specs=[vm] * 5 + [pl.BlockSpec(memory_space=pltpu.HBM)] * 2,
        out_specs=(vm,) * 5,
        scratch_shapes=[like(x) for x in (g2, w_enc)] + [
            pltpu.VMEM(gwp_shape, F32), like(gwo), pltpu.VMEM(gwp_shape, F32), like(da_t), like(loss), pltpu.VMEM(da_t.shape[::-1], BF16),
            pltpu.SemaphoreType.DMA((2,)),
            pltpu.SemaphoreType.DMA((7,)),
            pltpu.SemaphoreType.DMA((7,)),
        ],
        compiler_params=pltpu.CompilerParams(collective_id=1, has_side_effects=True, vmem_limit_bytes=REDUCE_VMEM),
        name="rnnt_reduce",
    )(in_vmem(gwo), in_vmem(dc_t), in_vmem(da_t), in_vmem(loss), in_vmem(f2), in_hbm(g2), in_hbm(w_enc))


def store_kernel(n, *refs):
    sems = refs[2 * n]
    copies = [pltpu.make_async_copy(refs[q], refs[n + q], sems.at[q]) for q in range(n)]
    for copy in copies:
        copy.start()
    for copy in copies:
        copy.wait()


def store_call(arrays):
    n = len(arrays)
    return pl.pallas_call(
        functools.partial(store_kernel, n),
        out_shape=tuple(pltpu.HBM(x.shape, x.dtype) for x in arrays),
        in_specs=[pl.BlockSpec(memory_space=pltpu.VMEM)] * n,
        out_specs=(pl.BlockSpec(memory_space=pltpu.HBM),) * n,
        scratch_shapes=[pltpu.SemaphoreType.DMA((n,))],
        compiler_params=pltpu.CompilerParams(vmem_limit_bytes=STORE_VMEM),
        name="rnnt_store",
    )(*[in_vmem(x) for x in arrays])


def core_kernel(n_t, n_u, flen_s, llen_s, flen_v, llen_v, ylab, c_buf, a_buf, wot, gwo_0, segu_0, segt_0, wo_h,
                loss_ref, dc_ref, da_ref, gwo_ref, segu, segt,
                wo_ref, wo_sem, hbuf, hpar, ebuf, fac, mch, sch, vsb, ypar, ybuf, idx, dzb, dpb, zrow, sk, abuf, t1buf, t2buf,
                gocc, gocb, tbl, off):
    n_utt = flen_s.shape[0]
    n_j = c_buf.shape[0]
    n_v = wo_ref.shape[1]
    step_u = WIN // 2 * n_u
    step_t = WIN // 2 * n_t
    per_tile = 128 // step_t
    gu = WIN * n_u
    n_win = n_utt * 2 // WIN - 1
    n_diag = n_t + n_u - 1
    n_kt = (n_diag + 1) * n_t
    n_ch = n_v // CHUNK

    load_wo = pltpu.make_async_copy(wo_h, wo_ref, wo_sem)
    load_wo.start()

    def off_step(b, total):
        off[b] = total
        return total + flen_s[b] * (llen_s[b] + 1)
    off[n_utt] = lax.fori_loop(0, n_utt, off_step, jnp.int32(0))

    total = off[n_utt]
    cut = lax.fori_loop(CORE_MIN, CORE_MAX, lambda b, n: n + jnp.where(off[b] + off[b + 1] <= total, 1, 0), jnp.int32(CORE_MIN))
    first_core = lax.axis_index('seq') % 2 == 0
    u_lo = jnp.where(first_core, 0, cut)
    u_hi = jnp.where(first_core, cut, n_utt)
    stop = off[u_hi]

    def utt_step(b, carry):
        win = jnp.minimum(b // (WIN // 2), n_win - 1)
        base = off[win * (WIN // 2)]
        last = jnp.minimum(off[win * (WIN // 2) + WIN], stop)

        def emit(c):
            n, pos = c
            end = jnp.minimum(pos + ROWS, last)
            tbl[0, n] = win
            tbl[1, n] = pos - base
            tbl[2, n] = end - base
            return n + 1, end
        return lax.while_loop(lambda c: c[1] < off[b + 1], emit, carry)
    n_blocks, _ = lax.fori_loop(u_lo, u_hi, utt_step, (jnp.int32(0), off[u_lo]))
    for past in range(3):
        for q in range(3):
            tbl[q, n_blocks + past] = 0

    sk[...] = jnp.zeros_like(sk)
    mch[...] = jnp.zeros_like(mch)
    sch[...] = jnp.ones_like(sch)
    zrow[...] = jnp.zeros_like(zrow)
    vsb[...] = jnp.zeros_like(vsb)
    dpb[...] = jnp.zeros_like(dpb)

    def onehot(n, index_row):
        return (lax.broadcasted_iota(jnp.int32, (n, ROWS), 0) == index_row)

    def as_bf16(mask):
        return jnp.where(mask, 1.0, 0.0).astype(BF16)

    def frame_onehot(index_row):
        n = WIN * n_t + 128 - step_t
        return jnp.concatenate([as_bf16(onehot(n, index_row)), jnp.zeros((256 - n, ROWS), BF16)], axis=0)

    sub8 = lax.broadcasted_iota(jnp.int32, (8, ROWS), 0)
    n_sub = CHUNK // 8

    def lanes_of(win):
        return pl.ds(pl.multiple_of(win * step_u, 128), gu)

    def frame_lanes_of(win):
        return pl.ds(pl.multiple_of(win // per_tile * 128, 128), 256)

    def spread3(idx_b, parts):
        mask = lax.broadcasted_iota(jnp.int32, (CORE_MAX, ROWS), 0) == idx_b
        return jnp.concatenate([jnp.where(mask, part, 0.0) for part in parts]
                               + [jnp.zeros((128 - 3 * CORE_MAX, ROWS), F32)], axis=0).astype(BF16)

    def locate(i):
        win = tbl[0, i]
        r = tbl[1, i] + lax.broadcasted_iota(jnp.int32, (1, ROWS), 1)
        end_r = tbl[2, i]
        start = jnp.int32(0)
        bl = jnp.full((1, ROWS), -1, jnp.int32)
        w = jnp.zeros((1, ROWS), jnp.int32)
        u1 = jnp.ones((1, ROWS), jnp.int32)
        for j in range(WIN):
            u1_j = llen_s[win * (WIN // 2) + j] + 1
            end = start + flen_s[win * (WIN // 2) + j] * u1_j
            inside = (r >= start) & (r < jnp.minimum(end, end_r))
            bl = jnp.where(inside, j, bl)
            w = jnp.where(inside, r - start, w)
            u1 = jnp.where(inside, u1_j, u1)
            start = end
        valid = bl >= 0
        t = jnp.zeros((1, ROWS), jnp.int32)
        for j in range(1, n_t):
            t = t + jnp.where(w >= j * u1, 1, 0)
        u = w - t * u1
        idx_u = jnp.where(valid, bl * n_u + u, -1)
        idx_t = jnp.where(valid, bl * n_t + t + win % per_tile * step_t, -1)
        idx_kt = jnp.where(valid, (t + u) * n_t + t, -1)
        idx_b = jnp.where(valid, win * (WIN // 2) + bl - u_lo, -1024)
        rows8 = lax.broadcasted_iota(jnp.int32, (8, ROWS), 0)
        idx[i] = jnp.where(rows8 == 0, idx_u, jnp.where(rows8 == 1, idx_t, jnp.where(rows8 == 2, idx_kt, idx_b)))

    half = n_j // 2

    def hidden(i, par):
        win = tbl[0, i]
        ohu = as_bf16(onehot(gu, idx[i, 0:1]))
        oht = frame_onehot(idx[i, 1:2])
        for q in range(2):
            rows = slice(q * half, (q + 1) * half)
            pre = dot(c_buf[rows, lanes_of(win)], ohu) + dot(a_buf[rows, frame_lanes_of(win)], oht)
            h = jnp.tanh(pre).astype(BF16)
            hpar[par, rows] = h
            hbuf[i, rows] = h
        yy = dot(ylab[win], ohu)
        y8 = jnp.broadcast_to((yy[0:1] * 32.0 + yy[1:2]).astype(jnp.int32), (8, ROWS))
        ypar[par] = y8
        ybuf[i] = y8

    def finish(i, par):
        idx_b = idx[i, 3:4]
        m_all = mch[par]
        m8 = jnp.max(m_all.reshape(n_ch, 8, ROWS), axis=0)
        m = jnp.max(m8, axis=0, keepdims=True)
        f_all = jnp.exp(m_all - m)
        s = jnp.sum(jnp.sum((sch[par] * f_all).reshape(n_ch, 8, ROWS), axis=0), axis=0, keepdims=True)
        fac[i] = f_all * (1.0 / s)
        lse = m + jnp.log(s)
        b_parts = split3(zrow[par, 8:9] - lse)
        l_parts = split3(jnp.sum(zrow[par, 0:8], axis=0, keepdims=True) - lse)
        vsb[par, 0:128] = spread3(idx_b, b_parts)
        vsb[par, 128:256] = spread3(idx_b, l_parts)

    def scatter(i, par, live):
        okt = as_bf16(onehot(n_kt, jnp.where(live, idx[i, 2:3], -1)))
        part = n_kt // 2
        for q in range(2):
            sk[q * part:(q + 1) * part] += dot(okt[q * part:(q + 1) * part], vsb[par], NT)

    def slot_of(i):
        return jnp.where(i < KEEP, i, KEEP + i % 2)

    def scores_of(i, par):
        y8 = ypar[par]
        y_tile = lax.shift_right_logical(y8, 3)
        slot = slot_of(i)
        lz = jnp.zeros((8, ROWS), F32)
        for c in range(n_ch):
            z = dot(wot[c * CHUNK:(c + 1) * CHUNK, :], hpar[par])
            z3 = z.reshape(n_sub, 8, ROWS)
            for k in range(n_sub):
                lz = jnp.where(y_tile == c * n_sub + k, z3[k], lz)
            if c == 0:
                zrow[par, 8:16] = z[0:8, :]
            m_c = jnp.max(z3, axis=0)
            e3 = jnp.exp(z3 - m_c[None])
            ebuf[slot, c * CHUNK:(c + 1) * CHUNK, :] = e3.reshape(CHUNK, ROWS)
            mch[par, c * 8:(c + 1) * 8, :] = m_c
            sch[par, c * 8:(c + 1) * 8, :] = jnp.sum(e3, axis=0)
        zrow[par, 0:8] = jnp.where(sub8 == jnp.bitwise_and(y8, 7), lz, 0.0)

    def fwd_pair(p, carry):
        i = 2 * p
        hidden(i + 1, 1)
        finish(jnp.maximum(i - 1, 0), 1)
        scatter(jnp.maximum(i - 2, 0), 0, i > 1)
        scores_of(i, 0)
        scatter(jnp.maximum(i - 1, 0), 1, i > 0)
        hidden(i + 2, 0)
        finish(i, 0)
        scores_of(i + 1, 1)
        locate(i + 3)
        locate(i + 4)
        return carry

    def fwd_odd(p, carry):
        i = n_blocks - 1
        finish(jnp.maximum(i - 1, 0), 1)
        scatter(jnp.maximum(i - 2, 0), 0, i > 1)
        scores_of(i, 0)
        scatter(jnp.maximum(i - 1, 0), 1, i > 0)
        finish(i, 0)
        scatter(i, 0, True)
        return carry

    def fwd_even(p, carry):
        finish(n_blocks - 1, 1)
        scatter(n_blocks - 2, 0, True)
        scatter(n_blocks - 1, 1, True)
        return carry

    for first in range(3):
        locate(jnp.int32(first))
    hidden(jnp.int32(0), 0)
    lax.fori_loop(0, n_blocks // 2, fwd_pair, 0)
    lax.fori_loop(0, n_blocks % 2, fwd_odd, 0)
    lax.fori_loop(0, 1 - n_blocks % 2, fwd_even, 0)

    tt = lax.broadcasted_iota(jnp.int32, (n_t, 128), 0)
    def own_lanes(ref):
        x = jnp.concatenate([ref[...], jnp.zeros((1, 128 - n_utt), jnp.int32)], axis=1).astype(F32)
        return pltpu.roll(jnp.broadcast_to(x, (n_t, 128)), (128 - u_lo) % 128, 1).astype(jnp.int32)
    t_len = own_lanes(flen_v)
    u_len = own_lanes(llen_v)

    def scores(k):
        lo = k * n_t
        x, y = (v + pltpu.roll(v, 128 - CORE_MAX, 1) + pltpu.roll(v, 128 - 2 * CORE_MAX, 1)
                for v in (sk[lo:lo + n_t, 0:128], sk[lo:lo + n_t, 128:256]))
        uu = k - tt
        ok = (uu >= 0) & (tt < t_len)
        bl_k = jnp.where(ok & (uu <= u_len), x, NEG)
        lb_k = jnp.where(ok & (uu < u_len), y, NEG)
        return bl_k, lb_k

    alpha = jnp.where(tt == 0, 0.0, NEG).astype(F32)
    abuf[0] = alpha
    beta = jnp.full((n_t, 128), NEG, F32)
    sc = [scores(k) for k in range(n_diag)]
    for step in range(n_diag):
        if step > 0:
            bl_k, lb_k = sc[step - 1]
            p1 = jnp.where(tt == 0, NEG, pltpu.roll(alpha + bl_k, 1, 0))
            alpha = logadd(p1, alpha + lb_k)
            abuf[step] = alpha
        k = n_diag - 1 - step
        bl_k, lb_k = sc[k]
        up = jnp.where(tt == n_t - 1, jnp.where(u_len == k + 1 - n_t, 0.0, NEG), pltpu.roll(beta, n_t - 1, 0))
        t1 = up + bl_k
        t2 = beta + lb_k
        t1buf[k] = t1
        t2buf[k] = t2
        beta = jnp.where(tt >= t_len, jnp.where(k - tt == u_len, 0.0, NEG), logadd(t1, t2))
    log_p = beta[0:1, :]
    lane = lax.broadcasted_iota(jnp.int32, (n_t, 128), 1)
    loss_ref[...] = pltpu.roll(jnp.where(lane < u_hi - u_lo, -log_p, 0.0), u_lo, 1)
    lane_ok = lane < CORE_MAX
    for k in range(n_diag):
        for which, buf in enumerate((t1buf, t2buf)):
            occ = jnp.where(lane_ok, jnp.exp(jnp.minimum(abuf[k] + buf[k] - log_p, 0.0)), 0.0)
            hi, mid, lo = split3(occ)
            lo_row = which * n_kt + k * n_t
            gocc[lo_row:lo_row + n_t, :] = hi + pltpu.roll(mid, CORE_MAX, 1) + pltpu.roll(lo, 2 * CORE_MAX, 1)
    for which in range(2):
        gocc[which * n_kt + n_diag * n_t:(which + 1) * n_kt, :] = jnp.zeros((n_kt - n_diag * n_t, 128), F32)
    gocb[...] = gocc[...].astype(BF16)

    def again(first, count):
        def one(q, carry):
            i = first + q

            @pl.when(i >= KEEP)
            def _():
                def chunk(c, carry):
                    rows = pl.ds(pl.multiple_of(c * CHUNK, CHUNK), CHUNK)
                    z3 = dot(wot[rows, :], hbuf[i]).reshape(n_sub, 8, ROWS)
                    ebuf[KEEP + i % 2, rows, :] = jnp.exp(z3 - jnp.max(z3, axis=0)[None]).reshape(CHUNK, ROWS)
                    return carry
                lax.fori_loop(0, n_ch, chunk, 0)
            return carry
        lax.fori_loop(0, count, one, 0)

    def occupancy(i, par):
        orep = spread3(idx[i, 3:4], (1.0, 1.0, 1.0))
        kt8 = jnp.broadcast_to(idx[i, 2:3], (8, ROWS))
        kt_tile = lax.shift_right_arithmetic(kt8, 3)
        kt_sub = sub8 == jnp.bitwise_and(kt8, 7)
        for which in range(2):
            gath = dot(gocb[which * n_kt:(which + 1) * n_kt], orep).reshape(n_kt // 8, 8, ROWS)
            occ = jnp.zeros((8, ROWS), F32)
            for k in range(n_diag):
                occ = jnp.where(kt_tile == k, gath[k], occ)
            occ = jnp.sum(jnp.where(kt_sub, occ, 0.0), axis=0, keepdims=True)
            zrow[par, which * 8:which * 8 + 8] = jnp.broadcast_to(occ, (8, ROWS))

    def d_logits(i, par):
        y8 = ybuf[i]
        y_tile = lax.shift_right_logical(y8, 3)
        gb = zrow[par, 0:8]
        gl = zrow[par, 8:16]
        occ = gb + gl
        gl_y = jnp.where(sub8 == jnp.bitwise_and(y8, 7), gl, 0.0)
        gb_0 = jnp.where(sub8 == 0, gb, 0.0)
        slot = slot_of(i)
        for c in range(n_ch):
            sc_c = fac[i, c * 8:(c + 1) * 8, :] * occ
            e3 = ebuf[slot, c * CHUNK:(c + 1) * CHUNK, :].reshape(n_sub, 8, ROWS)
            tiles = []
            for k in range(n_sub):
                d = e3[k] * sc_c
                if c == 0 and k == 0:
                    d = d - gb_0
                tiles.append(d - jnp.where(y_tile == c * n_sub + k, gl_y, 0.0))
            d = jnp.concatenate(tiles, axis=0)
            dzb[par, c * CHUNK:(c + 1) * CHUNK, :] = d.astype(BF16)

    def segments(i, par):
        win = tbl[0, i]
        ohu = as_bf16(onehot(gu, idx[i, 0:1]))
        oht = frame_onehot(idx[i, 1:2])
        for q in range(2):
            rows = slice(q * half, (q + 1) * half)
            segu[rows, lanes_of(win)] += dot(dpb[par, rows], ohu, NT)
            segt[rows, frame_lanes_of(win)] += dot(dpb[par, rows], oht, NT)

    def d_hidden(i, par):
        for q in range(2):
            rows = slice(q * half, (q + 1) * half)
            hf = hbuf[i, rows].astype(F32)
            dh = dot(wo_ref[rows], dzb[par])
            dpb[par, rows] = (dh * (1.0 - hf * hf)).astype(BF16)

    def out_grad(blocks):
        for c in range(n_v // 256):
            cols = slice(c * 256, (c + 1) * 256)
            new = None
            for i, par in blocks:
                term = dot(hbuf[i], dzb[par, cols, :], NT)
                new = term if new is None else new + term
            gwo_ref[:, cols] += new

    def bwd_pair(p, carry):
        i = 2 * p
        again(i + 2, 2)
        d_hidden(i, 0)
        d_hidden(i + 1, 1)
        out_grad(((i, 0), (i + 1, 1)))
        d_logits(i + 2, 0)
        segments(i, 0)
        d_logits(i + 3, 1)
        segments(i + 1, 1)
        occupancy(i + 4, 0)
        occupancy(i + 5, 1)
        return carry

    def bwd_odd(p, carry):
        d_hidden(n_blocks - 1, 0)
        out_grad(((n_blocks - 1, 0),))
        segments(n_blocks - 1, 0)
        return carry

    load_wo.wait()
    again(0, 2)
    for first in range(2):
        occupancy(jnp.int32(first), first)
        d_logits(jnp.int32(first), first)
        occupancy(jnp.int32(first + 2), first)
    lax.fori_loop(0, n_blocks // 2, bwd_pair, 0)
    lax.fori_loop(0, n_blocks % 2, bwd_odd, 0)

    dc_ref[...] = segu[...].astype(BF16)
    da_ref[...] = segt[:, 0:n_utt * n_t].astype(BF16)


def core_call(c_t, a_t, wot, ylab, gwo_0, segu_0, segt_0, w_out, flen, llen, n_t, n_u):
    n_utt = flen.shape[0]
    n_j = c_t.shape[0]
    n_v = w_out.shape[1]
    max_blk = n_utt // 2 * n_t * n_u // ROWS + 6
    n_kt = (n_t + n_u) * n_t
    n_st = n_v // CHUNK * 8
    vm = pl.BlockSpec(memory_space=pltpu.VMEM)
    sm = pl.BlockSpec(memory_space=pltpu.SMEM)
    return pl.pallas_call(
        functools.partial(core_kernel, n_t, n_u),
        out_shape=(
            pltpu.VMEM((8, 128), F32),
            pltpu.VMEM((n_j, n_utt * n_u), BF16),
            pltpu.VMEM((n_j, n_utt * n_t), BF16),
            pltpu.VMEM(w_out.shape, F32),
            pltpu.VMEM(segu_0.shape, F32),
            pltpu.VMEM(segt_0.shape, F32),
        ),
        in_specs=[sm, sm] + [vm] * 9 + [pl.BlockSpec(memory_space=pltpu.HBM)],
        out_specs=(vm,) * 6,
        input_output_aliases={8: 3, 9: 4, 10: 5},
        scratch_shapes=[
            pltpu.VMEM(w_out.shape, BF16),
            pltpu.SemaphoreType.DMA,
            pltpu.VMEM((max_blk, n_j, ROWS), BF16),
            pltpu.VMEM((2, n_j, ROWS), BF16),
            pltpu.VMEM((min(max_blk, KEEP + 2), n_v, ROWS), F32),
            pltpu.VMEM((max_blk, n_st, ROWS), F32),
            pltpu.VMEM((2, n_st, ROWS), F32),
            pltpu.VMEM((2, n_st, ROWS), F32),
            pltpu.VMEM((2, 256, ROWS), BF16),
            pltpu.VMEM((2, 8, ROWS), jnp.int32),
            pltpu.VMEM((max_blk, 8, ROWS), jnp.int32),
            pltpu.VMEM((max_blk, 8, ROWS), jnp.int32),
            pltpu.VMEM((2, n_v, ROWS), BF16),
            pltpu.VMEM((2, n_j, ROWS), BF16),
            pltpu.VMEM((2, 16, ROWS), F32),
            pltpu.VMEM((n_kt, 256), F32),
            pltpu.VMEM((n_t + n_u, n_t, 128), F32),
            pltpu.VMEM((n_t + n_u, n_t, 128), F32),
            pltpu.VMEM((n_t + n_u, n_t, 128), F32),
            pltpu.VMEM((2 * n_kt, 128), F32),
            pltpu.VMEM((2 * n_kt, 128), BF16),
            pltpu.SMEM((3, max_blk), jnp.int32),
            pltpu.SMEM((n_utt + 1,), jnp.int32),
        ],
        compiler_params=pltpu.CompilerParams(vmem_limit_bytes=CORE_VMEM),
        name="rnnt_core",
    )(flen, llen, flen.reshape(1, n_utt), llen.reshape(1, n_utt), *[in_vmem(x) for x in (ylab, c_t, a_t, wot, gwo_0, segu_0, segt_0)], in_hbm(w_out))


def solution(mesh):
    seq_size = mesh.shape['seq']

    def local_fn(enc_out, pred_out, w_enc, w_pred, w_out, labels, frame_len, label_len):
        n_utt, n_loc, n_h = enc_out.shape
        n_u = pred_out.shape[1]
        n_t = n_loc * seq_size
        g2 = pred_out.reshape(n_utt * n_u, n_h)
        c_t, a_t, wot, f2, *rest = gather_call(enc_out, g2, w_enc, w_pred, w_out, labels.T, seq_size, n_t, n_u)
        loss, dc_t, da_t, gwo, _, _ = core_call(c_t, a_t, wot, *rest, w_out, frame_len, label_len, n_t, n_u)
        loss, gf, gwe, gwp, gwo = store_call(reduce_call(gwo, dc_t, da_t, loss, g2, f2, w_enc, enc_out.shape, n_t))
        return loss.reshape(n_utt), gf, gwe, gwp, gwo

    in_specs = (P('dp', 'seq', None), P('dp', None, None), P(None, None), P(None, None), P(None, None), P('dp', None), P('dp'), P('dp'))
    out_specs = (P('dp'), P('dp', 'seq', None), P('dp', None), P('dp', None), P('dp', None))
    return jax.shard_map(local_fn, mesh=mesh, in_specs=in_specs, out_specs=out_specs, check_vma=False)
```

```python
import functools

import jax
import jax.numpy as jnp
from jax import lax
from jax.experimental import pallas as pl
from jax.experimental.pallas import tpu as pltpu
from jax.sharding import PartitionSpec as P

NEG = -1.0e30
ROWS = 256
WIN = 8
CHUNK = 128
CORE_MIN, CORE_MAX = 24, 40
GATHER_VMEM = 40 << 20
CORE_VMEM = 51 << 20
REDUCE_VMEM = 36 << 20
STORE_VMEM = 1 << 20
KEEP = 15
F32 = jnp.float32
BF16 = jnp.bfloat16
MESH = pl.DeviceIdType.MESH
NT = (((1,), (1,)), ((), ()))
NN = (((1,), (0,)), ((), ()))


def dot(a, b, dims=NN):
    return lax.dot_general(a, b, dims, preferred_element_type=F32)


def in_hbm(x):
    return pltpu.with_memory_space_constraint(x, pltpu.HBM)


def in_vmem(x):
    return pltpu.with_memory_space_constraint(x, pltpu.VMEM)


def split3(x):
    hi = x.astype(BF16).astype(F32)
    r1 = x - hi
    mid = r1.astype(BF16).astype(F32)
    return hi, mid, r1 - mid


def logadd(a, b):
    m = jnp.maximum(a, b)
    return m + jnp.log(1.0 + jnp.exp(jnp.minimum(a, b) - m))


def label_rows(n_u, lab_ref, ylab):
    n_utt = lab_ref.shape[1]
    step_u = WIN // 2 * n_u
    gu = WIN * n_u
    n_win = ylab.shape[0]
    lab = lab_ref[...]
    place = jnp.where(lax.broadcasted_iota(jnp.int32, (n_utt, n_utt * n_u), 1) // n_u
                      == lax.broadcasted_iota(jnp.int32, (n_utt, n_utt * n_u), 0), 1.0, 0.0).astype(BF16)
    mine = (lax.broadcasted_iota(jnp.int32, (lab.shape[0], n_utt * n_u), 1) % n_u
            == lax.broadcasted_iota(jnp.int32, (lab.shape[0], n_utt * n_u), 0))
    flat = []
    for part in (lax.shift_right_arithmetic(lab, 5), jnp.bitwise_and(lab, 31)):
        spread = dot(part.astype(F32).astype(BF16), place)
        flat.append(jnp.sum(jnp.where(mine, spread, 0.0), axis=0, keepdims=True))
    for w in range(n_win):
        row = lax.broadcasted_iota(jnp.int32, (16, gu), 0)
        hi, lo = (x[:, w * step_u:w * step_u + gu] for x in flat)
        ylab[w] = jnp.where(row == 0, hi, jnp.where(row == 1, lo, 0.0)).astype(BF16)


def gather_kernel(n_t, n_u, enc_h, g_h, we_h, wp_h, wo_h, lab_ref, c_ref, a_ref, wot_ref, f_ref, ylab,
                  enc_ref, g_ref, we_ref, wp_ref, wo_ref, fbuf, in_sem, send_sem, recv_sem):
    me = lax.axis_index('seq')
    n_seq = fbuf.shape[0]
    partner = me + 1 - 2 * (me % 2)
    peer = (me + 2) % n_seq
    load_enc, load_wo, load_wp, load_g, load_we = loads = [pltpu.make_async_copy(src, dst, in_sem.at[q]) for q, (src, dst) in enumerate(
        ((enc_h, enc_ref), (wo_h, wo_ref), (wp_h, wp_ref), (g_h, g_ref), (we_h, we_ref)))]
    for load in loads:
        load.start()
    barrier = pltpu.get_barrier_semaphore()
    for other in (partner, peer):
        pl.semaphore_signal(barrier, inc=1, device_id={'seq': other}, device_id_type=MESH)
    pl.semaphore_wait(barrier, 2)

    def send(src, slot, sem, other):
        return pltpu.make_async_remote_copy(src_ref=src, dst_ref=fbuf.at[slot], send_sem=send_sem.at[sem], recv_sem=recv_sem.at[sem],
                                            device_id={'seq': other}, device_id_type=MESH)
    load_enc.wait()
    to_peer = send(enc_ref, me, 0, peer)
    to_peer.start()
    to_partner = send(enc_ref, me, 1, partner)
    to_partner.start()
    fbuf[me] = enc_ref[...]
    load_wo.wait()
    wot_ref[...] = wo_ref[...].T
    load_wp.wait()
    load_g.wait()
    n_c = (CORE_MAX + WIN // 2) * n_u
    cols = pl.ds(pl.multiple_of(me % 2 * (c_ref.shape[1] - n_c), 128), n_c)
    c_ref[:, cols] = dot(wp_ref[...].T, g_ref[cols, :], NT).astype(BF16)
    load_we.wait()
    we_t = we_ref[...].T
    label_rows(n_u, lab_ref, ylab)
    n_f, n_h = f_ref.shape
    n_own = n_f // n_seq
    n_loc = n_t // n_seq
    row = lax.broadcasted_iota(jnp.int32, (n_own, n_f), 0)
    col = lax.broadcasted_iota(jnp.int32, (n_own, n_f), 1)

    def piece(p):
        rows = fbuf[p].reshape(n_own, n_h)
        f_ref[pl.ds(pl.multiple_of(p * n_own, n_own), n_own), :] = rows
        order = jnp.where(col == row // n_loc * n_t + p * n_loc + row % n_loc, 1.0, 0.0).astype(BF16)
        return dot(dot(we_t, rows, NT).astype(BF16), order)
    a_t = piece(me)
    to_partner.wait_recv()
    a_t = a_t + piece(partner)
    to_peer.wait_recv()
    relay = send(fbuf.at[peer], peer, 2, partner)
    relay.start()
    a_t = a_t + piece(peer)
    relay.wait_recv()
    a_ref[:, 0:n_f] = (a_t + piece((partner + 2) % n_seq)).astype(BF16)
    a_ref[:, n_f:] = jnp.zeros((a_ref.shape[0], a_ref.shape[1] - n_f), BF16)
    to_peer.wait_send()
    to_partner.wait_send()
    relay.wait_send()


def gather_call(enc, g2, w_enc, w_pred, w_out, labels_t, n_seq, n_t, n_u):
    n_utt, n_loc, n_h = enc.shape
    n_j = w_enc.shape[1]
    vm = pl.BlockSpec(memory_space=pltpu.VMEM)
    n_f = n_utt * n_loc * n_seq
    args = [in_hbm(x) for x in (enc, g2, w_enc, w_pred, w_out)]
    return pl.pallas_call(
        functools.partial(gather_kernel, n_t, n_u),
        out_shape=(
            pltpu.VMEM((n_j, g2.shape[0]), BF16),
            pltpu.VMEM((n_j, n_f + 128), BF16),
            pltpu.VMEM(w_out.shape[::-1], BF16),
            pltpu.VMEM((n_f, n_h), BF16),
            pltpu.VMEM((n_utt * 2 // WIN - 1, 16, WIN * n_u), BF16),
        ),
        in_specs=[pl.BlockSpec(memory_space=pltpu.HBM)] * 5 + [vm],
        out_specs=(vm,) * 5,
        scratch_shapes=[pltpu.VMEM(x.shape, x.dtype) for x in (enc, g2, w_enc, w_pred, w_out)] + [
            pltpu.VMEM((n_seq, n_utt, n_loc, n_h), BF16),
            pltpu.SemaphoreType.DMA((5,)),
            pltpu.SemaphoreType.DMA((3,)),
            pltpu.SemaphoreType.DMA((3,)),
        ],
        compiler_params=pltpu.CompilerParams(collective_id=0, has_side_effects=True, vmem_limit_bytes=GATHER_VMEM),
        name="rnnt_gather",
    )(*args, labels_t)


def reduce_kernel(n_t, gwo_v, dc_v, da_v, loss_v, f_v, g_p, we_p, loss_ref, gf_ref, gwe_ref, gwp_ref, gwo_ref,
                  g_v, we_v, gwp_v, rgwo, rgwp, rda, rloss, da_rows, in_sem, send_sem, recv_sem):
    me = lax.axis_index('seq')
    partner = me + 1 - 2 * (me % 2)
    loads = [pltpu.make_async_copy(src, dst, in_sem.at[q]) for q, (src, dst) in enumerate(((g_p, g_v), (we_p, we_v)))]
    for load in loads:
        load.start()
    barrier = pltpu.get_barrier_semaphore()
    pl.semaphore_signal(barrier, inc=1, device_id={'seq': partner}, device_id_type=MESH)
    pl.semaphore_wait(barrier, 1)

    def send(src, dst, sem):
        return pltpu.make_async_remote_copy(src_ref=src, dst_ref=dst, send_sem=send_sem.at[sem], recv_sem=recv_sem.at[sem],
                                            device_id={'seq': partner}, device_id_type=MESH)
    n_part = 4
    rows = gwo_v.shape[0] // n_part
    sends = [send(da_v, rda, 0), send(loss_v, rloss, 1)]
    sends += [send(gwo_v.at[pl.ds(q * rows, rows)], rgwo.at[pl.ds(q * rows, rows)], 2 + q) for q in range(n_part)]
    for s in sends:
        s.start()
    loads[0].wait()
    gwp_v[...] = dot(g_v[...].T, dc_v[...], NT)
    s_gwp = send(gwp_v, rgwp, 2 + n_part)
    loads[1].wait()
    sends[0].wait_recv()
    sends[1].wait_recv()
    loss_ref[...] = (loss_v[0:1, :] + rloss[0:1, :])[:, 0:loss_ref.shape[1]]
    da = (da_v[...].astype(F32) + rda[...].astype(F32)).astype(BF16)
    s_gwp.start()
    n_f = da.shape[1]
    n_loc = gf_ref.shape[1]
    n_own = gf_ref.shape[0] * n_loc
    row = lax.broadcasted_iota(jnp.int32, (n_f, n_f), 0)
    col = lax.broadcasted_iota(jnp.int32, (n_f, n_f), 1)
    order = jnp.where(col == row % n_own // n_loc * n_t + row // n_own * n_loc + row % n_loc, 1.0, 0.0).astype(BF16)
    da_f = dot(order, da, NT).astype(BF16)
    da_rows[...] = da_f
    gwe_ref[...] = dot(f_v[...].T, da_f)
    own = da_rows[pl.ds(pl.multiple_of(me * n_own, n_own), n_own), :]
    gf_ref[...] = dot(own, we_v[...], NT).astype(BF16).reshape(gf_ref.shape)
    for q in range(n_part):
        sends[2 + q].wait_recv()
        part = slice(q * rows, (q + 1) * rows)
        gwo_ref[part] = gwo_v[part] + rgwo[part]
    s_gwp.wait_recv()
    gwp_ref[...] = gwp_v[...] + rgwp[...]
    for s in sends + [s_gwp]:
        s.wait_send()


def reduce_call(gwo, dc_t, da_t, loss, g2, f2, w_enc, gf_shape, n_t):
    vm = pl.BlockSpec(memory_space=pltpu.VMEM)
    like = lambda x: pltpu.VMEM(x.shape, x.dtype)
    gwp_shape = (g2.shape[1], dc_t.shape[0])
    return pl.pallas_call(
        functools.partial(reduce_kernel, n_t),
        out_shape=(
            pltpu.VMEM((1, f2.shape[0] // n_t), F32),
            pltpu.VMEM(gf_shape, BF16),
            pltpu.VMEM(w_enc.shape, F32),
            pltpu.VMEM(gwp_shape, F32),
            pltpu.VMEM(gwo.shape, F32),
        ),
        in_specs=[vm] * 5 + [pl.BlockSpec(memory_space=pltpu.HBM)] * 2,
        out_specs=(vm,) * 5,
        scratch_shapes=[like(x) for x in (g2, w_enc)] + [
            pltpu.VMEM(gwp_shape, F32), like(gwo), pltpu.VMEM(gwp_shape, F32), like(da_t), like(loss), pltpu.VMEM(da_t.shape[::-1], BF16),
            pltpu.SemaphoreType.DMA((2,)),
            pltpu.SemaphoreType.DMA((7,)),
            pltpu.SemaphoreType.DMA((7,)),
        ],
        compiler_params=pltpu.CompilerParams(collective_id=1, has_side_effects=True, vmem_limit_bytes=REDUCE_VMEM),
        name="rnnt_reduce",
    )(in_vmem(gwo), in_vmem(dc_t), in_vmem(da_t), in_vmem(loss), in_vmem(f2), in_hbm(g2), in_hbm(w_enc))


def store_kernel(n, *refs):
    sems = refs[2 * n]
    copies = [pltpu.make_async_copy(refs[q], refs[n + q], sems.at[q]) for q in range(n)]
    for copy in copies:
        copy.start()
    for copy in copies:
        copy.wait()


def store_call(arrays):
    n = len(arrays)
    return pl.pallas_call(
        functools.partial(store_kernel, n),
        out_shape=tuple(pltpu.HBM(x.shape, x.dtype) for x in arrays),
        in_specs=[pl.BlockSpec(memory_space=pltpu.VMEM)] * n,
        out_specs=(pl.BlockSpec(memory_space=pltpu.HBM),) * n,
        scratch_shapes=[pltpu.SemaphoreType.DMA((n,))],
        compiler_params=pltpu.CompilerParams(vmem_limit_bytes=STORE_VMEM),
        name="rnnt_store",
    )(*[in_vmem(x) for x in arrays])


def core_kernel(n_t, n_u, flen_s, llen_s, flen_v, llen_v, ylab, c_buf, a_buf, wot, wo_h,
                loss_ref, dc_ref, da_ref, gwo_ref,
                wo_ref, wo_sem, hbuf, hpar, ebuf, fac, mch, sch, vsb, ypar, ybuf, idx, dzb, dpb, zrow, sk, abuf, t1buf, t2buf,
                gocc, gocb, segu, segt, tbl, off):
    n_utt = flen_s.shape[0]
    n_j = c_buf.shape[0]
    n_v = wo_ref.shape[1]
    step_u = WIN // 2 * n_u
    step_t = WIN // 2 * n_t
    per_tile = 128 // step_t
    gu = WIN * n_u
    n_win = n_utt * 2 // WIN - 1
    n_diag = n_t + n_u - 1
    n_kt = (n_diag + 1) * n_t
    n_ch = n_v // CHUNK

    load_wo = pltpu.make_async_copy(wo_h, wo_ref, wo_sem)
    load_wo.start()

    def off_step(b, total):
        off[b] = total
        return total + flen_s[b] * (llen_s[b] + 1)
    off[n_utt] = lax.fori_loop(0, n_utt, off_step, jnp.int32(0))

    total = off[n_utt]
    cut = lax.fori_loop(CORE_MIN, CORE_MAX, lambda b, n: n + jnp.where(off[b] + off[b + 1] <= total, 1, 0), jnp.int32(CORE_MIN))
    first_core = lax.axis_index('seq') % 2 == 0
    u_lo = jnp.where(first_core, 0, cut)
    u_hi = jnp.where(first_core, cut, n_utt)
    stop = off[u_hi]

    def utt_step(b, carry):
        win = jnp.minimum(b // (WIN // 2), n_win - 1)
        base = off[win * (WIN // 2)]
        last = jnp.minimum(off[win * (WIN // 2) + WIN], stop)

        def emit(c):
            n, pos = c
            end = jnp.minimum(pos + ROWS, last)
            tbl[0, n] = win
            tbl[1, n] = pos - base
            tbl[2, n] = end - base
            return n + 1, end
        return lax.while_loop(lambda c: c[1] < off[b + 1], emit, carry)
    n_blocks, _ = lax.fori_loop(u_lo, u_hi, utt_step, (jnp.int32(0), off[u_lo]))
    for past in range(3):
        for q in range(3):
            tbl[q, n_blocks + past] = 0

    sk[...] = jnp.zeros_like(sk)
    mch[...] = jnp.zeros_like(mch)
    sch[...] = jnp.ones_like(sch)
    zrow[...] = jnp.zeros_like(zrow)
    vsb[...] = jnp.zeros_like(vsb)
    dpb[...] = jnp.zeros_like(dpb)

    def onehot(n, index_row):
        return (lax.broadcasted_iota(jnp.int32, (n, ROWS), 0) == index_row)

    def as_bf16(mask):
        return jnp.where(mask, 1.0, 0.0).astype(BF16)

    def frame_onehot(index_row):
        n = WIN * n_t + 128 - step_t
        return jnp.concatenate([as_bf16(onehot(n, index_row)), jnp.zeros((256 - n, ROWS), BF16)], axis=0)

    sub8 = lax.broadcasted_iota(jnp.int32, (8, ROWS), 0)
    n_sub = CHUNK // 8

    def lanes_of(win):
        return pl.ds(pl.multiple_of(win * step_u, 128), gu)

    def frame_lanes_of(win):
        return pl.ds(pl.multiple_of(win // per_tile * 128, 128), 256)

    def spread3(idx_b, parts):
        mask = lax.broadcasted_iota(jnp.int32, (CORE_MAX, ROWS), 0) == idx_b
        return jnp.concatenate([jnp.where(mask, part, 0.0) for part in parts]
                               + [jnp.zeros((128 - 3 * CORE_MAX, ROWS), F32)], axis=0).astype(BF16)

    def locate(i):
        win = tbl[0, i]
        r = tbl[1, i] + lax.broadcasted_iota(jnp.int32, (1, ROWS), 1)
        end_r = tbl[2, i]
        start = jnp.int32(0)
        bl = jnp.full((1, ROWS), -1, jnp.int32)
        w = jnp.zeros((1, ROWS), jnp.int32)
        u1 = jnp.ones((1, ROWS), jnp.int32)
        for j in range(WIN):
            u1_j = llen_s[win * (WIN // 2) + j] + 1
            end = start + flen_s[win * (WIN // 2) + j] * u1_j
            inside = (r >= start) & (r < jnp.minimum(end, end_r))
            bl = jnp.where(inside, j, bl)
            w = jnp.where(inside, r - start, w)
            u1 = jnp.where(inside, u1_j, u1)
            start = end
        valid = bl >= 0
        t = jnp.zeros((1, ROWS), jnp.int32)
        for j in range(1, n_t):
            t = t + jnp.where(w >= j * u1, 1, 0)
        u = w - t * u1
        idx_u = jnp.where(valid, bl * n_u + u, -1)
        idx_t = jnp.where(valid, bl * n_t + t + win % per_tile * step_t, -1)
        idx_kt = jnp.where(valid, (t + u) * n_t + t, -1)
        idx_b = jnp.where(valid, win * (WIN // 2) + bl - u_lo, -1024)
        rows8 = lax.broadcasted_iota(jnp.int32, (8, ROWS), 0)
        idx[i] = jnp.where(rows8 == 0, idx_u, jnp.where(rows8 == 1, idx_t, jnp.where(rows8 == 2, idx_kt, idx_b)))

    half = n_j // 2

    def hidden(i, par):
        win = tbl[0, i]
        ohu = as_bf16(onehot(gu, idx[i, 0:1]))
        oht = frame_onehot(idx[i, 1:2])
        for q in range(2):
            rows = slice(q * half, (q + 1) * half)
            pre = dot(c_buf[rows, lanes_of(win)], ohu) + dot(a_buf[rows, frame_lanes_of(win)], oht)
            h = jnp.tanh(pre).astype(BF16)
            hpar[par, rows] = h
            hbuf[i, rows] = h
        yy = dot(ylab[win], ohu)
        y8 = jnp.broadcast_to((yy[0:1] * 32.0 + yy[1:2]).astype(jnp.int32), (8, ROWS))
        ypar[par] = y8
        ybuf[i] = y8

    def finish(i, par):
        idx_b = idx[i, 3:4]
        m_all = mch[par]
        m8 = jnp.max(m_all.reshape(n_ch, 8, ROWS), axis=0)
        m = jnp.max(m8, axis=0, keepdims=True)
        f_all = jnp.exp(m_all - m)
        s = jnp.sum(jnp.sum((sch[par] * f_all).reshape(n_ch, 8, ROWS), axis=0), axis=0, keepdims=True)
        fac[i] = f_all * (1.0 / s)
        lse = m + jnp.log(s)
        b_parts = split3(zrow[par, 8:9] - lse)
        l_parts = split3(jnp.sum(zrow[par, 0:8], axis=0, keepdims=True) - lse)
        vsb[par, 0:128] = spread3(idx_b, b_parts)
        vsb[par, 128:256] = spread3(idx_b, l_parts)

    def scatter(i, par, live):
        okt = as_bf16(onehot(n_kt, jnp.where(live, idx[i, 2:3], -1)))
        part = n_kt // 2
        for q in range(2):
            sk[q * part:(q + 1) * part] += dot(okt[q * part:(q + 1) * part], vsb[par], NT)

    def slot_of(i):
        return jnp.where(i < KEEP, i, KEEP + i % 2)

    def scores_of(i, par):
        y8 = ypar[par]
        y_tile = lax.shift_right_logical(y8, 3)
        slot = slot_of(i)
        lz = jnp.zeros((8, ROWS), F32)
        for c in range(n_ch):
            z = dot(wot[c * CHUNK:(c + 1) * CHUNK, :], hpar[par])
            z3 = z.reshape(n_sub, 8, ROWS)
            for k in range(n_sub):
                lz = jnp.where(y_tile == c * n_sub + k, z3[k], lz)
            if c == 0:
                zrow[par, 8:16] = z[0:8, :]
            m_c = jnp.max(z3, axis=0)
            e3 = jnp.exp(z3 - m_c[None])
            ebuf[slot, c * CHUNK:(c + 1) * CHUNK, :] = e3.reshape(CHUNK, ROWS)
            mch[par, c * 8:(c + 1) * 8, :] = m_c
            sch[par, c * 8:(c + 1) * 8, :] = jnp.sum(e3, axis=0)
        zrow[par, 0:8] = jnp.where(sub8 == jnp.bitwise_and(y8, 7), lz, 0.0)

    def fwd_pair(p, carry):
        i = 2 * p
        hidden(i + 1, 1)
        finish(jnp.maximum(i - 1, 0), 1)
        scatter(jnp.maximum(i - 2, 0), 0, i > 1)
        scores_of(i, 0)
        scatter(jnp.maximum(i - 1, 0), 1, i > 0)
        hidden(i + 2, 0)
        finish(i, 0)
        scores_of(i + 1, 1)
        locate(i + 3)
        locate(i + 4)
        return carry

    def fwd_odd(p, carry):
        i = n_blocks - 1
        finish(jnp.maximum(i - 1, 0), 1)
        scatter(jnp.maximum(i - 2, 0), 0, i > 1)
        scores_of(i, 0)
        scatter(jnp.maximum(i - 1, 0), 1, i > 0)
        finish(i, 0)
        scatter(i, 0, True)
        return carry

    def fwd_even(p, carry):
        finish(n_blocks - 1, 1)
        scatter(n_blocks - 2, 0, True)
        scatter(n_blocks - 1, 1, True)
        return carry

    for first in range(3):
        locate(jnp.int32(first))
    hidden(jnp.int32(0), 0)
    lax.fori_loop(0, n_blocks // 2, fwd_pair, 0)
    lax.fori_loop(0, n_blocks % 2, fwd_odd, 0)
    lax.fori_loop(0, 1 - n_blocks % 2, fwd_even, 0)

    tt = lax.broadcasted_iota(jnp.int32, (n_t, 128), 0)
    def own_lanes(ref):
        x = jnp.concatenate([ref[...], jnp.zeros((1, 128 - n_utt), jnp.int32)], axis=1).astype(F32)
        return pltpu.roll(jnp.broadcast_to(x, (n_t, 128)), (128 - u_lo) % 128, 1).astype(jnp.int32)
    t_len = own_lanes(flen_v)
    u_len = own_lanes(llen_v)

    def scores(k):
        lo = k * n_t
        x, y = (v + pltpu.roll(v, 128 - CORE_MAX, 1) + pltpu.roll(v, 128 - 2 * CORE_MAX, 1)
                for v in (sk[lo:lo + n_t, 0:128], sk[lo:lo + n_t, 128:256]))
        uu = k - tt
        ok = (uu >= 0) & (tt < t_len)
        bl_k = jnp.where(ok & (uu <= u_len), x, NEG)
        lb_k = jnp.where(ok & (uu < u_len), y, NEG)
        return bl_k, lb_k

    alpha = jnp.where(tt == 0, 0.0, NEG).astype(F32)
    abuf[0] = alpha
    beta = jnp.full((n_t, 128), NEG, F32)
    sc = [scores(k) for k in range(n_diag)]
    for step in range(n_diag):
        if step > 0:
            bl_k, lb_k = sc[step - 1]
            p1 = jnp.where(tt == 0, NEG, pltpu.roll(alpha + bl_k, 1, 0))
            alpha = logadd(p1, alpha + lb_k)
            abuf[step] = alpha
        k = n_diag - 1 - step
        bl_k, lb_k = sc[k]
        up = jnp.where(tt == n_t - 1, jnp.where(u_len == k + 1 - n_t, 0.0, NEG), pltpu.roll(beta, n_t - 1, 0))
        t1 = up + bl_k
        t2 = beta + lb_k
        t1buf[k] = t1
        t2buf[k] = t2
        beta = jnp.where(tt >= t_len, jnp.where(k - tt == u_len, 0.0, NEG), logadd(t1, t2))
    segu[...] = jnp.zeros_like(segu)
    segt[...] = jnp.zeros_like(segt)
    log_p = beta[0:1, :]
    lane = lax.broadcasted_iota(jnp.int32, (n_t, 128), 1)
    loss_ref[...] = pltpu.roll(jnp.where(lane < u_hi - u_lo, -log_p, 0.0), u_lo, 1)
    lane_ok = lane < CORE_MAX
    for k in range(n_diag):
        for which, buf in enumerate((t1buf, t2buf)):
            occ = jnp.where(lane_ok, jnp.exp(jnp.minimum(abuf[k] + buf[k] - log_p, 0.0)), 0.0)
            hi, mid, lo = split3(occ)
            lo_row = which * n_kt + k * n_t
            gocc[lo_row:lo_row + n_t, :] = hi + pltpu.roll(mid, CORE_MAX, 1) + pltpu.roll(lo, 2 * CORE_MAX, 1)
    for which in range(2):
        gocc[which * n_kt + n_diag * n_t:(which + 1) * n_kt, :] = jnp.zeros((n_kt - n_diag * n_t, 128), F32)
    gocb[...] = gocc[...].astype(BF16)

    def again(first, count):
        def one(q, carry):
            i = first + q

            @pl.when(i >= KEEP)
            def _():
                def chunk(c, carry):
                    rows = pl.ds(pl.multiple_of(c * CHUNK, CHUNK), CHUNK)
                    z3 = dot(wot[rows, :], hbuf[i]).reshape(n_sub, 8, ROWS)
                    ebuf[KEEP + i % 2, rows, :] = jnp.exp(z3 - jnp.max(z3, axis=0)[None]).reshape(CHUNK, ROWS)
                    return carry
                lax.fori_loop(0, n_ch, chunk, 0)
            return carry
        @pl.when(first + count > KEEP)
        def _():
            lax.fori_loop(0, count, one, 0)

    def occupancy(i, par):
        orep = spread3(idx[i, 3:4], (1.0, 1.0, 1.0))
        kt8 = jnp.broadcast_to(idx[i, 2:3], (8, ROWS))
        kt_tile = lax.shift_right_arithmetic(kt8, 3)
        kt_sub = sub8 == jnp.bitwise_and(kt8, 7)
        for which in range(2):
            gath = dot(gocb[which * n_kt:(which + 1) * n_kt], orep).reshape(n_kt // 8, 8, ROWS)
            occ = jnp.zeros((8, ROWS), F32)
            for k in range(n_diag):
                occ = jnp.where(kt_tile == k, gath[k], occ)
            occ = jnp.sum(jnp.where(kt_sub, occ, 0.0), axis=0, keepdims=True)
            zrow[par, which * 8:which * 8 + 8] = jnp.broadcast_to(occ, (8, ROWS))

    def d_logits(i, par):
        y8 = ybuf[i]
        y_tile = lax.shift_right_logical(y8, 3)
        gb = zrow[par, 0:8]
        gl = zrow[par, 8:16]
        occ = gb + gl
        gl_y = jnp.where(sub8 == jnp.bitwise_and(y8, 7), gl, 0.0)
        gb_0 = jnp.where(sub8 == 0, gb, 0.0)
        slot = slot_of(i)
        for c in range(n_ch):
            sc_c = fac[i, c * 8:(c + 1) * 8, :] * occ
            e3 = ebuf[slot, c * CHUNK:(c + 1) * CHUNK, :].reshape(n_sub, 8, ROWS)
            tiles = []
            for k in range(n_sub):
                d = e3[k] * sc_c
                if c == 0 and k == 0:
                    d = d - gb_0
                tiles.append(d - jnp.where(y_tile == c * n_sub + k, gl_y, 0.0))
            d = jnp.concatenate(tiles, axis=0)
            dzb[par, c * CHUNK:(c + 1) * CHUNK, :] = d.astype(BF16)

    def segments(i, par):
        win = tbl[0, i]
        ohu = as_bf16(onehot(gu, idx[i, 0:1]))
        oht = frame_onehot(idx[i, 1:2])
        for q in range(2):
            rows = slice(q * half, (q + 1) * half)
            segu[rows, lanes_of(win)] += dot(dpb[par, rows], ohu, NT)
            segt[rows, frame_lanes_of(win)] += dot(dpb[par, rows], oht, NT)

    def d_hidden(i, par):
        for q in range(2):
            rows = slice(q * half, (q + 1) * half)
            hf = hbuf[i, rows].astype(F32)
            dh = dot(wo_ref[rows], dzb[par])
            dpb[par, rows] = (dh * (1.0 - hf * hf)).astype(BF16)

    def out_grad(blocks, add):
        for c in range(n_v // 256):
            cols = slice(c * 256, (c + 1) * 256)
            new = None
            for i, par in blocks:
                term = dot(hbuf[i], dzb[par, cols, :], NT)
                new = term if new is None else new + term
            gwo_ref[:, cols] = jnp.where(add, gwo_ref[:, cols], 0.0) + new

    def bwd_pair(p, carry):
        i = 2 * p
        again(i + 2, 2)
        d_hidden(i, 0)
        d_hidden(i + 1, 1)
        out_grad(((i, 0), (i + 1, 1)), p > 0)
        d_logits(i + 2, 0)
        segments(i, 0)
        d_logits(i + 3, 1)
        segments(i + 1, 1)
        occupancy(i + 4, 0)
        occupancy(i + 5, 1)
        return carry

    def bwd_odd(p, carry):
        d_hidden(n_blocks - 1, 0)
        out_grad(((n_blocks - 1, 0),), n_blocks > 1)
        segments(n_blocks - 1, 0)
        return carry

    load_wo.wait()
    again(0, 2)
    for first in range(2):
        occupancy(jnp.int32(first), first)
        d_logits(jnp.int32(first), first)
        occupancy(jnp.int32(first + 2), first)
    lax.fori_loop(0, n_blocks // 2, bwd_pair, 0)
    lax.fori_loop(0, n_blocks % 2, bwd_odd, 0)

    dc_ref[...] = segu[...].astype(BF16)
    da_ref[...] = segt[:, 0:n_utt * n_t].astype(BF16)


def core_call(c_t, a_t, wot, ylab, w_out, flen, llen, n_t, n_u):
    n_utt = flen.shape[0]
    n_j = c_t.shape[0]
    n_v = w_out.shape[1]
    max_blk = n_utt // 2 * n_t * n_u // ROWS + 6
    n_kt = (n_t + n_u) * n_t
    n_st = n_v // CHUNK * 8
    vm = pl.BlockSpec(memory_space=pltpu.VMEM)
    sm = pl.BlockSpec(memory_space=pltpu.SMEM)
    return pl.pallas_call(
        functools.partial(core_kernel, n_t, n_u),
        out_shape=(
            pltpu.VMEM((8, 128), F32),
            pltpu.VMEM((n_j, n_utt * n_u), BF16),
            pltpu.VMEM((n_j, n_utt * n_t), BF16),
            pltpu.VMEM(w_out.shape, F32),
        ),
        in_specs=[sm, sm] + [vm] * 6 + [pl.BlockSpec(memory_space=pltpu.HBM)],
        out_specs=(vm,) * 4,
        scratch_shapes=[
            pltpu.VMEM(w_out.shape, BF16),
            pltpu.SemaphoreType.DMA,
            pltpu.VMEM((max_blk, n_j, ROWS), BF16),
            pltpu.VMEM((2, n_j, ROWS), BF16),
            pltpu.VMEM((min(max_blk, KEEP + 2), n_v, ROWS), F32),
            pltpu.VMEM((max_blk, n_st, ROWS), F32),
            pltpu.VMEM((2, n_st, ROWS), F32),
            pltpu.VMEM((2, n_st, ROWS), F32),
            pltpu.VMEM((2, 256, ROWS), BF16),
            pltpu.VMEM((2, 8, ROWS), jnp.int32),
            pltpu.VMEM((max_blk, 8, ROWS), jnp.int32),
            pltpu.VMEM((max_blk, 8, ROWS), jnp.int32),
            pltpu.VMEM((2, n_v, ROWS), BF16),
            pltpu.VMEM((2, n_j, ROWS), BF16),
            pltpu.VMEM((2, 16, ROWS), F32),
            pltpu.VMEM((n_kt, 256), F32),
            pltpu.VMEM((n_t + n_u, n_t, 128), F32),
            pltpu.VMEM((n_t + n_u, n_t, 128), F32),
            pltpu.VMEM((n_t + n_u, n_t, 128), F32),
            pltpu.VMEM((2 * n_kt, 128), F32),
            pltpu.VMEM((2 * n_kt, 128), BF16),
            pltpu.VMEM((n_j, n_utt * n_u), F32),
            pltpu.VMEM((n_j, n_utt * n_t + 128), F32),
            pltpu.SMEM((3, max_blk), jnp.int32),
            pltpu.SMEM((n_utt + 1,), jnp.int32),
        ],
        compiler_params=pltpu.CompilerParams(vmem_limit_bytes=CORE_VMEM),
        name="rnnt_core",
    )(flen, llen, flen.reshape(1, n_utt), llen.reshape(1, n_utt), *[in_vmem(x) for x in (ylab, c_t, a_t, wot)], in_hbm(w_out))


def solution(mesh):
    seq_size = mesh.shape['seq']

    def local_fn(enc_out, pred_out, w_enc, w_pred, w_out, labels, frame_len, label_len):
        n_utt, n_loc, n_h = enc_out.shape
        n_u = pred_out.shape[1]
        n_t = n_loc * seq_size
        g2 = pred_out.reshape(n_utt * n_u, n_h)
        c_t, a_t, wot, f2, *rest = gather_call(enc_out, g2, w_enc, w_pred, w_out, labels.T, seq_size, n_t, n_u)
        loss, dc_t, da_t, gwo = core_call(c_t, a_t, wot, *rest, w_out, frame_len, label_len, n_t, n_u)
        loss, gf, gwe, gwp, gwo = store_call(reduce_call(gwo, dc_t, da_t, loss, g2, f2, w_enc, enc_out.shape, n_t))
        return loss.reshape(n_utt), gf, gwe, gwp, gwo

    in_specs = (P('dp', 'seq', None), P('dp', None, None), P(None, None), P(None, None), P(None, None), P('dp', None), P('dp'), P('dp'))
    out_specs = (P('dp'), P('dp', 'seq', None), P('dp', None), P('dp', None), P('dp', None))
    return jax.shard_map(local_fn, mesh=mesh, in_specs=in_specs, out_specs=out_specs, check_vma=False)
```

```python
import functools

import jax
import jax.numpy as jnp
from jax import lax
from jax.experimental import pallas as pl
from jax.experimental.pallas import tpu as pltpu
from jax.sharding import PartitionSpec as P

NEG = -1.0e30
ROWS = 256
WIN = 8
CHUNK = 128
CORE_MIN, CORE_MAX = 24, 40
GATHER_VMEM = 40 << 20
CORE_VMEM = 51 << 20
REDUCE_VMEM = 36 << 20
STORE_VMEM = 1 << 20
KEEP = 15
F32 = jnp.float32
BF16 = jnp.bfloat16
MESH = pl.DeviceIdType.MESH
NT = (((1,), (1,)), ((), ()))
NN = (((1,), (0,)), ((), ()))


def dot(a, b, dims=NN):
    return lax.dot_general(a, b, dims, preferred_element_type=F32)


def in_hbm(x):
    return pltpu.with_memory_space_constraint(x, pltpu.HBM)


def in_vmem(x):
    return pltpu.with_memory_space_constraint(x, pltpu.VMEM)


def split3(x):
    hi = x.astype(BF16).astype(F32)
    r1 = x - hi
    mid = r1.astype(BF16).astype(F32)
    return hi, mid, r1 - mid


def logadd(a, b):
    m = jnp.maximum(a, b)
    return m + jnp.log(1.0 + jnp.exp(jnp.minimum(a, b) - m))


def label_rows(n_u, lab_ref, ylab):
    n_utt = lab_ref.shape[1]
    step_u = WIN // 2 * n_u
    gu = WIN * n_u
    n_win = ylab.shape[0]
    lab = lab_ref[...]
    place = jnp.where(lax.broadcasted_iota(jnp.int32, (n_utt, n_utt * n_u), 1) // n_u
                      == lax.broadcasted_iota(jnp.int32, (n_utt, n_utt * n_u), 0), 1.0, 0.0).astype(BF16)
    mine = (lax.broadcasted_iota(jnp.int32, (lab.shape[0], n_utt * n_u), 1) % n_u
            == lax.broadcasted_iota(jnp.int32, (lab.shape[0], n_utt * n_u), 0))
    flat = []
    for part in (lax.shift_right_arithmetic(lab, 5), jnp.bitwise_and(lab, 31)):
        spread = dot(part.astype(F32).astype(BF16), place)
        flat.append(jnp.sum(jnp.where(mine, spread, 0.0), axis=0, keepdims=True))
    for w in range(n_win):
        row = lax.broadcasted_iota(jnp.int32, (16, gu), 0)
        hi, lo = (x[:, w * step_u:w * step_u + gu] for x in flat)
        ylab[w] = jnp.where(row == 0, hi, jnp.where(row == 1, lo, 0.0)).astype(BF16)


def gather_kernel(n_t, n_u, enc_h, g_h, we_h, wp_h, wo_h, lab_h, c_ref, a_ref, wot_ref, f_ref, ylab,
                  enc_ref, g_ref, we_ref, wp_ref, wo_ref, lab_ref, fbuf, in_sem, send_sem, recv_sem):
    me = lax.axis_index('seq')
    n_seq = fbuf.shape[0]
    partner = me + 1 - 2 * (me % 2)
    peer = (me + 2) % n_seq
    load_enc, load_wo, load_wp, load_g, load_we, load_lab = loads = [pltpu.make_async_copy(src, dst, in_sem.at[q]) for q, (src, dst) in enumerate(
        ((enc_h, enc_ref), (wo_h, wo_ref), (wp_h, wp_ref), (g_h, g_ref), (we_h, we_ref), (lab_h, lab_ref)))]
    for load in loads:
        load.start()
    barrier = pltpu.get_barrier_semaphore()
    for other in (partner, peer):
        pl.semaphore_signal(barrier, inc=1, device_id={'seq': other}, device_id_type=MESH)
    pl.semaphore_wait(barrier, 2)

    def send(src, slot, sem, other):
        return pltpu.make_async_remote_copy(src_ref=src, dst_ref=fbuf.at[slot], send_sem=send_sem.at[sem], recv_sem=recv_sem.at[sem],
                                            device_id={'seq': other}, device_id_type=MESH)
    load_enc.wait()
    to_peer = send(enc_ref, me, 0, peer)
    to_peer.start()
    to_partner = send(enc_ref, me, 1, partner)
    to_partner.start()
    fbuf[me] = enc_ref[...]
    load_wo.wait()
    wot_ref[...] = wo_ref[...].T
    load_wp.wait()
    load_g.wait()
    n_c = (CORE_MAX + WIN // 2) * n_u
    cols = pl.ds(pl.multiple_of(me % 2 * (c_ref.shape[1] - n_c), 128), n_c)
    c_ref[:, cols] = dot(wp_ref[...].T, g_ref[cols, :], NT).astype(BF16)
    load_we.wait()
    we_t = we_ref[...].T
    load_lab.wait()
    label_rows(n_u, lab_ref, ylab)
    n_f, n_h = f_ref.shape
    n_own = n_f // n_seq
    n_loc = n_t // n_seq
    row = lax.broadcasted_iota(jnp.int32, (n_own, n_f), 0)
    col = lax.broadcasted_iota(jnp.int32, (n_own, n_f), 1)

    def piece(p):
        rows = fbuf[p].reshape(n_own, n_h)
        f_ref[pl.ds(pl.multiple_of(p * n_own, n_own), n_own), :] = rows
        order = jnp.where(col == row // n_loc * n_t + p * n_loc + row % n_loc, 1.0, 0.0).astype(BF16)
        return dot(dot(we_t, rows, NT).astype(BF16), order)
    a_t = piece(me)
    to_partner.wait_recv()
    a_t = a_t + piece(partner)
    to_peer.wait_recv()
    relay = send(fbuf.at[peer], peer, 2, partner)
    relay.start()
    a_t = a_t + piece(peer)
    relay.wait_recv()
    a_ref[:, 0:n_f] = (a_t + piece((partner + 2) % n_seq)).astype(BF16)
    a_ref[:, n_f:] = jnp.zeros((a_ref.shape[0], a_ref.shape[1] - n_f), BF16)
    to_peer.wait_send()
    to_partner.wait_send()
    relay.wait_send()


def gather_call(enc, g2, w_enc, w_pred, w_out, labels_t, n_seq, n_t, n_u):
    n_utt, n_loc, n_h = enc.shape
    n_j = w_enc.shape[1]
    vm = pl.BlockSpec(memory_space=pltpu.VMEM)
    n_f = n_utt * n_loc * n_seq
    args = [in_hbm(x) for x in (enc, g2, w_enc, w_pred, w_out, labels_t)]
    return pl.pallas_call(
        functools.partial(gather_kernel, n_t, n_u),
        out_shape=(
            pltpu.VMEM((n_j, g2.shape[0]), BF16),
            pltpu.VMEM((n_j, n_f + 128), BF16),
            pltpu.VMEM(w_out.shape[::-1], BF16),
            pltpu.VMEM((n_f, n_h), BF16),
            pltpu.VMEM((n_utt * 2 // WIN - 1, 16, WIN * n_u), BF16),
        ),
        in_specs=[pl.BlockSpec(memory_space=pltpu.HBM)] * 6,
        out_specs=(vm,) * 5,
        scratch_shapes=[pltpu.VMEM(x.shape, x.dtype) for x in (enc, g2, w_enc, w_pred, w_out, labels_t)] + [
            pltpu.VMEM((n_seq, n_utt, n_loc, n_h), BF16),
            pltpu.SemaphoreType.DMA((6,)),
            pltpu.SemaphoreType.DMA((3,)),
            pltpu.SemaphoreType.DMA((3,)),
        ],
        compiler_params=pltpu.CompilerParams(collective_id=0, has_side_effects=True, vmem_limit_bytes=GATHER_VMEM),
        name="rnnt_gather",
    )(*args)


def reduce_kernel(n_t, gwo_v, dc_v, da_v, loss_v, f_v, g_p, we_p, loss_ref, gf_ref, gwe_ref, gwp_ref, gwo_ref,
                  g_v, we_v, gwp_v, rgwo, rgwp, rda, rloss, da_rows, in_sem, send_sem, recv_sem):
    me = lax.axis_index('seq')
    partner = me + 1 - 2 * (me % 2)
    loads = [pltpu.make_async_copy(src, dst, in_sem.at[q]) for q, (src, dst) in enumerate(((g_p, g_v), (we_p, we_v)))]
    for load in loads:
        load.start()
    barrier = pltpu.get_barrier_semaphore()
    pl.semaphore_signal(barrier, inc=1, device_id={'seq': partner}, device_id_type=MESH)
    pl.semaphore_wait(barrier, 1)

    def send(src, dst, sem):
        return pltpu.make_async_remote_copy(src_ref=src, dst_ref=dst, send_sem=send_sem.at[sem], recv_sem=recv_sem.at[sem],
                                            device_id={'seq': partner}, device_id_type=MESH)
    n_part = 4
    rows = gwo_v.shape[0] // n_part
    n_da = CORE_MAX * n_t + 64
    da_lo = (da_v.shape[1] - n_da) * (me % 2)
    part = (slice(None), pl.ds(pl.multiple_of(da_lo, 128), n_da))
    sends = [send(da_v.at[part], rda.at[part], 0), send(loss_v, rloss, 1)]
    sends += [send(gwo_v.at[pl.ds(q * rows, rows)], rgwo.at[pl.ds(q * rows, rows)], 2 + q) for q in range(n_part)]
    for s in sends:
        s.start()
    loads[0].wait()
    gwp_v[...] = dot(g_v[...].T, dc_v[...], NT)
    s_gwp = send(gwp_v, rgwp, 2 + n_part)
    loads[1].wait()
    sends[0].wait_recv()
    sends[1].wait_recv()
    loss_ref[...] = (loss_v[0:1, :] + rloss[0:1, :])[:, 0:loss_ref.shape[1]]
    lane = lax.broadcasted_iota(jnp.int32, rda.shape, 1) - (da_v.shape[1] - n_da) * (partner % 2)
    other = jnp.where((lane >= 0) & (lane < n_da), rda[...].astype(F32), 0.0)
    da = (da_v[...].astype(F32) + other).astype(BF16)
    s_gwp.start()
    n_f = da.shape[1]
    n_loc = gf_ref.shape[1]
    n_own = gf_ref.shape[0] * n_loc
    row = lax.broadcasted_iota(jnp.int32, (n_f, n_f), 0)
    col = lax.broadcasted_iota(jnp.int32, (n_f, n_f), 1)
    order = jnp.where(col == row % n_own // n_loc * n_t + row // n_own * n_loc + row % n_loc, 1.0, 0.0).astype(BF16)
    da_f = dot(order, da, NT).astype(BF16)
    da_rows[...] = da_f
    gwe_ref[...] = dot(f_v[...].T, da_f)
    own = da_rows[pl.ds(pl.multiple_of(me * n_own, n_own), n_own), :]
    gf_ref[...] = dot(own, we_v[...], NT).astype(BF16).reshape(gf_ref.shape)
    for q in range(n_part):
        sends[2 + q].wait_recv()
        part = slice(q * rows, (q + 1) * rows)
        gwo_ref[part] = gwo_v[part] + rgwo[part]
    s_gwp.wait_recv()
    gwp_ref[...] = gwp_v[...] + rgwp[...]
    for s in sends + [s_gwp]:
        s.wait_send()


def reduce_call(gwo, dc_t, da_t, loss, g2, f2, w_enc, gf_shape, n_t):
    vm = pl.BlockSpec(memory_space=pltpu.VMEM)
    like = lambda x: pltpu.VMEM(x.shape, x.dtype)
    gwp_shape = (g2.shape[1], dc_t.shape[0])
    return pl.pallas_call(
        functools.partial(reduce_kernel, n_t),
        out_shape=(
            pltpu.VMEM((1, f2.shape[0] // n_t), F32),
            pltpu.VMEM(gf_shape, BF16),
            pltpu.VMEM(w_enc.shape, F32),
            pltpu.VMEM(gwp_shape, F32),
            pltpu.VMEM(gwo.shape, F32),
        ),
        in_specs=[vm] * 5 + [pl.BlockSpec(memory_space=pltpu.HBM)] * 2,
        out_specs=(vm,) * 5,
        scratch_shapes=[like(x) for x in (g2, w_enc)] + [
            pltpu.VMEM(gwp_shape, F32), like(gwo), pltpu.VMEM(gwp_shape, F32), like(da_t), like(loss), pltpu.VMEM(da_t.shape[::-1], BF16),
            pltpu.SemaphoreType.DMA((2,)),
            pltpu.SemaphoreType.DMA((7,)),
            pltpu.SemaphoreType.DMA((7,)),
        ],
        compiler_params=pltpu.CompilerParams(collective_id=1, has_side_effects=True, vmem_limit_bytes=REDUCE_VMEM),
        name="rnnt_reduce",
    )(in_vmem(gwo), in_vmem(dc_t), in_vmem(da_t), in_vmem(loss), in_vmem(f2), in_hbm(g2), in_hbm(w_enc))


def store_kernel(n, *refs):
    sems = refs[2 * n]
    copies = [pltpu.make_async_copy(refs[q], refs[n + q], sems.at[q]) for q in range(n)]
    for copy in copies:
        copy.start()
    for copy in copies:
        copy.wait()


def store_call(arrays):
    n = len(arrays)
    return pl.pallas_call(
        functools.partial(store_kernel, n),
        out_shape=tuple(pltpu.HBM(x.shape, x.dtype) for x in arrays),
        in_specs=[pl.BlockSpec(memory_space=pltpu.VMEM)] * n,
        out_specs=(pl.BlockSpec(memory_space=pltpu.HBM),) * n,
        scratch_shapes=[pltpu.SemaphoreType.DMA((n,))],
        compiler_params=pltpu.CompilerParams(vmem_limit_bytes=STORE_VMEM),
        name="rnnt_store",
    )(*[in_vmem(x) for x in arrays])


def core_kernel(n_t, n_u, flen_s, llen_s, flen_v, llen_v, ylab, c_buf, a_buf, wot, wo_h,
                loss_ref, dc_ref, da_ref, gwo_ref,
                wo_ref, wo_sem, hbuf, hpar, ebuf, fac, mch, sch, vsb, ypar, ybuf, idx, dzb, dpb, zrow, sk, abuf, t1buf, t2buf,
                gocc, gocb, segu, segt, tbl, off):
    n_utt = flen_s.shape[0]
    n_j = c_buf.shape[0]
    n_v = wo_ref.shape[1]
    step_u = WIN // 2 * n_u
    step_t = WIN // 2 * n_t
    per_tile = 128 // step_t
    gu = WIN * n_u
    n_win = n_utt * 2 // WIN - 1
    n_diag = n_t + n_u - 1
    n_kt = (n_diag + 1) * n_t
    n_ch = n_v // CHUNK

    load_wo = pltpu.make_async_copy(wo_h, wo_ref, wo_sem)
    load_wo.start()

    total = jnp.int32(0)
    for b in range(n_utt):
        off[b] = total
        total = total + flen_s[b] * (llen_s[b] + 1)
    off[n_utt] = total

    cut = jnp.int32(CORE_MIN)
    for b in range(CORE_MIN, CORE_MAX):
        cut = cut + jnp.where(off[b] + off[b + 1] <= total, 1, 0)
    first_core = lax.axis_index('seq') % 2 == 0
    u_lo = jnp.where(first_core, 0, cut)
    u_hi = jnp.where(first_core, cut, n_utt)
    stop = off[u_hi]

    def utt_step(b, carry):
        win = jnp.minimum(b // (WIN // 2), n_win - 1)
        base = off[win * (WIN // 2)]
        last = jnp.minimum(off[win * (WIN // 2) + WIN], stop)

        def emit(c):
            n, pos = c
            end = jnp.minimum(pos + ROWS, last)
            tbl[0, n] = win
            tbl[1, n] = pos - base
            tbl[2, n] = end - base
            return n + 1, end
        return lax.while_loop(lambda c: c[1] < off[b + 1], emit, carry)
    n_blocks, _ = lax.fori_loop(u_lo, u_hi, utt_step, (jnp.int32(0), off[u_lo]))
    for past in range(3):
        for q in range(3):
            tbl[q, n_blocks + past] = 0

    sk[...] = jnp.zeros_like(sk)
    mch[...] = jnp.zeros_like(mch)
    sch[...] = jnp.ones_like(sch)
    zrow[...] = jnp.zeros_like(zrow)
    vsb[...] = jnp.zeros_like(vsb)
    dpb[...] = jnp.zeros_like(dpb)

    def onehot(n, index_row):
        return (lax.broadcasted_iota(jnp.int32, (n, ROWS), 0) == index_row)

    def as_bf16(mask):
        return jnp.where(mask, 1.0, 0.0).astype(BF16)

    def frame_onehot(index_row):
        n = WIN * n_t + 128 - step_t
        return jnp.concatenate([as_bf16(onehot(n, index_row)), jnp.zeros((256 - n, ROWS), BF16)], axis=0)

    sub8 = lax.broadcasted_iota(jnp.int32, (8, ROWS), 0)
    n_sub = CHUNK // 8

    def lanes_of(win):
        return pl.ds(pl.multiple_of(win * step_u, 128), gu)

    def frame_lanes_of(win):
        return pl.ds(pl.multiple_of(win // per_tile * 128, 128), 256)

    def spread3(idx_b, parts):
        mask = lax.broadcasted_iota(jnp.int32, (CORE_MAX, ROWS), 0) == idx_b
        return jnp.concatenate([jnp.where(mask, part, 0.0) for part in parts]
                               + [jnp.zeros((128 - 3 * CORE_MAX, ROWS), F32)], axis=0).astype(BF16)

    def locate(i):
        win = tbl[0, i]
        r = tbl[1, i] + lax.broadcasted_iota(jnp.int32, (1, ROWS), 1)
        end_r = tbl[2, i]
        start = jnp.int32(0)
        bl = jnp.full((1, ROWS), -1, jnp.int32)
        w = jnp.zeros((1, ROWS), jnp.int32)
        u1 = jnp.ones((1, ROWS), jnp.int32)
        for j in range(WIN):
            u1_j = llen_s[win * (WIN // 2) + j] + 1
            end = start + flen_s[win * (WIN // 2) + j] * u1_j
            inside = (r >= start) & (r < jnp.minimum(end, end_r))
            bl = jnp.where(inside, j, bl)
            w = jnp.where(inside, r - start, w)
            u1 = jnp.where(inside, u1_j, u1)
            start = end
        valid = bl >= 0
        t = jnp.zeros((1, ROWS), jnp.int32)
        for j in range(1, n_t):
            t = t + jnp.where(w >= j * u1, 1, 0)
        u = w - t * u1
        idx_u = jnp.where(valid, bl * n_u + u, -1)
        idx_t = jnp.where(valid, bl * n_t + t + win % per_tile * step_t, -1)
        idx_kt = jnp.where(valid, (t + u) * n_t + t, -1)
        idx_b = jnp.where(valid, win * (WIN // 2) + bl - u_lo, -1024)
        rows8 = lax.broadcasted_iota(jnp.int32, (8, ROWS), 0)
        idx[i] = jnp.where(rows8 == 0, idx_u, jnp.where(rows8 == 1, idx_t, jnp.where(rows8 == 2, idx_kt, idx_b)))

    half = n_j // 2

    def hidden(i, par):
        win = tbl[0, i]
        ohu = as_bf16(onehot(gu, idx[i, 0:1]))
        oht = frame_onehot(idx[i, 1:2])
        for q in range(2):
            rows = slice(q * half, (q + 1) * half)
            pre = dot(c_buf[rows, lanes_of(win)], ohu) + dot(a_buf[rows, frame_lanes_of(win)], oht)
            h = jnp.tanh(pre).astype(BF16)
            hpar[par, rows] = h
            hbuf[i, rows] = h
        yy = dot(ylab[win], ohu)
        y8 = jnp.broadcast_to((yy[0:1] * 32.0 + yy[1:2]).astype(jnp.int32), (8, ROWS))
        ypar[par] = y8
        ybuf[i] = y8

    def finish(i, par):
        idx_b = idx[i, 3:4]
        m_all = mch[par]
        m8 = jnp.max(m_all.reshape(n_ch, 8, ROWS), axis=0)
        m = jnp.max(m8, axis=0, keepdims=True)
        f_all = jnp.exp(m_all - m)
        s = jnp.sum(jnp.sum((sch[par] * f_all).reshape(n_ch, 8, ROWS), axis=0), axis=0, keepdims=True)
        fac[i] = f_all * (1.0 / s)
        lse = m + jnp.log(s)
        b_parts = split3(zrow[par, 8:9] - lse)
        l_parts = split3(jnp.sum(zrow[par, 0:8], axis=0, keepdims=True) - lse)
        vsb[par, 0:128] = spread3(idx_b, b_parts)
        vsb[par, 128:256] = spread3(idx_b, l_parts)

    def scatter(i, par, live):
        okt = as_bf16(onehot(n_kt, jnp.where(live, idx[i, 2:3], -1)))
        part = n_kt // 2
        for q in range(2):
            sk[q * part:(q + 1) * part] += dot(okt[q * part:(q + 1) * part], vsb[par], NT)

    def slot_of(i):
        return jnp.where(i < KEEP, i, KEEP + i % 2)

    def scores_of(i, par):
        y8 = ypar[par]
        y_tile = lax.shift_right_logical(y8, 3)
        slot = slot_of(i)
        lz = jnp.zeros((8, ROWS), F32)
        for c in range(n_ch):
            z = dot(wot[c * CHUNK:(c + 1) * CHUNK, :], hpar[par])
            z3 = z.reshape(n_sub, 8, ROWS)
            for k in range(n_sub):
                lz = jnp.where(y_tile == c * n_sub + k, z3[k], lz)
            if c == 0:
                zrow[par, 8:16] = z[0:8, :]
            m_c = jnp.max(z3, axis=0)
            e3 = jnp.exp(z3 - m_c[None])
            ebuf[slot, c * CHUNK:(c + 1) * CHUNK, :] = e3.reshape(CHUNK, ROWS)
            mch[par, c * 8:(c + 1) * 8, :] = m_c
            sch[par, c * 8:(c + 1) * 8, :] = jnp.sum(e3, axis=0)
        zrow[par, 0:8] = jnp.where(sub8 == jnp.bitwise_and(y8, 7), lz, 0.0)

    def fwd_pair(p, carry):
        i = 2 * p
        hidden(i + 1, 1)
        finish(jnp.maximum(i - 1, 0), 1)
        scatter(jnp.maximum(i - 2, 0), 0, i > 1)
        scores_of(i, 0)
        hidden(i + 2, 0)
        scores_of(i + 1, 1)
        scatter(jnp.maximum(i - 1, 0), 1, i > 0)
        finish(i, 0)
        locate(i + 3)
        locate(i + 4)
        return carry

    def fwd_odd(p, carry):
        i = n_blocks - 1
        finish(jnp.maximum(i - 1, 0), 1)
        scatter(jnp.maximum(i - 2, 0), 0, i > 1)
        scores_of(i, 0)
        scatter(jnp.maximum(i - 1, 0), 1, i > 0)
        finish(i, 0)
        scatter(i, 0, True)
        return carry

    def fwd_even(p, carry):
        finish(n_blocks - 1, 1)
        scatter(n_blocks - 2, 0, True)
        scatter(n_blocks - 1, 1, True)
        return carry

    for first in range(3):
        locate(jnp.int32(first))
    hidden(jnp.int32(0), 0)
    lax.fori_loop(0, n_blocks // 2, fwd_pair, 0)
    lax.fori_loop(0, n_blocks % 2, fwd_odd, 0)
    lax.fori_loop(0, 1 - n_blocks % 2, fwd_even, 0)

    tt = lax.broadcasted_iota(jnp.int32, (n_t, 128), 0)
    def own_lanes(ref):
        x = jnp.concatenate([ref[...], jnp.zeros((1, 128 - n_utt), jnp.int32)], axis=1).astype(F32)
        return pltpu.roll(jnp.broadcast_to(x, (n_t, 128)), (128 - u_lo) % 128, 1).astype(jnp.int32)
    t_len = own_lanes(flen_v)
    u_len = own_lanes(llen_v)

    def scores(k):
        lo = k * n_t
        x, y = (v + pltpu.roll(v, 128 - CORE_MAX, 1) + pltpu.roll(v, 128 - 2 * CORE_MAX, 1)
                for v in (sk[lo:lo + n_t, 0:128], sk[lo:lo + n_t, 128:256]))
        uu = k - tt
        ok = (uu >= 0) & (tt < t_len)
        bl_k = jnp.where(ok & (uu <= u_len), x, NEG)
        lb_k = jnp.where(ok & (uu < u_len), y, NEG)
        return bl_k, lb_k

    alpha = jnp.where(tt == 0, 0.0, NEG).astype(F32)
    abuf[0] = alpha
    beta = jnp.full((n_t, 128), NEG, F32)
    sc = [scores(k) for k in range(n_diag)]
    for step in range(n_diag):
        if step > 0:
            bl_k, lb_k = sc[step - 1]
            p1 = jnp.where(tt == 0, NEG, pltpu.roll(alpha + bl_k, 1, 0))
            alpha = logadd(p1, alpha + lb_k)
            abuf[step] = alpha
        k = n_diag - 1 - step
        bl_k, lb_k = sc[k]
        up = jnp.where(tt == n_t - 1, jnp.where(u_len == k + 1 - n_t, 0.0, NEG), pltpu.roll(beta, n_t - 1, 0))
        t1 = up + bl_k
        t2 = beta + lb_k
        t1buf[k] = t1
        t2buf[k] = t2
        beta = jnp.where(tt >= t_len, jnp.where(k - tt == u_len, 0.0, NEG), logadd(t1, t2))
    segu[...] = jnp.zeros_like(segu)
    segt[...] = jnp.zeros_like(segt)
    log_p = beta[0:1, :]
    lane = lax.broadcasted_iota(jnp.int32, (n_t, 128), 1)
    loss_ref[...] = pltpu.roll(jnp.where(lane < u_hi - u_lo, -log_p, 0.0), u_lo, 1)
    lane_ok = lane < CORE_MAX
    for k in range(n_diag):
        for which, buf in enumerate((t1buf, t2buf)):
            occ = jnp.where(lane_ok, jnp.exp(jnp.minimum(abuf[k] + buf[k] - log_p, 0.0)), 0.0)
            hi, mid, lo = split3(occ)
            lo_row = which * n_kt + k * n_t
            gocc[lo_row:lo_row + n_t, :] = hi + pltpu.roll(mid, CORE_MAX, 1) + pltpu.roll(lo, 2 * CORE_MAX, 1)
    for which in range(2):
        gocc[which * n_kt + n_diag * n_t:(which + 1) * n_kt, :] = jnp.zeros((n_kt - n_diag * n_t, 128), F32)
    gocb[...] = gocc[...].astype(BF16)

    def again(first, count):
        def one(q, carry):
            i = first + q

            @pl.when(i >= KEEP)
            def _():
                def chunk(c, carry):
                    rows = pl.ds(pl.multiple_of(c * CHUNK, CHUNK), CHUNK)
                    z3 = dot(wot[rows, :], hbuf[i]).reshape(n_sub, 8, ROWS)
                    ebuf[KEEP + i % 2, rows, :] = jnp.exp(z3 - jnp.max(z3, axis=0)[None]).reshape(CHUNK, ROWS)
                    return carry
                lax.fori_loop(0, n_ch, chunk, 0)
            return carry
        @pl.when(first + count > KEEP)
        def _():
            lax.fori_loop(0, count, one, 0)

    def occupancy(i, par):
        orep = spread3(idx[i, 3:4], (1.0, 1.0, 1.0))
        kt8 = jnp.broadcast_to(idx[i, 2:3], (8, ROWS))
        kt_tile = lax.shift_right_arithmetic(kt8, 3)
        kt_sub = sub8 == jnp.bitwise_and(kt8, 7)
        for which in range(2):
            gath = dot(gocb[which * n_kt:(which + 1) * n_kt], orep).reshape(n_kt // 8, 8, ROWS)
            occ = jnp.zeros((8, ROWS), F32)
            for k in range(n_diag):
                occ = jnp.where(kt_tile == k, gath[k], occ)
            occ = jnp.sum(jnp.where(kt_sub, occ, 0.0), axis=0, keepdims=True)
            zrow[par, which * 8:which * 8 + 8] = jnp.broadcast_to(occ, (8, ROWS))

    def d_logits(i, par):
        y8 = ybuf[i]
        y_tile = lax.shift_right_logical(y8, 3)
        gb = zrow[par, 0:8]
        gl = zrow[par, 8:16]
        occ = gb + gl
        gl_y = jnp.where(sub8 == jnp.bitwise_and(y8, 7), gl, 0.0)
        gb_0 = jnp.where(sub8 == 0, gb, 0.0)
        slot = slot_of(i)
        for c in range(n_ch):
            sc_c = fac[i, c * 8:(c + 1) * 8, :] * occ
            e3 = ebuf[slot, c * CHUNK:(c + 1) * CHUNK, :].reshape(n_sub, 8, ROWS)
            tiles = []
            for k in range(n_sub):
                d = e3[k] * sc_c
                if c == 0 and k == 0:
                    d = d - gb_0
                tiles.append(d - jnp.where(y_tile == c * n_sub + k, gl_y, 0.0))
            d = jnp.concatenate(tiles, axis=0)
            dzb[par, c * CHUNK:(c + 1) * CHUNK, :] = d.astype(BF16)

    def segments(i, par):
        win = tbl[0, i]
        ohu = as_bf16(onehot(gu, idx[i, 0:1]))
        oht = frame_onehot(idx[i, 1:2])
        for q in range(2):
            rows = slice(q * half, (q + 1) * half)
            segu[rows, lanes_of(win)] += dot(dpb[par, rows], ohu, NT)
            segt[rows, frame_lanes_of(win)] += dot(dpb[par, rows], oht, NT)

    def d_hidden(i, par):
        for q in range(2):
            rows = slice(q * half, (q + 1) * half)
            hf = hbuf[i, rows].astype(F32)
            dh = dot(wo_ref[rows], dzb[par])
            dpb[par, rows] = (dh * (1.0 - hf * hf)).astype(BF16)

    def out_grad(blocks, add):
        for c in range(n_v // 256):
            cols = slice(c * 256, (c + 1) * 256)
            new = None
            for i, par in blocks:
                term = dot(hbuf[i], dzb[par, cols, :], NT)
                new = term if new is None else new + term
            gwo_ref[:, cols] = jnp.where(add, gwo_ref[:, cols], 0.0) + new

    def bwd_pair(p, carry):
        i = 2 * p
        again(i + 2, 2)
        d_hidden(i, 0)
        d_hidden(i + 1, 1)
        segments(i, 0)
        out_grad(((i, 0), (i + 1, 1)), p > 0)
        d_logits(i + 2, 0)
        segments(i + 1, 1)
        d_logits(i + 3, 1)
        occupancy(i + 4, 0)
        occupancy(i + 5, 1)
        return carry

    def bwd_odd(p, carry):
        d_hidden(n_blocks - 1, 0)
        out_grad(((n_blocks - 1, 0),), n_blocks > 1)
        segments(n_blocks - 1, 0)
        return carry

    load_wo.wait()
    again(0, 2)
    for first in range(2):
        occupancy(jnp.int32(first), first)
        d_logits(jnp.int32(first), first)
        occupancy(jnp.int32(first + 2), first)
    lax.fori_loop(0, n_blocks // 2, bwd_pair, 0)
    lax.fori_loop(0, n_blocks % 2, bwd_odd, 0)

    dc_ref[...] = segu[...].astype(BF16)
    da_ref[...] = segt[:, 0:n_utt * n_t].astype(BF16)


def core_call(c_t, a_t, wot, ylab, w_out, flen, llen, n_t, n_u):
    n_utt = flen.shape[0]
    n_j = c_t.shape[0]
    n_v = w_out.shape[1]
    max_blk = n_utt // 2 * n_t * n_u // ROWS + 6
    n_kt = (n_t + n_u) * n_t
    n_st = n_v // CHUNK * 8
    vm = pl.BlockSpec(memory_space=pltpu.VMEM)
    sm = pl.BlockSpec(memory_space=pltpu.SMEM)
    return pl.pallas_call(
        functools.partial(core_kernel, n_t, n_u),
        out_shape=(
            pltpu.VMEM((8, 128), F32),
            pltpu.VMEM((n_j, n_utt * n_u), BF16),
            pltpu.VMEM((n_j, n_utt * n_t), BF16),
            pltpu.VMEM(w_out.shape, F32),
        ),
        in_specs=[sm, sm] + [vm] * 6 + [pl.BlockSpec(memory_space=pltpu.HBM)],
        out_specs=(vm,) * 4,
        scratch_shapes=[
            pltpu.VMEM(w_out.shape, BF16),
            pltpu.SemaphoreType.DMA,
            pltpu.VMEM((max_blk, n_j, ROWS), BF16),
            pltpu.VMEM((2, n_j, ROWS), BF16),
            pltpu.VMEM((min(max_blk, KEEP + 2), n_v, ROWS), F32),
            pltpu.VMEM((max_blk, n_st, ROWS), F32),
            pltpu.VMEM((2, n_st, ROWS), F32),
            pltpu.VMEM((2, n_st, ROWS), F32),
            pltpu.VMEM((2, 256, ROWS), BF16),
            pltpu.VMEM((2, 8, ROWS), jnp.int32),
            pltpu.VMEM((max_blk, 8, ROWS), jnp.int32),
            pltpu.VMEM((max_blk, 8, ROWS), jnp.int32),
            pltpu.VMEM((2, n_v, ROWS), BF16),
            pltpu.VMEM((2, n_j, ROWS), BF16),
            pltpu.VMEM((2, 16, ROWS), F32),
            pltpu.VMEM((n_kt, 256), F32),
            pltpu.VMEM((n_t + n_u, n_t, 128), F32),
            pltpu.VMEM((n_t + n_u, n_t, 128), F32),
            pltpu.VMEM((n_t + n_u, n_t, 128), F32),
            pltpu.VMEM((2 * n_kt, 128), F32),
            pltpu.VMEM((2 * n_kt, 128), BF16),
            pltpu.VMEM((n_j, n_utt * n_u), F32),
            pltpu.VMEM((n_j, n_utt * n_t + 128), F32),
            pltpu.SMEM((3, max_blk), jnp.int32),
            pltpu.SMEM((n_utt + 1,), jnp.int32),
        ],
        compiler_params=pltpu.CompilerParams(vmem_limit_bytes=CORE_VMEM),
        name="rnnt_core",
    )(flen, llen, flen.reshape(1, n_utt), llen.reshape(1, n_utt), *[in_vmem(x) for x in (ylab, c_t, a_t, wot)], in_hbm(w_out))


def solution(mesh):
    seq_size = mesh.shape['seq']

    def local_fn(enc_out, pred_out, w_enc, w_pred, w_out, labels, frame_len, label_len):
        n_utt, n_loc, n_h = enc_out.shape
        n_u = pred_out.shape[1]
        n_t = n_loc * seq_size
        g2 = pred_out.reshape(n_utt * n_u, n_h)
        c_t, a_t, wot, f2, *rest = gather_call(enc_out, g2, w_enc, w_pred, w_out, labels.T, seq_size, n_t, n_u)
        loss, dc_t, da_t, gwo = core_call(c_t, a_t, wot, *rest, w_out, frame_len, label_len, n_t, n_u)
        loss, gf, gwe, gwp, gwo = store_call(reduce_call(gwo, dc_t, da_t, loss, g2, f2, w_enc, enc_out.shape, n_t))
        return loss.reshape(n_utt), gf, gwe, gwp, gwo

    in_specs = (P('dp', 'seq', None), P('dp', None, None), P(None, None), P(None, None), P(None, None), P('dp', None), P('dp'), P('dp'))
    out_specs = (P('dp'), P('dp', 'seq', None), P('dp', None), P('dp', None), P('dp', None))
    return jax.shard_map(local_fn, mesh=mesh, in_specs=in_specs, out_specs=out_specs, check_vma=False)
```

```python
import functools

import jax
import jax.numpy as jnp
from jax import lax
from jax.experimental import pallas as pl
from jax.experimental.pallas import tpu as pltpu
from jax.sharding import PartitionSpec as P

NEG = -1.0e30
ROWS = 256
WIN = 6
CHUNK = 128
CORE_MIN, CORE_MAX = 24, 40
GATHER_VMEM = 40 << 20
CORE_VMEM = 51 << 20
REDUCE_VMEM = 36 << 20
STORE_VMEM = 1 << 20
KEEP = 15
F32 = jnp.float32
BF16 = jnp.bfloat16
MESH = pl.DeviceIdType.MESH
NT = (((1,), (1,)), ((), ()))
NN = (((1,), (0,)), ((), ()))


def dot(a, b, dims=NN):
    return lax.dot_general(a, b, dims, preferred_element_type=F32)


def in_hbm(x):
    return pltpu.with_memory_space_constraint(x, pltpu.HBM)


def in_vmem(x):
    return pltpu.with_memory_space_constraint(x, pltpu.VMEM)


def split3(x):
    hi = x.astype(BF16).astype(F32)
    r1 = x - hi
    mid = r1.astype(BF16).astype(F32)
    return hi, mid, r1 - mid


def logadd(a, b):
    m = jnp.maximum(a, b)
    return m + jnp.log(1.0 + jnp.exp(jnp.minimum(a, b) - m))


def label_rows(n_u, first, n_rows, lab_ref):
    lab = lab_ref[...]
    n_lab, n_utt = lab.shape
    pad = jnp.zeros((n_u - n_lab, n_utt), F32)
    parts = [lax.shift_right_arithmetic(lab, 5).astype(F32), pad, jnp.bitwise_and(lab, 31).astype(F32), pad]
    both = jnp.concatenate(parts, axis=0).T.astype(BF16)
    row = lax.broadcasted_iota(jnp.int32, (n_rows, n_utt), 0)
    col = lax.broadcasted_iota(jnp.int32, (n_rows, n_utt), 1)
    spread = dot(jnp.where(row // n_u + first == col, 1.0, 0.0).astype(BF16), both)
    row = lax.broadcasted_iota(jnp.int32, (n_rows, 2 * n_u), 0)
    col = lax.broadcasted_iota(jnp.int32, (n_rows, 2 * n_u), 1)
    own = jnp.where(row % n_u == col % n_u, spread, 0.0).astype(BF16)
    place = (lax.broadcasted_iota(jnp.int32, (2 * n_u, 128), 0) // n_u == lax.broadcasted_iota(jnp.int32, (2 * n_u, 128), 1))
    return dot(own, jnp.where(place, 1.0, 0.0).astype(BF16)).astype(BF16)


def gather_kernel(n_t, n_u, enc_h, g_h, we_h, wp_h, wo_h, lab_h, c_ref, a_ref, wot_ref, f_ref, y_ref,
                  enc_ref, g_ref, we_ref, wp_ref, wo_ref, lab_ref, fbuf, in_sem, send_sem, recv_sem):
    me = lax.axis_index('seq')
    n_seq = fbuf.shape[0]
    partner = me + 1 - 2 * (me % 2)
    peer = (me + 2) % n_seq
    load_enc, load_wo, load_wp, load_g, load_we, load_lab = loads = [pltpu.make_async_copy(src, dst, in_sem.at[q]) for q, (src, dst) in enumerate(
        ((enc_h, enc_ref), (wo_h, wo_ref), (wp_h, wp_ref), (g_h, g_ref), (we_h, we_ref), (lab_h, lab_ref)))]
    for load in loads:
        load.start()
    barrier = pltpu.get_barrier_semaphore()
    for other in (partner, peer):
        pl.semaphore_signal(barrier, inc=1, device_id={'seq': other}, device_id_type=MESH)
    pl.semaphore_wait(barrier, 2)

    def send(src, slot, sem, other):
        return pltpu.make_async_remote_copy(src_ref=src, dst_ref=fbuf.at[slot], send_sem=send_sem.at[sem], recv_sem=recv_sem.at[sem],
                                            device_id={'seq': other}, device_id_type=MESH)
    load_enc.wait()
    to_peer = send(enc_ref, me, 0, peer)
    to_peer.start()
    to_partner = send(enc_ref, me, 1, partner)
    to_partner.start()
    fbuf[me] = enc_ref[...]
    load_wo.wait()
    wot_ref[...] = wo_ref[...].T
    load_wp.wait()
    load_g.wait()
    n_own_utt = CORE_MAX + WIN
    n_c = n_own_utt * n_u
    first = me % 2 * (c_ref.shape[0] // n_u - n_own_utt)
    rows_c = pl.ds(pl.multiple_of(first * n_u, 64), n_c)
    c_ref[rows_c, :] = dot(g_ref[rows_c, :], wp_ref[...]).astype(BF16)
    load_we.wait()
    load_lab.wait()
    y_ref[rows_c, :] = label_rows(n_u, first, n_c, lab_ref)
    n_f, n_h = f_ref.shape
    n_own = n_f // n_seq
    n_loc = n_t // n_seq
    col = lax.broadcasted_iota(jnp.int32, (n_f, n_own), 0)
    row = lax.broadcasted_iota(jnp.int32, (n_f, n_own), 1)

    def piece(p):
        rows = fbuf[p].reshape(n_own, n_h)
        f_ref[pl.ds(pl.multiple_of(p * n_own, n_own), n_own), :] = rows
        order = jnp.where(col == row // n_loc * n_t + p * n_loc + row % n_loc, 1.0, 0.0).astype(BF16)
        return dot(order, dot(rows, we_ref[...]).astype(BF16))
    a_t = piece(me)
    to_partner.wait_recv()
    a_t = a_t + piece(partner)
    to_peer.wait_recv()
    relay = send(fbuf.at[peer], peer, 2, partner)
    relay.start()
    a_t = a_t + piece(peer)
    relay.wait_recv()
    a_ref[...] = a_t + piece((partner + 2) % n_seq)
    to_peer.wait_send()
    to_partner.wait_send()
    relay.wait_send()


def gather_call(enc, g2, w_enc, w_pred, w_out, labels_t, n_seq, n_t, n_u):
    n_utt, n_loc, n_h = enc.shape
    n_j = w_enc.shape[1]
    vm = pl.BlockSpec(memory_space=pltpu.VMEM)
    n_f = n_utt * n_loc * n_seq
    args = [in_hbm(x) for x in (enc, g2, w_enc, w_pred, w_out, labels_t)]
    return pl.pallas_call(
        functools.partial(gather_kernel, n_t, n_u),
        out_shape=(
            pltpu.VMEM((g2.shape[0], n_j), BF16),
            pltpu.VMEM((n_f, n_j), F32),
            pltpu.VMEM(w_out.shape[::-1], BF16),
            pltpu.VMEM((n_f, n_h), BF16),
            pltpu.VMEM((g2.shape[0], 128), BF16),
        ),
        in_specs=[pl.BlockSpec(memory_space=pltpu.HBM)] * 6,
        out_specs=(vm,) * 5,
        scratch_shapes=[pltpu.VMEM(x.shape, x.dtype) for x in (enc, g2, w_enc, w_pred, w_out, labels_t)] + [
            pltpu.VMEM((n_seq, n_utt, n_loc, n_h), BF16),
            pltpu.SemaphoreType.DMA((6,)),
            pltpu.SemaphoreType.DMA((3,)),
            pltpu.SemaphoreType.DMA((3,)),
        ],
        compiler_params=pltpu.CompilerParams(collective_id=0, has_side_effects=True, vmem_limit_bytes=GATHER_VMEM),
        name="rnnt_gather",
    )(*args)


def reduce_kernel(n_t, gwo_v, dc_v, da_v, loss_v, f_v, g_p, we_p, loss_ref, gf_ref, gwe_ref, gwp_ref, gwo_ref,
                  g_v, we_v, gwp_v, rgwo, rgwp, rda, rloss, da_rows, in_sem, send_sem, recv_sem):
    me = lax.axis_index('seq')
    partner = me + 1 - 2 * (me % 2)
    loads = [pltpu.make_async_copy(src, dst, in_sem.at[q]) for q, (src, dst) in enumerate(((g_p, g_v), (we_p, we_v)))]
    for load in loads:
        load.start()
    barrier = pltpu.get_barrier_semaphore()
    pl.semaphore_signal(barrier, inc=1, device_id={'seq': partner}, device_id_type=MESH)
    pl.semaphore_wait(barrier, 1)

    def send(src, dst, sem):
        return pltpu.make_async_remote_copy(src_ref=src, dst_ref=dst, send_sem=send_sem.at[sem], recv_sem=recv_sem.at[sem],
                                            device_id={'seq': partner}, device_id_type=MESH)
    n_part = 4
    rows = gwo_v.shape[0] // n_part
    n_da = CORE_MAX * n_t
    da_lo = (da_v.shape[0] - n_da) * (me % 2)
    part = pl.ds(pl.multiple_of(da_lo, 64), n_da)
    sends = [send(da_v.at[part], rda.at[part], 0), send(loss_v, rloss, 1)]
    sends += [send(gwo_v.at[pl.ds(q * rows, rows)], rgwo.at[pl.ds(q * rows, rows)], 2 + q) for q in range(n_part)]
    for s in sends:
        s.start()
    loads[0].wait()
    gwp_v[...] = dot(g_v[...].T, dc_v[...])
    s_gwp = send(gwp_v, rgwp, 2 + n_part)
    loads[1].wait()
    sends[0].wait_recv()
    sends[1].wait_recv()
    loss_ref[...] = (loss_v[0:1, :] + rloss[0:1, :])[:, 0:loss_ref.shape[1]]
    row = lax.broadcasted_iota(jnp.int32, rda.shape, 0) - (da_v.shape[0] - n_da) * (partner % 2)
    other = jnp.where((row >= 0) & (row < n_da), rda[...].astype(F32), 0.0)
    da = (da_v[...].astype(F32) + other).astype(BF16)
    s_gwp.start()
    n_f = da.shape[0]
    n_loc = gf_ref.shape[1]
    n_own = gf_ref.shape[0] * n_loc
    row = lax.broadcasted_iota(jnp.int32, (n_f, n_f), 0)
    col = lax.broadcasted_iota(jnp.int32, (n_f, n_f), 1)
    order = jnp.where(col == row % n_own // n_loc * n_t + row // n_own * n_loc + row % n_loc, 1.0, 0.0).astype(BF16)
    da_f = dot(order, da).astype(BF16)
    da_rows[...] = da_f
    gwe_ref[...] = dot(f_v[...].T, da_f)
    own = da_rows[pl.ds(pl.multiple_of(me * n_own, n_own), n_own), :]
    gf_ref[...] = dot(own, we_v[...], NT).astype(BF16).reshape(gf_ref.shape)
    for q in range(n_part):
        sends[2 + q].wait_recv()
        part = slice(q * rows, (q + 1) * rows)
        gwo_ref[part] = gwo_v[part] + rgwo[part]
    s_gwp.wait_recv()
    gwp_ref[...] = gwp_v[...] + rgwp[...]
    for s in sends + [s_gwp]:
        s.wait_send()


def reduce_call(gwo, dc_t, da_t, loss, g2, f2, w_enc, gf_shape, n_t):
    vm = pl.BlockSpec(memory_space=pltpu.VMEM)
    like = lambda x: pltpu.VMEM(x.shape, x.dtype)
    gwp_shape = (g2.shape[1], dc_t.shape[1])
    return pl.pallas_call(
        functools.partial(reduce_kernel, n_t),
        out_shape=(
            pltpu.VMEM((1, f2.shape[0] // n_t), F32),
            pltpu.VMEM(gf_shape, BF16),
            pltpu.VMEM(w_enc.shape, F32),
            pltpu.VMEM(gwp_shape, F32),
            pltpu.VMEM(gwo.shape, F32),
        ),
        in_specs=[vm] * 5 + [pl.BlockSpec(memory_space=pltpu.HBM)] * 2,
        out_specs=(vm,) * 5,
        scratch_shapes=[like(x) for x in (g2, w_enc)] + [
            pltpu.VMEM(gwp_shape, F32), like(gwo), pltpu.VMEM(gwp_shape, F32), like(da_t), like(loss), like(da_t),
            pltpu.SemaphoreType.DMA((2,)),
            pltpu.SemaphoreType.DMA((7,)),
            pltpu.SemaphoreType.DMA((7,)),
        ],
        compiler_params=pltpu.CompilerParams(collective_id=1, has_side_effects=True, vmem_limit_bytes=REDUCE_VMEM),
        name="rnnt_reduce",
    )(in_vmem(gwo), in_vmem(dc_t), in_vmem(da_t), in_vmem(loss), in_vmem(f2), in_hbm(g2), in_hbm(w_enc))


def store_kernel(n, *refs):
    sems = refs[2 * n]
    copies = [pltpu.make_async_copy(refs[q], refs[n + q], sems.at[q]) for q in range(n)]
    for copy in copies:
        copy.start()
    for copy in copies:
        copy.wait()


def store_call(arrays):
    n = len(arrays)
    return pl.pallas_call(
        functools.partial(store_kernel, n),
        out_shape=tuple(pltpu.HBM(x.shape, x.dtype) for x in arrays),
        in_specs=[pl.BlockSpec(memory_space=pltpu.VMEM)] * n,
        out_specs=(pl.BlockSpec(memory_space=pltpu.HBM),) * n,
        scratch_shapes=[pltpu.SemaphoreType.DMA((n,))],
        compiler_params=pltpu.CompilerParams(vmem_limit_bytes=STORE_VMEM),
        name="rnnt_store",
    )(*[in_vmem(x) for x in arrays])


def core_kernel(n_t, n_u, flen_s, llen_s, flen_v, llen_v, y_buf, c_buf, a_buf, wot, wo_h,
                loss_ref, dc_ref, da_ref, gwo_ref,
                wo_ref, wo_sem, hbuf, hpar, ebuf, fac, mch, sch, vsb, ypar, ybuf, idx, dzb, dpb, zrow, sk, abuf, t1buf, t2buf,
                gocc, gocb, segu, segt, tbl, off):
    n_utt = flen_s.shape[0]
    n_j = c_buf.shape[1]
    n_v = wo_ref.shape[1]
    gu = WIN * n_u
    gt = WIN * n_t
    n_diag = n_t + n_u - 1
    n_kt = (n_diag + 1) * n_t
    n_ch = n_v // CHUNK

    load_wo = pltpu.make_async_copy(wo_h, wo_ref, wo_sem)
    load_wo.start()

    total = jnp.int32(0)
    for b in range(n_utt):
        off[b] = total
        total = total + flen_s[b] * (llen_s[b] + 1)
    off[n_utt] = total

    cut = jnp.int32(CORE_MIN)
    for b in range(CORE_MIN, CORE_MAX):
        cut = cut + jnp.where(off[b] + off[b + 1] <= total, 1, 0)
    first_core = lax.axis_index('seq') % 2 == 0
    u_lo = jnp.where(first_core, 0, cut)
    u_hi = jnp.where(first_core, cut, n_utt)
    stop = off[u_hi]

    def utt_step(b, carry):
        win = jnp.minimum(b, n_utt - WIN)
        base = off[win]
        last = jnp.minimum(off[win + WIN], stop)

        def emit(c):
            n, pos = c
            end = jnp.minimum(pos + ROWS, last)
            tbl[0, n] = win
            tbl[1, n] = pos - base
            tbl[2, n] = end - base
            return n + 1, end
        return lax.while_loop(lambda c: c[1] < off[b + 1], emit, carry)
    n_blocks, _ = lax.fori_loop(u_lo, u_hi, utt_step, (jnp.int32(0), off[u_lo]))
    for past in range(3):
        for q in range(3):
            tbl[q, n_blocks + past] = 0

    sk[...] = jnp.zeros_like(sk)
    mch[...] = jnp.zeros_like(mch)
    sch[...] = jnp.ones_like(sch)
    zrow[...] = jnp.zeros_like(zrow)
    vsb[...] = jnp.zeros_like(vsb)
    dpb[...] = jnp.zeros_like(dpb)

    def onehot(n, index_row):
        return (lax.broadcasted_iota(jnp.int32, (n, ROWS), 0) == index_row)

    def as_bf16(mask):
        return jnp.where(mask, 1.0, 0.0).astype(BF16)

    def block_onehot(i):
        iota = lax.broadcasted_iota(jnp.int32, (gu + gt, ROWS), 0)
        return jnp.concatenate([as_bf16(iota[0:gu] == idx[i, 0:1]), as_bf16(iota[gu:] == idx[i, 1:2])], axis=0)

    sub8 = lax.broadcasted_iota(jnp.int32, (8, ROWS), 0)
    n_sub = CHUNK // 8

    def rows_of(win, width):
        return pl.ds(pl.multiple_of(win * width, width), WIN * width)

    def spread3(idx_b, parts):
        mask = lax.broadcasted_iota(jnp.int32, (CORE_MAX, ROWS), 0) == idx_b
        return jnp.concatenate([jnp.where(mask, part, 0.0) for part in parts]
                               + [jnp.zeros((128 - 3 * CORE_MAX, ROWS), F32)], axis=0).astype(BF16)

    def locate(i):
        win = tbl[0, i]
        r = tbl[1, i] + lax.broadcasted_iota(jnp.int32, (1, ROWS), 1)
        end_r = tbl[2, i]
        start = jnp.int32(0)
        bl = jnp.full((1, ROWS), -1, jnp.int32)
        w = jnp.zeros((1, ROWS), jnp.int32)
        u1 = jnp.ones((1, ROWS), jnp.int32)
        for j in range(WIN):
            u1_j = llen_s[win + j] + 1
            end = start + flen_s[win + j] * u1_j
            inside = (r >= start) & (r < jnp.minimum(end, end_r))
            bl = jnp.where(inside, j, bl)
            w = jnp.where(inside, r - start, w)
            u1 = jnp.where(inside, u1_j, u1)
            start = end
        valid = bl >= 0
        t = jnp.zeros((1, ROWS), jnp.int32)
        for j in range(1, n_t):
            t = t + jnp.where(w >= j * u1, 1, 0)
        u = w - t * u1
        idx_u = jnp.where(valid, bl * n_u + u, -1)
        idx_t = jnp.where(valid, gu + bl * n_t + t, -1)
        idx_kt = jnp.where(valid, (t + u) * n_t + t, -1)
        idx_b = jnp.where(valid, win + bl - u_lo, -1024)
        rows8 = lax.broadcasted_iota(jnp.int32, (8, ROWS), 0)
        idx[i] = jnp.where(rows8 == 0, idx_u, jnp.where(rows8 == 1, idx_t, jnp.where(rows8 == 2, idx_kt, idx_b)))

    half = n_j // 2

    def hidden(i, par):
        win = tbl[0, i]
        oh = jnp.concatenate([block_onehot(i), jnp.zeros((256 - gu - gt, ROWS), BF16)], axis=0)
        none = jnp.zeros((256 - gu - gt, n_j), BF16)
        cols = jnp.concatenate([c_buf[rows_of(win, n_u)], a_buf[rows_of(win, n_t)].astype(BF16), none], axis=0).T
        for q in range(2):
            rows = slice(q * half, (q + 1) * half)
            pre = dot(cols[rows], oh)
            h = jnp.tanh(pre).astype(BF16)
            hpar[par, rows] = h
            hbuf[i, rows] = h
        yy = dot(jnp.concatenate(
            [y_buf[rows_of(win, n_u)], jnp.zeros((256 - gu, 128), BF16)], axis=0).T[0:16], oh)
        y8 = jnp.broadcast_to((yy[0:1] * 32.0 + yy[1:2]).astype(jnp.int32), (8, ROWS))
        ypar[par] = y8
        ybuf[i] = y8

    def finish(i, par):
        idx_b = idx[i, 3:4]
        m_all = mch[par]
        m8 = jnp.max(m_all.reshape(n_ch, 8, ROWS), axis=0)
        m = jnp.max(m8, axis=0, keepdims=True)
        f_all = jnp.exp(m_all - m)
        s = jnp.sum(jnp.sum((sch[par] * f_all).reshape(n_ch, 8, ROWS), axis=0), axis=0, keepdims=True)
        fac[i] = f_all * (1.0 / s)
        lse = m + jnp.log(s)
        b_parts = split3(zrow[par, 8:9] - lse)
        l_parts = split3(jnp.sum(zrow[par, 0:8], axis=0, keepdims=True) - lse)
        vsb[par, 0:128] = spread3(idx_b, b_parts)
        vsb[par, 128:256] = spread3(idx_b, l_parts)

    def scatter(i, par, live):
        okt = as_bf16(onehot(n_kt, jnp.where(live, idx[i, 2:3], -1)))
        part = n_kt // 2
        for q in range(2):
            sk[q * part:(q + 1) * part] += dot(okt[q * part:(q + 1) * part], vsb[par], NT)

    def slot_of(i):
        return jnp.where(i < KEEP, i, KEEP + i % 2)

    def scores_of(i, par):
        y8 = ypar[par]
        y_tile = lax.shift_right_logical(y8, 3)
        slot = slot_of(i)
        lz = jnp.zeros((8, ROWS), F32)
        for c in range(n_ch):
            z = dot(wot[c * CHUNK:(c + 1) * CHUNK, :], hpar[par])
            z3 = z.reshape(n_sub, 8, ROWS)
            for k in range(n_sub):
                lz = jnp.where(y_tile == c * n_sub + k, z3[k], lz)
            if c == 0:
                zrow[par, 8:16] = z[0:8, :]
            m_c = jnp.max(z3, axis=0)
            e3 = jnp.exp(z3 - m_c[None])
            ebuf[slot, c * CHUNK:(c + 1) * CHUNK, :] = e3.reshape(CHUNK, ROWS)
            mch[par, c * 8:(c + 1) * 8, :] = m_c
            sch[par, c * 8:(c + 1) * 8, :] = jnp.sum(e3, axis=0)
        zrow[par, 0:8] = jnp.where(sub8 == jnp.bitwise_and(y8, 7), lz, 0.0)

    def fwd_pair(p, carry):
        i = 2 * p
        hidden(i + 1, 1)
        finish(jnp.maximum(i - 1, 0), 1)
        scatter(jnp.maximum(i - 2, 0), 0, i > 1)
        scores_of(i, 0)
        hidden(i + 2, 0)
        scores_of(i + 1, 1)
        scatter(jnp.maximum(i - 1, 0), 1, i > 0)
        finish(i, 0)
        locate(i + 3)
        locate(i + 4)
        return carry

    def fwd_odd(p, carry):
        i = n_blocks - 1
        finish(jnp.maximum(i - 1, 0), 1)
        scatter(jnp.maximum(i - 2, 0), 0, i > 1)
        scores_of(i, 0)
        scatter(jnp.maximum(i - 1, 0), 1, i > 0)
        finish(i, 0)
        scatter(i, 0, True)
        return carry

    def fwd_even(p, carry):
        finish(n_blocks - 1, 1)
        scatter(n_blocks - 2, 0, True)
        scatter(n_blocks - 1, 1, True)
        return carry

    for first in range(3):
        locate(jnp.int32(first))
    hidden(jnp.int32(0), 0)
    lax.fori_loop(0, n_blocks // 2, fwd_pair, 0)
    lax.fori_loop(0, n_blocks % 2, fwd_odd, 0)
    lax.fori_loop(0, 1 - n_blocks % 2, fwd_even, 0)

    tt = lax.broadcasted_iota(jnp.int32, (n_t, 128), 0)
    def own_lanes(ref):
        x = jnp.concatenate([ref[...], jnp.zeros((1, 128 - n_utt), jnp.int32)], axis=1).astype(F32)
        return pltpu.roll(jnp.broadcast_to(x, (n_t, 128)), (128 - u_lo) % 128, 1).astype(jnp.int32)
    t_len = own_lanes(flen_v)
    u_len = own_lanes(llen_v)

    def scores(k):
        lo = k * n_t
        x, y = (v + pltpu.roll(v, 128 - CORE_MAX, 1) + pltpu.roll(v, 128 - 2 * CORE_MAX, 1)
                for v in (sk[lo:lo + n_t, 0:128], sk[lo:lo + n_t, 128:256]))
        uu = k - tt
        ok = (uu >= 0) & (tt < t_len)
        bl_k = jnp.where(ok & (uu <= u_len), x, NEG)
        lb_k = jnp.where(ok & (uu < u_len), y, NEG)
        return bl_k, lb_k

    alpha = jnp.where(tt == 0, 0.0, NEG).astype(F32)
    abuf[0] = alpha
    beta = jnp.full((n_t, 128), NEG, F32)
    sc = [scores(k) for k in range(n_diag)]
    for step in range(n_diag):
        if step > 0:
            bl_k, lb_k = sc[step - 1]
            p1 = jnp.where(tt == 0, NEG, pltpu.roll(alpha + bl_k, 1, 0))
            alpha = logadd(p1, alpha + lb_k)
            abuf[step] = alpha
        k = n_diag - 1 - step
        bl_k, lb_k = sc[k]
        up = jnp.where(tt == n_t - 1, jnp.where(u_len == k + 1 - n_t, 0.0, NEG), pltpu.roll(beta, n_t - 1, 0))
        t1 = up + bl_k
        t2 = beta + lb_k
        t1buf[k] = t1
        t2buf[k] = t2
        beta = jnp.where(tt >= t_len, jnp.where(k - tt == u_len, 0.0, NEG), logadd(t1, t2))
    segu[...] = jnp.zeros_like(segu)
    segt[...] = jnp.zeros_like(segt)
    log_p = beta[0:1, :]
    lane = lax.broadcasted_iota(jnp.int32, (n_t, 128), 1)
    loss_ref[...] = pltpu.roll(jnp.where(lane < u_hi - u_lo, -log_p, 0.0), u_lo, 1)
    lane_ok = lane < CORE_MAX
    for k in range(n_diag):
        for which, buf in enumerate((t1buf, t2buf)):
            occ = jnp.where(lane_ok, jnp.exp(jnp.minimum(abuf[k] + buf[k] - log_p, 0.0)), 0.0)
            hi, mid, lo = split3(occ)
            lo_row = which * n_kt + k * n_t
            gocc[lo_row:lo_row + n_t, :] = hi + pltpu.roll(mid, CORE_MAX, 1) + pltpu.roll(lo, 2 * CORE_MAX, 1)
    for which in range(2):
        gocc[which * n_kt + n_diag * n_t:(which + 1) * n_kt, :] = jnp.zeros((n_kt - n_diag * n_t, 128), F32)
    gocb[...] = gocc[...].astype(BF16)

    def again(first, count):
        def one(q, carry):
            i = first + q

            @pl.when(i >= KEEP)
            def _():
                def chunk(c, carry):
                    rows = pl.ds(pl.multiple_of(c * CHUNK, CHUNK), CHUNK)
                    z3 = dot(wot[rows, :], hbuf[i]).reshape(n_sub, 8, ROWS)
                    ebuf[KEEP + i % 2, rows, :] = jnp.exp(z3 - jnp.max(z3, axis=0)[None]).reshape(CHUNK, ROWS)
                    return carry
                lax.fori_loop(0, n_ch, chunk, 0)
            return carry
        @pl.when(first + count > KEEP)
        def _():
            lax.fori_loop(0, count, one, 0)

    def occupancy(i, par):
        orep = spread3(idx[i, 3:4], (1.0, 1.0, 1.0))
        kt8 = jnp.broadcast_to(idx[i, 2:3], (8, ROWS))
        kt_tile = lax.shift_right_arithmetic(kt8, 3)
        kt_sub = sub8 == jnp.bitwise_and(kt8, 7)
        for which in range(2):
            gath = dot(gocb[which * n_kt:(which + 1) * n_kt], orep).reshape(n_kt // 8, 8, ROWS)
            occ = jnp.zeros((8, ROWS), F32)
            for k in range(n_diag):
                occ = jnp.where(kt_tile == k, gath[k], occ)
            occ = jnp.sum(jnp.where(kt_sub, occ, 0.0), axis=0, keepdims=True)
            zrow[par, which * 8:which * 8 + 8] = jnp.broadcast_to(occ, (8, ROWS))

    def d_logits(i, par):
        y8 = ybuf[i]
        y_tile = lax.shift_right_logical(y8, 3)
        gb = zrow[par, 0:8]
        gl = zrow[par, 8:16]
        occ = gb + gl
        gl_y = jnp.where(sub8 == jnp.bitwise_and(y8, 7), gl, 0.0)
        gb_0 = jnp.where(sub8 == 0, gb, 0.0)
        slot = slot_of(i)
        for c in range(n_ch):
            sc_c = fac[i, c * 8:(c + 1) * 8, :] * occ
            e3 = ebuf[slot, c * CHUNK:(c + 1) * CHUNK, :].reshape(n_sub, 8, ROWS)
            tiles = []
            for k in range(n_sub):
                d = e3[k] * sc_c
                if c == 0 and k == 0:
                    d = d - gb_0
                tiles.append(d - jnp.where(y_tile == c * n_sub + k, gl_y, 0.0))
            d = jnp.concatenate(tiles, axis=0)
            dzb[par, c * CHUNK:(c + 1) * CHUNK, :] = d.astype(BF16)

    def segments(i, par):
        win = tbl[0, i]
        oh = block_onehot(i)
        for lo in range(0, n_j, 256):
            cols = slice(lo, min(lo + 256, n_j))
            sums = dot(oh, dpb[par, cols], NT)
            segu[rows_of(win, n_u), cols] += sums[0:gu]
            segt[rows_of(win, n_t), cols] += sums[gu:]

    def d_hidden(i, par):
        for q in range(2):
            rows = slice(q * half, (q + 1) * half)
            hf = hbuf[i, rows].astype(F32)
            dh = dot(wo_ref[rows], dzb[par])
            dpb[par, rows] = (dh * (1.0 - hf * hf)).astype(BF16)

    def out_grad(blocks, add):
        for c in range(n_v // 256):
            cols = slice(c * 256, (c + 1) * 256)
            new = None
            for i, par in blocks:
                term = dot(hbuf[i], dzb[par, cols, :], NT)
                new = term if new is None else new + term
            gwo_ref[:, cols] = jnp.where(add, gwo_ref[:, cols], 0.0) + new

    def bwd_pair(p, carry):
        i = 2 * p
        again(i + 2, 2)
        d_hidden(i, 0)
        d_hidden(i + 1, 1)
        segments(i, 0)
        out_grad(((i, 0), (i + 1, 1)), p > 0)
        d_logits(i + 2, 0)
        segments(i + 1, 1)
        d_logits(i + 3, 1)
        occupancy(i + 4, 0)
        occupancy(i + 5, 1)
        return carry

    def bwd_odd(p, carry):
        d_hidden(n_blocks - 1, 0)
        out_grad(((n_blocks - 1, 0),), n_blocks > 1)
        segments(n_blocks - 1, 0)
        return carry

    load_wo.wait()
    again(0, 2)
    for first in range(2):
        occupancy(jnp.int32(first), first)
        d_logits(jnp.int32(first), first)
        occupancy(jnp.int32(first + 2), first)
    lax.fori_loop(0, n_blocks // 2, bwd_pair, 0)
    lax.fori_loop(0, n_blocks % 2, bwd_odd, 0)

    dc_ref[...] = segu[...].astype(BF16)
    da_ref[...] = segt[...].astype(BF16)


def core_call(c_t, a_t, wot, ylab, w_out, flen, llen, n_t, n_u):
    n_utt = flen.shape[0]
    n_j = c_t.shape[1]
    n_v = w_out.shape[1]
    max_blk = n_utt // 2 * n_t * n_u // ROWS + 6
    n_kt = (n_t + n_u) * n_t
    n_st = n_v // CHUNK * 8
    vm = pl.BlockSpec(memory_space=pltpu.VMEM)
    sm = pl.BlockSpec(memory_space=pltpu.SMEM)
    return pl.pallas_call(
        functools.partial(core_kernel, n_t, n_u),
        out_shape=(
            pltpu.VMEM((8, 128), F32),
            pltpu.VMEM((n_utt * n_u, n_j), BF16),
            pltpu.VMEM((n_utt * n_t, n_j), BF16),
            pltpu.VMEM(w_out.shape, F32),
        ),
        in_specs=[sm, sm] + [vm] * 6 + [pl.BlockSpec(memory_space=pltpu.HBM)],
        out_specs=(vm,) * 4,
        scratch_shapes=[
            pltpu.VMEM(w_out.shape, BF16),
            pltpu.SemaphoreType.DMA,
            pltpu.VMEM((max_blk, n_j, ROWS), BF16),
            pltpu.VMEM((2, n_j, ROWS), BF16),
            pltpu.VMEM((min(max_blk, KEEP + 2), n_v, ROWS), F32),
            pltpu.VMEM((max_blk, n_st, ROWS), F32),
            pltpu.VMEM((2, n_st, ROWS), F32),
            pltpu.VMEM((2, n_st, ROWS), F32),
            pltpu.VMEM((2, 256, ROWS), BF16),
            pltpu.VMEM((2, 8, ROWS), jnp.int32),
            pltpu.VMEM((max_blk, 8, ROWS), jnp.int32),
            pltpu.VMEM((max_blk, 8, ROWS), jnp.int32),
            pltpu.VMEM((2, n_v, ROWS), BF16),
            pltpu.VMEM((2, n_j, ROWS), BF16),
            pltpu.VMEM((2, 16, ROWS), F32),
            pltpu.VMEM((n_kt, 256), F32),
            pltpu.VMEM((n_t + n_u, n_t, 128), F32),
            pltpu.VMEM((n_t + n_u, n_t, 128), F32),
            pltpu.VMEM((n_t + n_u, n_t, 128), F32),
            pltpu.VMEM((2 * n_kt, 128), F32),
            pltpu.VMEM((2 * n_kt, 128), BF16),
            pltpu.VMEM((n_utt * n_u, n_j), F32),
            pltpu.VMEM((n_utt * n_t, n_j), F32),
            pltpu.SMEM((3, max_blk), jnp.int32),
            pltpu.SMEM((n_utt + 1,), jnp.int32),
        ],
        compiler_params=pltpu.CompilerParams(vmem_limit_bytes=CORE_VMEM),
        name="rnnt_core",
    )(flen, llen, flen.reshape(1, n_utt), llen.reshape(1, n_utt), *[in_vmem(x) for x in (ylab, c_t, a_t, wot)], in_hbm(w_out))


def solution(mesh):
    seq_size = mesh.shape['seq']

    def local_fn(enc_out, pred_out, w_enc, w_pred, w_out, labels, frame_len, label_len):
        n_utt, n_loc, n_h = enc_out.shape
        n_u = pred_out.shape[1]
        n_t = n_loc * seq_size
        g2 = pred_out.reshape(n_utt * n_u, n_h)
        c_t, a_t, wot, f2, *rest = gather_call(enc_out, g2, w_enc, w_pred, w_out, labels.T, seq_size, n_t, n_u)
        loss, dc_t, da_t, gwo = core_call(c_t, a_t, wot, *rest, w_out, frame_len, label_len, n_t, n_u)
        loss, gf, gwe, gwp, gwo = store_call(reduce_call(gwo, dc_t, da_t, loss, g2, f2, w_enc, enc_out.shape, n_t))
        return loss.reshape(n_utt), gf, gwe, gwp, gwo

    in_specs = (P('dp', 'seq', None), P('dp', None, None), P(None, None), P(None, None), P(None, None), P('dp', None), P('dp'), P('dp'))
    out_specs = (P('dp'), P('dp', 'seq', None), P('dp', None), P('dp', None), P('dp', None))
    return jax.shard_map(local_fn, mesh=mesh, in_specs=in_specs, out_specs=out_specs, check_vma=False)
```

```python
import functools

import jax
import jax.numpy as jnp
from jax import lax
from jax.experimental import pallas as pl
from jax.experimental.pallas import tpu as pltpu
from jax.sharding import PartitionSpec as P

NEG = -1.0e30
ROWS = 256
WIN = 6
CHUNK = 256
CORE_MIN, CORE_MAX = 24, 40
GATHER_VMEM = 40 << 20
CORE_VMEM = 47 << 20
REDUCE_VMEM = 36 << 20
STORE_VMEM = 1 << 20
KEEP = 15
F32 = jnp.float32
BF16 = jnp.bfloat16
MESH = pl.DeviceIdType.MESH
NT = (((1,), (1,)), ((), ()))
NN = (((1,), (0,)), ((), ()))


def dot(a, b, dims=NN):
    return lax.dot_general(a, b, dims, preferred_element_type=F32)


def in_hbm(x):
    return pltpu.with_memory_space_constraint(x, pltpu.HBM)


def in_vmem(x):
    return pltpu.with_memory_space_constraint(x, pltpu.VMEM)


def split3(x):
    hi = x.astype(BF16).astype(F32)
    r1 = x - hi
    mid = r1.astype(BF16).astype(F32)
    return hi, mid, r1 - mid


def logadd(a, b):
    m = jnp.maximum(a, b)
    return m + jnp.log(1.0 + jnp.exp(jnp.minimum(a, b) - m))


def label_rows(n_u, first, n_rows, lab_ref):
    lab = lab_ref[...]
    n_lab, n_utt = lab.shape
    pad = jnp.zeros((n_u - n_lab, n_utt), F32)
    parts = [lax.shift_right_arithmetic(lab, 5).astype(F32), pad, jnp.bitwise_and(lab, 31).astype(F32), pad]
    both = jnp.concatenate(parts, axis=0).T.astype(BF16)
    row = lax.broadcasted_iota(jnp.int32, (n_rows, n_utt), 0)
    col = lax.broadcasted_iota(jnp.int32, (n_rows, n_utt), 1)
    spread = dot(jnp.where(row // n_u + first == col, 1.0, 0.0).astype(BF16), both)
    row = lax.broadcasted_iota(jnp.int32, (n_rows, 2 * n_u), 0)
    col = lax.broadcasted_iota(jnp.int32, (n_rows, 2 * n_u), 1)
    own = jnp.where(row % n_u == col % n_u, spread, 0.0).astype(BF16)
    place = (lax.broadcasted_iota(jnp.int32, (2 * n_u, 128), 0) // n_u == lax.broadcasted_iota(jnp.int32, (2 * n_u, 128), 1))
    return dot(own, jnp.where(place, 1.0, 0.0).astype(BF16)).astype(BF16)


def gather_kernel(n_t, n_u, enc_h, g_h, we_h, wp_h, wo_h, lab_h, c_ref, a_ref, wot_ref, f_ref, y_ref,
                  enc_ref, g_ref, we_ref, wp_ref, wo_ref, lab_ref, fbuf, in_sem, send_sem, recv_sem):
    me = lax.axis_index('seq')
    n_seq = fbuf.shape[0]
    partner = me + 1 - 2 * (me % 2)
    peer = (me + 2) % n_seq
    load_enc, load_wo, load_wp, load_g, load_we, load_lab = loads = [pltpu.make_async_copy(src, dst, in_sem.at[q]) for q, (src, dst) in enumerate(
        ((enc_h, enc_ref), (wo_h, wo_ref), (wp_h, wp_ref), (g_h, g_ref), (we_h, we_ref), (lab_h, lab_ref)))]
    for load in loads:
        load.start()
    barrier = pltpu.get_barrier_semaphore()
    for other in (partner, peer):
        pl.semaphore_signal(barrier, inc=1, device_id={'seq': other}, device_id_type=MESH)
    pl.semaphore_wait(barrier, 2)

    def send(src, slot, sem, other):
        return pltpu.make_async_remote_copy(src_ref=src, dst_ref=fbuf.at[slot], send_sem=send_sem.at[sem], recv_sem=recv_sem.at[sem],
                                            device_id={'seq': other}, device_id_type=MESH)
    load_enc.wait()
    to_peer = send(enc_ref, me, 0, peer)
    to_peer.start()
    to_partner = send(enc_ref, me, 1, partner)
    to_partner.start()
    fbuf[me] = enc_ref[...]
    load_wo.wait()
    wot_ref[...] = wo_ref[...].T
    load_wp.wait()
    load_g.wait()
    n_own_utt = CORE_MAX + WIN
    n_c = n_own_utt * n_u
    first = me % 2 * (c_ref.shape[0] // n_u - n_own_utt)
    rows_c = pl.ds(pl.multiple_of(first * n_u, 64), n_c)
    c_ref[rows_c, :] = dot(g_ref[rows_c, :], wp_ref[...]).astype(BF16)
    load_we.wait()
    load_lab.wait()
    y_ref[rows_c, :] = label_rows(n_u, first, n_c, lab_ref)
    n_f, n_h = f_ref.shape
    n_own = n_f // n_seq
    n_loc = n_t // n_seq
    col = lax.broadcasted_iota(jnp.int32, (n_f, n_own), 0)
    row = lax.broadcasted_iota(jnp.int32, (n_f, n_own), 1)

    def piece(p):
        rows = fbuf[p].reshape(n_own, n_h)
        f_ref[pl.ds(pl.multiple_of(p * n_own, n_own), n_own), :] = rows
        order = jnp.where(col == row // n_loc * n_t + p * n_loc + row % n_loc, 1.0, 0.0).astype(BF16)
        return dot(order, dot(rows, we_ref[...]).astype(BF16))
    a_t = piece(me)
    to_partner.wait_recv()
    a_t = a_t + piece(partner)
    to_peer.wait_recv()
    relay = send(fbuf.at[peer], peer, 2, partner)
    relay.start()
    a_t = a_t + piece(peer)
    relay.wait_recv()
    a_ref[...] = a_t + piece((partner + 2) % n_seq)
    to_peer.wait_send()
    to_partner.wait_send()
    relay.wait_send()


def gather_call(enc, g2, w_enc, w_pred, w_out, labels_t, n_seq, n_t, n_u):
    n_utt, n_loc, n_h = enc.shape
    n_j = w_enc.shape[1]
    vm = pl.BlockSpec(memory_space=pltpu.VMEM)
    n_f = n_utt * n_loc * n_seq
    args = [in_hbm(x) for x in (enc, g2, w_enc, w_pred, w_out, labels_t)]
    return pl.pallas_call(
        functools.partial(gather_kernel, n_t, n_u),
        out_shape=(
            pltpu.VMEM((g2.shape[0], n_j), BF16),
            pltpu.VMEM((n_f, n_j), F32),
            pltpu.VMEM(w_out.shape[::-1], BF16),
            pltpu.VMEM((n_f, n_h), BF16),
            pltpu.VMEM((g2.shape[0], 128), BF16),
        ),
        in_specs=[pl.BlockSpec(memory_space=pltpu.HBM)] * 6,
        out_specs=(vm,) * 5,
        scratch_shapes=[pltpu.VMEM(x.shape, x.dtype) for x in (enc, g2, w_enc, w_pred, w_out, labels_t)] + [
            pltpu.VMEM((n_seq, n_utt, n_loc, n_h), BF16),
            pltpu.SemaphoreType.DMA((6,)),
            pltpu.SemaphoreType.DMA((3,)),
            pltpu.SemaphoreType.DMA((3,)),
        ],
        compiler_params=pltpu.CompilerParams(collective_id=0, has_side_effects=True, vmem_limit_bytes=GATHER_VMEM),
        name="rnnt_gather",
    )(*args)


def reduce_kernel(n_t, gwo_v, dc_v, da_v, loss_v, f_v, g_p, we_p, loss_ref, gf_ref, gwe_ref, gwp_ref, gwo_ref,
                  g_v, we_v, gwp_v, rgwo, rgwp, rda, rloss, da_rows, in_sem, send_sem, recv_sem):
    me = lax.axis_index('seq')
    partner = me + 1 - 2 * (me % 2)
    loads = [pltpu.make_async_copy(src, dst, in_sem.at[q]) for q, (src, dst) in enumerate(((g_p, g_v), (we_p, we_v)))]
    for load in loads:
        load.start()
    barrier = pltpu.get_barrier_semaphore()
    pl.semaphore_signal(barrier, inc=1, device_id={'seq': partner}, device_id_type=MESH)
    pl.semaphore_wait(barrier, 1)

    def send(src, dst, sem):
        return pltpu.make_async_remote_copy(src_ref=src, dst_ref=dst, send_sem=send_sem.at[sem], recv_sem=recv_sem.at[sem],
                                            device_id={'seq': partner}, device_id_type=MESH)
    n_part = 4
    rows = gwo_v.shape[0] // n_part
    n_da = CORE_MAX * n_t
    da_lo = (da_v.shape[0] - n_da) * (me % 2)
    part = pl.ds(pl.multiple_of(da_lo, 64), n_da)
    sends = [send(da_v.at[part], rda.at[part], 0), send(loss_v, rloss, 1)]
    sends += [send(gwo_v.at[pl.ds(q * rows, rows)], rgwo.at[pl.ds(q * rows, rows)], 2 + q) for q in range(n_part)]
    for s in sends:
        s.start()
    loads[0].wait()
    gwp_v[...] = dot(g_v[...].T, dc_v[...].astype(BF16))
    s_gwp = send(gwp_v, rgwp, 2 + n_part)
    loads[1].wait()
    sends[0].wait_recv()
    sends[1].wait_recv()
    loss_ref[...] = (loss_v[0:1, :] + rloss[0:1, :])[:, 0:loss_ref.shape[1]]
    row = lax.broadcasted_iota(jnp.int32, rda.shape, 0) - (da_v.shape[0] - n_da) * (partner % 2)
    other = jnp.where((row >= 0) & (row < n_da), rda[...].astype(F32), 0.0)
    da = (da_v[...].astype(F32) + other).astype(BF16)
    s_gwp.start()
    n_f = da.shape[0]
    n_loc = gf_ref.shape[1]
    n_own = gf_ref.shape[0] * n_loc
    row = lax.broadcasted_iota(jnp.int32, (n_f, n_f), 0)
    col = lax.broadcasted_iota(jnp.int32, (n_f, n_f), 1)
    order = jnp.where(col == row % n_own // n_loc * n_t + row // n_own * n_loc + row % n_loc, 1.0, 0.0).astype(BF16)
    da_f = dot(order, da).astype(BF16)
    da_rows[...] = da_f
    gwe_ref[...] = dot(f_v[...].T, da_f)
    own = da_rows[pl.ds(pl.multiple_of(me * n_own, n_own), n_own), :]
    gf_ref[...] = dot(own, we_v[...], NT).astype(BF16).reshape(gf_ref.shape)
    for q in range(n_part):
        sends[2 + q].wait_recv()
        part = slice(q * rows, (q + 1) * rows)
        gwo_ref[part] = gwo_v[part] + rgwo[part]
    s_gwp.wait_recv()
    gwp_ref[...] = gwp_v[...] + rgwp[...]
    for s in sends + [s_gwp]:
        s.wait_send()


def reduce_call(gwo, dc_t, da_t, loss, g2, f2, w_enc, gf_shape, n_t):
    vm = pl.BlockSpec(memory_space=pltpu.VMEM)
    like = lambda x: pltpu.VMEM(x.shape, x.dtype)
    gwp_shape = (g2.shape[1], dc_t.shape[1])
    return pl.pallas_call(
        functools.partial(reduce_kernel, n_t),
        out_shape=(
            pltpu.VMEM((1, f2.shape[0] // n_t), F32),
            pltpu.VMEM(gf_shape, BF16),
            pltpu.VMEM(w_enc.shape, F32),
            pltpu.VMEM(gwp_shape, F32),
            pltpu.VMEM(gwo.shape, F32),
        ),
        in_specs=[vm] * 5 + [pl.BlockSpec(memory_space=pltpu.HBM)] * 2,
        out_specs=(vm,) * 5,
        scratch_shapes=[like(x) for x in (g2, w_enc)] + [
            pltpu.VMEM(gwp_shape, F32), like(gwo), pltpu.VMEM(gwp_shape, F32), like(da_t), like(loss), like(da_t),
            pltpu.SemaphoreType.DMA((2,)),
            pltpu.SemaphoreType.DMA((7,)),
            pltpu.SemaphoreType.DMA((7,)),
        ],
        compiler_params=pltpu.CompilerParams(collective_id=1, has_side_effects=True, vmem_limit_bytes=REDUCE_VMEM),
        name="rnnt_reduce",
    )(in_vmem(gwo), in_vmem(dc_t), in_vmem(da_t), in_vmem(loss), in_vmem(f2), in_hbm(g2), in_hbm(w_enc))


def store_kernel(n, *refs):
    sems = refs[2 * n]
    copies = [pltpu.make_async_copy(refs[q], refs[n + q], sems.at[q]) for q in range(n)]
    for copy in copies:
        copy.start()
    for copy in copies:
        copy.wait()


def store_call(arrays):
    n = len(arrays)
    return pl.pallas_call(
        functools.partial(store_kernel, n),
        out_shape=tuple(pltpu.HBM(x.shape, x.dtype) for x in arrays),
        in_specs=[pl.BlockSpec(memory_space=pltpu.VMEM)] * n,
        out_specs=(pl.BlockSpec(memory_space=pltpu.HBM),) * n,
        scratch_shapes=[pltpu.SemaphoreType.DMA((n,))],
        compiler_params=pltpu.CompilerParams(vmem_limit_bytes=STORE_VMEM),
        name="rnnt_store",
    )(*[in_vmem(x) for x in arrays])


def core_kernel(n_t, n_u, flen_s, llen_s, flen_v, llen_v, y_buf, c_buf, a_buf, wot, wo_h,
                loss_ref, segu, da_ref, gwo_ref,
                wo_ref, wo_sem, hbuf, hpar, ebuf, fac, mch, sch, vsb, ypar, ybuf, idx, dzb, dpb, zrow, sk, abuf, t1buf, t2buf,
                gocc, gocb, segt, tbl, off):
    n_utt = flen_s.shape[0]
    n_j = c_buf.shape[1]
    n_v = wo_ref.shape[1]
    gu = WIN * n_u
    gt = WIN * n_t
    n_diag = n_t + n_u - 1
    n_kt = (n_diag + 1) * n_t
    n_ch = n_v // CHUNK

    load_wo = pltpu.make_async_copy(wo_h, wo_ref, wo_sem)
    load_wo.start()

    total = jnp.int32(0)
    for b in range(n_utt):
        off[b] = total
        total = total + flen_s[b] * (llen_s[b] + 1)
    off[n_utt] = total

    cut = jnp.int32(CORE_MIN)
    for b in range(CORE_MIN, CORE_MAX):
        cut = cut + jnp.where(off[b] + off[b + 1] <= total, 1, 0)
    first_core = lax.axis_index('seq') % 2 == 0
    u_lo = jnp.where(first_core, 0, cut)
    u_hi = jnp.where(first_core, cut, n_utt)
    stop = off[u_hi]

    def utt_step(b, carry):
        win = jnp.minimum(b, n_utt - WIN)
        base = off[win]
        last = jnp.minimum(off[win + WIN], stop)

        def emit(c):
            n, pos = c
            end = jnp.minimum(pos + ROWS, last)
            tbl[0, n] = win
            tbl[1, n] = pos - base
            tbl[2, n] = end - base
            return n + 1, end
        return lax.while_loop(lambda c: c[1] < off[b + 1], emit, carry)
    n_blocks, _ = lax.fori_loop(u_lo, u_hi, utt_step, (jnp.int32(0), off[u_lo]))
    for past in range(3):
        for q in range(3):
            tbl[q, n_blocks + past] = 0

    sk[...] = jnp.zeros_like(sk)
    mch[...] = jnp.zeros_like(mch)
    sch[...] = jnp.ones_like(sch)
    zrow[...] = jnp.zeros_like(zrow)
    vsb[...] = jnp.zeros_like(vsb)
    dpb[...] = jnp.zeros_like(dpb)

    def onehot(n, index_row):
        return (lax.broadcasted_iota(jnp.int32, (n, ROWS), 0) == index_row)

    def as_bf16(mask):
        return jnp.where(mask, 1.0, 0.0).astype(BF16)

    def block_onehot(i):
        iota = lax.broadcasted_iota(jnp.int32, (gu + gt, ROWS), 0)
        return jnp.concatenate([as_bf16(iota[0:gu] == idx[i, 0:1]), as_bf16(iota[gu:] == idx[i, 1:2])], axis=0)

    sub8 = lax.broadcasted_iota(jnp.int32, (8, ROWS), 0)
    n_sub = CHUNK // 8

    def rows_of(win, width):
        return pl.ds(pl.multiple_of(win * width, width), WIN * width)

    def spread3(idx_b, parts):
        mask = lax.broadcasted_iota(jnp.int32, (CORE_MAX, ROWS), 0) == idx_b
        return jnp.concatenate([jnp.where(mask, part, 0.0) for part in parts]
                               + [jnp.zeros((128 - 3 * CORE_MAX, ROWS), F32)], axis=0).astype(BF16)

    def locate(i):
        win = tbl[0, i]
        r = tbl[1, i] + lax.broadcasted_iota(jnp.int32, (1, ROWS), 1)
        end_r = tbl[2, i]
        start = jnp.int32(0)
        bl = jnp.full((1, ROWS), -1, jnp.int32)
        w = jnp.zeros((1, ROWS), jnp.int32)
        u1 = jnp.ones((1, ROWS), jnp.int32)
        for j in range(WIN):
            u1_j = llen_s[win + j] + 1
            end = start + flen_s[win + j] * u1_j
            inside = (r >= start) & (r < jnp.minimum(end, end_r))
            bl = jnp.where(inside, j, bl)
            w = jnp.where(inside, r - start, w)
            u1 = jnp.where(inside, u1_j, u1)
            start = end
        valid = bl >= 0
        t = jnp.zeros((1, ROWS), jnp.int32)
        for j in range(1, n_t):
            t = t + jnp.where(w >= j * u1, 1, 0)
        u = w - t * u1
        idx_u = jnp.where(valid, bl * n_u + u, -1)
        idx_t = jnp.where(valid, gu + bl * n_t + t, -1)
        idx_kt = jnp.where(valid, (t + u) * n_t + t, -1)
        idx_b = jnp.where(valid, win + bl - u_lo, -1024)
        rows8 = lax.broadcasted_iota(jnp.int32, (8, ROWS), 0)
        idx[i] = jnp.where(rows8 == 0, idx_u, jnp.where(rows8 == 1, idx_t, jnp.where(rows8 == 2, idx_kt, idx_b)))

    half = n_j // 2

    def hidden(i, par):
        win = tbl[0, i]
        oh = jnp.concatenate([block_onehot(i), jnp.zeros((256 - gu - gt, ROWS), BF16)], axis=0)
        none = jnp.zeros((256 - gu - gt, n_j), BF16)
        cols = jnp.concatenate([c_buf[rows_of(win, n_u)], a_buf[rows_of(win, n_t)].astype(BF16), none], axis=0).T
        for q in range(2):
            rows = slice(q * half, (q + 1) * half)
            pre = dot(cols[rows], oh)
            h = jnp.tanh(pre).astype(BF16)
            hpar[par, rows] = h
            hbuf[i, rows] = h
        yy = dot(jnp.concatenate(
            [y_buf[rows_of(win, n_u)], jnp.zeros((256 - gu, 128), BF16)], axis=0).T[0:16], oh)
        y8 = jnp.broadcast_to((yy[0:1] * 32.0 + yy[1:2]).astype(jnp.int32), (8, ROWS))
        ypar[par] = y8
        ybuf[i] = y8

    def finish(i, par):
        idx_b = idx[i, 3:4]
        m_all = mch[par]
        m8 = jnp.max(m_all.reshape(n_ch, 8, ROWS), axis=0)
        m = jnp.max(m8, axis=0, keepdims=True)
        f_all = jnp.exp(m_all - m)
        s = jnp.sum(jnp.sum((sch[par] * f_all).reshape(n_ch, 8, ROWS), axis=0), axis=0, keepdims=True)
        fac[i] = f_all * (1.0 / s)
        lse = m + jnp.log(s)
        b_parts = split3(zrow[par, 8:9] - lse)
        l_parts = split3(jnp.sum(zrow[par, 0:8], axis=0, keepdims=True) - lse)
        vsb[par, 0:128] = spread3(idx_b, b_parts)
        vsb[par, 128:256] = spread3(idx_b, l_parts)

    def scatter(i, par, live):
        okt = as_bf16(onehot(n_kt, jnp.where(live, idx[i, 2:3], -1)))
        part = n_kt // 2
        for q in range(2):
            sk[q * part:(q + 1) * part] += dot(okt[q * part:(q + 1) * part], vsb[par], NT)

    def slot_of(i):
        return jnp.where(i < KEEP, i, KEEP + i % 2)

    def scores_part(i, par, chunks, lz):
        y8 = ypar[par]
        y_tile = lax.shift_right_logical(y8, 3)
        slot = slot_of(i)
        for c in chunks:
            z = dot(wot[c * CHUNK:(c + 1) * CHUNK, :], hpar[par])
            z3 = z.reshape(n_sub, 8, ROWS)
            for k in range(n_sub):
                lz = jnp.where(y_tile == c * n_sub + k, z3[k], lz)
            if c == 0:
                zrow[par, 8:16] = z[0:8, :]
            m_c = jnp.max(z3, axis=0)
            e3 = jnp.exp(z3 - m_c[None])
            ebuf[slot, c * CHUNK:(c + 1) * CHUNK, :] = e3.reshape(CHUNK, ROWS)
            mch[par, c * 8:(c + 1) * 8, :] = m_c
            sch[par, c * 8:(c + 1) * 8, :] = jnp.sum(e3, axis=0)
        if chunks[-1] == n_ch - 1:
            zrow[par, 0:8] = jnp.where(sub8 == jnp.bitwise_and(y8, 7), lz, 0.0)
        return lz

    def scores_of(i, par):
        scores_part(i, par, range(n_ch), jnp.zeros((8, ROWS), F32))

    def fwd_pair(p, carry):
        i = 2 * p
        finish(jnp.maximum(i - 1, 0), 1)
        hidden(i + 1, 1)
        scatter(jnp.maximum(i - 2, 0), 0, i > 1)
        scores_of(i, 0)
        hidden(i + 2, 0)
        scores_of(i + 1, 1)
        scatter(jnp.maximum(i - 1, 0), 1, i > 0)
        finish(i, 0)
        locate(i + 3)
        locate(i + 4)
        return carry

    def fwd_odd(p, carry):
        i = n_blocks - 1
        finish(jnp.maximum(i - 1, 0), 1)
        scatter(jnp.maximum(i - 2, 0), 0, i > 1)
        scores_of(i, 0)
        scatter(jnp.maximum(i - 1, 0), 1, i > 0)
        finish(i, 0)
        scatter(i, 0, True)
        return carry

    def fwd_even(p, carry):
        finish(n_blocks - 1, 1)
        scatter(n_blocks - 2, 0, True)
        scatter(n_blocks - 1, 1, True)
        return carry

    for first in range(3):
        locate(jnp.int32(first))
    hidden(jnp.int32(0), 0)
    lax.fori_loop(0, n_blocks // 2, fwd_pair, 0)
    lax.fori_loop(0, n_blocks % 2, fwd_odd, 0)
    lax.fori_loop(0, 1 - n_blocks % 2, fwd_even, 0)

    tt = lax.broadcasted_iota(jnp.int32, (n_t, 128), 0)
    def own_lanes(ref):
        x = jnp.concatenate([ref[...], jnp.zeros((1, 128 - n_utt), jnp.int32)], axis=1).astype(F32)
        return pltpu.roll(jnp.broadcast_to(x, (n_t, 128)), (128 - u_lo) % 128, 1).astype(jnp.int32)
    t_len = own_lanes(flen_v)
    u_len = own_lanes(llen_v)

    def scores(k):
        lo = k * n_t
        x, y = (v + pltpu.roll(v, 128 - CORE_MAX, 1) + pltpu.roll(v, 128 - 2 * CORE_MAX, 1)
                for v in (sk[lo:lo + n_t, 0:128], sk[lo:lo + n_t, 128:256]))
        uu = k - tt
        ok = (uu >= 0) & (tt < t_len)
        bl_k = jnp.where(ok & (uu <= u_len), x, NEG)
        lb_k = jnp.where(ok & (uu < u_len), y, NEG)
        return bl_k, lb_k

    alpha = jnp.where(tt == 0, 0.0, NEG).astype(F32)
    abuf[0] = alpha
    beta = jnp.full((n_t, 128), NEG, F32)
    sc = [scores(k) for k in range(n_diag)]
    for step in range(n_diag):
        if step > 0:
            bl_k, lb_k = sc[step - 1]
            p1 = jnp.where(tt == 0, NEG, pltpu.roll(alpha + bl_k, 1, 0))
            alpha = logadd(p1, alpha + lb_k)
            abuf[step] = alpha
        k = n_diag - 1 - step
        bl_k, lb_k = sc[k]
        up = jnp.where(tt == n_t - 1, jnp.where(u_len == k + 1 - n_t, 0.0, NEG), pltpu.roll(beta, n_t - 1, 0))
        t1 = up + bl_k
        t2 = beta + lb_k
        t1buf[k] = t1
        t2buf[k] = t2
        beta = jnp.where(tt >= t_len, jnp.where(k - tt == u_len, 0.0, NEG), logadd(t1, t2))
    segu[...] = jnp.zeros_like(segu)
    segt[...] = jnp.zeros_like(segt)
    log_p = beta[0:1, :]
    lane = lax.broadcasted_iota(jnp.int32, (n_t, 128), 1)
    loss_ref[...] = pltpu.roll(jnp.where(lane < u_hi - u_lo, -log_p, 0.0), u_lo, 1)
    lane_ok = lane < CORE_MAX
    for k in range(n_diag):
        for which, buf in enumerate((t1buf, t2buf)):
            occ = jnp.where(lane_ok, jnp.exp(jnp.minimum(abuf[k] + buf[k] - log_p, 0.0)), 0.0)
            hi, mid, lo = split3(occ)
            lo_row = which * n_kt + k * n_t
            gocc[lo_row:lo_row + n_t, :] = hi + pltpu.roll(mid, CORE_MAX, 1) + pltpu.roll(lo, 2 * CORE_MAX, 1)
    for which in range(2):
        gocc[which * n_kt + n_diag * n_t:(which + 1) * n_kt, :] = jnp.zeros((n_kt - n_diag * n_t, 128), F32)
    gocb[...] = gocc[...].astype(BF16)

    def again(first, count):
        def one(q, carry):
            i = first + q

            @pl.when(i >= KEEP)
            def _():
                def chunk(c, carry):
                    rows = pl.ds(pl.multiple_of(c * CHUNK, CHUNK), CHUNK)
                    z3 = dot(wot[rows, :], hbuf[i]).reshape(n_sub, 8, ROWS)
                    ebuf[KEEP + i % 2, rows, :] = jnp.exp(z3 - jnp.max(z3, axis=0)[None]).reshape(CHUNK, ROWS)
                    return carry
                lax.fori_loop(0, n_ch, chunk, 0)
            return carry
        @pl.when(first + count > KEEP)
        def _():
            lax.fori_loop(0, count, one, 0)

    def occupancy(i, par):
        orep = spread3(idx[i, 3:4], (1.0, 1.0, 1.0))
        kt8 = jnp.broadcast_to(idx[i, 2:3], (8, ROWS))
        kt_tile = lax.shift_right_arithmetic(kt8, 3)
        kt_sub = sub8 == jnp.bitwise_and(kt8, 7)
        for which in range(2):
            gath = dot(gocb[which * n_kt:(which + 1) * n_kt], orep).reshape(n_kt // 8, 8, ROWS)
            occ = jnp.zeros((8, ROWS), F32)
            for k in range(n_diag):
                occ = jnp.where(kt_tile == k, gath[k], occ)
            occ = jnp.sum(jnp.where(kt_sub, occ, 0.0), axis=0, keepdims=True)
            zrow[par, which * 8:which * 8 + 8] = jnp.broadcast_to(occ, (8, ROWS))

    def d_logits(i, par):
        y8 = ybuf[i]
        y_tile = lax.shift_right_logical(y8, 3)
        gb = zrow[par, 0:8]
        gl = zrow[par, 8:16]
        occ = gb + gl
        gl_y = jnp.where(sub8 == jnp.bitwise_and(y8, 7), gl, 0.0)
        gb_0 = jnp.where(sub8 == 0, gb, 0.0)
        slot = slot_of(i)
        for c in range(n_ch):
            sc_c = fac[i, c * 8:(c + 1) * 8, :] * occ
            e3 = ebuf[slot, c * CHUNK:(c + 1) * CHUNK, :].reshape(n_sub, 8, ROWS)
            tiles = []
            for k in range(n_sub):
                d = e3[k] * sc_c
                if c == 0 and k == 0:
                    d = d - gb_0
                tiles.append(d - jnp.where(y_tile == c * n_sub + k, gl_y, 0.0))
            d = jnp.concatenate(tiles, axis=0)
            dzb[par, c * CHUNK:(c + 1) * CHUNK, :] = d.astype(BF16)

    def segments(i, par):
        win = tbl[0, i]
        oh = block_onehot(i)
        for lo in range(0, n_j, 256):
            cols = slice(lo, min(lo + 256, n_j))
            sums = dot(oh, dpb[par, cols], NT)
            segu[rows_of(win, n_u), cols] += sums[0:gu]
            segt[rows_of(win, n_t), cols] += sums[gu:]

    def d_hidden(i, par):
        for q in range(2):
            rows = slice(q * half, (q + 1) * half)
            hf = hbuf[i, rows].astype(F32)
            dh = dot(wo_ref[rows], dzb[par])
            dpb[par, rows] = (dh * (1.0 - hf * hf)).astype(BF16)

    def out_grad(blocks, add):
        for c in range(n_v // 256):
            cols = slice(c * 256, (c + 1) * 256)
            new = None
            for i, par in blocks:
                term = dot(hbuf[i], dzb[par, cols, :], NT)
                new = term if new is None else new + term
            gwo_ref[:, cols] = jnp.where(add, gwo_ref[:, cols], 0.0) + new

    def bwd_pair(p, carry):
        i = 2 * p
        again(i + 2, 2)
        d_hidden(i, 0)
        d_hidden(i + 1, 1)
        segments(i, 0)
        segments(i + 1, 1)
        out_grad(((i, 0), (i + 1, 1)), p > 0)
        d_logits(i + 2, 0)
        d_logits(i + 3, 1)
        occupancy(i + 4, 0)
        occupancy(i + 5, 1)
        return carry

    def bwd_odd(p, carry):
        d_hidden(n_blocks - 1, 0)
        out_grad(((n_blocks - 1, 0),), n_blocks > 1)
        segments(n_blocks - 1, 0)
        return carry

    load_wo.wait()
    again(0, 2)
    for first in range(2):
        occupancy(jnp.int32(first), first)
        d_logits(jnp.int32(first), first)
        occupancy(jnp.int32(first + 2), first)
    lax.fori_loop(0, n_blocks // 2, bwd_pair, 0)
    lax.fori_loop(0, n_blocks % 2, bwd_odd, 0)

    da_ref[...] = segt[...].astype(BF16)


def core_call(c_t, a_t, wot, ylab, w_out, flen, llen, n_t, n_u):
    n_utt = flen.shape[0]
    n_j = c_t.shape[1]
    n_v = w_out.shape[1]
    max_blk = n_utt // 2 * n_t * n_u // ROWS + 6
    n_kt = (n_t + n_u) * n_t
    n_st = n_v // CHUNK * 8
    vm = pl.BlockSpec(memory_space=pltpu.VMEM)
    sm = pl.BlockSpec(memory_space=pltpu.SMEM)
    return pl.pallas_call(
        functools.partial(core_kernel, n_t, n_u),
        out_shape=(
            pltpu.VMEM((8, 128), F32),
            pltpu.VMEM((n_utt * n_u, n_j), F32),
            pltpu.VMEM((n_utt * n_t, n_j), BF16),
            pltpu.VMEM(w_out.shape, F32),
        ),
        in_specs=[sm, sm] + [vm] * 6 + [pl.BlockSpec(memory_space=pltpu.HBM)],
        out_specs=(vm,) * 4,
        scratch_shapes=[
            pltpu.VMEM(w_out.shape, BF16),
            pltpu.SemaphoreType.DMA,
            pltpu.VMEM((max_blk, n_j, ROWS), BF16),
            pltpu.VMEM((2, n_j, ROWS), BF16),
            pltpu.VMEM((min(max_blk, KEEP + 2), n_v, ROWS), F32),
            pltpu.VMEM((max_blk, n_st, ROWS), F32),
            pltpu.VMEM((2, n_st, ROWS), F32),
            pltpu.VMEM((2, n_st, ROWS), F32),
            pltpu.VMEM((2, 256, ROWS), BF16),
            pltpu.VMEM((2, 8, ROWS), jnp.int32),
            pltpu.VMEM((max_blk, 8, ROWS), jnp.int32),
            pltpu.VMEM((max_blk, 8, ROWS), jnp.int32),
            pltpu.VMEM((2, n_v, ROWS), BF16),
            pltpu.VMEM((2, n_j, ROWS), BF16),
            pltpu.VMEM((2, 16, ROWS), F32),
            pltpu.VMEM((n_kt, 256), F32),
            pltpu.VMEM((n_t + n_u, n_t, 128), F32),
            pltpu.VMEM((n_t + n_u, n_t, 128), F32),
            pltpu.VMEM((n_t + n_u, n_t, 128), F32),
            pltpu.VMEM((2 * n_kt, 128), F32),
            pltpu.VMEM((2 * n_kt, 128), BF16),
            pltpu.VMEM((n_utt * n_t, n_j), F32),
            pltpu.SMEM((3, max_blk), jnp.int32),
            pltpu.SMEM((n_utt + 1,), jnp.int32),
        ],
        compiler_params=pltpu.CompilerParams(vmem_limit_bytes=CORE_VMEM),
        name="rnnt_core",
    )(flen, llen, flen.reshape(1, n_utt), llen.reshape(1, n_utt), *[in_vmem(x) for x in (ylab, c_t, a_t, wot)], in_hbm(w_out))


def solution(mesh):
    seq_size = mesh.shape['seq']

    def local_fn(enc_out, pred_out, w_enc, w_pred, w_out, labels, frame_len, label_len):
        n_utt, n_loc, n_h = enc_out.shape
        n_u = pred_out.shape[1]
        n_t = n_loc * seq_size
        g2 = pred_out.reshape(n_utt * n_u, n_h)
        c_t, a_t, wot, f2, *rest = gather_call(enc_out, g2, w_enc, w_pred, w_out, labels.T, seq_size, n_t, n_u)
        loss, dc_t, da_t, gwo = core_call(c_t, a_t, wot, *rest, w_out, frame_len, label_len, n_t, n_u)
        loss, gf, gwe, gwp, gwo = store_call(reduce_call(gwo, dc_t, da_t, loss, g2, f2, w_enc, enc_out.shape, n_t))
        return loss.reshape(n_utt), gf, gwe, gwp, gwo

    in_specs = (P('dp', 'seq', None), P('dp', None, None), P(None, None), P(None, None), P(None, None), P('dp', None), P('dp'), P('dp'))
    out_specs = (P('dp'), P('dp', 'seq', None), P('dp', None), P('dp', None), P('dp', None))
    return jax.shard_map(local_fn, mesh=mesh, in_specs=in_specs, out_specs=out_specs, check_vma=False)
```

```python
import functools

import jax
import jax.numpy as jnp
from jax import lax
from jax.experimental import pallas as pl
from jax.experimental.pallas import tpu as pltpu
from jax.sharding import PartitionSpec as P

NEG = -1.0e30
ROWS = 256
WIN = 6
CHUNK = 256
CORE_MIN, CORE_MAX = 24, 40
GATHER_VMEM = 40 << 20
CORE_VMEM = 47 << 20
REDUCE_VMEM = 36 << 20
STORE_VMEM = 1 << 20
KEEP = 15
F32 = jnp.float32
BF16 = jnp.bfloat16
MESH = pl.DeviceIdType.MESH
NT = (((1,), (1,)), ((), ()))
NN = (((1,), (0,)), ((), ()))


def dot(a, b, dims=NN):
    return lax.dot_general(a, b, dims, preferred_element_type=F32)


def in_hbm(x):
    return pltpu.with_memory_space_constraint(x, pltpu.HBM)


def in_vmem(x):
    return pltpu.with_memory_space_constraint(x, pltpu.VMEM)


def split3(x):
    hi = x.astype(BF16).astype(F32)
    r1 = x - hi
    mid = r1.astype(BF16).astype(F32)
    return hi, mid, r1 - mid


def logadd(a, b):
    m = jnp.maximum(a, b)
    return m + jnp.log(1.0 + jnp.exp(jnp.minimum(a, b) - m))


def label_rows(n_u, first, n_rows, lab_ref):
    lab = lab_ref[...]
    n_lab, n_utt = lab.shape
    pad = jnp.zeros((n_u - n_lab, n_utt), F32)
    parts = [lax.shift_right_arithmetic(lab, 5).astype(F32), pad, jnp.bitwise_and(lab, 31).astype(F32), pad]
    both = jnp.concatenate(parts, axis=0).T.astype(BF16)
    row = lax.broadcasted_iota(jnp.int32, (n_rows, n_utt), 0)
    col = lax.broadcasted_iota(jnp.int32, (n_rows, n_utt), 1)
    spread = dot(jnp.where(row // n_u + first == col, 1.0, 0.0).astype(BF16), both)
    row = lax.broadcasted_iota(jnp.int32, (n_rows, 2 * n_u), 0)
    col = lax.broadcasted_iota(jnp.int32, (n_rows, 2 * n_u), 1)
    own = jnp.where(row % n_u == col % n_u, spread, 0.0).astype(BF16)
    place = (lax.broadcasted_iota(jnp.int32, (2 * n_u, 128), 0) // n_u == lax.broadcasted_iota(jnp.int32, (2 * n_u, 128), 1))
    return dot(own, jnp.where(place, 1.0, 0.0).astype(BF16)).astype(BF16)


def gather_kernel(n_t, n_u, enc_h, g_h, we_h, wp_h, wo_h, lab_h, c_ref, a_ref, wot_ref, f_ref, y_ref,
                  enc_ref, g_ref, we_ref, wp_ref, wo_ref, lab_ref, fbuf, in_sem, send_sem, recv_sem):
    me = lax.axis_index('seq')
    n_seq = fbuf.shape[0]
    partner = me + 1 - 2 * (me % 2)
    peer = (me + 2) % n_seq
    load_enc, load_wo, load_wp, load_g, load_we, load_lab = loads = [pltpu.make_async_copy(src, dst, in_sem.at[q]) for q, (src, dst) in enumerate(
        ((enc_h, enc_ref), (wo_h, wo_ref), (wp_h, wp_ref), (g_h, g_ref), (we_h, we_ref), (lab_h, lab_ref)))]
    for load in loads:
        load.start()
    diag = (partner + 2) % n_seq
    barrier = pltpu.get_barrier_semaphore()
    for other in (partner, peer, diag):
        pl.semaphore_signal(barrier, inc=1, device_id={'seq': other}, device_id_type=MESH)
    pl.semaphore_wait(barrier, 3)

    core = me % 2
    n_utt = enc_ref.shape[0]
    n_need = CORE_MAX + 8
    n_edge = n_utt - n_need
    middle = pl.ds(n_edge, n_utt - 2 * n_edge)
    edge = lambda c: pl.ds(c * n_need, n_edge)

    def send(src, slot, part, sem, other):
        return pltpu.make_async_remote_copy(src_ref=src.at[part], dst_ref=fbuf.at[slot, part], send_sem=send_sem.at[sem],
                                            recv_sem=recv_sem.at[sem], device_id={'seq': other}, device_id_type=MESH)
    load_enc.wait()
    sends = [
        send(enc_ref, me, middle, 0, peer),
        send(enc_ref, me, edge(core), 1, peer),
        send(enc_ref, me, edge(1 - core), 2, diag),
        send(enc_ref, me, pl.ds((1 - core) * n_edge, n_need), 3, partner),
    ]
    for s in sends:
        s.start()
    fbuf[:, edge(1 - core)] = jnp.zeros((n_seq, n_edge) + fbuf.shape[2:], BF16)
    fbuf[me] = enc_ref[...]
    load_wo.wait()
    wot_ref[...] = wo_ref[...].T
    load_wp.wait()
    load_g.wait()
    n_c = n_need * n_u
    first = core * n_edge
    rows_c = pl.ds(pl.multiple_of(first * n_u, 64), n_c)
    c_ref[rows_c, :] = dot(g_ref[rows_c, :], wp_ref[...]).astype(BF16)
    load_we.wait()
    load_lab.wait()
    y_ref[rows_c, :] = label_rows(n_u, first, n_c, lab_ref)
    n_f, n_h = f_ref.shape
    n_own = n_f // n_seq
    n_loc = n_t // n_seq
    col = lax.broadcasted_iota(jnp.int32, (n_f, n_own), 0)
    row = lax.broadcasted_iota(jnp.int32, (n_f, n_own), 1)

    def piece(p):
        rows = fbuf[p].reshape(n_own, n_h)
        f_ref[pl.ds(pl.multiple_of(p * n_own, n_own), n_own), :] = rows
        order = jnp.where(col == row // n_loc * n_t + p * n_loc + row % n_loc, 1.0, 0.0).astype(BF16)
        return dot(order, dot(rows, we_ref[...]).astype(BF16))
    a_t = piece(me)
    sends[3].wait_recv()
    a_t = a_t + piece(partner)
    sends[0].wait_recv()
    relay = send(fbuf.at[peer], peer, middle, 4, partner)
    relay.start()
    sends[1].wait_recv()
    a_t = a_t + piece(peer)
    sends[2].wait_recv()
    relay.wait_recv()
    a_ref[...] = a_t + piece(diag)
    for s in sends + [relay]:
        s.wait_send()


def gather_call(enc, g2, w_enc, w_pred, w_out, labels_t, n_seq, n_t, n_u):
    n_utt, n_loc, n_h = enc.shape
    n_j = w_enc.shape[1]
    vm = pl.BlockSpec(memory_space=pltpu.VMEM)
    n_f = n_utt * n_loc * n_seq
    args = [in_hbm(x) for x in (enc, g2, w_enc, w_pred, w_out, labels_t)]
    return pl.pallas_call(
        functools.partial(gather_kernel, n_t, n_u),
        out_shape=(
            pltpu.VMEM((g2.shape[0], n_j), BF16),
            pltpu.VMEM((n_f, n_j), F32),
            pltpu.VMEM(w_out.shape[::-1], BF16),
            pltpu.VMEM((n_f, n_h), BF16),
            pltpu.VMEM((g2.shape[0], 128), BF16),
        ),
        in_specs=[pl.BlockSpec(memory_space=pltpu.HBM)] * 6,
        out_specs=(vm,) * 5,
        scratch_shapes=[pltpu.VMEM(x.shape, x.dtype) for x in (enc, g2, w_enc, w_pred, w_out, labels_t)] + [
            pltpu.VMEM((n_seq, n_utt, n_loc, n_h), BF16),
            pltpu.SemaphoreType.DMA((6,)),
            pltpu.SemaphoreType.DMA((5,)),
            pltpu.SemaphoreType.DMA((5,)),
        ],
        compiler_params=pltpu.CompilerParams(collective_id=0, has_side_effects=True, vmem_limit_bytes=GATHER_VMEM),
        name="rnnt_gather",
    )(*args)


def reduce_kernel(n_t, gwo_v, dc_v, da_v, loss_v, f_v, g_p, we_p, loss_ref, gf_ref, gwe_ref, gwp_ref, gwo_ref,
                  g_v, we_v, gwp_v, rgwo, rgwp, rda, rloss, da_rows, rf, f_all, in_sem, send_sem, recv_sem):
    me = lax.axis_index('seq')
    partner = me + 1 - 2 * (me % 2)
    loads = [pltpu.make_async_copy(src, dst, in_sem.at[q]) for q, (src, dst) in enumerate(((g_p, g_v), (we_p, we_v)))]
    for load in loads:
        load.start()
    barrier = pltpu.get_barrier_semaphore()
    pl.semaphore_signal(barrier, inc=1, device_id={'seq': partner}, device_id_type=MESH)
    pl.semaphore_wait(barrier, 1)

    def send(src, dst, sem):
        return pltpu.make_async_remote_copy(src_ref=src, dst_ref=dst, send_sem=send_sem.at[sem], recv_sem=recv_sem.at[sem],
                                            device_id={'seq': partner}, device_id_type=MESH)
    n_part = 4
    rows = gwo_v.shape[0] // n_part
    n_da = CORE_MAX * n_t
    da_lo = (da_v.shape[0] - n_da) * (me % 2)
    part = pl.ds(pl.multiple_of(da_lo, 64), n_da)
    sends = [send(da_v.at[part], rda.at[part], 0), send(loss_v, rloss, 1)]
    sends += [send(gwo_v.at[pl.ds(q * rows, rows)], rgwo.at[pl.ds(q * rows, rows)], 2 + q) for q in range(n_part)]
    n_dev = n_t // gf_ref.shape[1]
    n_blk = f_v.shape[0] // n_dev
    n_edge = rf.shape[0] // n_dev
    edge_lo = lambda p, c: pl.multiple_of(p * n_blk + c * (n_blk - n_edge), 16)
    f_sends = [send(f_v.at[pl.ds(edge_lo(p, me % 2), n_edge)], rf.at[pl.ds(p * n_edge, n_edge)], 3 + n_part + p) for p in range(n_dev)]
    for s in sends + f_sends:
        s.start()
    loads[0].wait()
    gwp_v[...] = dot(g_v[...].T, dc_v[...].astype(BF16))
    s_gwp = send(gwp_v, rgwp, 2 + n_part)
    loads[1].wait()
    sends[0].wait_recv()
    sends[1].wait_recv()
    loss_ref[...] = (loss_v[0:1, :] + rloss[0:1, :])[:, 0:loss_ref.shape[1]]
    row = lax.broadcasted_iota(jnp.int32, rda.shape, 0) - (da_v.shape[0] - n_da) * (partner % 2)
    other = jnp.where((row >= 0) & (row < n_da), rda[...].astype(F32), 0.0)
    da = (da_v[...].astype(F32) + other).astype(BF16)
    s_gwp.start()
    n_f = da.shape[0]
    n_loc = gf_ref.shape[1]
    n_own = gf_ref.shape[0] * n_loc
    row = lax.broadcasted_iota(jnp.int32, (n_f, n_f), 0)
    col = lax.broadcasted_iota(jnp.int32, (n_f, n_f), 1)
    order = jnp.where(col == row % n_own // n_loc * n_t + row // n_own * n_loc + row % n_loc, 1.0, 0.0).astype(BF16)
    da_f = dot(order, da).astype(BF16)
    da_rows[...] = da_f
    f_all[...] = f_v[...]
    for p in range(n_dev):
        f_sends[p].wait_recv()
        f_all[pl.ds(edge_lo(p, partner % 2), n_edge), :] = rf[p * n_edge:(p + 1) * n_edge]
    gwe_ref[...] = dot(f_all[...].T, da_f)
    own = da_rows[pl.ds(pl.multiple_of(me * n_own, n_own), n_own), :]
    gf_ref[...] = dot(own, we_v[...], NT).astype(BF16).reshape(gf_ref.shape)
    for q in range(n_part):
        sends[2 + q].wait_recv()
        part = slice(q * rows, (q + 1) * rows)
        gwo_ref[part] = gwo_v[part] + rgwo[part]
    s_gwp.wait_recv()
    gwp_ref[...] = gwp_v[...] + rgwp[...]
    for s in sends + f_sends + [s_gwp]:
        s.wait_send()


def reduce_call(gwo, dc_t, da_t, loss, g2, f2, w_enc, gf_shape, n_t):
    vm = pl.BlockSpec(memory_space=pltpu.VMEM)
    like = lambda x: pltpu.VMEM(x.shape, x.dtype)
    gwp_shape = (g2.shape[1], dc_t.shape[1])
    return pl.pallas_call(
        functools.partial(reduce_kernel, n_t),
        out_shape=(
            pltpu.VMEM((1, f2.shape[0] // n_t), F32),
            pltpu.VMEM(gf_shape, BF16),
            pltpu.VMEM(w_enc.shape, F32),
            pltpu.VMEM(gwp_shape, F32),
            pltpu.VMEM(gwo.shape, F32),
        ),
        in_specs=[vm] * 5 + [pl.BlockSpec(memory_space=pltpu.HBM)] * 2,
        out_specs=(vm,) * 5,
        scratch_shapes=[like(x) for x in (g2, w_enc)] + [
            pltpu.VMEM(gwp_shape, F32), like(gwo), pltpu.VMEM(gwp_shape, F32), like(da_t), like(loss), like(da_t), pltpu.VMEM(((gf_shape[0] - CORE_MAX - 8) * n_t, f2.shape[1]), BF16), like(f2),
            pltpu.SemaphoreType.DMA((2,)),
            pltpu.SemaphoreType.DMA((11,)),
            pltpu.SemaphoreType.DMA((11,)),
        ],
        compiler_params=pltpu.CompilerParams(collective_id=1, has_side_effects=True, vmem_limit_bytes=REDUCE_VMEM),
        name="rnnt_reduce",
    )(in_vmem(gwo), in_vmem(dc_t), in_vmem(da_t), in_vmem(loss), in_vmem(f2), in_hbm(g2), in_hbm(w_enc))


def store_kernel(n, *refs):
    sems = refs[2 * n]
    copies = [pltpu.make_async_copy(refs[q], refs[n + q], sems.at[q]) for q in range(n)]
    for copy in copies:
        copy.start()
    for copy in copies:
        copy.wait()


def store_call(arrays):
    n = len(arrays)
    return pl.pallas_call(
        functools.partial(store_kernel, n),
        out_shape=tuple(pltpu.HBM(x.shape, x.dtype) for x in arrays),
        in_specs=[pl.BlockSpec(memory_space=pltpu.VMEM)] * n,
        out_specs=(pl.BlockSpec(memory_space=pltpu.HBM),) * n,
        scratch_shapes=[pltpu.SemaphoreType.DMA((n,))],
        compiler_params=pltpu.CompilerParams(vmem_limit_bytes=STORE_VMEM),
        name="rnnt_store",
    )(*[in_vmem(x) for x in arrays])


def core_kernel(n_t, n_u, flen_s, llen_s, flen_v, llen_v, y_buf, c_buf, a_buf, wot, wo_h,
                loss_ref, segu, da_ref, gwo_ref,
                wo_ref, wo_sem, hbuf, hpar, ebuf, fac, mch, sch, vsb, ypar, ybuf, idx, dzb, dpb, zrow, sk, abuf, t1buf, t2buf,
                gocc, gocb, segt, tbl, off):
    n_utt = flen_s.shape[0]
    n_j = c_buf.shape[1]
    n_v = wo_ref.shape[1]
    gu = WIN * n_u
    gt = WIN * n_t
    n_diag = n_t + n_u - 1
    n_kt = (n_diag + 1) * n_t
    n_ch = n_v // CHUNK

    load_wo = pltpu.make_async_copy(wo_h, wo_ref, wo_sem)
    load_wo.start()

    total = jnp.int32(0)
    for b in range(n_utt):
        off[b] = total
        total = total + flen_s[b] * (llen_s[b] + 1)
    off[n_utt] = total

    cut = jnp.int32(CORE_MIN)
    for b in range(CORE_MIN, CORE_MAX):
        cut = cut + jnp.where(off[b] + off[b + 1] <= total, 1, 0)
    first_core = lax.axis_index('seq') % 2 == 0
    u_lo = jnp.where(first_core, 0, cut)
    u_hi = jnp.where(first_core, cut, n_utt)
    stop = off[u_hi]

    def utt_step(b, carry):
        win = jnp.minimum(b, n_utt - WIN)
        base = off[win]
        last = jnp.minimum(off[win + WIN], stop)

        def emit(c):
            n, pos = c
            end = jnp.minimum(pos + ROWS, last)
            tbl[0, n] = win
            tbl[1, n] = pos - base
            tbl[2, n] = end - base
            return n + 1, end
        return lax.while_loop(lambda c: c[1] < off[b + 1], emit, carry)
    n_blocks, _ = lax.fori_loop(u_lo, u_hi, utt_step, (jnp.int32(0), off[u_lo]))
    for past in range(3):
        for q in range(3):
            tbl[q, n_blocks + past] = 0

    sk[...] = jnp.zeros_like(sk)
    mch[...] = jnp.zeros_like(mch)
    sch[...] = jnp.ones_like(sch)
    zrow[...] = jnp.zeros_like(zrow)
    vsb[...] = jnp.zeros_like(vsb)
    dpb[...] = jnp.zeros_like(dpb)

    def onehot(n, index_row):
        return (lax.broadcasted_iota(jnp.int32, (n, ROWS), 0) == index_row)

    def as_bf16(mask):
        return jnp.where(mask, 1.0, 0.0).astype(BF16)

    def block_onehot(i):
        iota = lax.broadcasted_iota(jnp.int32, (gu + gt, ROWS), 0)
        return jnp.concatenate([as_bf16(iota[0:gu] == idx[i, 0:1]), as_bf16(iota[gu:] == idx[i, 1:2])], axis=0)

    sub8 = lax.broadcasted_iota(jnp.int32, (8, ROWS), 0)
    n_sub = CHUNK // 8

    def rows_of(win, width):
        return pl.ds(pl.multiple_of(win * width, width), WIN * width)

    def spread3(idx_b, parts):
        mask = lax.broadcasted_iota(jnp.int32, (CORE_MAX, ROWS), 0) == idx_b
        return jnp.concatenate([jnp.where(mask, part, 0.0) for part in parts]
                               + [jnp.zeros((128 - 3 * CORE_MAX, ROWS), F32)], axis=0).astype(BF16)

    def locate(i):
        win = tbl[0, i]
        r = tbl[1, i] + lax.broadcasted_iota(jnp.int32, (1, ROWS), 1)
        end_r = tbl[2, i]
        start = jnp.int32(0)
        bl = jnp.full((1, ROWS), -1, jnp.int32)
        w = jnp.zeros((1, ROWS), jnp.int32)
        u1 = jnp.ones((1, ROWS), jnp.int32)
        for j in range(WIN):
            u1_j = llen_s[win + j] + 1
            end = start + flen_s[win + j] * u1_j
            inside = (r >= start) & (r < jnp.minimum(end, end_r))
            bl = jnp.where(inside, j, bl)
            w = jnp.where(inside, r - start, w)
            u1 = jnp.where(inside, u1_j, u1)
            start = end
        valid = bl >= 0
        t = jnp.zeros((1, ROWS), jnp.int32)
        for j in range(1, n_t):
            t = t + jnp.where(w >= j * u1, 1, 0)
        u = w - t * u1
        idx_u = jnp.where(valid, bl * n_u + u, -1)
        idx_t = jnp.where(valid, gu + bl * n_t + t, -1)
        idx_kt = jnp.where(valid, (t + u) * n_t + t, -1)
        idx_b = jnp.where(valid, win + bl - u_lo, -1024)
        rows8 = lax.broadcasted_iota(jnp.int32, (8, ROWS), 0)
        idx[i] = jnp.where(rows8 == 0, idx_u, jnp.where(rows8 == 1, idx_t, jnp.where(rows8 == 2, idx_kt, idx_b)))

    half = n_j // 2

    def hidden(i, par):
        win = tbl[0, i]
        oh = jnp.concatenate([block_onehot(i), jnp.zeros((256 - gu - gt, ROWS), BF16)], axis=0)
        none = jnp.zeros((256 - gu - gt, n_j), BF16)
        cols = jnp.concatenate([c_buf[rows_of(win, n_u)], a_buf[rows_of(win, n_t)].astype(BF16), none], axis=0).T
        for q in range(2):
            rows = slice(q * half, (q + 1) * half)
            pre = dot(cols[rows], oh)
            h = jnp.tanh(pre).astype(BF16)
            hpar[par, rows] = h
            hbuf[i, rows] = h
        yy = dot(jnp.concatenate(
            [y_buf[rows_of(win, n_u)], jnp.zeros((256 - gu, 128), BF16)], axis=0).T[0:16], oh)
        y8 = jnp.broadcast_to((yy[0:1] * 32.0 + yy[1:2]).astype(jnp.int32), (8, ROWS))
        ypar[par] = y8
        ybuf[i] = y8

    def finish(i, par):
        idx_b = idx[i, 3:4]
        m_all = mch[par]
        m8 = jnp.max(m_all.reshape(n_ch, 8, ROWS), axis=0)
        m = jnp.max(m8, axis=0, keepdims=True)
        f_all = jnp.exp(m_all - m)
        s = jnp.sum(jnp.sum((sch[par] * f_all).reshape(n_ch, 8, ROWS), axis=0), axis=0, keepdims=True)
        fac[i] = f_all * (1.0 / s)
        lse = m + jnp.log(s)
        b_parts = split3(zrow[par, 8:9] - lse)
        l_parts = split3(jnp.sum(zrow[par, 0:8], axis=0, keepdims=True) - lse)
        vsb[par, 0:128] = spread3(idx_b, b_parts)
        vsb[par, 128:256] = spread3(idx_b, l_parts)

    def scatter(i, par, live):
        okt = as_bf16(onehot(n_kt, jnp.where(live, idx[i, 2:3], -1)))
        part = n_kt // 2
        for q in range(2):
            sk[q * part:(q + 1) * part] += dot(okt[q * part:(q + 1) * part], vsb[par], NT)

    def slot_of(i):
        return jnp.where(i < KEEP, i, KEEP + i % 2)

    def scores_part(i, par, chunks, lz):
        y8 = ypar[par]
        y_tile = lax.shift_right_logical(y8, 3)
        slot = slot_of(i)
        for c in chunks:
            z = dot(wot[c * CHUNK:(c + 1) * CHUNK, :], hpar[par])
            z3 = z.reshape(n_sub, 8, ROWS)
            for k in range(n_sub):
                lz = jnp.where(y_tile == c * n_sub + k, z3[k], lz)
            if c == 0:
                zrow[par, 8:16] = z[0:8, :]
            m_c = jnp.max(z3, axis=0)
            e3 = jnp.exp(z3 - m_c[None])
            ebuf[slot, c * CHUNK:(c + 1) * CHUNK, :] = e3.reshape(CHUNK, ROWS)
            mch[par, c * 8:(c + 1) * 8, :] = m_c
            sch[par, c * 8:(c + 1) * 8, :] = jnp.sum(e3, axis=0)
        if chunks[-1] == n_ch - 1:
            zrow[par, 0:8] = jnp.where(sub8 == jnp.bitwise_and(y8, 7), lz, 0.0)
        return lz

    def scores_of(i, par):
        scores_part(i, par, range(n_ch), jnp.zeros((8, ROWS), F32))

    def fwd_pair(p, carry):
        i = 2 * p
        finish(jnp.maximum(i - 1, 0), 1)
        hidden(i + 1, 1)
        scatter(jnp.maximum(i - 2, 0), 0, i > 1)
        scores_of(i, 0)
        hidden(i + 2, 0)
        scores_of(i + 1, 1)
        scatter(jnp.maximum(i - 1, 0), 1, i > 0)
        finish(i, 0)
        locate(i + 3)
        locate(i + 4)
        return carry

    def fwd_odd(p, carry):
        i = n_blocks - 1
        finish(jnp.maximum(i - 1, 0), 1)
        scatter(jnp.maximum(i - 2, 0), 0, i > 1)
        scores_of(i, 0)
        scatter(jnp.maximum(i - 1, 0), 1, i > 0)
        finish(i, 0)
        scatter(i, 0, True)
        return carry

    def fwd_even(p, carry):
        finish(n_blocks - 1, 1)
        scatter(n_blocks - 2, 0, True)
        scatter(n_blocks - 1, 1, True)
        return carry

    for first in range(3):
        locate(jnp.int32(first))
    hidden(jnp.int32(0), 0)
    lax.fori_loop(0, n_blocks // 2, fwd_pair, 0)
    lax.fori_loop(0, n_blocks % 2, fwd_odd, 0)
    lax.fori_loop(0, 1 - n_blocks % 2, fwd_even, 0)

    tt = lax.broadcasted_iota(jnp.int32, (n_t, 128), 0)
    def own_lanes(ref):
        x = jnp.concatenate([ref[...], jnp.zeros((1, 128 - n_utt), jnp.int32)], axis=1).astype(F32)
        return pltpu.roll(jnp.broadcast_to(x, (n_t, 128)), (128 - u_lo) % 128, 1).astype(jnp.int32)
    t_len = own_lanes(flen_v)
    u_len = own_lanes(llen_v)

    def scores(k):
        lo = k * n_t
        x, y = (v + pltpu.roll(v, 128 - CORE_MAX, 1) + pltpu.roll(v, 128 - 2 * CORE_MAX, 1)
                for v in (sk[lo:lo + n_t, 0:128], sk[lo:lo + n_t, 128:256]))
        uu = k - tt
        ok = (uu >= 0) & (tt < t_len)
        bl_k = jnp.where(ok & (uu <= u_len), x, NEG)
        lb_k = jnp.where(ok & (uu < u_len), y, NEG)
        return bl_k, lb_k

    alpha = jnp.where(tt == 0, 0.0, NEG).astype(F32)
    abuf[0] = alpha
    beta = jnp.full((n_t, 128), NEG, F32)
    sc = [scores(k) for k in range(n_diag)]
    for step in range(n_diag):
        if step > 0:
            bl_k, lb_k = sc[step - 1]
            p1 = jnp.where(tt == 0, NEG, pltpu.roll(alpha + bl_k, 1, 0))
            alpha = logadd(p1, alpha + lb_k)
            abuf[step] = alpha
        k = n_diag - 1 - step
        bl_k, lb_k = sc[k]
        up = jnp.where(tt == n_t - 1, jnp.where(u_len == k + 1 - n_t, 0.0, NEG), pltpu.roll(beta, n_t - 1, 0))
        t1 = up + bl_k
        t2 = beta + lb_k
        t1buf[k] = t1
        t2buf[k] = t2
        beta = jnp.where(tt >= t_len, jnp.where(k - tt == u_len, 0.0, NEG), logadd(t1, t2))
    segu[...] = jnp.zeros_like(segu)
    segt[...] = jnp.zeros_like(segt)
    log_p = beta[0:1, :]
    lane = lax.broadcasted_iota(jnp.int32, (n_t, 128), 1)
    loss_ref[...] = pltpu.roll(jnp.where(lane < u_hi - u_lo, -log_p, 0.0), u_lo, 1)
    lane_ok = lane < CORE_MAX
    for k in range(n_diag):
        for which, buf in enumerate((t1buf, t2buf)):
            occ = jnp.where(lane_ok, jnp.exp(jnp.minimum(abuf[k] + buf[k] - log_p, 0.0)), 0.0)
            hi, mid, lo = split3(occ)
            lo_row = which * n_kt + k * n_t
            gocc[lo_row:lo_row + n_t, :] = hi + pltpu.roll(mid, CORE_MAX, 1) + pltpu.roll(lo, 2 * CORE_MAX, 1)
    for which in range(2):
        gocc[which * n_kt + n_diag * n_t:(which + 1) * n_kt, :] = jnp.zeros((n_kt - n_diag * n_t, 128), F32)
    gocb[...] = gocc[...].astype(BF16)

    def again(first, count):
        def one(q, carry):
            i = first + q

            @pl.when(i >= KEEP)
            def _():
                def chunk(c, carry):
                    rows = pl.ds(pl.multiple_of(c * CHUNK, CHUNK), CHUNK)
                    z3 = dot(wot[rows, :], hbuf[i]).reshape(n_sub, 8, ROWS)
                    ebuf[KEEP + i % 2, rows, :] = jnp.exp(z3 - jnp.max(z3, axis=0)[None]).reshape(CHUNK, ROWS)
                    return carry
                lax.fori_loop(0, n_ch, chunk, 0)
            return carry
        @pl.when(first + count > KEEP)
        def _():
            lax.fori_loop(0, count, one, 0)

    def occupancy(i, par):
        orep = spread3(idx[i, 3:4], (1.0, 1.0, 1.0))
        kt8 = jnp.broadcast_to(idx[i, 2:3], (8, ROWS))
        kt_tile = lax.shift_right_arithmetic(kt8, 3)
        kt_sub = sub8 == jnp.bitwise_and(kt8, 7)
        for which in range(2):
            gath = dot(gocb[which * n_kt:(which + 1) * n_kt], orep).reshape(n_kt // 8, 8, ROWS)
            occ = jnp.zeros((8, ROWS), F32)
            for k in range(n_diag):
                occ = jnp.where(kt_tile == k, gath[k], occ)
            occ = jnp.sum(jnp.where(kt_sub, occ, 0.0), axis=0, keepdims=True)
            zrow[par, which * 8:which * 8 + 8] = jnp.broadcast_to(occ, (8, ROWS))

    def d_logits(i, par):
        y8 = ybuf[i]
        y_tile = lax.shift_right_logical(y8, 3)
        gb = zrow[par, 0:8]
        gl = zrow[par, 8:16]
        occ = gb + gl
        gl_y = jnp.where(sub8 == jnp.bitwise_and(y8, 7), gl, 0.0)
        gb_0 = jnp.where(sub8 == 0, gb, 0.0)
        slot = slot_of(i)
        for c in range(n_ch):
            sc_c = fac[i, c * 8:(c + 1) * 8, :] * occ
            e3 = ebuf[slot, c * CHUNK:(c + 1) * CHUNK, :].reshape(n_sub, 8, ROWS)
            tiles = []
            for k in range(n_sub):
                d = e3[k] * sc_c
                if c == 0 and k == 0:
                    d = d - gb_0
                tiles.append(d - jnp.where(y_tile == c * n_sub + k, gl_y, 0.0))
            d = jnp.concatenate(tiles, axis=0)
            dzb[par, c * CHUNK:(c + 1) * CHUNK, :] = d.astype(BF16)

    def segments(i, par):
        win = tbl[0, i]
        oh = block_onehot(i)
        for lo in range(0, n_j, 256):
            cols = slice(lo, min(lo + 256, n_j))
            sums = dot(oh, dpb[par, cols], NT)
            segu[rows_of(win, n_u), cols] += sums[0:gu]
            segt[rows_of(win, n_t), cols] += sums[gu:]

    def d_hidden(i, par):
        for q in range(2):
            rows = slice(q * half, (q + 1) * half)
            hf = hbuf[i, rows].astype(F32)
            dh = dot(wo_ref[rows], dzb[par])
            dpb[par, rows] = (dh * (1.0 - hf * hf)).astype(BF16)

    def out_grad(blocks, add):
        for c in range(n_v // 256):
            cols = slice(c * 256, (c + 1) * 256)
            new = None
            for i, par in blocks:
                term = dot(hbuf[i], dzb[par, cols, :], NT)
                new = term if new is None else new + term
            gwo_ref[:, cols] = jnp.where(add, gwo_ref[:, cols], 0.0) + new

    def bwd_pair(p, carry):
        i = 2 * p
        again(i + 2, 2)
        d_hidden(i, 0)
        d_hidden(i + 1, 1)
        segments(i, 0)
        segments(i + 1, 1)
        out_grad(((i, 0), (i + 1, 1)), p > 0)
        d_logits(i + 2, 0)
        d_logits(i + 3, 1)
        occupancy(i + 4, 0)
        occupancy(i + 5, 1)
        return carry

    def bwd_odd(p, carry):
        d_hidden(n_blocks - 1, 0)
        out_grad(((n_blocks - 1, 0),), n_blocks > 1)
        segments(n_blocks - 1, 0)
        return carry

    load_wo.wait()
    again(0, 2)
    for first in range(2):
        occupancy(jnp.int32(first), first)
        d_logits(jnp.int32(first), first)
        occupancy(jnp.int32(first + 2), first)
    lax.fori_loop(0, n_blocks // 2, bwd_pair, 0)
    lax.fori_loop(0, n_blocks % 2, bwd_odd, 0)

    da_ref[...] = segt[...].astype(BF16)


def core_call(c_t, a_t, wot, ylab, w_out, flen, llen, n_t, n_u):
    n_utt = flen.shape[0]
    n_j = c_t.shape[1]
    n_v = w_out.shape[1]
    max_blk = n_utt // 2 * n_t * n_u // ROWS + 6
    n_kt = (n_t + n_u) * n_t
    n_st = n_v // CHUNK * 8
    vm = pl.BlockSpec(memory_space=pltpu.VMEM)
    sm = pl.BlockSpec(memory_space=pltpu.SMEM)
    return pl.pallas_call(
        functools.partial(core_kernel, n_t, n_u),
        out_shape=(
            pltpu.VMEM((8, 128), F32),
            pltpu.VMEM((n_utt * n_u, n_j), F32),
            pltpu.VMEM((n_utt * n_t, n_j), BF16),
            pltpu.VMEM(w_out.shape, F32),
        ),
        in_specs=[sm, sm] + [vm] * 6 + [pl.BlockSpec(memory_space=pltpu.HBM)],
        out_specs=(vm,) * 4,
        scratch_shapes=[
            pltpu.VMEM(w_out.shape, BF16),
            pltpu.SemaphoreType.DMA,
            pltpu.VMEM((max_blk, n_j, ROWS), BF16),
            pltpu.VMEM((2, n_j, ROWS), BF16),
            pltpu.VMEM((min(max_blk, KEEP + 2), n_v, ROWS), F32),
            pltpu.VMEM((max_blk, n_st, ROWS), F32),
            pltpu.VMEM((2, n_st, ROWS), F32),
            pltpu.VMEM((2, n_st, ROWS), F32),
            pltpu.VMEM((2, 256, ROWS), BF16),
            pltpu.VMEM((2, 8, ROWS), jnp.int32),
            pltpu.VMEM((max_blk, 8, ROWS), jnp.int32),
            pltpu.VMEM((max_blk, 8, ROWS), jnp.int32),
            pltpu.VMEM((2, n_v, ROWS), BF16),
            pltpu.VMEM((2, n_j, ROWS), BF16),
            pltpu.VMEM((2, 16, ROWS), F32),
            pltpu.VMEM((n_kt, 256), F32),
            pltpu.VMEM((n_t + n_u, n_t, 128), F32),
            pltpu.VMEM((n_t + n_u, n_t, 128), F32),
            pltpu.VMEM((n_t + n_u, n_t, 128), F32),
            pltpu.VMEM((2 * n_kt, 128), F32),
            pltpu.VMEM((2 * n_kt, 128), BF16),
            pltpu.VMEM((n_utt * n_t, n_j), F32),
            pltpu.SMEM((3, max_blk), jnp.int32),
            pltpu.SMEM((n_utt + 1,), jnp.int32),
        ],
        compiler_params=pltpu.CompilerParams(vmem_limit_bytes=CORE_VMEM),
        name="rnnt_core",
    )(flen, llen, flen.reshape(1, n_utt), llen.reshape(1, n_utt), *[in_vmem(x) for x in (ylab, c_t, a_t, wot)], in_hbm(w_out))


def solution(mesh):
    seq_size = mesh.shape['seq']

    def local_fn(enc_out, pred_out, w_enc, w_pred, w_out, labels, frame_len, label_len):
        n_utt, n_loc, n_h = enc_out.shape
        n_u = pred_out.shape[1]
        n_t = n_loc * seq_size
        g2 = pred_out.reshape(n_utt * n_u, n_h)
        c_t, a_t, wot, f2, *rest = gather_call(enc_out, g2, w_enc, w_pred, w_out, labels.T, seq_size, n_t, n_u)
        loss, dc_t, da_t, gwo = core_call(c_t, a_t, wot, *rest, w_out, frame_len, label_len, n_t, n_u)
        loss, gf, gwe, gwp, gwo = store_call(reduce_call(gwo, dc_t, da_t, loss, g2, f2, w_enc, enc_out.shape, n_t))
        return loss.reshape(n_utt), gf, gwe, gwp, gwo

    in_specs = (P('dp', 'seq', None), P('dp', None, None), P(None, None), P(None, None), P(None, None), P('dp', None), P('dp'), P('dp'))
    out_specs = (P('dp'), P('dp', 'seq', None), P('dp', None), P('dp', None), P('dp', None))
    return jax.shard_map(local_fn, mesh=mesh, in_specs=in_specs, out_specs=out_specs, check_vma=False)
```

```python
import functools

import jax
import jax.numpy as jnp
from jax import lax
from jax.experimental import pallas as pl
from jax.experimental.pallas import tpu as pltpu
from jax.sharding import PartitionSpec as P

NEG = -1.0e30
ROWS = 256
WIN = 6
CHUNK = 256
CORE_MIN, CORE_MAX = 24, 40
GATHER_VMEM = 40 << 20
CORE_VMEM = 47 << 20
REDUCE_VMEM = 36 << 20
STORE_VMEM = 1 << 20
KEEP = 15
F32 = jnp.float32
BF16 = jnp.bfloat16
MESH = pl.DeviceIdType.MESH
NT = (((1,), (1,)), ((), ()))
NN = (((1,), (0,)), ((), ()))


def dot(a, b, dims=NN):
    return lax.dot_general(a, b, dims, preferred_element_type=F32)


def in_hbm(x):
    return pltpu.with_memory_space_constraint(x, pltpu.HBM)


def in_vmem(x):
    return pltpu.with_memory_space_constraint(x, pltpu.VMEM)


def split3(x):
    hi = x.astype(BF16).astype(F32)
    r1 = x - hi
    mid = r1.astype(BF16).astype(F32)
    return hi, mid, r1 - mid


def logadd(a, b):
    m = jnp.maximum(a, b)
    return m + jnp.log(1.0 + jnp.exp(jnp.minimum(a, b) - m))


def label_rows(n_u, first, n_rows, lab_ref):
    lab = lab_ref[...]
    n_lab, n_utt = lab.shape
    pad = jnp.zeros((n_u - n_lab, n_utt), F32)
    parts = [lax.shift_right_arithmetic(lab, 5).astype(F32), pad, jnp.bitwise_and(lab, 31).astype(F32), pad]
    both = jnp.concatenate(parts, axis=0).T.astype(BF16)
    row = lax.broadcasted_iota(jnp.int32, (n_rows, n_utt), 0)
    col = lax.broadcasted_iota(jnp.int32, (n_rows, n_utt), 1)
    spread = dot(jnp.where(row // n_u + first == col, 1.0, 0.0).astype(BF16), both)
    row = lax.broadcasted_iota(jnp.int32, (n_rows, 2 * n_u), 0)
    col = lax.broadcasted_iota(jnp.int32, (n_rows, 2 * n_u), 1)
    own = jnp.where(row % n_u == col % n_u, spread, 0.0).astype(BF16)
    place = (lax.broadcasted_iota(jnp.int32, (2 * n_u, 128), 0) // n_u == lax.broadcasted_iota(jnp.int32, (2 * n_u, 128), 1))
    return dot(own, jnp.where(place, 1.0, 0.0).astype(BF16)).astype(BF16)


def gather_kernel(n_t, n_u, enc_h, g_h, we_h, wp_h, wo_h, lab_h, c_ref, a_ref, wot_ref, f_ref, y_ref,
                  enc_ref, g_ref, we_ref, wp_ref, wo_ref, lab_ref, fbuf, in_sem, send_sem, recv_sem):
    me = lax.axis_index('seq')
    n_seq = fbuf.shape[0]
    partner = me + 1 - 2 * (me % 2)
    peer = (me + 2) % n_seq
    core = me % 2
    n_utt = enc_ref.shape[0]
    n_need = CORE_MAX + 8
    n_edge = n_utt - n_need
    n_c = n_need * n_u
    first = core * n_edge
    rows_c = pl.ds(pl.multiple_of(first * n_u, 64), n_c)
    load_enc, load_wo, load_wp, load_g, load_we, load_lab = loads = [pltpu.make_async_copy(src, dst, in_sem.at[q]) for q, (src, dst) in enumerate(
        ((enc_h, enc_ref), (wo_h, wo_ref), (wp_h, wp_ref), (g_h.at[rows_c], g_ref.at[rows_c]), (we_h, we_ref), (lab_h, lab_ref)))]
    for load in loads:
        load.start()
    diag = (partner + 2) % n_seq
    barrier = pltpu.get_barrier_semaphore()
    for other in (partner, peer, diag):
        pl.semaphore_signal(barrier, inc=1, device_id={'seq': other}, device_id_type=MESH)
    pl.semaphore_wait(barrier, 3)

    middle = pl.ds(n_edge, n_utt - 2 * n_edge)
    edge = lambda c: pl.ds(c * n_need, n_edge)

    def send(src, slot, part, sem, other):
        return pltpu.make_async_remote_copy(src_ref=src.at[part], dst_ref=fbuf.at[slot, part], send_sem=send_sem.at[sem],
                                            recv_sem=recv_sem.at[sem], device_id={'seq': other}, device_id_type=MESH)
    load_enc.wait()
    sends = [
        send(enc_ref, me, middle, 0, peer),
        send(enc_ref, me, edge(core), 1, peer),
        send(enc_ref, me, edge(1 - core), 2, diag),
        send(enc_ref, me, pl.ds((1 - core) * n_edge, n_need), 3, partner),
    ]
    for s in sends:
        s.start()
    fbuf[:, edge(1 - core)] = jnp.zeros((n_seq, n_edge) + fbuf.shape[2:], BF16)
    fbuf[me] = enc_ref[...]
    load_wo.wait()
    wot_ref[...] = wo_ref[...].T
    load_wp.wait()
    load_g.wait()
    c_ref[rows_c, :] = dot(g_ref[rows_c, :], wp_ref[...]).astype(BF16)
    load_we.wait()
    load_lab.wait()
    y_ref[rows_c, :] = label_rows(n_u, first, n_c, lab_ref)
    n_f, n_h = f_ref.shape
    n_own = n_f // n_seq
    n_loc = n_t // n_seq
    col = lax.broadcasted_iota(jnp.int32, (n_f, n_own), 0)
    row = lax.broadcasted_iota(jnp.int32, (n_f, n_own), 1)

    def piece(p):
        rows = fbuf[p].reshape(n_own, n_h)
        f_ref[pl.ds(pl.multiple_of(p * n_own, n_own), n_own), :] = rows
        order = jnp.where(col == row // n_loc * n_t + p * n_loc + row % n_loc, 1.0, 0.0).astype(BF16)
        return dot(order, dot(rows, we_ref[...]).astype(BF16))
    a_t = piece(me)
    sends[3].wait_recv()
    a_t = a_t + piece(partner)
    sends[0].wait_recv()
    relay = send(fbuf.at[peer], peer, middle, 4, partner)
    relay.start()
    sends[1].wait_recv()
    a_t = a_t + piece(peer)
    sends[2].wait_recv()
    relay.wait_recv()
    a_ref[...] = a_t + piece(diag)
    for s in sends + [relay]:
        s.wait_send()


def gather_call(enc, g2, w_enc, w_pred, w_out, labels_t, n_seq, n_t, n_u):
    n_utt, n_loc, n_h = enc.shape
    n_j = w_enc.shape[1]
    vm = pl.BlockSpec(memory_space=pltpu.VMEM)
    n_f = n_utt * n_loc * n_seq
    args = [in_hbm(x) for x in (enc, g2, w_enc, w_pred, w_out, labels_t)]
    return pl.pallas_call(
        functools.partial(gather_kernel, n_t, n_u),
        out_shape=(
            pltpu.VMEM((g2.shape[0], n_j), BF16),
            pltpu.VMEM((n_f, n_j), F32),
            pltpu.VMEM(w_out.shape[::-1], BF16),
            pltpu.VMEM((n_f, n_h), BF16),
            pltpu.VMEM((g2.shape[0], 128), BF16),
        ),
        in_specs=[pl.BlockSpec(memory_space=pltpu.HBM)] * 6,
        out_specs=(vm,) * 5,
        scratch_shapes=[pltpu.VMEM(x.shape, x.dtype) for x in (enc, g2, w_enc, w_pred, w_out, labels_t)] + [
            pltpu.VMEM((n_seq, n_utt, n_loc, n_h), BF16),
            pltpu.SemaphoreType.DMA((6,)),
            pltpu.SemaphoreType.DMA((5,)),
            pltpu.SemaphoreType.DMA((5,)),
        ],
        compiler_params=pltpu.CompilerParams(collective_id=0, has_side_effects=True, vmem_limit_bytes=GATHER_VMEM),
        name="rnnt_gather",
    )(*args)


def reduce_kernel(n_t, gwo_v, dc_v, da_v, loss_v, f_v, g_p, we_p, loss_ref, gf_ref, gwe_ref, gwp_ref, gwo_ref,
                  g_v, we_v, gwp_v, rgwo, rgwp, rda, rloss, da_rows, rf, f_all, in_sem, send_sem, recv_sem):
    me = lax.axis_index('seq')
    partner = me + 1 - 2 * (me % 2)
    n_need = g_v.shape[0]
    mine = pl.ds(pl.multiple_of(me % 2 * (dc_v.shape[0] - n_need), 64), n_need)
    loads = [pltpu.make_async_copy(src, dst, in_sem.at[q]) for q, (src, dst) in enumerate(((g_p.at[mine], g_v), (we_p, we_v)))]
    for load in loads:
        load.start()
    barrier = pltpu.get_barrier_semaphore()
    pl.semaphore_signal(barrier, inc=1, device_id={'seq': partner}, device_id_type=MESH)
    pl.semaphore_wait(barrier, 1)

    def send(src, dst, sem):
        return pltpu.make_async_remote_copy(src_ref=src, dst_ref=dst, send_sem=send_sem.at[sem], recv_sem=recv_sem.at[sem],
                                            device_id={'seq': partner}, device_id_type=MESH)
    n_part = 4
    rows = gwo_v.shape[0] // n_part
    n_da = CORE_MAX * n_t
    da_lo = (da_v.shape[0] - n_da) * (me % 2)
    part = pl.ds(pl.multiple_of(da_lo, 64), n_da)
    sends = [send(da_v.at[part], rda.at[part], 0), send(loss_v, rloss, 1)]
    sends += [send(gwo_v.at[pl.ds(q * rows, rows)], rgwo.at[pl.ds(q * rows, rows)], 2 + q) for q in range(n_part)]
    n_dev = n_t // gf_ref.shape[1]
    n_blk = f_v.shape[0] // n_dev
    n_edge = rf.shape[0] // n_dev
    edge_lo = lambda p, c: pl.multiple_of(p * n_blk + c * (n_blk - n_edge), 16)
    f_sends = [send(f_v.at[pl.ds(edge_lo(p, me % 2), n_edge)], rf.at[pl.ds(p * n_edge, n_edge)], 3 + n_part + p) for p in range(n_dev)]
    for s in sends + f_sends:
        s.start()
    loads[0].wait()
    gwp_v[...] = dot(g_v[...].T, dc_v[mine, :].astype(BF16))
    s_gwp = send(gwp_v, rgwp, 2 + n_part)
    loads[1].wait()
    sends[0].wait_recv()
    sends[1].wait_recv()
    loss_ref[...] = (loss_v[0:1, :] + rloss[0:1, :])[:, 0:loss_ref.shape[1]]
    row = lax.broadcasted_iota(jnp.int32, rda.shape, 0) - (da_v.shape[0] - n_da) * (partner % 2)
    other = jnp.where((row >= 0) & (row < n_da), rda[...].astype(F32), 0.0)
    da = (da_v[...].astype(F32) + other).astype(BF16)
    s_gwp.start()
    n_f = da.shape[0]
    n_loc = gf_ref.shape[1]
    n_own = gf_ref.shape[0] * n_loc
    row = lax.broadcasted_iota(jnp.int32, (n_f, n_f), 0)
    col = lax.broadcasted_iota(jnp.int32, (n_f, n_f), 1)
    order = jnp.where(col == row % n_own // n_loc * n_t + row // n_own * n_loc + row % n_loc, 1.0, 0.0).astype(BF16)
    da_f = dot(order, da).astype(BF16)
    da_rows[...] = da_f
    f_all[...] = f_v[...]
    for p in range(n_dev):
        f_sends[p].wait_recv()
        f_all[pl.ds(edge_lo(p, partner % 2), n_edge), :] = rf[p * n_edge:(p + 1) * n_edge]
    gwe_ref[...] = dot(f_all[...].T, da_f)
    own = da_rows[pl.ds(pl.multiple_of(me * n_own, n_own), n_own), :]
    gf_ref[...] = dot(own, we_v[...], NT).astype(BF16).reshape(gf_ref.shape)
    for q in range(n_part):
        sends[2 + q].wait_recv()
        part = slice(q * rows, (q + 1) * rows)
        gwo_ref[part] = gwo_v[part] + rgwo[part]
    s_gwp.wait_recv()
    gwp_ref[...] = gwp_v[...] + rgwp[...]
    for s in sends + f_sends + [s_gwp]:
        s.wait_send()


def reduce_call(gwo, dc_t, da_t, loss, g2, f2, w_enc, gf_shape, n_t):
    vm = pl.BlockSpec(memory_space=pltpu.VMEM)
    like = lambda x: pltpu.VMEM(x.shape, x.dtype)
    gwp_shape = (g2.shape[1], dc_t.shape[1])
    return pl.pallas_call(
        functools.partial(reduce_kernel, n_t),
        out_shape=(
            pltpu.VMEM((1, f2.shape[0] // n_t), F32),
            pltpu.VMEM(gf_shape, BF16),
            pltpu.VMEM(w_enc.shape, F32),
            pltpu.VMEM(gwp_shape, F32),
            pltpu.VMEM(gwo.shape, F32),
        ),
        in_specs=[vm] * 5 + [pl.BlockSpec(memory_space=pltpu.HBM)] * 2,
        out_specs=(vm,) * 5,
        scratch_shapes=[pltpu.VMEM((g2.shape[0] // gf_shape[0] * (CORE_MAX + 8), g2.shape[1]), BF16), like(w_enc)] + [
            pltpu.VMEM(gwp_shape, F32), like(gwo), pltpu.VMEM(gwp_shape, F32), like(da_t), like(loss), like(da_t), pltpu.VMEM(((gf_shape[0] - CORE_MAX - 8) * n_t, f2.shape[1]), BF16), like(f2),
            pltpu.SemaphoreType.DMA((2,)),
            pltpu.SemaphoreType.DMA((11,)),
            pltpu.SemaphoreType.DMA((11,)),
        ],
        compiler_params=pltpu.CompilerParams(collective_id=1, has_side_effects=True, vmem_limit_bytes=REDUCE_VMEM),
        name="rnnt_reduce",
    )(in_vmem(gwo), in_vmem(dc_t), in_vmem(da_t), in_vmem(loss), in_vmem(f2), in_hbm(g2), in_hbm(w_enc))


def store_kernel(n, *refs):
    sems = refs[2 * n]
    copies = [pltpu.make_async_copy(refs[q], refs[n + q], sems.at[q]) for q in range(n)]
    for copy in copies:
        copy.start()
    for copy in copies:
        copy.wait()


def store_call(arrays):
    n = len(arrays)
    return pl.pallas_call(
        functools.partial(store_kernel, n),
        out_shape=tuple(pltpu.HBM(x.shape, x.dtype) for x in arrays),
        in_specs=[pl.BlockSpec(memory_space=pltpu.VMEM)] * n,
        out_specs=(pl.BlockSpec(memory_space=pltpu.HBM),) * n,
        scratch_shapes=[pltpu.SemaphoreType.DMA((n,))],
        compiler_params=pltpu.CompilerParams(vmem_limit_bytes=STORE_VMEM),
        name="rnnt_store",
    )(*[in_vmem(x) for x in arrays])


def core_kernel(n_t, n_u, flen_s, llen_s, flen_v, llen_v, y_buf, c_buf, a_buf, wot, wo_h,
                loss_ref, segu, da_ref, gwo_ref,
                wo_ref, wo_sem, hbuf, hpar, ebuf, fac, mch, sch, vsb, ypar, ybuf, idx, dzb, dpb, zrow, sk, abuf, t1buf, t2buf,
                gocc, gocb, segt, tbl, off):
    n_utt = flen_s.shape[0]
    n_j = c_buf.shape[1]
    n_v = wo_ref.shape[1]
    gu = WIN * n_u
    gt = WIN * n_t
    n_diag = n_t + n_u - 1
    n_kt = (n_diag + 1) * n_t
    n_ch = n_v // CHUNK

    load_wo = pltpu.make_async_copy(wo_h, wo_ref, wo_sem)
    load_wo.start()

    total = jnp.int32(0)
    for b in range(n_utt):
        off[b] = total
        total = total + flen_s[b] * (llen_s[b] + 1)
    off[n_utt] = total

    cut = jnp.int32(CORE_MIN)
    for b in range(CORE_MIN, CORE_MAX):
        cut = cut + jnp.where(off[b] + off[b + 1] <= total, 1, 0)
    first_core = lax.axis_index('seq') % 2 == 0
    u_lo = jnp.where(first_core, 0, cut)
    u_hi = jnp.where(first_core, cut, n_utt)
    stop = off[u_hi]

    def utt_step(b, carry):
        win = jnp.minimum(b, n_utt - WIN)
        base = off[win]
        last = jnp.minimum(off[win + WIN], stop)

        def emit(c):
            n, pos = c
            end = jnp.minimum(pos + ROWS, last)
            tbl[0, n] = win
            tbl[1, n] = pos - base
            tbl[2, n] = end - base
            return n + 1, end
        return lax.while_loop(lambda c: c[1] < off[b + 1], emit, carry)
    n_blocks, _ = lax.fori_loop(u_lo, u_hi, utt_step, (jnp.int32(0), off[u_lo]))
    for past in range(3):
        for q in range(3):
            tbl[q, n_blocks + past] = 0

    sk[...] = jnp.zeros_like(sk)
    mch[...] = jnp.zeros_like(mch)
    sch[...] = jnp.ones_like(sch)
    zrow[...] = jnp.zeros_like(zrow)
    vsb[...] = jnp.zeros_like(vsb)
    dpb[...] = jnp.zeros_like(dpb)

    def onehot(n, index_row):
        return (lax.broadcasted_iota(jnp.int32, (n, ROWS), 0) == index_row)

    def as_bf16(mask):
        return jnp.where(mask, 1.0, 0.0).astype(BF16)

    def block_onehot(i):
        iota = lax.broadcasted_iota(jnp.int32, (gu + gt, ROWS), 0)
        return jnp.concatenate([as_bf16(iota[0:gu] == idx[i, 0:1]), as_bf16(iota[gu:] == idx[i, 1:2])], axis=0)

    sub8 = lax.broadcasted_iota(jnp.int32, (8, ROWS), 0)
    n_sub = CHUNK // 8

    def rows_of(win, width):
        return pl.ds(pl.multiple_of(win * width, width), WIN * width)

    def spread3(idx_b, parts):
        mask = lax.broadcasted_iota(jnp.int32, (CORE_MAX, ROWS), 0) == idx_b
        return jnp.concatenate([jnp.where(mask, part, 0.0) for part in parts]
                               + [jnp.zeros((128 - 3 * CORE_MAX, ROWS), F32)], axis=0).astype(BF16)

    def locate(i):
        win = tbl[0, i]
        r = tbl[1, i] + lax.broadcasted_iota(jnp.int32, (1, ROWS), 1)
        end_r = tbl[2, i]
        start = jnp.int32(0)
        bl = jnp.full((1, ROWS), -1, jnp.int32)
        w = jnp.zeros((1, ROWS), jnp.int32)
        u1 = jnp.ones((1, ROWS), jnp.int32)
        for j in range(WIN):
            u1_j = llen_s[win + j] + 1
            end = start + flen_s[win + j] * u1_j
            inside = (r >= start) & (r < jnp.minimum(end, end_r))
            bl = jnp.where(inside, j, bl)
            w = jnp.where(inside, r - start, w)
            u1 = jnp.where(inside, u1_j, u1)
            start = end
        valid = bl >= 0
        t = jnp.zeros((1, ROWS), jnp.int32)
        for j in range(1, n_t):
            t = t + jnp.where(w >= j * u1, 1, 0)
        u = w - t * u1
        idx_u = jnp.where(valid, bl * n_u + u, -1)
        idx_t = jnp.where(valid, gu + bl * n_t + t, -1)
        idx_kt = jnp.where(valid, (t + u) * n_t + t, -1)
        idx_b = jnp.where(valid, win + bl - u_lo, -1024)
        rows8 = lax.broadcasted_iota(jnp.int32, (8, ROWS), 0)
        idx[i] = jnp.where(rows8 == 0, idx_u, jnp.where(rows8 == 1, idx_t, jnp.where(rows8 == 2, idx_kt, idx_b)))

    half = n_j // 2

    def hidden(i, par):
        win = tbl[0, i]
        oh = jnp.concatenate([block_onehot(i), jnp.zeros((256 - gu - gt, ROWS), BF16)], axis=0)
        none = jnp.zeros((256 - gu - gt, n_j), BF16)
        cols = jnp.concatenate([c_buf[rows_of(win, n_u)], a_buf[rows_of(win, n_t)].astype(BF16), none], axis=0).T
        for q in range(2):
            rows = slice(q * half, (q + 1) * half)
            pre = dot(cols[rows], oh)
            h = jnp.tanh(pre).astype(BF16)
            hpar[par, rows] = h
            hbuf[i, rows] = h
        yy = dot(jnp.concatenate(
            [y_buf[rows_of(win, n_u)], jnp.zeros((256 - gu, 128), BF16)], axis=0).T[0:16], oh)
        y8 = jnp.broadcast_to((yy[0:1] * 32.0 + yy[1:2]).astype(jnp.int32), (8, ROWS))
        ypar[par] = y8
        ybuf[i] = y8

    def finish(i, par):
        idx_b = idx[i, 3:4]
        m_all = mch[par]
        m8 = jnp.max(m_all.reshape(n_ch, 8, ROWS), axis=0)
        m = jnp.max(m8, axis=0, keepdims=True)
        f_all = jnp.exp(m_all - m)
        s = jnp.sum(jnp.sum((sch[par] * f_all).reshape(n_ch, 8, ROWS), axis=0), axis=0, keepdims=True)
        fac[i] = f_all * (1.0 / s)
        lse = m + jnp.log(s)
        b_parts = split3(zrow[par, 8:9] - lse)
        l_parts = split3(jnp.sum(zrow[par, 0:8], axis=0, keepdims=True) - lse)
        vsb[par, 0:128] = spread3(idx_b, b_parts)
        vsb[par, 128:256] = spread3(idx_b, l_parts)

    def scatter(i, par, live):
        okt = as_bf16(onehot(n_kt, jnp.where(live, idx[i, 2:3], -1)))
        part = n_kt // 2
        for q in range(2):
            sk[q * part:(q + 1) * part] += dot(okt[q * part:(q + 1) * part], vsb[par], NT)

    def slot_of(i):
        return jnp.where(i < KEEP, i, KEEP + i % 2)

    def scores_part(i, par, chunks, lz):
        y8 = ypar[par]
        y_tile = lax.shift_right_logical(y8, 3)
        slot = slot_of(i)
        for c in chunks:
            z = dot(wot[c * CHUNK:(c + 1) * CHUNK, :], hpar[par])
            z3 = z.reshape(n_sub, 8, ROWS)
            for k in range(n_sub):
                lz = jnp.where(y_tile == c * n_sub + k, z3[k], lz)
            if c == 0:
                zrow[par, 8:16] = z[0:8, :]
            m_c = jnp.max(z3, axis=0)
            e3 = jnp.exp(z3 - m_c[None])
            ebuf[slot, c * CHUNK:(c + 1) * CHUNK, :] = e3.reshape(CHUNK, ROWS)
            mch[par, c * 8:(c + 1) * 8, :] = m_c
            sch[par, c * 8:(c + 1) * 8, :] = jnp.sum(e3, axis=0)
        if chunks[-1] == n_ch - 1:
            zrow[par, 0:8] = jnp.where(sub8 == jnp.bitwise_and(y8, 7), lz, 0.0)
        return lz

    def scores_of(i, par):
        scores_part(i, par, range(n_ch), jnp.zeros((8, ROWS), F32))

    def fwd_pair(p, carry):
        i = 2 * p
        finish(jnp.maximum(i - 1, 0), 1)
        hidden(i + 1, 1)
        scatter(jnp.maximum(i - 2, 0), 0, i > 1)
        scores_of(i, 0)
        hidden(i + 2, 0)
        scores_of(i + 1, 1)
        scatter(jnp.maximum(i - 1, 0), 1, i > 0)
        finish(i, 0)
        locate(i + 3)
        locate(i + 4)
        return carry

    def fwd_odd(p, carry):
        i = n_blocks - 1
        finish(jnp.maximum(i - 1, 0), 1)
        scatter(jnp.maximum(i - 2, 0), 0, i > 1)
        scores_of(i, 0)
        scatter(jnp.maximum(i - 1, 0), 1, i > 0)
        finish(i, 0)
        scatter(i, 0, True)
        return carry

    def fwd_even(p, carry):
        finish(n_blocks - 1, 1)
        scatter(n_blocks - 2, 0, True)
        scatter(n_blocks - 1, 1, True)
        return carry

    for first in range(3):
        locate(jnp.int32(first))
    hidden(jnp.int32(0), 0)
    lax.fori_loop(0, n_blocks // 2, fwd_pair, 0)
    lax.fori_loop(0, n_blocks % 2, fwd_odd, 0)
    lax.fori_loop(0, 1 - n_blocks % 2, fwd_even, 0)

    tt = lax.broadcasted_iota(jnp.int32, (n_t, 128), 0)
    def own_lanes(ref):
        x = jnp.concatenate([ref[...], jnp.zeros((1, 128 - n_utt), jnp.int32)], axis=1).astype(F32)
        return pltpu.roll(jnp.broadcast_to(x, (n_t, 128)), (128 - u_lo) % 128, 1).astype(jnp.int32)
    t_len = own_lanes(flen_v)
    u_len = own_lanes(llen_v)

    def scores(k):
        lo = k * n_t
        x, y = (v + pltpu.roll(v, 128 - CORE_MAX, 1) + pltpu.roll(v, 128 - 2 * CORE_MAX, 1)
                for v in (sk[lo:lo + n_t, 0:128], sk[lo:lo + n_t, 128:256]))
        uu = k - tt
        ok = (uu >= 0) & (tt < t_len)
        bl_k = jnp.where(ok & (uu <= u_len), x, NEG)
        lb_k = jnp.where(ok & (uu < u_len), y, NEG)
        return bl_k, lb_k

    alpha = jnp.where(tt == 0, 0.0, NEG).astype(F32)
    abuf[0] = alpha
    beta = jnp.full((n_t, 128), NEG, F32)
    sc = [scores(k) for k in range(n_diag)]
    for step in range(n_diag):
        if step > 0:
            bl_k, lb_k = sc[step - 1]
            p1 = jnp.where(tt == 0, NEG, pltpu.roll(alpha + bl_k, 1, 0))
            alpha = logadd(p1, alpha + lb_k)
            abuf[step] = alpha
        k = n_diag - 1 - step
        bl_k, lb_k = sc[k]
        up = jnp.where(tt == n_t - 1, jnp.where(u_len == k + 1 - n_t, 0.0, NEG), pltpu.roll(beta, n_t - 1, 0))
        t1 = up + bl_k
        t2 = beta + lb_k
        t1buf[k] = t1
        t2buf[k] = t2
        beta = jnp.where(tt >= t_len, jnp.where(k - tt == u_len, 0.0, NEG), logadd(t1, t2))
    n_need = (CORE_MAX + 8) * n_u
    mine = pl.ds(pl.multiple_of(jnp.where(first_core, 0, segu.shape[0] - n_need), 64), n_need)
    segu[mine, :] = jnp.zeros((n_need, n_j), F32)
    segt[...] = jnp.zeros_like(segt)
    log_p = beta[0:1, :]
    lane = lax.broadcasted_iota(jnp.int32, (n_t, 128), 1)
    loss_ref[...] = pltpu.roll(jnp.where(lane < u_hi - u_lo, -log_p, 0.0), u_lo, 1)
    lane_ok = lane < CORE_MAX
    for k in range(n_diag):
        for which, buf in enumerate((t1buf, t2buf)):
            occ = jnp.where(lane_ok, jnp.exp(jnp.minimum(abuf[k] + buf[k] - log_p, 0.0)), 0.0)
            hi, mid, lo = split3(occ)
            lo_row = which * n_kt + k * n_t
            gocc[lo_row:lo_row + n_t, :] = hi + pltpu.roll(mid, CORE_MAX, 1) + pltpu.roll(lo, 2 * CORE_MAX, 1)
    for which in range(2):
        gocc[which * n_kt + n_diag * n_t:(which + 1) * n_kt, :] = jnp.zeros((n_kt - n_diag * n_t, 128), F32)
    gocb[...] = gocc[...].astype(BF16)

    def again(first, count):
        def one(q, carry):
            i = first + q

            @pl.when(i >= KEEP)
            def _():
                def chunk(c, carry):
                    rows = pl.ds(pl.multiple_of(c * CHUNK, CHUNK), CHUNK)
                    z3 = dot(wot[rows, :], hbuf[i]).reshape(n_sub, 8, ROWS)
                    ebuf[KEEP + i % 2, rows, :] = jnp.exp(z3 - jnp.max(z3, axis=0)[None]).reshape(CHUNK, ROWS)
                    return carry
                lax.fori_loop(0, n_ch, chunk, 0)
            return carry
        @pl.when(first + count > KEEP)
        def _():
            lax.fori_loop(0, count, one, 0)

    def occupancy(i, par):
        orep = spread3(idx[i, 3:4], (1.0, 1.0, 1.0))
        kt8 = jnp.broadcast_to(idx[i, 2:3], (8, ROWS))
        kt_tile = lax.shift_right_arithmetic(kt8, 3)
        kt_sub = sub8 == jnp.bitwise_and(kt8, 7)
        for which in range(2):
            gath = dot(gocb[which * n_kt:(which + 1) * n_kt], orep).reshape(n_kt // 8, 8, ROWS)
            occ = jnp.zeros((8, ROWS), F32)
            for k in range(n_diag):
                occ = jnp.where(kt_tile == k, gath[k], occ)
            occ = jnp.sum(jnp.where(kt_sub, occ, 0.0), axis=0, keepdims=True)
            zrow[par, which * 8:which * 8 + 8] = jnp.broadcast_to(occ, (8, ROWS))

    def d_logits(i, par):
        y8 = ybuf[i]
        y_tile = lax.shift_right_logical(y8, 3)
        gb = zrow[par, 0:8]
        gl = zrow[par, 8:16]
        occ = gb + gl
        gl_y = jnp.where(sub8 == jnp.bitwise_and(y8, 7), gl, 0.0)
        gb_0 = jnp.where(sub8 == 0, gb, 0.0)
        slot = slot_of(i)
        for c in range(n_ch):
            sc_c = fac[i, c * 8:(c + 1) * 8, :] * occ
            e3 = ebuf[slot, c * CHUNK:(c + 1) * CHUNK, :].reshape(n_sub, 8, ROWS)
            tiles = []
            for k in range(n_sub):
                d = e3[k] * sc_c
                if c == 0 and k == 0:
                    d = d - gb_0
                tiles.append(d - jnp.where(y_tile == c * n_sub + k, gl_y, 0.0))
            d = jnp.concatenate(tiles, axis=0)
            dzb[par, c * CHUNK:(c + 1) * CHUNK, :] = d.astype(BF16)

    def segments(i, par):
        win = tbl[0, i]
        oh = block_onehot(i)
        for lo in range(0, n_j, 256):
            cols = slice(lo, min(lo + 256, n_j))
            sums = dot(oh, dpb[par, cols], NT)
            segu[rows_of(win, n_u), cols] += sums[0:gu]
            segt[rows_of(win, n_t), cols] += sums[gu:]

    def d_hidden(i, par):
        for q in range(2):
            rows = slice(q * half, (q + 1) * half)
            hf = hbuf[i, rows].astype(F32)
            dh = dot(wo_ref[rows], dzb[par])
            dpb[par, rows] = (dh * (1.0 - hf * hf)).astype(BF16)

    def out_grad(blocks, add):
        for c in range(n_v // 256):
            cols = slice(c * 256, (c + 1) * 256)
            new = None
            for i, par in blocks:
                term = dot(hbuf[i], dzb[par, cols, :], NT)
                new = term if new is None else new + term
            gwo_ref[:, cols] = jnp.where(add, gwo_ref[:, cols], 0.0) + new

    def bwd_pair(p, carry):
        i = 2 * p
        again(i + 2, 2)
        d_hidden(i, 0)
        d_hidden(i + 1, 1)
        segments(i, 0)
        segments(i + 1, 1)
        out_grad(((i, 0), (i + 1, 1)), p > 0)
        d_logits(i + 2, 0)
        d_logits(i + 3, 1)
        occupancy(i + 4, 0)
        occupancy(i + 5, 1)
        return carry

    def bwd_odd(p, carry):
        d_hidden(n_blocks - 1, 0)
        out_grad(((n_blocks - 1, 0),), n_blocks > 1)
        segments(n_blocks - 1, 0)
        return carry

    load_wo.wait()
    again(0, 2)
    for first in range(2):
        occupancy(jnp.int32(first), first)
        d_logits(jnp.int32(first), first)
        occupancy(jnp.int32(first + 2), first)
    lax.fori_loop(0, n_blocks // 2, bwd_pair, 0)
    lax.fori_loop(0, n_blocks % 2, bwd_odd, 0)

    da_ref[...] = segt[...].astype(BF16)


def core_call(c_t, a_t, wot, ylab, w_out, flen, llen, n_t, n_u):
    n_utt = flen.shape[0]
    n_j = c_t.shape[1]
    n_v = w_out.shape[1]
    max_blk = n_utt // 2 * n_t * n_u // ROWS + 6
    n_kt = (n_t + n_u) * n_t
    n_st = n_v // CHUNK * 8
    vm = pl.BlockSpec(memory_space=pltpu.VMEM)
    sm = pl.BlockSpec(memory_space=pltpu.SMEM)
    return pl.pallas_call(
        functools.partial(core_kernel, n_t, n_u),
        out_shape=(
            pltpu.VMEM((8, 128), F32),
            pltpu.VMEM((n_utt * n_u, n_j), F32),
            pltpu.VMEM((n_utt * n_t, n_j), BF16),
            pltpu.VMEM(w_out.shape, F32),
        ),
        in_specs=[sm, sm] + [vm] * 6 + [pl.BlockSpec(memory_space=pltpu.HBM)],
        out_specs=(vm,) * 4,
        scratch_shapes=[
            pltpu.VMEM(w_out.shape, BF16),
            pltpu.SemaphoreType.DMA,
            pltpu.VMEM((max_blk, n_j, ROWS), BF16),
            pltpu.VMEM((2, n_j, ROWS), BF16),
            pltpu.VMEM((min(max_blk, KEEP + 2), n_v, ROWS), F32),
            pltpu.VMEM((max_blk, n_st, ROWS), F32),
            pltpu.VMEM((2, n_st, ROWS), F32),
            pltpu.VMEM((2, n_st, ROWS), F32),
            pltpu.VMEM((2, 256, ROWS), BF16),
            pltpu.VMEM((2, 8, ROWS), jnp.int32),
            pltpu.VMEM((max_blk, 8, ROWS), jnp.int32),
            pltpu.VMEM((max_blk, 8, ROWS), jnp.int32),
            pltpu.VMEM((2, n_v, ROWS), BF16),
            pltpu.VMEM((2, n_j, ROWS), BF16),
            pltpu.VMEM((2, 16, ROWS), F32),
            pltpu.VMEM((n_kt, 256), F32),
            pltpu.VMEM((n_t + n_u, n_t, 128), F32),
            pltpu.VMEM((n_t + n_u, n_t, 128), F32),
            pltpu.VMEM((n_t + n_u, n_t, 128), F32),
            pltpu.VMEM((2 * n_kt, 128), F32),
            pltpu.VMEM((2 * n_kt, 128), BF16),
            pltpu.VMEM((n_utt * n_t, n_j), F32),
            pltpu.SMEM((3, max_blk), jnp.int32),
            pltpu.SMEM((n_utt + 1,), jnp.int32),
        ],
        compiler_params=pltpu.CompilerParams(vmem_limit_bytes=CORE_VMEM),
        name="rnnt_core",
    )(flen, llen, flen.reshape(1, n_utt), llen.reshape(1, n_utt), *[in_vmem(x) for x in (ylab, c_t, a_t, wot)], in_hbm(w_out))


def solution(mesh):
    seq_size = mesh.shape['seq']

    def local_fn(enc_out, pred_out, w_enc, w_pred, w_out, labels, frame_len, label_len):
        n_utt, n_loc, n_h = enc_out.shape
        n_u = pred_out.shape[1]
        n_t = n_loc * seq_size
        g2 = pred_out.reshape(n_utt * n_u, n_h)
        c_t, a_t, wot, f2, *rest = gather_call(enc_out, g2, w_enc, w_pred, w_out, labels.T, seq_size, n_t, n_u)
        loss, dc_t, da_t, gwo = core_call(c_t, a_t, wot, *rest, w_out, frame_len, label_len, n_t, n_u)
        loss, gf, gwe, gwp, gwo = store_call(reduce_call(gwo, dc_t, da_t, loss, g2, f2, w_enc, enc_out.shape, n_t))
        return loss.reshape(n_utt), gf, gwe, gwp, gwo

    in_specs = (P('dp', 'seq', None), P('dp', None, None), P(None, None), P(None, None), P(None, None), P('dp', None), P('dp'), P('dp'))
    out_specs = (P('dp'), P('dp', 'seq', None), P('dp', None), P('dp', None), P('dp', None))
    return jax.shard_map(local_fn, mesh=mesh, in_specs=in_specs, out_specs=out_specs, check_vma=False)
```

```python
import functools

import jax
import jax.numpy as jnp
from jax import lax
from jax.experimental import pallas as pl
from jax.experimental.pallas import tpu as pltpu
from jax.sharding import PartitionSpec as P

NEG = -1.0e30
ROWS = 256
WIN = 6
CHUNK = 256
CORE_MIN, CORE_MAX = 24, 40
GATHER_VMEM = 40 << 20
CORE_VMEM = 47 << 20
REDUCE_VMEM = 36 << 20
STORE_VMEM = 1 << 20
KEEP = 17
F32 = jnp.float32
BF16 = jnp.bfloat16
MESH = pl.DeviceIdType.MESH
NT = (((1,), (1,)), ((), ()))
NN = (((1,), (0,)), ((), ()))


def dot(a, b, dims=NN):
    return lax.dot_general(a, b, dims, preferred_element_type=F32)


def in_hbm(x):
    return pltpu.with_memory_space_constraint(x, pltpu.HBM)


def in_vmem(x):
    return pltpu.with_memory_space_constraint(x, pltpu.VMEM)


def split3(x):
    hi = x.astype(BF16).astype(F32)
    r1 = x - hi
    mid = r1.astype(BF16).astype(F32)
    return hi, mid, r1 - mid


def logadd(a, b):
    m = jnp.maximum(a, b)
    return m + jnp.log(1.0 + jnp.exp(jnp.minimum(a, b) - m))


def label_rows(n_u, first, n_rows, lab_ref):
    lab = lab_ref[...]
    n_lab, n_utt = lab.shape
    pad = jnp.zeros((n_u - n_lab, n_utt), F32)
    parts = [lax.shift_right_arithmetic(lab, 5).astype(F32), pad, jnp.bitwise_and(lab, 31).astype(F32), pad]
    both = jnp.concatenate(parts, axis=0).T.astype(BF16)
    row = lax.broadcasted_iota(jnp.int32, (n_rows, n_utt), 0)
    col = lax.broadcasted_iota(jnp.int32, (n_rows, n_utt), 1)
    spread = dot(jnp.where(row // n_u + first == col, 1.0, 0.0).astype(BF16), both)
    row = lax.broadcasted_iota(jnp.int32, (n_rows, 2 * n_u), 0)
    col = lax.broadcasted_iota(jnp.int32, (n_rows, 2 * n_u), 1)
    own = jnp.where(row % n_u == col % n_u, spread, 0.0).astype(BF16)
    place = (lax.broadcasted_iota(jnp.int32, (2 * n_u, 128), 0) // n_u == lax.broadcasted_iota(jnp.int32, (2 * n_u, 128), 1))
    return dot(own, jnp.where(place, 1.0, 0.0).astype(BF16)).astype(BF16)


def gather_kernel(n_t, n_u, enc_h, g_h, we_h, wp_h, wo_h, lab_h, c_ref, a_ref, wot_ref, f_ref, y_ref,
                  enc_ref, g_ref, we_ref, wp_ref, wo_ref, lab_ref, fbuf, in_sem, send_sem, recv_sem):
    me = lax.axis_index('seq')
    n_seq = fbuf.shape[0]
    partner = me + 1 - 2 * (me % 2)
    peer = (me + 2) % n_seq
    core = me % 2
    n_utt = enc_ref.shape[0]
    n_need = CORE_MAX + 8
    n_edge = n_utt - n_need
    n_c = n_need * n_u
    first = core * n_edge
    rows_c = pl.ds(pl.multiple_of(first * n_u, 64), n_c)
    load_enc, load_wo, load_wp, load_g, load_we, load_lab = loads = [pltpu.make_async_copy(src, dst, in_sem.at[q]) for q, (src, dst) in enumerate(
        ((enc_h, enc_ref), (wo_h, wo_ref), (wp_h, wp_ref), (g_h.at[rows_c], g_ref.at[rows_c]), (we_h, we_ref), (lab_h, lab_ref)))]
    for load in loads:
        load.start()
    diag = (partner + 2) % n_seq
    barrier = pltpu.get_barrier_semaphore()
    for other in (partner, peer, diag):
        pl.semaphore_signal(barrier, inc=1, device_id={'seq': other}, device_id_type=MESH)
    pl.semaphore_wait(barrier, 3)

    middle = pl.ds(n_edge, n_utt - 2 * n_edge)
    edge = lambda c: pl.ds(c * n_need, n_edge)

    def send(src, slot, part, sem, other):
        return pltpu.make_async_remote_copy(src_ref=src.at[part], dst_ref=fbuf.at[slot, part], send_sem=send_sem.at[sem],
                                            recv_sem=recv_sem.at[sem], device_id={'seq': other}, device_id_type=MESH)
    load_enc.wait()
    sends = [
        send(enc_ref, me, middle, 0, peer),
        send(enc_ref, me, edge(core), 1, peer),
        send(enc_ref, me, edge(1 - core), 2, diag),
        send(enc_ref, me, pl.ds((1 - core) * n_edge, n_need), 3, partner),
    ]
    for s in sends:
        s.start()
    fbuf[:, edge(1 - core)] = jnp.zeros((n_seq, n_edge) + fbuf.shape[2:], BF16)
    fbuf[me] = enc_ref[...]
    load_wo.wait()
    wot_ref[...] = wo_ref[...].T
    load_wp.wait()
    load_g.wait()
    c_ref[rows_c, :] = dot(g_ref[rows_c, :], wp_ref[...]).astype(BF16)
    load_we.wait()
    load_lab.wait()
    y_ref[rows_c, :] = label_rows(n_u, first, n_c, lab_ref)
    n_f, n_h = f_ref.shape
    n_own = n_f // n_seq
    n_loc = n_t // n_seq
    col = lax.broadcasted_iota(jnp.int32, (n_f, n_own), 0)
    row = lax.broadcasted_iota(jnp.int32, (n_f, n_own), 1)

    def piece(p):
        rows = fbuf[p].reshape(n_own, n_h)
        f_ref[pl.ds(pl.multiple_of(p * n_own, n_own), n_own), :] = rows
        order = jnp.where(col == row // n_loc * n_t + p * n_loc + row % n_loc, 1.0, 0.0).astype(BF16)
        return dot(order, dot(rows, we_ref[...]).astype(BF16))
    a_t = piece(me)
    sends[3].wait_recv()
    a_t = a_t + piece(partner)
    sends[0].wait_recv()
    relay = send(fbuf.at[peer], peer, middle, 4, partner)
    relay.start()
    sends[1].wait_recv()
    a_t = a_t + piece(peer)
    sends[2].wait_recv()
    relay.wait_recv()
    a_ref[...] = a_t + piece(diag)
    for s in sends + [relay]:
        s.wait_send()


def gather_call(enc, g2, w_enc, w_pred, w_out, labels_t, n_seq, n_t, n_u):
    n_utt, n_loc, n_h = enc.shape
    n_j = w_enc.shape[1]
    vm = pl.BlockSpec(memory_space=pltpu.VMEM)
    n_f = n_utt * n_loc * n_seq
    args = [in_hbm(x) for x in (enc, g2, w_enc, w_pred, w_out, labels_t)]
    return pl.pallas_call(
        functools.partial(gather_kernel, n_t, n_u),
        out_shape=(
            pltpu.VMEM((g2.shape[0], n_j), BF16),
            pltpu.VMEM((n_f, n_j), F32),
            pltpu.VMEM(w_out.shape[::-1], BF16),
            pltpu.VMEM((n_f, n_h), BF16),
            pltpu.VMEM((g2.shape[0], 128), BF16),
        ),
        in_specs=[pl.BlockSpec(memory_space=pltpu.HBM)] * 6,
        out_specs=(vm,) * 5,
        scratch_shapes=[pltpu.VMEM(x.shape, x.dtype) for x in (enc, g2, w_enc, w_pred, w_out, labels_t)] + [
            pltpu.VMEM((n_seq, n_utt, n_loc, n_h), BF16),
            pltpu.SemaphoreType.DMA((6,)),
            pltpu.SemaphoreType.DMA((5,)),
            pltpu.SemaphoreType.DMA((5,)),
        ],
        compiler_params=pltpu.CompilerParams(collective_id=0, has_side_effects=True, vmem_limit_bytes=GATHER_VMEM),
        name="rnnt_gather",
    )(*args)


def reduce_kernel(n_t, gwo_v, dc_v, da_v, loss_v, f_v, g_p, we_p, loss_ref, gf_ref, gwe_ref, gwp_ref, gwo_ref,
                  g_v, we_v, gwp_v, rgwo, rgwp, rda, rloss, da_rows, rf, f_all, in_sem, send_sem, recv_sem):
    me = lax.axis_index('seq')
    partner = me + 1 - 2 * (me % 2)
    n_need = g_v.shape[0]
    mine = pl.ds(pl.multiple_of(me % 2 * (dc_v.shape[0] - n_need), 64), n_need)
    loads = [pltpu.make_async_copy(src, dst, in_sem.at[q]) for q, (src, dst) in enumerate(((g_p.at[mine], g_v), (we_p, we_v)))]
    for load in loads:
        load.start()
    barrier = pltpu.get_barrier_semaphore()
    pl.semaphore_signal(barrier, inc=1, device_id={'seq': partner}, device_id_type=MESH)
    pl.semaphore_wait(barrier, 1)

    def send(src, dst, sem):
        return pltpu.make_async_remote_copy(src_ref=src, dst_ref=dst, send_sem=send_sem.at[sem], recv_sem=recv_sem.at[sem],
                                            device_id={'seq': partner}, device_id_type=MESH)
    n_part = 4
    rows = gwo_v.shape[0] // n_part
    n_da = CORE_MAX * n_t
    da_lo = (da_v.shape[0] - n_da) * (me % 2)
    part = pl.ds(pl.multiple_of(da_lo, 64), n_da)
    sends = [send(da_v.at[part], rda.at[part], 0), send(loss_v, rloss, 1)]
    sends += [send(gwo_v.at[pl.ds(q * rows, rows)], rgwo.at[pl.ds(q * rows, rows)], 2 + q) for q in range(n_part)]
    n_dev = n_t // gf_ref.shape[1]
    n_blk = f_v.shape[0] // n_dev
    n_edge = rf.shape[0] // n_dev
    edge_lo = lambda p, c: pl.multiple_of(p * n_blk + c * (n_blk - n_edge), 16)
    f_sends = [send(f_v.at[pl.ds(edge_lo(p, me % 2), n_edge)], rf.at[pl.ds(p * n_edge, n_edge)], 3 + n_part + p) for p in range(n_dev)]
    for s in sends + f_sends:
        s.start()
    loads[0].wait()
    gwp_v[...] = dot(g_v[...].T, dc_v[mine, :].astype(BF16))
    s_gwp = send(gwp_v, rgwp, 2 + n_part)
    loads[1].wait()
    sends[0].wait_recv()
    sends[1].wait_recv()
    loss_ref[...] = (loss_v[0:1, :] + rloss[0:1, :])[:, 0:loss_ref.shape[1]]
    row = lax.broadcasted_iota(jnp.int32, rda.shape, 0) - (da_v.shape[0] - n_da) * (partner % 2)
    other = jnp.where((row >= 0) & (row < n_da), rda[...].astype(F32), 0.0)
    da = (da_v[...].astype(F32) + other).astype(BF16)
    s_gwp.start()
    n_f = da.shape[0]
    n_loc = gf_ref.shape[1]
    n_own = gf_ref.shape[0] * n_loc
    row = lax.broadcasted_iota(jnp.int32, (n_f, n_f), 0)
    col = lax.broadcasted_iota(jnp.int32, (n_f, n_f), 1)
    order = jnp.where(col == row % n_own // n_loc * n_t + row // n_own * n_loc + row % n_loc, 1.0, 0.0).astype(BF16)
    da_f = dot(order, da).astype(BF16)
    da_rows[...] = da_f
    f_all[...] = f_v[...]
    for p in range(n_dev):
        f_sends[p].wait_recv()
        f_all[pl.ds(edge_lo(p, partner % 2), n_edge), :] = rf[p * n_edge:(p + 1) * n_edge]
    gwe_ref[...] = dot(f_all[...].T, da_f)
    own = da_rows[pl.ds(pl.multiple_of(me * n_own, n_own), n_own), :]
    gf_ref[...] = dot(own, we_v[...], NT).astype(BF16).reshape(gf_ref.shape)
    for q in range(n_part):
        sends[2 + q].wait_recv()
        part = slice(q * rows, (q + 1) * rows)
        gwo_ref[part] = gwo_v[part] + rgwo[part]
    s_gwp.wait_recv()
    gwp_ref[...] = gwp_v[...] + rgwp[...]
    for s in sends + f_sends + [s_gwp]:
        s.wait_send()


def reduce_call(gwo, dc_t, da_t, loss, g2, f2, w_enc, gf_shape, n_t):
    vm = pl.BlockSpec(memory_space=pltpu.VMEM)
    like = lambda x: pltpu.VMEM(x.shape, x.dtype)
    gwp_shape = (g2.shape[1], dc_t.shape[1])
    return pl.pallas_call(
        functools.partial(reduce_kernel, n_t),
        out_shape=(
            pltpu.VMEM((1, f2.shape[0] // n_t), F32),
            pltpu.VMEM(gf_shape, BF16),
            pltpu.VMEM(w_enc.shape, F32),
            pltpu.VMEM(gwp_shape, F32),
            pltpu.VMEM(gwo.shape, F32),
        ),
        in_specs=[vm] * 5 + [pl.BlockSpec(memory_space=pltpu.HBM)] * 2,
        out_specs=(vm,) * 5,
        scratch_shapes=[pltpu.VMEM((g2.shape[0] // gf_shape[0] * (CORE_MAX + 8), g2.shape[1]), BF16), like(w_enc)] + [
            pltpu.VMEM(gwp_shape, F32), like(gwo), pltpu.VMEM(gwp_shape, F32), like(da_t), like(loss), like(da_t), pltpu.VMEM(((gf_shape[0] - CORE_MAX - 8) * n_t, f2.shape[1]), BF16), like(f2),
            pltpu.SemaphoreType.DMA((2,)),
            pltpu.SemaphoreType.DMA((11,)),
            pltpu.SemaphoreType.DMA((11,)),
        ],
        compiler_params=pltpu.CompilerParams(collective_id=1, has_side_effects=True, vmem_limit_bytes=REDUCE_VMEM),
        name="rnnt_reduce",
    )(in_vmem(gwo), in_vmem(dc_t), in_vmem(da_t), in_vmem(loss), in_vmem(f2), in_hbm(g2), in_hbm(w_enc))


def store_kernel(n, *refs):
    sems = refs[2 * n]
    copies = [pltpu.make_async_copy(refs[q], refs[n + q], sems.at[q]) for q in range(n)]
    for copy in copies:
        copy.start()
    for copy in copies:
        copy.wait()


def store_call(arrays):
    n = len(arrays)
    return pl.pallas_call(
        functools.partial(store_kernel, n),
        out_shape=tuple(pltpu.HBM(x.shape, x.dtype) for x in arrays),
        in_specs=[pl.BlockSpec(memory_space=pltpu.VMEM)] * n,
        out_specs=(pl.BlockSpec(memory_space=pltpu.HBM),) * n,
        scratch_shapes=[pltpu.SemaphoreType.DMA((n,))],
        compiler_params=pltpu.CompilerParams(vmem_limit_bytes=STORE_VMEM),
        name="rnnt_store",
    )(*[in_vmem(x) for x in arrays])


def core_kernel(n_t, n_u, flen_s, llen_s, flen_v, llen_v, y_buf, c_buf, a_buf, wot, wo_h,
                loss_ref, segu, da_ref, gwo_ref,
                wo_ref, wo_sem, hbuf, hpar, ebuf, fac, mch, sch, vsb, ypar, ybuf, idx, dzb, dpb, zrow, sk, abuf, t1buf, t2buf,
                gocc, gocb, segt, tbl, off):
    n_utt = flen_s.shape[0]
    n_j = c_buf.shape[1]
    n_v = wo_ref.shape[1]
    gu = WIN * n_u
    gt = WIN * n_t
    n_diag = n_t + n_u - 1
    n_kt = (n_diag + 1) * n_t
    n_ch = n_v // CHUNK

    load_wo = pltpu.make_async_copy(wo_h, wo_ref, wo_sem)
    load_wo.start()

    total = jnp.int32(0)
    for b in range(n_utt):
        off[b] = total
        total = total + flen_s[b] * (llen_s[b] + 1)
    off[n_utt] = total

    cut = jnp.int32(CORE_MIN)
    for b in range(CORE_MIN, CORE_MAX):
        cut = cut + jnp.where(off[b] + off[b + 1] <= total, 1, 0)
    first_core = lax.axis_index('seq') % 2 == 0
    u_lo = jnp.where(first_core, 0, cut)
    u_hi = jnp.where(first_core, cut, n_utt)
    stop = off[u_hi]

    def utt_step(b, carry):
        win = jnp.minimum(b, n_utt - WIN)
        base = off[win]
        last = jnp.minimum(off[win + WIN], stop)

        def emit(c):
            n, pos = c
            end = jnp.minimum(pos + ROWS, last)
            tbl[0, n] = win
            tbl[1, n] = pos - base
            tbl[2, n] = end - base
            return n + 1, end
        return lax.while_loop(lambda c: c[1] < off[b + 1], emit, carry)
    n_blocks, _ = lax.fori_loop(u_lo, u_hi, utt_step, (jnp.int32(0), off[u_lo]))
    for past in range(3):
        for q in range(3):
            tbl[q, n_blocks + past] = 0

    sk[...] = jnp.zeros_like(sk)
    mch[...] = jnp.zeros_like(mch)
    sch[...] = jnp.ones_like(sch)
    zrow[...] = jnp.zeros_like(zrow)
    vsb[...] = jnp.zeros_like(vsb)
    dpb[...] = jnp.zeros_like(dpb)

    def onehot(n, index_row):
        return (lax.broadcasted_iota(jnp.int32, (n, ROWS), 0) == index_row)

    def as_bf16(mask):
        return jnp.where(mask, 1.0, 0.0).astype(BF16)

    def block_onehot(i):
        iota = lax.broadcasted_iota(jnp.int32, (gu + gt, ROWS), 0)
        return jnp.concatenate([as_bf16(iota[0:gu] == idx[i, 0:1]), as_bf16(iota[gu:] == idx[i, 1:2])], axis=0)

    sub8 = lax.broadcasted_iota(jnp.int32, (8, ROWS), 0)
    n_sub = CHUNK // 8

    def rows_of(win, width):
        return pl.ds(pl.multiple_of(win * width, width), WIN * width)

    def spread3(idx_b, parts):
        mask = lax.broadcasted_iota(jnp.int32, (CORE_MAX, ROWS), 0) == idx_b
        return jnp.concatenate([jnp.where(mask, part, 0.0) for part in parts]
                               + [jnp.zeros((128 - 3 * CORE_MAX, ROWS), F32)], axis=0).astype(BF16)

    def locate(i):
        win = tbl[0, i]
        r = tbl[1, i] + lax.broadcasted_iota(jnp.int32, (1, ROWS), 1)
        end_r = tbl[2, i]
        start = jnp.int32(0)
        bl = jnp.full((1, ROWS), -1, jnp.int32)
        w = jnp.zeros((1, ROWS), jnp.int32)
        u1 = jnp.ones((1, ROWS), jnp.int32)
        for j in range(WIN):
            u1_j = llen_s[win + j] + 1
            end = start + flen_s[win + j] * u1_j
            inside = (r >= start) & (r < jnp.minimum(end, end_r))
            bl = jnp.where(inside, j, bl)
            w = jnp.where(inside, r - start, w)
            u1 = jnp.where(inside, u1_j, u1)
            start = end
        valid = bl >= 0
        t = jnp.zeros((1, ROWS), jnp.int32)
        for j in range(1, n_t):
            t = t + jnp.where(w >= j * u1, 1, 0)
        u = w - t * u1
        idx_u = jnp.where(valid, bl * n_u + u, -1)
        idx_t = jnp.where(valid, gu + bl * n_t + t, -1)
        idx_kt = jnp.where(valid, (t + u) * n_t + t, -1)
        idx_b = jnp.where(valid, win + bl - u_lo, -1024)
        rows8 = lax.broadcasted_iota(jnp.int32, (8, ROWS), 0)
        idx[i] = jnp.where(rows8 == 0, idx_u, jnp.where(rows8 == 1, idx_t, jnp.where(rows8 == 2, idx_kt, idx_b)))

    half = n_j // 2

    def hidden(i, par):
        win = tbl[0, i]
        oh = jnp.concatenate([block_onehot(i), jnp.zeros((256 - gu - gt, ROWS), BF16)], axis=0)
        none = jnp.zeros((256 - gu - gt, n_j), BF16)
        cols = jnp.concatenate([c_buf[rows_of(win, n_u)], a_buf[rows_of(win, n_t)].astype(BF16), none], axis=0).T
        for q in range(2):
            rows = slice(q * half, (q + 1) * half)
            pre = dot(cols[rows], oh)
            h = jnp.tanh(pre).astype(BF16)
            hpar[par, rows] = h
            hbuf[i, rows] = h
        yy = dot(jnp.concatenate(
            [y_buf[rows_of(win, n_u)], jnp.zeros((256 - gu, 128), BF16)], axis=0).T[0:16], oh)
        y8 = jnp.broadcast_to((yy[0:1] * 32.0 + yy[1:2]).astype(jnp.int32), (8, ROWS))
        ypar[par] = y8
        ybuf[i] = y8

    def finish(i, par):
        idx_b = idx[i, 3:4]
        m_all = mch[par]
        m8 = jnp.max(m_all.reshape(n_ch, 8, ROWS), axis=0)
        m = jnp.max(m8, axis=0, keepdims=True)
        f_all = jnp.exp(m_all - m)
        s = jnp.sum(jnp.sum((sch[par] * f_all).reshape(n_ch, 8, ROWS), axis=0), axis=0, keepdims=True)
        fac[i] = f_all * (1.0 / s)
        lse = m + jnp.log(s)
        b_parts = split3(zrow[par, 8:9] - lse)
        l_parts = split3(jnp.sum(zrow[par, 0:8], axis=0, keepdims=True) - lse)
        vsb[par, 0:128] = spread3(idx_b, b_parts)
        vsb[par, 128:256] = spread3(idx_b, l_parts)

    def scatter(i, par, live):
        okt = as_bf16(onehot(n_kt, jnp.where(live, idx[i, 2:3], -1)))
        part = n_kt // 2
        for q in range(2):
            sk[q * part:(q + 1) * part] += dot(okt[q * part:(q + 1) * part], vsb[par], NT)

    def slot_of(i):
        return jnp.where(i < KEEP, i, KEEP + i % 2)

    def scores_part(i, par, chunks, lz):
        y8 = ypar[par]
        y_tile = lax.shift_right_logical(y8, 3)
        slot = slot_of(i)
        for c in chunks:
            z = dot(wot[c * CHUNK:(c + 1) * CHUNK, :], hpar[par])
            z3 = z.reshape(n_sub, 8, ROWS)
            for k in range(n_sub):
                lz = jnp.where(y_tile == c * n_sub + k, z3[k], lz)
            if c == 0:
                zrow[par, 8:16] = z[0:8, :]
            m_c = jnp.max(z3, axis=0)
            e3 = jnp.exp(z3 - m_c[None])
            ebuf[slot, c * CHUNK:(c + 1) * CHUNK, :] = e3.reshape(CHUNK, ROWS)
            mch[par, c * 8:(c + 1) * 8, :] = m_c
            sch[par, c * 8:(c + 1) * 8, :] = jnp.sum(e3, axis=0)
        if chunks[-1] == n_ch - 1:
            zrow[par, 0:8] = jnp.where(sub8 == jnp.bitwise_and(y8, 7), lz, 0.0)
        return lz

    def scores_of(i, par):
        scores_part(i, par, range(n_ch), jnp.zeros((8, ROWS), F32))

    def fwd_pair(p, carry):
        i = 2 * p
        finish(jnp.maximum(i - 1, 0), 1)
        hidden(i + 1, 1)
        scatter(jnp.maximum(i - 2, 0), 0, i > 1)
        scores_of(i, 0)
        hidden(i + 2, 0)
        scores_of(i + 1, 1)
        scatter(jnp.maximum(i - 1, 0), 1, i > 0)
        finish(i, 0)
        locate(i + 3)
        locate(i + 4)
        return carry

    def fwd_odd(p, carry):
        i = n_blocks - 1
        finish(jnp.maximum(i - 1, 0), 1)
        scatter(jnp.maximum(i - 2, 0), 0, i > 1)
        scores_of(i, 0)
        scatter(jnp.maximum(i - 1, 0), 1, i > 0)
        finish(i, 0)
        scatter(i, 0, True)
        return carry

    def fwd_even(p, carry):
        finish(n_blocks - 1, 1)
        scatter(n_blocks - 2, 0, True)
        scatter(n_blocks - 1, 1, True)
        return carry

    for first in range(3):
        locate(jnp.int32(first))
    hidden(jnp.int32(0), 0)
    lax.fori_loop(0, n_blocks // 2, fwd_pair, 0)
    lax.fori_loop(0, n_blocks % 2, fwd_odd, 0)
    lax.fori_loop(0, 1 - n_blocks % 2, fwd_even, 0)

    tt = lax.broadcasted_iota(jnp.int32, (n_t, 128), 0)
    def own_lanes(ref):
        x = jnp.concatenate([ref[...], jnp.zeros((1, 128 - n_utt), jnp.int32)], axis=1).astype(F32)
        return pltpu.roll(jnp.broadcast_to(x, (n_t, 128)), (128 - u_lo) % 128, 1).astype(jnp.int32)
    t_len = own_lanes(flen_v)
    u_len = own_lanes(llen_v)

    def scores(k):
        lo = k * n_t
        x, y = (v + pltpu.roll(v, 128 - CORE_MAX, 1) + pltpu.roll(v, 128 - 2 * CORE_MAX, 1)
                for v in (sk[lo:lo + n_t, 0:128], sk[lo:lo + n_t, 128:256]))
        uu = k - tt
        ok = (uu >= 0) & (tt < t_len)
        bl_k = jnp.where(ok & (uu <= u_len), x, NEG)
        lb_k = jnp.where(ok & (uu < u_len), y, NEG)
        return bl_k, lb_k

    alpha = jnp.where(tt == 0, 0.0, NEG).astype(F32)
    abuf[0] = alpha
    beta = jnp.full((n_t, 128), NEG, F32)
    sc = [scores(k) for k in range(n_diag)]
    for step in range(n_diag):
        if step > 0:
            bl_k, lb_k = sc[step - 1]
            p1 = jnp.where(tt == 0, NEG, pltpu.roll(alpha + bl_k, 1, 0))
            alpha = logadd(p1, alpha + lb_k)
            abuf[step] = alpha
        k = n_diag - 1 - step
        bl_k, lb_k = sc[k]
        up = jnp.where(tt == n_t - 1, jnp.where(u_len == k + 1 - n_t, 0.0, NEG), pltpu.roll(beta, n_t - 1, 0))
        t1 = up + bl_k
        t2 = beta + lb_k
        t1buf[k] = t1
        t2buf[k] = t2
        beta = jnp.where(tt >= t_len, jnp.where(k - tt == u_len, 0.0, NEG), logadd(t1, t2))
    n_need = (CORE_MAX + 8) * n_u
    mine = pl.ds(pl.multiple_of(jnp.where(first_core, 0, segu.shape[0] - n_need), 64), n_need)
    segu[mine, :] = jnp.zeros((n_need, n_j), F32)
    segt[...] = jnp.zeros_like(segt)
    log_p = beta[0:1, :]
    lane = lax.broadcasted_iota(jnp.int32, (n_t, 128), 1)
    loss_ref[...] = pltpu.roll(jnp.where(lane < u_hi - u_lo, -log_p, 0.0), u_lo, 1)
    lane_ok = lane < CORE_MAX
    for k in range(n_diag):
        for which, buf in enumerate((t1buf, t2buf)):
            occ = jnp.where(lane_ok, jnp.exp(jnp.minimum(abuf[k] + buf[k] - log_p, 0.0)), 0.0)
            hi, mid, lo = split3(occ)
            lo_row = which * n_kt + k * n_t
            gocc[lo_row:lo_row + n_t, :] = hi + pltpu.roll(mid, CORE_MAX, 1) + pltpu.roll(lo, 2 * CORE_MAX, 1)
    for which in range(2):
        gocc[which * n_kt + n_diag * n_t:(which + 1) * n_kt, :] = jnp.zeros((n_kt - n_diag * n_t, 128), F32)
    gocb[...] = gocc[...].astype(BF16)

    def again(first, count):
        def one(q, carry):
            i = first + q

            @pl.when((i >= KEEP) & (i < n_blocks))
            def _():
                def chunk(c, carry):
                    rows = pl.ds(pl.multiple_of(c * CHUNK, CHUNK), CHUNK)
                    z3 = dot(wot[rows, :], hbuf[i]).reshape(n_sub, 8, ROWS)
                    ebuf[KEEP + i % 2, rows, :] = jnp.exp(z3 - jnp.max(z3, axis=0)[None]).reshape(CHUNK, ROWS)
                    return carry
                lax.fori_loop(0, n_ch, chunk, 0)
            return carry
        @pl.when((first + count > KEEP) & (n_blocks > KEEP))
        def _():
            lax.fori_loop(0, count, one, 0)

    def occupancy(i, par):
        orep = spread3(idx[i, 3:4], (1.0, 1.0, 1.0))
        kt8 = jnp.broadcast_to(idx[i, 2:3], (8, ROWS))
        kt_tile = lax.shift_right_arithmetic(kt8, 3)
        kt_sub = sub8 == jnp.bitwise_and(kt8, 7)
        for which in range(2):
            gath = dot(gocb[which * n_kt:(which + 1) * n_kt], orep).reshape(n_kt // 8, 8, ROWS)
            occ = jnp.zeros((8, ROWS), F32)
            for k in range(n_diag):
                occ = jnp.where(kt_tile == k, gath[k], occ)
            occ = jnp.sum(jnp.where(kt_sub, occ, 0.0), axis=0, keepdims=True)
            zrow[par, which * 8:which * 8 + 8] = jnp.broadcast_to(occ, (8, ROWS))

    def d_logits(i, par):
        y8 = ybuf[i]
        y_tile = lax.shift_right_logical(y8, 3)
        gb = zrow[par, 0:8]
        gl = zrow[par, 8:16]
        occ = gb + gl
        gl_y = jnp.where(sub8 == jnp.bitwise_and(y8, 7), gl, 0.0)
        gb_0 = jnp.where(sub8 == 0, gb, 0.0)
        slot = slot_of(i)
        for c in range(n_ch):
            sc_c = fac[i, c * 8:(c + 1) * 8, :] * occ
            e3 = ebuf[slot, c * CHUNK:(c + 1) * CHUNK, :].reshape(n_sub, 8, ROWS)
            tiles = []
            for k in range(n_sub):
                d = e3[k] * sc_c
                if c == 0 and k == 0:
                    d = d - gb_0
                tiles.append(d - jnp.where(y_tile == c * n_sub + k, gl_y, 0.0))
            d = jnp.concatenate(tiles, axis=0)
            dzb[par, c * CHUNK:(c + 1) * CHUNK, :] = d.astype(BF16)

    def segments(i, par):
        win = tbl[0, i]
        oh = block_onehot(i)
        for lo in range(0, n_j, 256):
            cols = slice(lo, min(lo + 256, n_j))
            sums = dot(oh, dpb[par, cols], NT)
            segu[rows_of(win, n_u), cols] += sums[0:gu]
            segt[rows_of(win, n_t), cols] += sums[gu:]

    def d_hidden(i, par):
        for q in range(2):
            rows = slice(q * half, (q + 1) * half)
            hf = hbuf[i, rows].astype(F32)
            dh = dot(wo_ref[rows], dzb[par])
            dpb[par, rows] = (dh * (1.0 - hf * hf)).astype(BF16)

    def out_grad(blocks, add):
        for c in range(n_v // 256):
            cols = slice(c * 256, (c + 1) * 256)
            new = None
            for i, par in blocks:
                term = dot(hbuf[i], dzb[par, cols, :], NT)
                new = term if new is None else new + term
            gwo_ref[:, cols] = jnp.where(add, gwo_ref[:, cols], 0.0) + new

    def bwd_pair(p, carry):
        i = 2 * p
        again(i + 2, 2)
        d_hidden(i, 0)
        d_hidden(i + 1, 1)
        segments(i, 0)
        segments(i + 1, 1)
        out_grad(((i, 0), (i + 1, 1)), p > 0)
        d_logits(i + 2, 0)
        d_logits(i + 3, 1)
        occupancy(i + 4, 0)
        occupancy(i + 5, 1)
        return carry

    def bwd_odd(p, carry):
        d_hidden(n_blocks - 1, 0)
        out_grad(((n_blocks - 1, 0),), n_blocks > 1)
        segments(n_blocks - 1, 0)
        return carry

    load_wo.wait()
    again(0, 2)
    for first in range(2):
        occupancy(jnp.int32(first), first)
        d_logits(jnp.int32(first), first)
        occupancy(jnp.int32(first + 2), first)
    lax.fori_loop(0, n_blocks // 2, bwd_pair, 0)
    lax.fori_loop(0, n_blocks % 2, bwd_odd, 0)

    da_ref[...] = segt[...].astype(BF16)


def core_call(c_t, a_t, wot, ylab, w_out, flen, llen, n_t, n_u):
    n_utt = flen.shape[0]
    n_j = c_t.shape[1]
    n_v = w_out.shape[1]
    max_blk = n_utt // 2 * n_t * n_u // ROWS + 6
    n_kt = (n_t + n_u) * n_t
    n_st = n_v // CHUNK * 8
    vm = pl.BlockSpec(memory_space=pltpu.VMEM)
    sm = pl.BlockSpec(memory_space=pltpu.SMEM)
    return pl.pallas_call(
        functools.partial(core_kernel, n_t, n_u),
        out_shape=(
            pltpu.VMEM((8, 128), F32),
            pltpu.VMEM((n_utt * n_u, n_j), F32),
            pltpu.VMEM((n_utt * n_t, n_j), BF16),
            pltpu.VMEM(w_out.shape, F32),
        ),
        in_specs=[sm, sm] + [vm] * 6 + [pl.BlockSpec(memory_space=pltpu.HBM)],
        out_specs=(vm,) * 4,
        scratch_shapes=[
            pltpu.VMEM(w_out.shape, BF16),
            pltpu.SemaphoreType.DMA,
            pltpu.VMEM((max_blk, n_j, ROWS), BF16),
            pltpu.VMEM((2, n_j, ROWS), BF16),
            pltpu.VMEM((min(max_blk, KEEP + 2), n_v, ROWS), F32),
            pltpu.VMEM((max_blk, n_st, ROWS), F32),
            pltpu.VMEM((2, n_st, ROWS), F32),
            pltpu.VMEM((2, n_st, ROWS), F32),
            pltpu.VMEM((2, 256, ROWS), BF16),
            pltpu.VMEM((2, 8, ROWS), jnp.int32),
            pltpu.VMEM((max_blk, 8, ROWS), jnp.int32),
            pltpu.VMEM((max_blk, 8, ROWS), jnp.int32),
            pltpu.VMEM((2, n_v, ROWS), BF16),
            pltpu.VMEM((2, n_j, ROWS), BF16),
            pltpu.VMEM((2, 16, ROWS), F32),
            pltpu.VMEM((n_kt, 256), F32),
            pltpu.VMEM((n_t + n_u, n_t, 128), F32),
            pltpu.VMEM((n_t + n_u, n_t, 128), F32),
            pltpu.VMEM((n_t + n_u, n_t, 128), F32),
            pltpu.VMEM((2 * n_kt, 128), F32),
            pltpu.VMEM((2 * n_kt, 128), BF16),
            pltpu.VMEM((n_utt * n_t, n_j), F32),
            pltpu.SMEM((3, max_blk), jnp.int32),
            pltpu.SMEM((n_utt + 1,), jnp.int32),
        ],
        compiler_params=pltpu.CompilerParams(vmem_limit_bytes=CORE_VMEM),
        name="rnnt_core",
    )(flen, llen, flen.reshape(1, n_utt), llen.reshape(1, n_utt), *[in_vmem(x) for x in (ylab, c_t, a_t, wot)], in_hbm(w_out))


def solution(mesh):
    seq_size = mesh.shape['seq']

    def local_fn(enc_out, pred_out, w_enc, w_pred, w_out, labels, frame_len, label_len):
        n_utt, n_loc, n_h = enc_out.shape
        n_u = pred_out.shape[1]
        n_t = n_loc * seq_size
        g2 = pred_out.reshape(n_utt * n_u, n_h)
        c_t, a_t, wot, f2, *rest = gather_call(enc_out, g2, w_enc, w_pred, w_out, labels.T, seq_size, n_t, n_u)
        loss, dc_t, da_t, gwo = core_call(c_t, a_t, wot, *rest, w_out, frame_len, label_len, n_t, n_u)
        loss, gf, gwe, gwp, gwo = store_call(reduce_call(gwo, dc_t, da_t, loss, g2, f2, w_enc, enc_out.shape, n_t))
        return loss.reshape(n_utt), gf, gwe, gwp, gwo

    in_specs = (P('dp', 'seq', None), P('dp', None, None), P(None, None), P(None, None), P(None, None), P('dp', None), P('dp'), P('dp'))
    out_specs = (P('dp'), P('dp', 'seq', None), P('dp', None), P('dp', None), P('dp', None))
    return jax.shard_map(local_fn, mesh=mesh, in_specs=in_specs, out_specs=out_specs, check_vma=False)
```
